8 devices in a mesh: dp: 1 (over z), tp: 8 (over y, x, core).
Axes of the slice: x: 2, y: 2, z: 1, core: 2. Of those that a mesh axis runs over, the one named last changes fastest.
Arguments:
- hidden: bfloat16 [4096, 4096], P(('dp', 'tp'))
- w_head: bfloat16 [4096, 32768], P(None, 'tp')
- labels: int32 [4096], P(('dp', 'tp'))
Outputs:
- output 1: float32 [1], P('dp')
- output 2: bfloat16 [4096, 4096], P(('dp', 'tp'))
- output 3: bfloat16 [4096, 32768], P('dp', 'tp')
All inputs are finite; a program needn't handle non-finite values.
Results may differ from the reference program's by a relative error of at most 0.001.
Values are sent between devices in bfloat16 or wider.
A program may use at most 1 GiB of HBM per device.

```python
import math
import jax
import jax.numpy as jnp
from jax import lax

HIDDEN = 4096
VOCAB = 32768
TOKENS = 4096

ROW_BLOCK = math.gcd(TOKENS, 64)


def setup_inputs(seed: int = 0, part: int = 0) -> dict:
    base_key = jax.random.key(seed)
    key_w, key_parts = jax.random.split(base_key)
    key_x, key_lab = jax.random.split(jax.random.fold_in(key_parts, part))
    w_head = jax.random.normal(key_w, (HIDDEN, VOCAB), jnp.float32) * HIDDEN ** -0.5
    labels = jax.random.randint(key_lab, (TOKENS,), 0, VOCAB, dtype=jnp.int32)
    label_boost = math.log(VOCAB) - 1.0
    noise_x = jax.random.normal(key_x, (TOKENS, HIDDEN), jnp.float32)
    hidden = noise_x + label_boost * jnp.take(w_head, labels, axis=1).T
    return {"hidden": hidden.astype(jnp.bfloat16), "w_head": w_head.astype(jnp.bfloat16), "labels": labels}


def reference(hidden, w_head, labels):
    inv_tokens = 1.0 / TOKENS
    num_blocks = TOKENS // ROW_BLOCK
    hid_blocks = hidden.reshape(num_blocks, ROW_BLOCK, HIDDEN)
    lab_blocks = labels.reshape(num_blocks, ROW_BLOCK)
    vocab_ids = jnp.arange(VOCAB, dtype=jnp.int32)
    w_trans = w_head.T

    def row_step(acc_dw, block):
        hid_blk, lab_blk = block
        logits = jnp.dot(hid_blk, w_head, preferred_element_type=jnp.float32)
        row_max = jnp.max(logits, axis=1, keepdims=True)
        shifted = jnp.exp(logits - row_max)
        row_sum = jnp.sum(shifted, axis=1, keepdims=True)
        onehot = (vocab_ids[None, :] == lab_blk[:, None]).astype(jnp.float32)
        target = jnp.sum(logits * onehot, axis=1)
        token_loss = row_max[:, 0] + jnp.log(row_sum[:, 0]) - target
        grad_out = ((shifted / row_sum - onehot) * inv_tokens).astype(jnp.bfloat16)
        acc_dw = acc_dw + jnp.dot(hid_blk.T, grad_out, preferred_element_type=jnp.float32)
        dx_blk = jnp.dot(grad_out, w_trans, preferred_element_type=jnp.float32)
        return acc_dw, (token_loss, dx_blk.astype(jnp.bfloat16))

    zero_dw = jnp.zeros((HIDDEN, VOCAB), jnp.float32)
    acc_dw, (losses, dx_blocks) = lax.scan(row_step, zero_dw, (hid_blocks, lab_blocks))
    mean_loss = (jnp.sum(losses) * inv_tokens).reshape(1)
    return mean_loss, dx_blocks.reshape(TOKENS, HIDDEN), acc_dw.astype(jnp.bfloat16)
```

```python
import functools

import jax
import jax.numpy as jnp
from jax import lax
from jax.experimental import pallas as pl
from jax.experimental.pallas import tpu as pltpu
from jax.sharding import PartitionSpec as P

F32, BF16, I32 = jnp.float32, jnp.bfloat16, jnp.int32
MESH = pl.DeviceIdType.MESH
ANY = pl.ANY

TOK = 4096
HID = 4096
VOC = 4096
BLK = 256
HALF = 2048
NBLK = TOK // BLK
LANE = 128
PIECE = 512
INV = 1.0 / TOK


def _copy(src, dst, sem):
    return pltpu.make_async_copy(src, dst, sem)


def _send(src, dst, send_sem, recv_sem, dev):
    return pltpu.make_async_remote_copy(
        src_ref=src, dst_ref=dst, send_sem=send_sem, recv_sem=recv_sem, device_id={"tp": dev}, device_id_type=MESH
    )


def _product(lhs, rhs, put, jobs, transposed):
    pl.when(lax.axis_index("tp") < 8)(functools.partial(_pieces, lhs, rhs, put, jobs, transposed))


def _pieces(lhs, rhs, put, jobs, transposed):
    dims = (((1,), (1,)), ((), ())) if transposed else (((1,), (0,)), ((), ()))
    pieces = HALF // PIECE
    deep = 8
    for nt in range(pieces):
        acc = None
        for kt in range(deep):
            part = lax.dot_general(lhs(kt), rhs(nt, kt), dims, preferred_element_type=F32)
            acc = part if acc is None else acc + part
            for job in jobs[nt * deep + kt]:
                job()
        put(nt, acc)


def _wide(v, times=HALF // LANE):
    return jnp.concatenate([v] * times, axis=1)


def _fold(v):
    width = v.shape[1] // 2
    while width >= LANE:
        v = v[:, :width] + v[:, width:]
        width //= 2
    return v


def _column(row):
    return jnp.transpose(jnp.broadcast_to(row, (LANE, LANE)))


def _head_kernel(
    x_hbm, lab_hbm, w_hbm,
    xall, gall, s_n1b, s_self, y2, r1a, loss_out,
    zst, s_d, s_n1a, s_n2, r1n2,
    wv, xg, ga, gb, zb, pbuf, rbuf, sbuf, ab, bb, cb, lab_v, la, lb, st_new, st_all, ml, mk, sl, tl, comb,
    w_sem, lab_sem, labtx_sem, rx, tx, xl_sem, xs_sem, zo_sem, st_sem, sttx_sem,
    zi_sem, rr, ps, ss_sem, s1tx, r1s, r1as, ab_sem, cb_sem, g_sem,
):
    me = lax.axis_index("tp")
    chip = me // 2
    c = me % 2
    x = chip % 2
    y = chip // 2
    oc = 1 - c
    partner = me + 1 - 2 * c
    dx, dy = 2 - 4 * x, 4 - 8 * y
    n1 = me + oc * dx + c * dy
    n2 = me + c * dx + oc * dy
    n1kind = 1 + c

    def chip_of(kind):
        return chip + (kind % 2) * (1 - 2 * x) + (kind // 2) * (2 - 4 * y)

    def order1(i):
        mid, end = (i // 4 + 1) // 2 % 2, i // 12
        return mid * (1 + i % 2) + 3 * end, mid * ((i - 4) // 2) + (1 - mid) * (i % 4)

    def order2(i):
        mid, end = (i // 4 + 1) // 2 % 2, i // 12
        return mid * (1 + i % 2) + 3 * (1 - mid) * (1 - end), mid * ((i - 4) // 2) + (1 - mid) * (i % 4)

    def block_id(kind, q):
        return chip_of(kind) * 4 + q

    def xrows(kind, q, part):
        return xall.at[pl.ds(pl.multiple_of(block_id(kind, q) * BLK + part * LANE, LANE), LANE)]

    def xblock(kind, q):
        return xall.at[pl.ds(pl.multiple_of(block_id(kind, q) * BLK, BLK), BLK)]

    def own(q):
        return x_hbm.at[pl.ds(pl.multiple_of(q * LANE, LANE), LANE)]

    def rxs(kind, q, part):
        return rx.at[kind * 8 + q * 2 + part]

    def wcopy(h):
        return _copy(w_hbm.at[:, pl.ds(h * HALF, HALF)], wv.at[:, pl.ds(h * HALF, HALF)], w_sem.at[h])

    wcopy(0).start()
    wcopy(1).start()

    barrier = pltpu.get_barrier_semaphore()
    for d in range(1, 8):
        pl.semaphore_signal(barrier, inc=1, device_id={"tp": (me + d) % 8}, device_id_type=MESH)
    pl.semaphore_wait(barrier, 7)

    for q in range(4):
        _send(own(q), xrows(0, q, c), tx, rxs(0, q, c), partner).start()
        _send(own(q), xrows_at(xall, me, q), tx, rxs(n1kind, q, c), n1).start()
        _send(own(q), xrows_at(xall, me, q), tx, rxs(3 - n1kind, q, c), n2).start()
    for d in range(1, 8):
        _send(lab_hbm, lab_v.at[me], labtx_sem, lab_sem, (me + d) % 8).start()
    _copy(lab_hbm, lab_v.at[me], lab_sem).start()

    def load_x(b):
        kind, q = order1(b)
        slot = b % 2

        @pl.when(kind == 0)
        def _():
            _copy(own(q), xg.at[slot, pl.ds(pl.multiple_of(c * LANE, LANE), LANE)], xl_sem.at[slot]).start()
            _copy(xrows(0, q, oc), xg.at[slot, pl.ds(pl.multiple_of(oc * LANE, LANE), LANE)], xl_sem.at[slot]).start()

        @pl.when(kind != 0)
        def _():
            _copy(xblock(kind, q), xg.at[slot], xl_sem.at[slot]).start()

    def wait_rows(kind, q, part):
        _copy(xrows(kind, q, part), xrows(kind, q, part), rxs(kind, q, part)).wait()

    def zcopy(b, h):
        kind, q = order1(b)
        return _copy(zb.at[h], zst.at[block_id(kind, q), h], zo_sem.at[h])

    def own_store(b):
        slot = b % 2
        return _copy(xg.at[slot, pl.ds(pl.multiple_of(c * LANE, LANE), LANE)], xrows(0, b % 4, c), xs_sem.at[slot])

    def label_column(blk, part):
        return _column(lab_v[2 * (blk // 4) + part, pl.ds(blk % 4, 1), :])

    def lane_stats(col, h, r):
        rows = pl.ds(r, 8)
        z = zb[h, rows, :]
        m = ml[h, rows, :]
        hit = _wide(col[rows, :] - (me * VOC + h * HALF)) == lax.broadcasted_iota(I32, (8, HALF), 1)
        s = _fold(jnp.exp(z - _wide(m)))
        t = _fold(jnp.where(hit, z, 0.0))
        if h == 1:
            m0 = mk[0, rows, :]
            mm = jnp.maximum(m0, m)
            s = sl[0, rows, :] * jnp.exp(m0 - mm) + s * jnp.exp(m - mm)
            t = tl[0, rows, :] + t
            m = mm
        mk[h, rows, :] = m
        sl[h, rows, :] = s
        tl[h, rows, :] = t

    def label_columns(blk, col, part):
        col[pl.ds(part * LANE, LANE), :] = label_column(blk, part)

    def row_stats(part):
        rows = pl.ds(part * LANE, LANE)
        m = jnp.transpose(mk[1, rows, :])
        top = jnp.max(m, axis=0, keepdims=True)
        st_new[part : part + 1, :] = top
        st_new[2 + part : 3 + part, :] = jnp.sum(jnp.transpose(sl[1, rows, :]) * jnp.exp(m - top), axis=0, keepdims=True)
        st_new[4 + part : 5 + part, :] = jnp.sum(jnp.transpose(tl[1, rows, :]), axis=0, keepdims=True)

    def send_stats(blk):
        for d in range(1, 8):
            _send(st_new, st_all.at[blk, me], sttx_sem, st_sem.at[blk], (me + d) % 8).start()
        st_all[blk, me] = st_new[...]

    def stats_sent():
        _copy(st_all.at[0, pl.ds(0, 7)], st_all.at[0, pl.ds(0, 7)], sttx_sem).wait()

    def logits(b, h, jobs):
        slot = b % 2
        def put(nt, z):
            zb[h, :, nt * PIECE : (nt + 1) * PIECE] = z
            m = z[:, :LANE]
            for j in range(1, 4):
                m = jnp.maximum(m, z[:, j * LANE : (j + 1) * LANE])
            if nt:
                m = jnp.maximum(m, ml[h])
            ml[h] = m

        _product(
            lambda kt: xg[slot, :, kt * PIECE : (kt + 1) * PIECE],
            lambda nt, kt: wv[kt * PIECE : (kt + 1) * PIECE, h * HALF + nt * PIECE : h * HALF + (nt + 1) * PIECE],
            put,
            jobs,
            False,
        )

    _copy(own(0), xg.at[0, pl.ds(pl.multiple_of(c * LANE, LANE), LANE)], xl_sem.at[0]).start()
    wait_rows(0, 0, oc)
    _copy(xrows(0, 0, oc), xg.at[0, pl.ds(pl.multiple_of(oc * LANE, LANE), LANE)], xl_sem.at[0]).start()
    _copy(lab_v, lab_v, lab_sem).wait()
    wcopy(0).wait()

    def phase1(i, carry):
        slot = i % 2
        kind, q = order1(i)
        kprev, qprev = order1((i + NBLK - 2) % NBLK)
        kn, qn = order1((i + 1) % NBLK)

        _copy(xg.at[slot], xg.at[slot], xl_sem.at[slot]).wait()

        @pl.when(i < 4)
        def _():
            own_store(i).start()

        @pl.when(i > 0)
        def _():
            zcopy(i - 1, 1).start()
            zcopy(i - 1, 0).wait()

        @pl.when(i > 1)
        def _():
            send_stats(block_id(kprev, qprev))

        @pl.when((i >= 3) & (i < NBLK - 1))
        def _():
            wait_rows(kn, qn, c)
            _send(xrows(kn, qn, c), xrows(kn, qn, c), tx, rxs(kn, qn, c), partner).start()

            @pl.when(kn == n1kind)
            def _():
                _send(xrows(kn, qn, c), xrows(kn, qn, c), tx, rxs(3, qn, c), n2).start()

        jobs = [[] for _ in range(32)]
        for r in range(32):
            jobs[r].append(functools.partial(lane_stats, la, 1, r * 8))
        for part in range(2):
            jobs[4 + 4 * part].append(functools.partial(label_columns, block_id(kind, q), lb, part))
        logits(i, 0, jobs)

        zcopy(i, 0).start()

        @pl.when(i == 0)
        def _():
            wcopy(1).wait()

        @pl.when(i > 0)
        def _():
            zcopy(i - 1, 1).wait()

        @pl.when(i > 1)
        def _():
            stats_sent()

        @pl.when(i < NBLK - 1)
        def _():
            wait_rows(kn, qn, oc)

            @pl.when((i >= 1) & (i < 5))
            def _():
                own_store(i - 1).wait()

            load_x(i + 1)

        la[...] = lb[...]
        jobs = [[] for _ in range(32)]
        for r in range(32):
            jobs[r].append(functools.partial(lane_stats, lb, 0, r * 8))
        for part in range(2):
            jobs[8 + 8 * part].append(functools.partial(row_stats, part))
        logits(i, 1, jobs)
        return carry

    lax.fori_loop(0, NBLK, phase1, 0)
    last = NBLK - 1
    klast, qlast = order1(jnp.int32(last))
    zcopy(last, 1).start()
    zcopy(last, 0).wait()
    kprev, qprev = order1(jnp.int32(last - 1))
    send_stats(block_id(kprev, qprev))
    stats_sent()
    for r in range(32):
        lane_stats(la, 1, r * 8)
    for part in range(2):
        row_stats(part)
    zcopy(last, 1).wait()
    send_stats(block_id(klast, qlast))

    def zload(k, n):
        kind, q = order2(k)
        return _copy(zst.at[block_id(kind, q), n], zb.at[n], zi_sem.at[n])

    zload(0, 0).start()
    zload(0, 1).start()

    def combine(b, acc):
        _copy(st_all.at[b, pl.ds(0, 7)], st_all.at[b, pl.ds(0, 7)], st_sem.at[b]).wait()
        top = st_all[b, 0, 0:2, :]
        for d in range(1, 8):
            top = jnp.maximum(top, st_all[b, d, 0:2, :])
        s = jnp.zeros((2, LANE), F32)
        t = jnp.zeros((2, LANE), F32)
        for d in range(8):
            s = s + st_all[b, d, 2:4, :] * jnp.exp(st_all[b, d, 0:2, :] - top)
            t = t + st_all[b, d, 4:6, :]
        comb[b, 0:2, :] = top
        comb[b, 2:4, :] = INV / s
        return acc + (top + jnp.log(s) - t)

    token_loss = lax.fori_loop(0, NBLK, combine, jnp.zeros((2, LANE), F32))
    loss_out[...] = jnp.full((8, LANE), jnp.sum(token_loss) * INV, F32)

    gbufs = (ga, gb)

    def columns(k, par, part):
        kind, q = order2(k)
        blk = block_id(kind, q)
        rows = pl.ds(part * LANE, LANE)
        (la if par == 0 else lb)[rows, :] = label_column(blk, part)
        ml[par, rows, :] = _column(comb[blk, part : part + 1, :])
        sl[par, rows, :] = _column(comb[blk, 2 + part : 3 + part, :])

    def gradient(n, par, r, j):
        rows = pl.ds(r, 16)
        col = (la if par == 0 else lb)[rows, :] - (me * VOC + n * HALF + j)
        p = jnp.exp(zb[n, rows, j : j + 1024] - _wide(ml[par, rows, :], 8)) * _wide(sl[par, rows, :], 8)
        g = jnp.where(_wide(col, 8) == lax.broadcasted_iota(I32, (16, 1024), 1), p - INV, p)
        gbufs[par][rows, n * HALF + j : n * HALF + j + 1024] = g.astype(BF16)

    def gstore(k, par):
        kind, q = order2(k)
        return _copy(gbufs[par], gall.at[pl.ds(pl.multiple_of(block_id(kind, q) * BLK, BLK), BLK)], g_sem.at[par])

    def tile(ref, q, n):
        return ref.at[pl.ds(pl.multiple_of(q * LANE, LANE), LANE), pl.ds(pl.multiple_of(n * HALF, HALF), HALF)]

    def spair(k, n):
        return _send(
            pbuf.at[n, pl.ds(pl.multiple_of(oc * LANE, LANE), LANE)], rbuf.at[k % 2, n], ps.at[n], rr.at[(k % 2) * 2 + n], partner
        )

    def sstore_start(k, n):
        kind, q = order2(k)
        sem = ss_sem.at[n]

        @pl.when(kind == 3)
        def _():
            _copy(sbuf.at[n], tile(s_d, q, n), sem).start()

        @pl.when((kind == n1kind) & (q < 2))
        def _():
            _copy(sbuf.at[n], tile(s_n1a, q % 2, n), sem).start()

        @pl.when((kind == n1kind) & (q >= 2))
        def _():
            _copy(sbuf.at[n], tile(s_n1b, q % 2, n), sem).start()

        @pl.when(kind == 3 - n1kind)
        def _():
            _copy(sbuf.at[n], tile(s_n2, q, n), sem).start()

        @pl.when(kind == 0)
        def _():
            _copy(sbuf.at[n], tile(s_self, q, n), sem).start()

    def sstore_done(k, n):
        kind, q = order2(k)
        _copy(sbuf.at[n], tile(s_d, 0, n), ss_sem.at[n]).wait()

        @pl.when(kind == 3)
        def _():
            _send(tile(s_d, q, n), tile(r1n2, q, n), s1tx, r1s.at[q * 2 + n], n1).start()

        @pl.when((kind == n1kind) & (q < 2))
        def _():
            _send(tile(s_n1a, q % 2, n), tile(r1a, q % 2, n), s1tx, r1as.at[(q % 2) * 2 + n], n1).start()

    def stage2_load(q, n):
        _copy(tile(r1n2, q, n), tile(r1n2, q, n), r1s.at[q * 2 + n]).wait()
        _copy(tile(s_n2, q, n), ab.at[n], ab_sem.at[n * 2]).start()
        _copy(tile(r1n2, q, n), bb.at[n], ab_sem.at[n * 2 + 1]).start()

    def pair_sum(k, n, r):
        sbuf[n, pl.ds(r, 16), :] = pbuf[n, pl.ds(pl.multiple_of(c * LANE + r, 16), 16), :] + rbuf[k % 2, n, pl.ds(r, 16), :]

    def stage2_sum(n, r):
        cb[pl.ds(r, 16), :] = ab[n, pl.ds(r, 16), :] + bb[n, pl.ds(r, 16), :]

    def rwait(k, n):
        _copy(rbuf.at[k % 2, n], rbuf.at[k % 2, n], rr.at[(k % 2) * 2 + n]).wait()

    for part in range(2):
        columns(jnp.int32(0), 0, part)
        columns(jnp.int32(1), 1, part)
    for n in range(2):
        zload(0, n).wait()
        for r in range(0, BLK, 16):
            gradient(n, 0, r, 0)
            gradient(n, 0, r, 1024)
    gstore(0, 0).start()
    zload(1, 0).start()
    zload(1, 1).start()

    def sub(k, cur):
        nxt = 1 - cur

        @pl.when(k >= 1)
        def _():
            gstore(k - 1, nxt).wait()

        def trip(n):
            @pl.when(k < NBLK - 1)
            def _():
                zload(k + 1, n).wait()

            @pl.when(k >= 1)
            def _():
                rwait(k - 1, n)
                spair(k - 1, n).wait_send()

            @pl.when(k >= 12)
            def _():
                _copy(tile(s_n2, 0, n), ab.at[n], ab_sem.at[n * 2]).wait()
                _copy(tile(r1n2, 0, n), bb.at[n], ab_sem.at[n * 2 + 1]).wait()

            @pl.when(k >= 13 - n)
            def _():
                _copy(cb, tile(y2, 0, n), cb_sem).wait()

            jobs = [[] for _ in range(32)]
            for r in range(8):
                jobs[r // 2].append(functools.partial(pair_sum, k - 1, n, r * 16))
                jobs[20 + r].append(functools.partial(stage2_sum, n, r * 16))
            for r in range(32):
                jobs[4 + r * 7 // 8].append(functools.partial(gradient, n, nxt, r // 2 * 16, r % 2 * 1024))
            for part in range(2):
                jobs[8 + 8 * part].append(functools.partial(columns, (k + 2) % NBLK, cur, part))

            def put(nt, acc):
                pbuf[n, :, nt * PIECE : (nt + 1) * PIECE] = acc

            _product(
                lambda kt: gbufs[cur][:, kt * PIECE : (kt + 1) * PIECE],
                lambda nt, kt: wv[pl.ds(pl.multiple_of(n * HALF + nt * PIECE, PIECE), PIECE), kt * PIECE : (kt + 1) * PIECE],
                put,
                jobs,
                True,
            )

            spair(k, n).start()

            @pl.when(k < NBLK - 2)
            def _():
                zload(k + 2, n).start()

            @pl.when(k >= 2 - n)
            def _():
                sstore_done(k - 2 + n, 1 - n)

            @pl.when(k >= 1)
            def _():
                sstore_start(k - 1, n)

            @pl.when(k >= 12)
            def _():
                _copy(cb, tile(y2, k - 12, n), cb_sem).start()

            @pl.when((k >= 11) & (k < NBLK - 1))
            def _():
                stage2_load(k - 11, n)

        trip(0)
        trip(1)

        @pl.when(k < NBLK - 1)
        def _():
            gstore(k + 1, nxt).start()

    def pair(p, carry):
        sub(2 * p, 0)
        sub(2 * p + 1, 1)
        return carry

    lax.fori_loop(0, NBLK // 2, pair, 0)

    kl = jnp.int32(NBLK - 1)
    for n in range(2):
        rwait(kl, n)
        spair(kl, n).wait_send()
        if n == 0:
            sstore_done(kl - 1, 1)
        for r in range(8):
            pair_sum(kl, n, r * 16)
        sstore_start(kl, n)
    for n in range(2):
        sstore_done(kl, n)
    gstore(kl, 1).wait()
    _copy(cb, tile(y2, 0, 0), cb_sem).wait()

    for i in range(4):
        _copy(tile(r1a, i // 2, i % 2), tile(r1a, i // 2, i % 2), r1as.at[i]).wait()
    _copy(s_d, s_d, s1tx).wait()
    _copy(s_n1a, s_n1a, s1tx).wait()
    _copy(xall.at[pl.ds(0, 28 * LANE)], xall.at[pl.ds(0, 28 * LANE)], tx).wait()
    for d in range(7):
        _copy(lab_v.at[d], lab_v.at[d], labtx_sem).wait()
    stats_sent()


def xrows_at(xall, dev, q):
    return xall.at[pl.ds(pl.multiple_of((dev // 2) * 1024 + q * BLK + (dev % 2) * LANE, LANE), LANE)]


def _head(hid, lab, w):
    hbm = pl.BlockSpec(memory_space=ANY)
    sd = jax.ShapeDtypeStruct
    dma = pltpu.SemaphoreType.DMA
    vmem = pltpu.VMEM
    quarter = (LANE, HALF)
    return pl.pallas_call(
        _head_kernel,
        out_shape=(
            sd((TOK, HID), BF16),
            sd((TOK, VOC), BF16),
            sd((256, HID), F32),
            sd((PIECE, HID), F32),
            sd((PIECE, HID), F32),
            sd((256, HID), F32),
            sd((8, LANE), F32),
            sd((NBLK, 2, BLK, HALF), F32),
            sd((PIECE, HID), F32),
            sd((256, HID), F32),
            sd((PIECE, HID), F32),
            sd((PIECE, HID), F32),
        ),
        in_specs=[hbm] * 3,
        out_specs=(hbm,) * 6 + (pl.BlockSpec(memory_space=vmem),) + (hbm,) * 5,
        scratch_shapes=[
            vmem((HID, VOC), BF16),
            vmem((2, BLK, HID), BF16),
            vmem((BLK, VOC), BF16),
            vmem((BLK, VOC), BF16),
            vmem((2, BLK, HALF), F32),
            vmem((2, BLK, HALF), F32),
            vmem((2, 2) + quarter, F32),
            vmem((2,) + quarter, F32),
            vmem((2,) + quarter, F32),
            vmem((2,) + quarter, F32),
            vmem(quarter, F32),
            vmem((8, 4, LANE), I32),
            vmem((BLK, LANE), I32),
            vmem((BLK, LANE), I32),
            vmem((8, LANE), F32),
            vmem((NBLK, 8, 8, LANE), F32),
            vmem((2, BLK, LANE), F32),
            vmem((2, BLK, LANE), F32),
            vmem((2, BLK, LANE), F32),
            vmem((2, BLK, LANE), F32),
            vmem((NBLK, 8, LANE), F32),
            dma((2,)),
            dma(()),
            dma(()),
            dma((32,)),
            dma(()),
            dma((2,)),
            dma((2,)),
            dma((2,)),
            dma((NBLK,)),
            dma(()),
            dma((2,)),
            dma((4,)),
            dma((2,)),
            dma((2,)),
            dma(()),
            dma((8,)),
            dma((4,)),
            dma((4,)),
            dma(()),
            dma((2,)),
        ],
        compiler_params=pltpu.CompilerParams(collective_id=0, has_side_effects=True, vmem_limit_bytes=67_043_328),
        cost_estimate=pl.CostEstimate(flops=4 * TOK * HID * VOC, bytes_accessed=400 * 2**20, transcendentals=2 * TOK * VOC),
        name="head",
    )(hid, lab, w)


def _dhead_kernel(x_ref, g_ref, o_ref):
    o_ref[...] = lax.dot_general(x_ref[...], g_ref[...], (((0,), (0,)), ((), ())), preferred_element_type=F32).astype(BF16)


def _dhead(xall, gall):
    bm, bn = PIECE, 1024
    return pl.pallas_call(
        _dhead_kernel,
        grid=(VOC // bn, HID // bm),
        in_specs=[pl.BlockSpec((TOK, bm), lambda j, i: (0, i)), pl.BlockSpec((TOK, bn), lambda j, i: (0, j))],
        out_specs=pl.BlockSpec((bm, bn), lambda j, i: (i, j)),
        out_shape=jax.ShapeDtypeStruct((HID, VOC), BF16),
        compiler_params=pltpu.CompilerParams(vmem_limit_bytes=60 * 2**20, dimension_semantics=("arbitrary", "arbitrary")),
        cost_estimate=pl.CostEstimate(flops=2 * TOK * HID * VOC, bytes_accessed=200 * 2**20, transcendentals=0),
        name="dhead",
    )(xall, gall)


def solution(mesh):
    def device(y, x, core):
        return (y % 2) * 4 + (x % 2) * 2 + core

    first, second = [], []
    for yy in range(2):
        for xx in range(2):
            along_x = [(device(yy, xx, k), device(yy, xx + 1, k)) for k in range(2)]
            along_y = [(device(yy, xx, k), device(yy + 1, xx, k)) for k in range(2)]
            first += [along_x[0], along_y[1]]
            second += [along_y[0], along_x[1]]

    def local_step(hid, w, lab):
        xall, gall, s_n1b, s_self, y2, r1a, loss = _head(hid, lab.reshape(4, LANE), w)[:7]
        r1b = lax.ppermute(s_n1b, "tp", first)
        r2 = lax.ppermute(y2, "tp", second)
        d_head = _dhead(xall, gall)
        d_hidden = (s_self + jnp.concatenate([r1a, r1b], axis=0) + r2).astype(BF16)
        return loss[0, :1], d_hidden, d_head

    return jax.shard_map(
        local_step,
        mesh=mesh,
        in_specs=(P(("dp", "tp"), None), P(None, "tp"), P(("dp", "tp"))),
        out_specs=(P("dp"), P(("dp", "tp"), None), P("dp", "tp")),
        check_vma=False,
    )
```

```python
import functools

import jax
import jax.numpy as jnp
from jax import lax
from jax.experimental import pallas as pl
from jax.experimental.pallas import tpu as pltpu
from jax.sharding import PartitionSpec as P

F32, BF16, I32 = jnp.float32, jnp.bfloat16, jnp.int32
MESH = pl.DeviceIdType.MESH
ANY = pl.ANY

TOK = 4096
HID = 4096
VOC = 4096
BLK = 256
HALF = 2048
NBLK = TOK // BLK
LANE = 128
MIB = 1 << 20
TWO = (2,)
PAIR = (0, 1)
TILE = (8, LANE)
SUB = 16
FOUR = range(4)
PIECE = 512
INV = 1.0 / TOK


def _copy(src, dst, sem):
    return pltpu.make_async_copy(src, dst, sem)


def _send(src, dst, send_sem, recv_sem, dev):
    return pltpu.make_async_remote_copy(
        src_ref=src, dst_ref=dst, send_sem=send_sem, recv_sem=recv_sem, device_id={"tp": dev}, device_id_type=MESH
    )


def _product(lhs, rhs, put, jobs, transposed):
    pl.when(lax.axis_index("tp") < 8)(functools.partial(_pieces, lhs, rhs, put, jobs, transposed))


def _pieces(lhs, rhs, put, jobs, transposed):
    dims = (((1,), (1,)), ((), ())) if transposed else (((1,), (0,)), ((), ()))
    pieces = HALF // PIECE
    deep = 8
    for nt in range(pieces):
        acc = None
        for kt in range(deep):
            part = lax.dot_general(lhs(kt), rhs(nt, kt), dims, preferred_element_type=F32)
            acc = part if acc is None else acc + part
            for job in jobs[nt * deep + kt]:
                job()
        put(nt, acc)


def _wide(v, times=HALF // LANE):
    return jnp.concatenate([v] * times, axis=1)


def _fold(v):
    width = v.shape[1] // 2
    while width >= LANE:
        v = v[:, :width] + v[:, width:]
        width //= 2
    return v


def _column(row):
    return jnp.transpose(jnp.broadcast_to(row, (LANE, LANE)))


def _head_kernel(
    x_hbm, lab_hbm, w_hbm,
    xall, gall, s_n1b, s_self, y2, r1a, loss_out,
    zst, s_d, s_n1a, s_n2, r1n2,
    wv, xg, ga, gb, zb, pbuf, rbuf, sbuf, ab, bb, cb, lab_v, la, lb, st_new, st_loc, st_all, ml, mk, sl, tl, comb, c_lab, c_top, c_scale, loss_acc,
    w_sem, lab_sem, labtx_sem, rx, tx, xl_sem, xs_sem, zo_sem, st_sem, sttx_sem,
    zi_sem, rr, ps, ss_sem, s1tx, r1s, r1as, ab_sem, cb_sem, g_sem,
):
    me = lax.axis_index("tp")
    chip = me // 2
    c = me % 2
    x = chip % 2
    y = chip // 2
    oc = 1 - c
    partner = me + 1 - 2 * c
    dx, dy = 2 - 4 * x, 4 - 8 * y
    n1 = me + oc * dx + c * dy
    n2 = me + c * dx + oc * dy
    n1kind = 1 + c

    def chip_of(kind):
        return chip + (kind % 2) * (1 - 2 * x) + (kind // 2) * (2 - 4 * y)

    def order1(i):
        mid, end = (i // 4 + 1) // 2 % 2, i // 12
        return mid * (1 + i % 2) + 3 * end, mid * ((i - 4) // 2) + (1 - mid) * (i % 4)

    def order2(i):
        mid, end = (i // 4 + 1) // 2 % 2, i // 12
        return mid * (1 + i % 2) + 3 * (1 - mid) * (1 - end), mid * ((i - 4) // 2) + (1 - mid) * (i % 4)

    def block_id(kind, q):
        return chip_of(kind) * 4 + q

    def xrows(kind, q, part):
        return xall.at[pl.ds(pl.multiple_of(block_id(kind, q) * BLK + part * LANE, LANE), LANE)]

    def xblock(kind, q):
        return xall.at[pl.ds(pl.multiple_of(block_id(kind, q) * BLK, BLK), BLK)]

    def own(q):
        return x_hbm.at[pl.ds(pl.multiple_of(q * LANE, LANE), LANE)]

    def rxs(kind, q, part):
        return rx.at[kind * 8 + q * 2 + part]

    def wcopy(j):
        cols = pl.ds(j * PIECE, PIECE)
        return _copy(w_hbm.at[:, cols], wv.at[:, cols], w_sem.at[j])

    _copy(own(0), xg.at[0, pl.ds(pl.multiple_of(c * LANE, LANE), LANE)], xl_sem.at[0]).start()
    for j in FOUR:
        wcopy(j).start()

    barrier = pltpu.get_barrier_semaphore()
    for d in range(1, 8):
        pl.semaphore_signal(barrier, inc=1, device_id={"tp": (me + d) % 8}, device_id_type=MESH)
    pl.semaphore_wait(barrier, 7)

    for d in range(1, 8):
        _send(lab_hbm, lab_v.at[me], labtx_sem, lab_sem, (me + d) % 8).start()
    _copy(lab_hbm, lab_v.at[me], lab_sem).start()
    for q in FOUR:
        _send(own(q), xrows(0, q, c), tx, rxs(0, q, c), partner).start()
    for q in FOUR:
        _send(own(q), xrows_at(xall, me, q), tx, rxs(n1kind, q, c), n1).start()
        _send(own(q), xrows_at(xall, me, q), tx, rxs(3 - n1kind, q, c), n2).start()

    def load_x(b):
        kind, q = order1(b)
        slot = b % 2

        @pl.when(kind == 0)
        def _():
            _copy(own(q), xg.at[slot, pl.ds(pl.multiple_of(c * LANE, LANE), LANE)], xl_sem.at[slot]).start()
            _copy(xrows(0, q, oc), xg.at[slot, pl.ds(pl.multiple_of(oc * LANE, LANE), LANE)], xl_sem.at[slot]).start()

        @pl.when(kind != 0)
        def _():
            _copy(xblock(kind, q), xg.at[slot], xl_sem.at[slot]).start()

    def wait_rows(kind, q, part):
        _copy(xrows(kind, q, part), xrows(kind, q, part), rxs(kind, q, part)).wait()

    def take_rows(kind, q):
        wait_rows(kind, q, c)
        _send(xrows(kind, q, c), xrows(kind, q, c), tx, rxs(kind, q, c), partner).start()

    def part_load(b, part):
        kind, q = order1(b)
        return _copy(xrows(kind, q, part), xg.at[b % 2, pl.ds(pl.multiple_of(part * LANE, LANE), LANE)], xl_sem.at[b % 2])

    def zcopy(b, h):
        kind, q = order1(b)
        return _copy(zb.at[h], zst.at[block_id(kind, q), h], zo_sem.at[h])

    def own_store(b):
        slot = b % 2
        return _copy(xg.at[slot, pl.ds(pl.multiple_of(c * LANE, LANE), LANE)], xrows(0, b % 4, c), xs_sem.at[slot])

    def label_column(blk, part):
        return _column(lab_v[2 * (blk // 4) + part, pl.ds(blk % 4, 1), :])

    def lane_stats(col, h, r):
        rows = pl.ds(r, 8)
        z = zb[h, rows, :]
        m = ml[h, rows, :]
        hit = _wide(col[rows, :] - (me * VOC + h * HALF)) == lax.broadcasted_iota(I32, (8, HALF), 1)
        s = _fold(jnp.exp(z - _wide(m)))
        t = _fold(jnp.where(hit, z, 0.0))
        if h == 1:
            m0 = mk[0, rows, :]
            mm = jnp.maximum(m0, m)
            s = sl[0, rows, :] * jnp.exp(m0 - mm) + s * jnp.exp(m - mm)
            t = tl[0, rows, :] + t
            m = mm
        mk[h, rows, :] = m
        sl[h, rows, :] = s
        tl[h, rows, :] = t

    def label_columns(blk, col, part):
        col[pl.ds(part * LANE, LANE), :] = label_column(blk, part)

    def row_stats(part):
        rows = pl.ds(part * LANE, LANE)
        m = jnp.transpose(mk[1, rows, :])
        top = jnp.max(m, axis=0, keepdims=True)
        st_new[part : part + 1, :] = top
        st_new[2 + part : 3 + part, :] = jnp.sum(jnp.transpose(sl[1, rows, :]) * jnp.exp(m - top), axis=0, keepdims=True)
        st_new[4 + part : 5 + part, :] = jnp.sum(jnp.transpose(tl[1, rows, :]), axis=0, keepdims=True)

    def send_stats(blk):
        for d in range(1, 8):
            _send(st_loc.at[blk], st_all.at[blk, me], sttx_sem, st_sem.at[blk], (me + d) % 8).start()

    def keep_stats(blk):
        st_loc[blk] = st_new[...]
        st_all[blk, me] = st_new[...]

    def combine(blk):
        top = st_all[blk, 0, 0:2, :]
        for d in range(1, 8):
            top = jnp.maximum(top, st_all[blk, d, 0:2, :])
        s = jnp.zeros((2, LANE), F32)
        t = jnp.zeros((2, LANE), F32)
        for d in range(8):
            s = s + st_all[blk, d, 2:4, :] * jnp.exp(st_all[blk, d, 0:2, :] - top)
            t = t + st_all[blk, d, 4:6, :]
        comb[0:2, :] = top
        comb[2:4, :] = INV / s
        return top + jnp.log(s) - t

    def stats_arrived(blk):
        _copy(st_all.at[blk, pl.ds(0, 7)], st_all.at[blk, pl.ds(0, 7)], st_sem.at[blk]).wait()

    def columns(blk, par, part):
        rows = pl.ds(part * LANE, LANE)
        c_lab[par, rows, :] = label_column(blk, part)
        c_top[par, rows, :] = _column(comb[part : part + 1, :])
        c_scale[par, rows, :] = _column(comb[2 + part : 3 + part, :])

    def gradient(src, n, par, r, j):
        rows = pl.ds(pl.multiple_of(r, SUB), SUB)
        col = c_lab[par, rows, :] - (me * VOC + n * HALF + j)
        p = jnp.exp(src[n, rows, j : j + 1024] - _wide(c_top[par, rows, :], 8)) * _wide(c_scale[par, rows, :], 8)
        g = jnp.where(_wide(col, 8) == lax.broadcasted_iota(I32, (SUB, 1024), 1), p - INV, p)
        gbufs[par][rows, n * HALF + j : n * HALF + j + 1024] = g.astype(BF16)

    def gradient_jobs(src, n, par):
        return [functools.partial(gradient, src, n, par, r, j) for r in range(0, BLK, SUB) for j in (0, 1024)]

    gbufs = (ga, gb)

    def gstore(k, par):
        kind, q = order2(k)
        return _copy(gbufs[par], gall.at[pl.ds(pl.multiple_of(block_id(kind, q) * BLK, BLK), BLK)], g_sem.at[par])

    def zload(k, dst, n):
        kind, q = order2(k)
        return _copy(zst.at[block_id(kind, q), n], dst.at[n], zi_sem.at[n])

    first_kind, first_q = order2(me * 0)
    first_blk = block_id(first_kind, first_q)

    def logits(b, h, jobs):
        slot = b % 2
        def put(nt, z):
            zb[h, :, nt * PIECE : (nt + 1) * PIECE] = z
            m = z[:, :LANE]
            for j in range(1, 4):
                m = jnp.maximum(m, z[:, j * LANE : (j + 1) * LANE])
            if nt:
                m = jnp.maximum(m, ml[h])
            ml[h] = m

        _product(
            lambda kt: xg[slot, :, kt * PIECE : (kt + 1) * PIECE],
            lambda nt, kt: wv[kt * PIECE : (kt + 1) * PIECE, h * HALF + nt * PIECE : h * HALF + (nt + 1) * PIECE],
            put,
            jobs,
            False,
        )

    wait_rows(0, 0, oc)
    _copy(xrows(0, 0, oc), xg.at[0, pl.ds(pl.multiple_of(oc * LANE, LANE), LANE)], xl_sem.at[0]).start()
    _copy(lab_v, lab_v, lab_sem).wait()
    for j in FOUR:
        wcopy(j).wait()
    for j in range(4, 8):
        wcopy(j).start()

    def phase1(i, carry):
        slot = i % 2
        kind, q = order1(i)
        kprev, qprev = order1((i + NBLK - 2) % NBLK)
        kn, qn = order1((i + 1) % NBLK)

        @pl.when(i == NBLK - 1)
        def _():
            wait_rows(kind, q, oc)
            part_load(i, oc).start()

        _copy(xg.at[slot], xg.at[slot], xl_sem.at[slot]).wait()

        @pl.when(i < 4)
        def _():
            own_store(i).start()

        @pl.when(i > 0)
        def _():
            zcopy(i - 1, 1).start()
            zcopy(i - 1, 0).wait()

        @pl.when(i > 1)
        def _():
            keep_stats(block_id(kprev, qprev))

        @pl.when(i == NBLK - 2)
        def _():
            zload(0, pbuf, 0).start()
            zload(0, pbuf, 1).start()

        @pl.when(i == NBLK - 1)
        def _():
            stats_arrived(first_blk)
            loss_acc[...] = combine(first_blk)
            for part in PAIR:
                columns(first_blk, 0, part)
            for n in PAIR:
                zload(0, pbuf, n).wait()

                def some(r, carry, n=n):
                    for j in FOUR:
                        gradient(pbuf, n, 0, r * 32 + j // 2 * SUB, j % 2 * 1024)
                    return carry

                lax.fori_loop(0, 8, some, 0)

            gstore(0, 0).start()

        @pl.when((i >= 3) & (i < NBLK - 2))
        def _():
            take_rows(kn, qn)

            @pl.when(kn == n1kind)
            def _():
                _send(xrows(kn, qn, c), xrows(kn, qn, c), tx, rxs(3, qn, c), n2).start()

        jobs = [[] for _ in range(32)]
        for r in range(32):
            jobs[r].append(functools.partial(lane_stats, la, 1, r * 8))
        for part in PAIR:
            jobs[4 + 4 * part].append(functools.partial(label_columns, block_id(kind, q), lb, part))
        logits(i, 0, jobs)

        zcopy(i, 0).start()

        @pl.when(i == 0)
        def _():
            for j in range(4, 8):
                wcopy(j).wait()

        @pl.when(i > 0)
        def _():
            zcopy(i - 1, 1).wait()

        @pl.when(i > 1)
        def _():
            send_stats(block_id(kprev, qprev))

        @pl.when(i == NBLK - 2)
        def _():
            take_rows(kn, qn)
            part_load(i + 1, c).start()

        @pl.when(i < NBLK - 2)
        def _():
            wait_rows(kn, qn, oc)

            @pl.when((i >= 1) & (i < 5))
            def _():
                own_store(i - 1).wait()

            load_x(i + 1)

        la[...] = lb[...]
        jobs = [[] for _ in range(32)]
        for r in range(32):
            jobs[r].append(functools.partial(lane_stats, lb, 0, r * 8))
        for part in PAIR:
            jobs[8 + 8 * part].append(functools.partial(row_stats, part))
        logits(i, 1, jobs)
        return carry

    lax.fori_loop(0, NBLK, phase1, 0)
    last = NBLK - 1
    klast, qlast = order1(jnp.int32(last))
    kprev, qprev = order1(jnp.int32(last - 1))
    bprev, blast = block_id(kprev, qprev), block_id(klast, qlast)
    zcopy(last, 1).start()
    zcopy(last, 0).wait()
    zload(1, zb, 0).start()
    keep_stats(bprev)
    for r in range(32):
        lane_stats(la, 1, r * 8)
    send_stats(bprev)
    for part in PAIR:
        row_stats(part)
    keep_stats(blast)
    zcopy(last, 1).wait()
    zload(1, zb, 1).start()
    send_stats(blast)
    second_kind, second_q = order2(jnp.int32(1))
    second_blk = block_id(second_kind, second_q)
    stats_arrived(second_blk)
    loss_acc[...] += combine(second_blk)
    for part in PAIR:
        columns(second_blk, 1, part)

    def tile(ref, q, n):
        return ref.at[pl.ds(pl.multiple_of(q * LANE, LANE), LANE), pl.ds(pl.multiple_of(n * HALF, HALF), HALF)]

    def spair(k, n):
        return _send(
            pbuf.at[n, pl.ds(pl.multiple_of(oc * LANE, LANE), LANE)], rbuf.at[k % 2, n], ps.at[n], rr.at[(k % 2) * 2 + n], partner
        )

    def sstore_start(k, n):
        kind, q = order2(k)
        sem = ss_sem.at[n]

        @pl.when(kind == 3)
        def _():
            _copy(sbuf.at[n], tile(s_d, q, n), sem).start()

        @pl.when((kind == n1kind) & (q < 2))
        def _():
            _copy(sbuf.at[n], tile(s_n1a, q % 2, n), sem).start()

        @pl.when((kind == n1kind) & (q >= 2))
        def _():
            _copy(sbuf.at[n], tile(s_n1b, q % 2, n), sem).start()

        @pl.when(kind == 3 - n1kind)
        def _():
            _copy(sbuf.at[n], tile(s_n2, q, n), sem).start()

        @pl.when(kind == 0)
        def _():
            _copy(sbuf.at[n], tile(s_self, q, n), sem).start()

    def sstore_done(k, n):
        kind, q = order2(k)
        _copy(sbuf.at[n], tile(s_d, 0, n), ss_sem.at[n]).wait()

        @pl.when(kind == 3)
        def _():
            _send(tile(s_d, q, n), tile(r1n2, q, n), s1tx, r1s.at[q * 2 + n], n1).start()

        @pl.when((kind == n1kind) & (q < 2))
        def _():
            _send(tile(s_n1a, q % 2, n), tile(r1a, q % 2, n), s1tx, r1as.at[(q % 2) * 2 + n], n1).start()

    def stage2_load(q, n):
        _copy(tile(r1n2, q, n), tile(r1n2, q, n), r1s.at[q * 2 + n]).wait()
        _copy(tile(s_n2, q, n), ab.at[n], ab_sem.at[n * 2]).start()
        _copy(tile(r1n2, q, n), bb.at[n], ab_sem.at[n * 2 + 1]).start()

    def pair_sum(k, n, r):
        sbuf[n, pl.ds(r, SUB), :] = pbuf[n, pl.ds(pl.multiple_of(c * LANE + r, SUB), SUB), :] + rbuf[k % 2, n, pl.ds(r, SUB), :]

    def stage2_sum(n, r):
        cb[n, pl.ds(r, SUB), :] = ab[n, pl.ds(r, SUB), :] + bb[n, pl.ds(r, SUB), :]

    def rwait(k, n):
        _copy(rbuf.at[k % 2, n], rbuf.at[k % 2, n], rr.at[(k % 2) * 2 + n]).wait()

    def loss_part(k, blk):
        loss_acc[...] += jnp.where(k < NBLK - 2, combine(blk), 0.0)

    def sub(k, cur):
        nxt = 1 - cur
        kind2, q2 = order2((k + 2) % NBLK)
        blk2 = block_id(kind2, q2)

        def trip(n):
            @pl.when(k < NBLK - 1)
            def _():
                zload(k + 1, zb, n).wait()

            @pl.when(k >= 1)
            def _():
                rwait(k - 1, n)
                spair(k - 1, n).wait_send()
                if n == 0:
                    gstore(k - 1, nxt).wait()

            if n == 0:

                @pl.when(k < NBLK - 2)
                def _():
                    stats_arrived(blk2)

            @pl.when(k >= 12)
            def _():
                _copy(tile(s_n2, 0, n), ab.at[n], ab_sem.at[n * 2]).wait()
                _copy(tile(r1n2, 0, n), bb.at[n], ab_sem.at[n * 2 + 1]).wait()

            @pl.when(k >= 13)
            def _():
                _copy(cb.at[n], tile(y2, 0, n), cb_sem.at[n]).wait()

            jobs = [[] for _ in range(32)]
            for r in range(8):
                jobs[r // 2].append(functools.partial(pair_sum, k - 1, n, r * SUB))
                jobs[20 + r].append(functools.partial(stage2_sum, n, r * SUB))
            for r, job in enumerate(gradient_jobs(zb, n, nxt)):
                jobs[4 + r * 7 // 8].append(job)
            if n == 0:
                jobs[8].append(lambda: loss_part(k, blk2))
            else:
                for part in PAIR:
                    jobs[8 + 8 * part].append(functools.partial(columns, blk2, cur, part))

            def put(nt, acc):
                pbuf[n, :, nt * PIECE : (nt + 1) * PIECE] = acc

            _product(
                lambda kt: gbufs[cur][:, kt * PIECE : (kt + 1) * PIECE],
                lambda nt, kt: wv[pl.ds(pl.multiple_of(n * HALF + nt * PIECE, PIECE), PIECE), kt * PIECE : (kt + 1) * PIECE],
                put,
                jobs,
                True,
            )

            spair(k, n).start()

            @pl.when(k < NBLK - 2)
            def _():
                zload(k + 2, zb, n).start()

            @pl.when(k >= 2 - n)
            def _():
                sstore_done(k - 2 + n, 1 - n)

            @pl.when(k >= 1)
            def _():
                sstore_start(k - 1, n)

            @pl.when(k >= 12)
            def _():
                _copy(cb.at[n], tile(y2, k - 12, n), cb_sem.at[n]).start()

            @pl.when((k >= 11) & (k < NBLK - 1))
            def _():
                stage2_load(k - 11, n)


        trip(0)
        trip(1)

        @pl.when(k < NBLK - 1)
        def _():
            gstore(k + 1, nxt).start()

    def pair(p, carry):
        sub(2 * p, 0)
        sub(2 * p + 1, 1)
        return carry

    lax.fori_loop(0, NBLK // 2, pair, 0)

    kl = jnp.int32(NBLK - 1)
    for n in PAIR:
        rwait(kl, n)
        spair(kl, n).wait_send()
        if n == 0:
            sstore_done(kl - 1, 1)
        for r in range(8):
            pair_sum(kl, n, r * SUB)
        sstore_start(kl, n)
    for n in PAIR:
        sstore_done(kl, n)
    gstore(kl, 1).wait()
    for n in PAIR:
        _copy(cb.at[n], tile(y2, 0, n), cb_sem.at[n]).wait()

    loss_out[...] = jnp.full(TILE, jnp.sum(loss_acc[...]) * INV, F32)

    for i in FOUR:
        _copy(tile(r1a, i // 2, i % 2), tile(r1a, i // 2, i % 2), r1as.at[i]).wait()
    _copy(s_d, s_d, s1tx).wait()
    _copy(s_n1a, s_n1a, s1tx).wait()
    _copy(xall.at[pl.ds(0, 28 * LANE)], xall.at[pl.ds(0, 28 * LANE)], tx).wait()
    for d in range(7):
        _copy(lab_v.at[d], lab_v.at[d], labtx_sem).wait()
        _copy(st_loc, st_loc, sttx_sem).wait()


def xrows_at(xall, dev, q):
    return xall.at[pl.ds(pl.multiple_of((dev // 2) * 1024 + q * BLK + (dev % 2) * LANE, LANE), LANE)]


def _head(hid, lab, w):
    hbm = pl.BlockSpec(memory_space=ANY)
    sd = jax.ShapeDtypeStruct
    dma = pltpu.SemaphoreType.DMA
    vmem = pltpu.VMEM
    quarter = (LANE, HALF)
    return pl.pallas_call(
        _head_kernel,
        out_shape=(
            sd((TOK, HID), BF16),
            sd((TOK, VOC), BF16),
            sd((256, HID), F32),
            sd((PIECE, HID), F32),
            sd((PIECE, HID), F32),
            sd((256, HID), F32),
            sd(TILE, F32),
            sd((NBLK, 2, BLK, HALF), F32),
            sd((PIECE, HID), F32),
            sd((256, HID), F32),
            sd((PIECE, HID), F32),
            sd((PIECE, HID), F32),
        ),
        in_specs=[hbm] * 3,
        out_specs=(hbm,) * 6 + (pl.BlockSpec(memory_space=vmem),) + (hbm,) * 5,
        scratch_shapes=[
            vmem((HID, VOC), BF16),
            vmem((2, BLK, HID), BF16),
            vmem((BLK, VOC), BF16),
            vmem((BLK, VOC), BF16),
            vmem((2, BLK, HALF), F32),
            vmem((2, BLK, HALF), F32),
            vmem((2, 2) + quarter, F32),
            vmem(TWO + quarter, F32),
            vmem(TWO + quarter, F32),
            vmem(TWO + quarter, F32),
            vmem(TWO + quarter, F32),
            vmem((8, 4, LANE), I32),
            vmem((BLK, LANE), I32),
            vmem((BLK, LANE), I32),
            vmem(TILE, F32),
            vmem((NBLK,) + TILE, F32),
            vmem((NBLK, 8) + TILE, F32),
            vmem((2, BLK, LANE), F32),
            vmem((2, BLK, LANE), F32),
            vmem((2, BLK, LANE), F32),
            vmem((2, BLK, LANE), F32),
            vmem(TILE, F32),
            vmem((2, BLK, LANE), I32),
            vmem((2, BLK, LANE), F32),
            vmem((2, BLK, LANE), F32),
            vmem((2, LANE), F32),
            dma((8,)),
            dma(()),
            dma(()),
            dma((32,)),
            dma(()),
            dma(TWO),
            dma(TWO),
            dma(TWO),
            dma((NBLK,)),
            dma(()),
            dma(TWO),
            dma((4,)),
            dma(TWO),
            dma(TWO),
            dma(()),
            dma((8,)),
            dma((4,)),
            dma((4,)),
            dma(TWO),
            dma(TWO),
        ],
        compiler_params=pltpu.CompilerParams(collective_id=0, has_side_effects=True, vmem_limit_bytes=67_043_328),
        cost_estimate=pl.CostEstimate(flops=4 * TOK * HID * VOC, bytes_accessed=400 * MIB, transcendentals=2 * TOK * VOC),
        name="head",
    )(hid, lab, w)


def _dhead_kernel(x_hbm, g_hbm, o_hbm, gv, xb, ob, x_sem, g_sem, o_sem):
    rows = HID // PIECE

    def xload(b):
        return _copy(x_hbm.at[:, pl.ds(pl.multiple_of(b * PIECE, PIECE), PIECE)], xb.at[b % 2], x_sem.at[b % 2])

    def gload(j):
        cols = pl.ds(pl.multiple_of(j * PIECE, PIECE), PIECE)
        return _copy(g_hbm.at[:, cols], gv.at[:, cols], g_sem.at[j])

    def ostore(b, n):
        dst = o_hbm.at[pl.ds(pl.multiple_of(b * PIECE, PIECE), PIECE), pl.ds(pl.multiple_of(n * HALF, HALF), HALF)]
        return _copy(ob.at[n], dst, o_sem.at[n])

    def dot(lhs, rhs):
        return lax.dot_general(lhs, rhs, (((0,), (0,)), ((), ())), preferred_element_type=F32).astype(BF16)

    xload(0).start()
    gload(0).start()
    gload(1).start()
    xload(0).wait()

    def first(j, carry):
        gload(j).wait()

        @pl.when(j < 6)
        def _():
            gload(j + 2).start()

        @pl.when(j == 6)
        def _():
            xload(1).start()

        cols = pl.ds(pl.multiple_of(j % 4 * PIECE, PIECE), PIECE)
        ob[j // 4, :, cols] = dot(xb[0], gv[:, pl.ds(pl.multiple_of(j * PIECE, PIECE), PIECE)])
        return carry

    lax.fori_loop(0, 8, first, 0)
    ostore(0, 0).start()
    ostore(0, 1).start()

    def block(b, carry):
        xload(b).wait()

        @pl.when(b < rows - 1)
        def _():
            xload(b + 1).start()

        def half(n, carry):
            ostore(b - 1, n).wait()

            @pl.when(b < rows)
            def _():
                ob[n] = dot(xb[b % 2], gv[:, pl.ds(pl.multiple_of(n * HALF, HALF), HALF)])

            ostore(b, n).start()
            return carry

        return lax.fori_loop(0, 2, half, carry)

    lax.fori_loop(1, rows, block, 0)
    ostore(rows - 1, 0).wait()
    ostore(rows - 1, 1).wait()


def _dhead(xall, gall):
    hbm = pl.BlockSpec(memory_space=ANY)
    dma = pltpu.SemaphoreType.DMA
    return pl.pallas_call(
        _dhead_kernel,
        in_specs=[hbm, hbm],
        out_specs=hbm,
        out_shape=jax.ShapeDtypeStruct((HID, VOC), BF16),
        scratch_shapes=[
            pltpu.VMEM((TOK, VOC), BF16),
            pltpu.VMEM((2, TOK, PIECE), BF16),
            pltpu.VMEM((2, PIECE, HALF), BF16),
            dma(TWO),
            dma((8,)),
            dma(TWO),
        ],
        compiler_params=pltpu.CompilerParams(vmem_limit_bytes=60 * MIB),
        cost_estimate=pl.CostEstimate(flops=2 * TOK * HID * VOC, bytes_accessed=200 * MIB, transcendentals=0),
        name="dhead",
    )(xall, gall)


def _final_kernel(s_ref, a_ref, b_ref, r_ref, l_ref, o_ref, loss_ref):
    i = pl.program_id(0)
    half = pl.num_programs(0) // 2

    @pl.when(i < half)
    def _():
        o_ref[...] = (s_ref[...] + a_ref[...] + r_ref[...]).astype(BF16)

    @pl.when(i >= half)
    def _():
        o_ref[...] = (s_ref[...] + b_ref[...] + r_ref[...]).astype(BF16)

    loss_ref[0] = l_ref[0, 0]


def _final(s_self, r1a, r1b, r2, loss):
    steps = 8
    rows = PIECE // steps
    spec = functools.partial(pl.BlockSpec, (rows, HID))
    return pl.pallas_call(
        _final_kernel,
        grid=(steps,),
        in_specs=[
            spec(lambda i: (i, 0)),
            spec(lambda i: (jnp.minimum(i, steps // 2 - 1), 0)),
            spec(lambda i: (jnp.maximum(i - steps // 2, 0), 0)),
            spec(lambda i: (i, 0)),
            pl.BlockSpec(TILE, lambda i: (0, 0)),
        ],
        out_specs=(spec(lambda i: (i, 0)), pl.BlockSpec(memory_space=pltpu.SMEM)),
        out_shape=(jax.ShapeDtypeStruct((PIECE, HID), BF16), jax.ShapeDtypeStruct((1,), F32)),
        compiler_params=pltpu.CompilerParams(vmem_limit_bytes=62 * MIB),
        cost_estimate=pl.CostEstimate(flops=3 * PIECE * HID, bytes_accessed=28 * MIB, transcendentals=0),
        name="final",
    )(s_self, r1a, r1b, r2, loss)


def solution(mesh):
    def device(y, x, core):
        return (y % 2) * 4 + (x % 2) * 2 + core

    first, second = [], []
    for yy in PAIR:
        for xx in PAIR:
            along_x = [(device(yy, xx, k), device(yy, xx + 1, k)) for k in PAIR]
            along_y = [(device(yy, xx, k), device(yy + 1, xx, k)) for k in PAIR]
            first += [along_x[0], along_y[1]]
            second += [along_y[0], along_x[1]]

    def local_step(hid, w, lab):
        xall, gall, s_n1b, s_self, y2, r1a, loss = _head(hid, lab.reshape(4, LANE), w)[:7]
        r1b = lax.ppermute(s_n1b, "tp", first)
        r2 = lax.ppermute(y2, "tp", second)
        d_head = _dhead(xall, gall)
        d_hidden, mean_loss = _final(s_self, r1a, r1b, r2, loss)
        return mean_loss, d_hidden, d_head

    return jax.shard_map(
        local_step,
        mesh=mesh,
        in_specs=(P(("dp", "tp"), None), P(None, "tp"), P(("dp", "tp"))),
        out_specs=(P("dp"), P(("dp", "tp"), None), P("dp", "tp")),
        check_vma=False,
    )
```

```python
import functools

import jax
import jax.numpy as jnp
from jax import lax
from jax.experimental import pallas as pl
from jax.experimental.pallas import tpu as pltpu
from jax.sharding import PartitionSpec as P

F32, BF16, I32 = jnp.float32, jnp.bfloat16, jnp.int32
MESH = pl.DeviceIdType.MESH
ANY = pl.ANY

TOK = 4096
HID = 4096
VOC = 4096
BLK = 256
HALF = 2048
NBLK = TOK // BLK
LANE = 128
MIB = 1 << 20
TWO = (2,)
PAIR = (0, 1)
TILE = (8, LANE)
SUB = 16
FOUR = range(4)
LATE = 9
PIECE = 512
INV = 1.0 / TOK


def _copy(src, dst, sem):
    return pltpu.make_async_copy(src, dst, sem)


def _send(src, dst, send_sem, recv_sem, dev):
    return pltpu.make_async_remote_copy(
        src_ref=src, dst_ref=dst, send_sem=send_sem, recv_sem=recv_sem, device_id={"tp": dev}, device_id_type=MESH
    )


def _product(lhs, rhs, put, jobs, transposed):
    pl.when(lax.axis_index("tp") < 8)(functools.partial(_pieces, lhs, rhs, put, jobs, transposed))


def _pieces(lhs, rhs, put, jobs, transposed):
    dims = (((1,), (1,)), ((), ())) if transposed else (((1,), (0,)), ((), ()))
    pieces = HALF // PIECE
    deep = 8
    for nt in range(pieces):
        acc = None
        for kt in range(deep):
            part = lax.dot_general(lhs(kt), rhs(nt, kt), dims, preferred_element_type=F32)
            acc = part if acc is None else acc + part
            for job in jobs[nt * deep + kt]:
                job()
        put(nt, acc)


def _wide(v, times=HALF // LANE):
    return jnp.concatenate([v] * times, axis=1)


def _fold(v):
    width = v.shape[1] // 2
    while width >= LANE:
        v = v[:, :width] + v[:, width:]
        width //= 2
    return v


def _column(row):
    return jnp.transpose(jnp.broadcast_to(row, (LANE, LANE)))


def _head_kernel(
    x_hbm, lab_hbm, w_hbm,
    xall, gall, s_n1b, s_self, y2, r1a, loss_out,
    zst, s_d, s_n1a, s_n2, r1n2,
    wv, xg, ga, gb, zb, pbuf, rbuf, sbuf, ab, bb, cb, lab_v, la, lb, st_new, st_loc, st_all, ml, mk, sl, tl, comb, c_lab, c_top, c_scale, loss_acc,
    w_sem, lab_sem, labtx_sem, rx, tx, xl_sem, xs_sem, zo_sem, st_sem, sttx_sem,
    zi_sem, rr, ps, ss_sem, s1tx, r1s, r1as, ab_sem, cb_sem, g_sem,
):
    me = lax.axis_index("tp")
    chip = me // 2
    c = me % 2
    x = chip % 2
    y = chip // 2
    oc = 1 - c
    partner = me + 1 - 2 * c
    dx, dy = 2 - 4 * x, 4 - 8 * y
    n1 = me + oc * dx + c * dy
    n2 = me + c * dx + oc * dy
    n1kind = 1 + c

    def chip_of(kind):
        return chip + (kind % 2) * (1 - 2 * x) + (kind // 2) * (2 - 4 * y)

    def order1(i):
        mid, end = (i // 4 + 1) // 2 % 2, i // 12
        return mid * (1 + i % 2) + 3 * end, mid * ((i - 4) // 2) + (1 - mid) * (i % 4)

    def order2(i):
        mid, end = (i // 4 + 1) // 2 % 2, i // 12
        return mid * (1 + i % 2) + 3 * (1 - mid) * (1 - end), mid * ((i - 4) // 2) + (1 - mid) * (i % 4)

    def block_id(kind, q):
        return chip_of(kind) * 4 + q

    def xrows(kind, q, part):
        return xall.at[pl.ds(pl.multiple_of(block_id(kind, q) * BLK + part * LANE, LANE), LANE)]

    def xblock(kind, q):
        return xall.at[pl.ds(pl.multiple_of(block_id(kind, q) * BLK, BLK), BLK)]

    def own(q):
        return x_hbm.at[pl.ds(pl.multiple_of(q * LANE, LANE), LANE)]

    def rxs(kind, q, part):
        return rx.at[kind * 8 + q * 2 + part]

    def wcopy(j):
        cols = pl.ds(j * PIECE, PIECE)
        return _copy(w_hbm.at[:, cols], wv.at[:, cols], w_sem.at[j])

    _copy(own(0), xg.at[0, pl.ds(pl.multiple_of(c * LANE, LANE), LANE)], xl_sem.at[0]).start()
    for j in FOUR:
        wcopy(j).start()

    barrier = pltpu.get_barrier_semaphore()
    for d in range(1, 8):
        pl.semaphore_signal(barrier, inc=1, device_id={"tp": (me + d) % 8}, device_id_type=MESH)
    pl.semaphore_wait(barrier, 7)

    for d in range(1, 8):
        _send(lab_hbm, lab_v.at[me], labtx_sem, lab_sem, (me + d) % 8).start()
    _copy(lab_hbm, lab_v.at[me], lab_sem).start()
    for q in FOUR:
        _send(own(q), xrows(0, q, c), tx, rxs(0, q, c), partner).start()
    for q in FOUR:
        _send(own(q), xrows_at(xall, me, q), tx, rxs(n1kind, q, c), n1).start()
        _send(own(q), xrows_at(xall, me, q), tx, rxs(3 - n1kind, q, c), n2).start()

    def load_x(b):
        kind, q = order1(b)
        slot = b % 2

        @pl.when(kind == 0)
        def _():
            _copy(own(q), xg.at[slot, pl.ds(pl.multiple_of(c * LANE, LANE), LANE)], xl_sem.at[slot]).start()
            _copy(xrows(0, q, oc), xg.at[slot, pl.ds(pl.multiple_of(oc * LANE, LANE), LANE)], xl_sem.at[slot]).start()

        @pl.when(kind != 0)
        def _():
            _copy(xblock(kind, q), xg.at[slot], xl_sem.at[slot]).start()

    def wait_rows(kind, q, part):
        _copy(xrows(kind, q, part), xrows(kind, q, part), rxs(kind, q, part)).wait()

    def take_rows(kind, q):
        wait_rows(kind, q, c)
        _send(xrows(kind, q, c), xrows(kind, q, c), tx, rxs(kind, q, c), partner).start()

        @pl.when(kind == n1kind)
        def _():
            _send(xrows(kind, q, c), xrows(kind, q, c), tx, rxs(3, q, c), n2).start()

    def part_load(b, part):
        kind, q = order1(b)
        return _copy(xrows(kind, q, part), xg.at[b % 2, pl.ds(pl.multiple_of(part * LANE, LANE), LANE)], xl_sem.at[b % 2])

    def zcopy(b, h):
        kind, q = order1(b)
        return _copy(zb.at[h], zst.at[block_id(kind, q), h], zo_sem.at[h])

    def own_store(b):
        slot = b % 2
        return _copy(xg.at[slot, pl.ds(pl.multiple_of(c * LANE, LANE), LANE)], xrows(0, b % 4, c), xs_sem.at[slot])

    def label_column(blk, part):
        return _column(lab_v[2 * (blk // 4) + part, pl.ds(blk % 4, 1), :])

    def lane_stats(col, h, r):
        rows = pl.ds(r, 8)
        z = zb[h, rows, :]
        m = ml[h, rows, :]
        hit = _wide(col[rows, :] - (me * VOC + h * HALF)) == lax.broadcasted_iota(I32, (8, HALF), 1)
        s = _fold(jnp.exp(z - _wide(m)))
        t = _fold(jnp.where(hit, z, 0.0))
        if h == 1:
            m0 = mk[0, rows, :]
            mm = jnp.maximum(m0, m)
            s = sl[0, rows, :] * jnp.exp(m0 - mm) + s * jnp.exp(m - mm)
            t = tl[0, rows, :] + t
            m = mm
        mk[h, rows, :] = m
        sl[h, rows, :] = s
        tl[h, rows, :] = t

    def label_columns(blk, col, part):
        col[pl.ds(part * LANE, LANE), :] = label_column(blk, part)

    def row_stats(part):
        rows = pl.ds(part * LANE, LANE)
        m = jnp.transpose(mk[1, rows, :])
        top = jnp.max(m, axis=0, keepdims=True)
        st_new[part : part + 1, :] = top
        st_new[2 + part : 3 + part, :] = jnp.sum(jnp.transpose(sl[1, rows, :]) * jnp.exp(m - top), axis=0, keepdims=True)
        st_new[4 + part : 5 + part, :] = jnp.sum(jnp.transpose(tl[1, rows, :]), axis=0, keepdims=True)

    def send_stats(blk):
        for d in range(1, 8):
            _send(st_loc.at[blk], st_all.at[blk, me], sttx_sem, st_sem.at[blk], (me + d) % 8).start()

    def keep_stats(blk):
        st_loc[blk] = st_new[...]
        st_all[blk, me] = st_new[...]

    def combine(blk):
        top = st_all[blk, 0, 0:2, :]
        for d in range(1, 8):
            top = jnp.maximum(top, st_all[blk, d, 0:2, :])
        s = jnp.zeros((2, LANE), F32)
        t = jnp.zeros((2, LANE), F32)
        for d in range(8):
            s = s + st_all[blk, d, 2:4, :] * jnp.exp(st_all[blk, d, 0:2, :] - top)
            t = t + st_all[blk, d, 4:6, :]
        comb[0:2, :] = top
        comb[2:4, :] = INV / s
        return top + jnp.log(s) - t

    def stats_arrived(blk):
        _copy(st_all.at[blk, pl.ds(0, 7)], st_all.at[blk, pl.ds(0, 7)], st_sem.at[blk]).wait()

    def columns(blk, par, part):
        rows = pl.ds(part * LANE, LANE)
        c_lab[par, rows, :] = label_column(blk, part)
        c_top[par, rows, :] = _column(comb[part : part + 1, :])
        c_scale[par, rows, :] = _column(comb[2 + part : 3 + part, :])

    def gradient(src, n, par, r, j):
        rows = pl.ds(pl.multiple_of(r, SUB), SUB)
        col = c_lab[par, rows, :] - (me * VOC + n * HALF + j)
        p = jnp.exp(src[n, rows, j : j + 1024] - _wide(c_top[par, rows, :], 8)) * _wide(c_scale[par, rows, :], 8)
        g = jnp.where(_wide(col, 8) == lax.broadcasted_iota(I32, (SUB, 1024), 1), p - INV, p)
        gbufs[par][rows, n * HALF + j : n * HALF + j + 1024] = g.astype(BF16)

    def gradient_jobs(src, n, par):
        return [functools.partial(gradient, src, n, par, r, j) for r in range(0, BLK, SUB) for j in (0, 1024)]

    gbufs = (ga, gb)

    def gstore(k, par):
        kind, q = order2(k)
        return _copy(gbufs[par], gall.at[pl.ds(pl.multiple_of(block_id(kind, q) * BLK, BLK), BLK)], g_sem.at[par])

    def zload(k, dst, n):
        kind, q = order2(k)
        return _copy(zst.at[block_id(kind, q), n], dst.at[n], zi_sem.at[n])

    first_kind, first_q = order2(me * 0)
    first_blk = block_id(first_kind, first_q)

    def logits(b, h, jobs):
        slot = b % 2
        def put(nt, z):
            zb[h, :, nt * PIECE : (nt + 1) * PIECE] = z
            m = z[:, :LANE]
            for j in range(1, 4):
                m = jnp.maximum(m, z[:, j * LANE : (j + 1) * LANE])
            if nt:
                m = jnp.maximum(m, ml[h])
            ml[h] = m

        _product(
            lambda kt: xg[slot, :, kt * PIECE : (kt + 1) * PIECE],
            lambda nt, kt: wv[kt * PIECE : (kt + 1) * PIECE, h * HALF + nt * PIECE : h * HALF + (nt + 1) * PIECE],
            put,
            jobs,
            False,
        )

    wait_rows(0, 0, oc)
    _copy(xrows(0, 0, oc), xg.at[0, pl.ds(pl.multiple_of(oc * LANE, LANE), LANE)], xl_sem.at[0]).start()
    _copy(lab_v, lab_v, lab_sem).wait()
    for j in FOUR:
        wcopy(j).wait()
    for j in range(4, 8):
        wcopy(j).start()

    def phase1(i, carry):
        slot = i % 2
        kind, q = order1(i)
        kprev, qprev = order1((i + NBLK - 2) % NBLK)
        kn, qn = order1((i + 1) % NBLK)

        @pl.when((i == LATE + 1) | (i == NBLK - 1))
        def _():
            wait_rows(kind, q, oc)
            part_load(i, oc).start()

        _copy(xg.at[slot], xg.at[slot], xl_sem.at[slot]).wait()

        @pl.when(i < 4)
        def _():
            own_store(i).start()

        @pl.when(i > 0)
        def _():
            zcopy(i - 1, 1).start()
            zcopy(i - 1, 0).wait()

        @pl.when(i > 1)
        def _():
            keep_stats(block_id(kprev, qprev))

        @pl.when(i == NBLK - 2)
        def _():
            zload(0, pbuf, 0).start()
            zload(0, pbuf, 1).start()

        @pl.when(i == NBLK - 1)
        def _():
            stats_arrived(first_blk)
            loss_acc[...] = combine(first_blk)
            for part in PAIR:
                columns(first_blk, 0, part)
            for n in PAIR:
                zload(0, pbuf, n).wait()

                def some(r, carry, n=n):
                    for j in FOUR:
                        gradient(pbuf, n, 0, r * 32 + j // 2 * SUB, j % 2 * 1024)
                    return carry

                lax.fori_loop(0, 8, some, 0)

            gstore(0, 0).start()

        @pl.when((i >= 3) & (i != LATE) & (i < NBLK - 2))
        def _():
            take_rows(kn, qn)

        jobs = [[] for _ in range(32)]
        for r in range(32):
            jobs[r].append(functools.partial(lane_stats, la, 1, r * 8))
        for part in PAIR:
            jobs[4 + 4 * part].append(functools.partial(label_columns, block_id(kind, q), lb, part))
        logits(i, 0, jobs)

        zcopy(i, 0).start()

        @pl.when(i == 0)
        def _():
            for j in range(4, 8):
                wcopy(j).wait()

        @pl.when(i > 0)
        def _():
            zcopy(i - 1, 1).wait()

        @pl.when(i > 1)
        def _():
            send_stats(block_id(kprev, qprev))

        @pl.when((i == LATE) | (i == NBLK - 2))
        def _():
            take_rows(kn, qn)
            part_load(i + 1, c).start()

        @pl.when((i != LATE) & (i < NBLK - 2))
        def _():
            wait_rows(kn, qn, oc)

            @pl.when((i >= 1) & (i < 5))
            def _():
                own_store(i - 1).wait()

            load_x(i + 1)

        la[...] = lb[...]
        jobs = [[] for _ in range(32)]
        for r in range(32):
            jobs[r].append(functools.partial(lane_stats, lb, 0, r * 8))
        for part in PAIR:
            jobs[8 + 8 * part].append(functools.partial(row_stats, part))
        logits(i, 1, jobs)
        return carry

    lax.fori_loop(0, NBLK, phase1, 0)
    last = NBLK - 1
    klast, qlast = order1(jnp.int32(last))
    kprev, qprev = order1(jnp.int32(last - 1))
    bprev, blast = block_id(kprev, qprev), block_id(klast, qlast)
    zcopy(last, 1).start()
    zcopy(last, 0).wait()
    zload(1, zb, 0).start()
    keep_stats(bprev)
    for r in range(32):
        lane_stats(la, 1, r * 8)
    send_stats(bprev)
    for part in PAIR:
        row_stats(part)
    keep_stats(blast)
    zcopy(last, 1).wait()
    zload(1, zb, 1).start()
    send_stats(blast)
    second_kind, second_q = order2(jnp.int32(1))
    second_blk = block_id(second_kind, second_q)
    stats_arrived(second_blk)
    loss_acc[...] += combine(second_blk)
    for part in PAIR:
        columns(second_blk, 1, part)

    def tile(ref, q, n):
        return ref.at[pl.ds(pl.multiple_of(q * LANE, LANE), LANE), pl.ds(pl.multiple_of(n * HALF, HALF), HALF)]

    def spair(k, n):
        return _send(
            pbuf.at[n, pl.ds(pl.multiple_of(oc * LANE, LANE), LANE)], rbuf.at[k % 2, n], ps.at[n], rr.at[(k % 2) * 2 + n], partner
        )

    def sstore_start(k, n):
        kind, q = order2(k)
        sem = ss_sem.at[n]

        @pl.when(kind == 3)
        def _():
            _copy(sbuf.at[n], tile(s_d, q, n), sem).start()

        @pl.when((kind == n1kind) & (q < 2))
        def _():
            _copy(sbuf.at[n], tile(s_n1a, q % 2, n), sem).start()

        @pl.when((kind == n1kind) & (q >= 2))
        def _():
            _copy(sbuf.at[n], tile(s_n1b, q % 2, n), sem).start()

        @pl.when(kind == 3 - n1kind)
        def _():
            _copy(sbuf.at[n], tile(s_n2, q, n), sem).start()

        @pl.when(kind == 0)
        def _():
            _copy(sbuf.at[n], tile(s_self, q, n), sem).start()

    def sstore_done(k, n):
        kind, q = order2(k)
        _copy(sbuf.at[n], tile(s_d, 0, n), ss_sem.at[n]).wait()

        @pl.when(kind == 3)
        def _():
            _send(tile(s_d, q, n), tile(r1n2, q, n), s1tx, r1s.at[q * 2 + n], n1).start()

        @pl.when((kind == n1kind) & (q < 2))
        def _():
            _send(tile(s_n1a, q % 2, n), tile(r1a, q % 2, n), s1tx, r1as.at[(q % 2) * 2 + n], n1).start()

    def stage2_load(q, n):
        _copy(tile(r1n2, q, n), tile(r1n2, q, n), r1s.at[q * 2 + n]).wait()
        _copy(tile(s_n2, q, n), ab.at[n], ab_sem.at[n * 2]).start()
        _copy(tile(r1n2, q, n), bb.at[n], ab_sem.at[n * 2 + 1]).start()

    def pair_sum(k, n, r):
        sbuf[n, pl.ds(r, SUB), :] = pbuf[n, pl.ds(pl.multiple_of(c * LANE + r, SUB), SUB), :] + rbuf[k % 2, n, pl.ds(r, SUB), :]

    def stage2_sum(n, r):
        cb[n, pl.ds(r, SUB), :] = ab[n, pl.ds(r, SUB), :] + bb[n, pl.ds(r, SUB), :]

    def rwait(k, n):
        _copy(rbuf.at[k % 2, n], rbuf.at[k % 2, n], rr.at[(k % 2) * 2 + n]).wait()

    def loss_part(k, blk):
        loss_acc[...] += jnp.where(k < NBLK - 2, combine(blk), 0.0)

    def sub(k, cur):
        nxt = 1 - cur
        kind2, q2 = order2((k + 2) % NBLK)
        blk2 = block_id(kind2, q2)

        def trip(n):
            @pl.when(k < NBLK - 1)
            def _():
                zload(k + 1, zb, n).wait()

            @pl.when(k >= 1)
            def _():
                rwait(k - 1, n)
                spair(k - 1, n).wait_send()
                if n == 0:
                    gstore(k - 1, nxt).wait()

            if n == 0:

                @pl.when(k < NBLK - 2)
                def _():
                    stats_arrived(blk2)

            @pl.when(k >= 12)
            def _():
                _copy(tile(s_n2, 0, n), ab.at[n], ab_sem.at[n * 2]).wait()
                _copy(tile(r1n2, 0, n), bb.at[n], ab_sem.at[n * 2 + 1]).wait()

            @pl.when(k >= 13)
            def _():
                _copy(cb.at[n], tile(y2, 0, n), cb_sem.at[n]).wait()

            jobs = [[] for _ in range(32)]
            for r in range(8):
                jobs[r // 2].append(functools.partial(pair_sum, k - 1, n, r * SUB))
                jobs[20 + r].append(functools.partial(stage2_sum, n, r * SUB))
            for r, job in enumerate(gradient_jobs(zb, n, nxt)):
                jobs[4 + r * 7 // 8].append(job)
            if n == 0:
                jobs[8].append(lambda: loss_part(k, blk2))
            else:
                for part in PAIR:
                    jobs[8 + 8 * part].append(functools.partial(columns, blk2, cur, part))

            def put(nt, acc):
                pbuf[n, :, nt * PIECE : (nt + 1) * PIECE] = acc

            _product(
                lambda kt: gbufs[cur][:, kt * PIECE : (kt + 1) * PIECE],
                lambda nt, kt: wv[pl.ds(pl.multiple_of(n * HALF + nt * PIECE, PIECE), PIECE), kt * PIECE : (kt + 1) * PIECE],
                put,
                jobs,
                True,
            )

            spair(k, n).start()

            @pl.when(k < NBLK - 2)
            def _():
                zload(k + 2, zb, n).start()

            @pl.when(k >= 2 - n)
            def _():
                sstore_done(k - 2 + n, 1 - n)

            @pl.when(k >= 1)
            def _():
                sstore_start(k - 1, n)

            @pl.when(k >= 12)
            def _():
                _copy(cb.at[n], tile(y2, k - 12, n), cb_sem.at[n]).start()

            @pl.when((k >= 11) & (k < NBLK - 1))
            def _():
                stage2_load(k - 11, n)


        trip(0)
        trip(1)

        @pl.when(k < NBLK - 1)
        def _():
            gstore(k + 1, nxt).start()

    def pair(p, carry):
        sub(2 * p, 0)
        sub(2 * p + 1, 1)
        return carry

    lax.fori_loop(0, NBLK // 2, pair, 0)

    kl = jnp.int32(NBLK - 1)
    for n in PAIR:
        rwait(kl, n)
        spair(kl, n).wait_send()
        if n == 0:
            sstore_done(kl - 1, 1)
        for r in range(8):
            pair_sum(kl, n, r * SUB)
        sstore_start(kl, n)
    for n in PAIR:
        sstore_done(kl, n)
    gstore(kl, 1).wait()
    for n in PAIR:
        _copy(cb.at[n], tile(y2, 0, n), cb_sem.at[n]).wait()

    loss_out[...] = jnp.full(TILE, jnp.sum(loss_acc[...]) * INV, F32)

    for i in FOUR:
        _copy(tile(r1a, i // 2, i % 2), tile(r1a, i // 2, i % 2), r1as.at[i]).wait()
    _copy(s_d, s_d, s1tx).wait()
    _copy(s_n1a, s_n1a, s1tx).wait()
    _copy(xall.at[pl.ds(0, 28 * LANE)], xall.at[pl.ds(0, 28 * LANE)], tx).wait()
    for d in range(7):
        _copy(lab_v.at[d], lab_v.at[d], labtx_sem).wait()
        _copy(st_loc, st_loc, sttx_sem).wait()


def xrows_at(xall, dev, q):
    return xall.at[pl.ds(pl.multiple_of((dev // 2) * 1024 + q * BLK + (dev % 2) * LANE, LANE), LANE)]


def _head(hid, lab, w):
    hbm = pl.BlockSpec(memory_space=ANY)
    sd = jax.ShapeDtypeStruct
    dma = pltpu.SemaphoreType.DMA
    vmem = pltpu.VMEM
    quarter = (LANE, HALF)
    return pl.pallas_call(
        _head_kernel,
        out_shape=(
            sd((TOK, HID), BF16),
            sd((TOK, VOC), BF16),
            sd((256, HID), F32),
            sd((PIECE, HID), F32),
            sd((PIECE, HID), F32),
            sd((256, HID), F32),
            sd(TILE, F32),
            sd((NBLK, 2, BLK, HALF), F32),
            sd((PIECE, HID), F32),
            sd((256, HID), F32),
            sd((PIECE, HID), F32),
            sd((PIECE, HID), F32),
        ),
        in_specs=[hbm] * 3,
        out_specs=(hbm,) * 6 + (pl.BlockSpec(memory_space=vmem),) + (hbm,) * 5,
        scratch_shapes=[
            vmem((HID, VOC), BF16),
            vmem((2, BLK, HID), BF16),
            vmem((BLK, VOC), BF16),
            vmem((BLK, VOC), BF16),
            vmem((2, BLK, HALF), F32),
            vmem((2, BLK, HALF), F32),
            vmem((2, 2) + quarter, F32),
            vmem(TWO + quarter, F32),
            vmem(TWO + quarter, F32),
            vmem(TWO + quarter, F32),
            vmem(TWO + quarter, F32),
            vmem((8, 4, LANE), I32),
            vmem((BLK, LANE), I32),
            vmem((BLK, LANE), I32),
            vmem(TILE, F32),
            vmem((NBLK,) + TILE, F32),
            vmem((NBLK, 8) + TILE, F32),
            vmem((2, BLK, LANE), F32),
            vmem((2, BLK, LANE), F32),
            vmem((2, BLK, LANE), F32),
            vmem((2, BLK, LANE), F32),
            vmem(TILE, F32),
            vmem((2, BLK, LANE), I32),
            vmem((2, BLK, LANE), F32),
            vmem((2, BLK, LANE), F32),
            vmem((2, LANE), F32),
            dma((8,)),
            dma(()),
            dma(()),
            dma((32,)),
            dma(()),
            dma(TWO),
            dma(TWO),
            dma(TWO),
            dma((NBLK,)),
            dma(()),
            dma(TWO),
            dma((4,)),
            dma(TWO),
            dma(TWO),
            dma(()),
            dma((8,)),
            dma((4,)),
            dma((4,)),
            dma(TWO),
            dma(TWO),
        ],
        compiler_params=pltpu.CompilerParams(collective_id=0, has_side_effects=True, vmem_limit_bytes=67_043_328),
        cost_estimate=pl.CostEstimate(flops=4 * TOK * HID * VOC, bytes_accessed=400 * MIB, transcendentals=2 * TOK * VOC),
        name="head",
    )(hid, lab, w)


def _dhead_kernel(x_hbm, g_hbm, o_hbm, gv, xb, ob, x_sem, g_sem, o_sem):
    rows = HID // PIECE

    def xload(b):
        return _copy(x_hbm.at[:, pl.ds(pl.multiple_of(b * PIECE, PIECE), PIECE)], xb.at[b % 2], x_sem.at[b % 2])

    def gload(j):
        cols = pl.ds(pl.multiple_of(j * PIECE, PIECE), PIECE)
        return _copy(g_hbm.at[:, cols], gv.at[:, cols], g_sem.at[j])

    def ostore(b, n):
        dst = o_hbm.at[pl.ds(pl.multiple_of(b * PIECE, PIECE), PIECE), pl.ds(pl.multiple_of(n * HALF, HALF), HALF)]
        return _copy(ob.at[n], dst, o_sem.at[n])

    def dot(lhs, rhs):
        return lax.dot_general(lhs, rhs, (((0,), (0,)), ((), ())), preferred_element_type=F32).astype(BF16)

    xload(0).start()
    gload(0).start()
    gload(1).start()
    xload(0).wait()

    def first(j, carry):
        gload(j).wait()

        @pl.when(j < 6)
        def _():
            gload(j + 2).start()

        @pl.when(j == 6)
        def _():
            xload(1).start()

        cols = pl.ds(pl.multiple_of(j % 4 * PIECE, PIECE), PIECE)
        ob[j // 4, :, cols] = dot(xb[0], gv[:, pl.ds(pl.multiple_of(j * PIECE, PIECE), PIECE)])
        return carry

    lax.fori_loop(0, 8, first, 0)
    ostore(0, 0).start()
    ostore(0, 1).start()

    def block(b, carry):
        xload(b).wait()

        @pl.when(b < rows - 1)
        def _():
            xload(b + 1).start()

        def half(n, carry):
            ostore(b - 1, n).wait()

            @pl.when(b < rows)
            def _():
                ob[n] = dot(xb[b % 2], gv[:, pl.ds(pl.multiple_of(n * HALF, HALF), HALF)])

            ostore(b, n).start()
            return carry

        return lax.fori_loop(0, 2, half, carry)

    lax.fori_loop(1, rows, block, 0)
    ostore(rows - 1, 0).wait()
    ostore(rows - 1, 1).wait()


def _dhead(xall, gall):
    hbm = pl.BlockSpec(memory_space=ANY)
    dma = pltpu.SemaphoreType.DMA
    return pl.pallas_call(
        _dhead_kernel,
        in_specs=[hbm, hbm],
        out_specs=hbm,
        out_shape=jax.ShapeDtypeStruct((HID, VOC), BF16),
        scratch_shapes=[
            pltpu.VMEM((TOK, VOC), BF16),
            pltpu.VMEM((2, TOK, PIECE), BF16),
            pltpu.VMEM((2, PIECE, HALF), BF16),
            dma(TWO),
            dma((8,)),
            dma(TWO),
        ],
        compiler_params=pltpu.CompilerParams(vmem_limit_bytes=60 * MIB),
        cost_estimate=pl.CostEstimate(flops=2 * TOK * HID * VOC, bytes_accessed=200 * MIB, transcendentals=0),
        name="dhead",
    )(xall, gall)


def _final_kernel(s_hbm, a_hbm, b_hbm, r_hbm, l_ref, o_hbm, loss_ref, terms, ov, in_sem, o_sem):
    rows = PIECE // SUB

    def chunk(ref, i):
        return ref.at[pl.ds(pl.multiple_of(i * rows, rows), rows)]

    for i in range(SUB):
        half = (a_hbm, b_hbm)[i * 2 // SUB]
        for t, src in enumerate((chunk(s_hbm, i), chunk(half, i % (SUB // 2)), chunk(r_hbm, i))):
            _copy(src, chunk(terms.at[t], i), in_sem.at[t, i]).start()
    loss_ref[0] = l_ref[0, 0]

    def add(i, carry):
        for t in range(3):
            _copy(chunk(s_hbm, i), chunk(terms.at[t], i), in_sem.at[t, i]).wait()
        rs = pl.ds(pl.multiple_of(i * rows, rows), rows)
        ov[rs, :] = (terms[0, rs, :] + terms[1, rs, :] + terms[2, rs, :]).astype(BF16)
        _copy(chunk(ov, i), chunk(o_hbm, i), o_sem).start()
        return carry

    lax.fori_loop(0, SUB, add, 0)
    _copy(ov, o_hbm, o_sem).wait()


def _final(s_self, r1a, r1b, r2, loss):
    hbm = pl.BlockSpec(memory_space=ANY)
    dma = pltpu.SemaphoreType.DMA
    return pl.pallas_call(
        _final_kernel,
        in_specs=[hbm] * 4 + [pl.BlockSpec(memory_space=pltpu.VMEM)],
        out_specs=(hbm, pl.BlockSpec(memory_space=pltpu.SMEM)),
        out_shape=(jax.ShapeDtypeStruct((PIECE, HID), BF16), jax.ShapeDtypeStruct((1,), F32)),
        scratch_shapes=[
            pltpu.VMEM((3, PIECE, HID), F32),
            pltpu.VMEM((PIECE, HID), BF16),
            dma((3, SUB)),
            dma(()),
        ],
        compiler_params=pltpu.CompilerParams(vmem_limit_bytes=62 * MIB),
        cost_estimate=pl.CostEstimate(flops=3 * PIECE * HID, bytes_accessed=28 * MIB, transcendentals=0),
        name="final",
    )(s_self, r1a, r1b, r2, loss)


def solution(mesh):
    def device(y, x, core):
        return (y % 2) * 4 + (x % 2) * 2 + core

    first, second = [], []
    for yy in PAIR:
        for xx in PAIR:
            along_x = [(device(yy, xx, k), device(yy, xx + 1, k)) for k in PAIR]
            along_y = [(device(yy, xx, k), device(yy + 1, xx, k)) for k in PAIR]
            first += [along_x[0], along_y[1]]
            second += [along_y[0], along_x[1]]

    def local_step(hid, w, lab):
        xall, gall, s_n1b, s_self, y2, r1a, loss = _head(hid, lab.reshape(4, LANE), w)[:7]
        r1b = lax.ppermute(s_n1b, "tp", first)
        r2 = lax.ppermute(y2, "tp", second)
        d_head = _dhead(xall, gall)
        d_hidden, mean_loss = _final(s_self, r1a, r1b, r2, loss)
        return mean_loss, d_hidden, d_head

    return jax.shard_map(
        local_step,
        mesh=mesh,
        in_specs=(P(("dp", "tp"), None), P(None, "tp"), P(("dp", "tp"))),
        out_specs=(P("dp"), P(("dp", "tp"), None), P("dp", "tp")),
        check_vma=False,
    )
```

```python
import functools

import jax
import jax.numpy as jnp
from jax import lax
from jax.experimental import pallas as pl
from jax.experimental.pallas import tpu as pltpu
from jax.sharding import PartitionSpec as P

F32, BF16, I32 = jnp.float32, jnp.bfloat16, jnp.int32
MESH = pl.DeviceIdType.MESH
ANY = pl.ANY

TOK = 4096
HID = 4096
VOC = 4096
BLK = 256
HALF = 2048
NBLK = TOK // BLK
LANE = 128
MIB = 1 << 20
TWO = (2,)
PAIR = (0, 1)
TILE = (8, LANE)
SUB = 16
FOUR = range(4)
LATE = 9
PIECE = 512
INV = 1.0 / TOK


def _div(a, b):
    return lax.div(jnp.int32(a), jnp.int32(b))


def _rem(a, b):
    return lax.rem(jnp.int32(a), jnp.int32(b))


def _copy(src, dst, sem):
    return pltpu.make_async_copy(src, dst, sem)


def _send(src, dst, send_sem, recv_sem, dev):
    return pltpu.make_async_remote_copy(
        src_ref=src, dst_ref=dst, send_sem=send_sem, recv_sem=recv_sem, device_id={"tp": dev}, device_id_type=MESH
    )


def _product(lhs, rhs, put, jobs, transposed):
    pl.when(lax.axis_index("tp") < 8)(functools.partial(_pieces, lhs, rhs, put, jobs, transposed))


def _pieces(lhs, rhs, put, jobs, transposed):
    dims = (((1,), (1,)), ((), ())) if transposed else (((1,), (0,)), ((), ()))
    pieces = HALF // PIECE
    deep = 8
    for nt in range(pieces):
        acc = None
        for kt in range(deep):
            part = lax.dot_general(lhs(kt), rhs(nt, kt), dims, preferred_element_type=F32)
            acc = part if acc is None else acc + part
            for job in jobs[nt * deep + kt]:
                job()
        put(nt, acc)


def _wide(v, times=HALF // LANE):
    return jnp.concatenate([v] * times, axis=1)


def _fold(v):
    width = v.shape[1] // 2
    while width >= LANE:
        v = v[:, :width] + v[:, width:]
        width //= 2
    return v


def _column(row):
    return jnp.transpose(jnp.broadcast_to(row, (LANE, LANE)))


def _head_kernel(
    x_hbm, lab_hbm, w_hbm,
    xall, gall, s_n1b, s_self, y2, r1a, loss_out,
    zst, s_d, s_n1a, s_n2, r1n2,
    wv, xg, ga, gb, zb, pbuf, rbuf, sbuf, ab, bb, cb, lab_v, la, lb, st_new, st_loc, st_all, ml, mk, sl, tl, comb, c_lab, c_top, c_scale, loss_acc,
    w_sem, lab_sem, labtx_sem, rx, tx, xl_sem, xs_sem, zo_sem, st_sem, sttx_sem,
    zi_sem, rr, ps, ss_sem, s1tx, r1s, r1as, ab_sem, cb_sem, g_sem,
):
    me = lax.axis_index("tp")
    chip = _div(me, 2)
    c = _rem(me, 2)
    x = _rem(chip, 2)
    y = _div(chip, 2)
    oc = 1 - c
    partner = me + 1 - 2 * c
    dx, dy = 2 - 4 * x, 4 - 8 * y
    n1 = me + oc * dx + c * dy
    n2 = me + c * dx + oc * dy
    n1kind = 1 + c

    def chip_of(kind):
        return chip + _rem(kind, 2) * (1 - 2 * x) + _div(kind, 2) * (2 - 4 * y)

    def order(i, first, last):
        a = _div(i, 4)
        mid, end = _rem(_div(a + 1, 2), 2), _div(a, 3)
        kind = mid * (1 + _rem(i, 2)) + first * (1 - mid) * (1 - end) + last * end
        return kind, mid * _div(i - 4, 2) + (1 - mid) * _rem(i, 4)

    def order1(i):
        return order(i, 0, 3)

    def order2(i):
        return order(i, 3, 0)

    def block_id(kind, q):
        return chip_of(kind) * 4 + q

    def xrows(kind, q, part):
        return xall.at[pl.ds(pl.multiple_of(block_id(kind, q) * BLK + part * LANE, LANE), LANE)]

    def xblock(kind, q):
        return xall.at[pl.ds(pl.multiple_of(block_id(kind, q) * BLK, BLK), BLK)]

    def own(q):
        return x_hbm.at[pl.ds(pl.multiple_of(q * LANE, LANE), LANE)]

    def rxs(kind, q, part):
        return rx.at[kind * 8 + q * 2 + part]

    def wcopy(j):
        cols = pl.ds(j * PIECE, PIECE)
        return _copy(w_hbm.at[:, cols], wv.at[:, cols], w_sem.at[j])

    _copy(own(0), xg.at[0, pl.ds(pl.multiple_of(c * LANE, LANE), LANE)], xl_sem.at[0]).start()
    for j in FOUR:
        wcopy(j).start()

    barrier = pltpu.get_barrier_semaphore()
    for d in range(1, 8):
        pl.semaphore_signal(barrier, inc=1, device_id={"tp": _rem(me + d, 8)}, device_id_type=MESH)
    pl.semaphore_wait(barrier, 7)

    for d in range(1, 8):
        _send(lab_hbm, lab_v.at[me], labtx_sem, lab_sem, _rem(me + d, 8)).start()
    _copy(lab_hbm, lab_v.at[me], lab_sem).start()
    for q in FOUR:
        _send(own(q), xrows(0, q, c), tx, rxs(0, q, c), partner).start()
    for q in FOUR:
        _send(own(q), xrows_at(xall, me, q), tx, rxs(n1kind, q, c), n1).start()
        _send(own(q), xrows_at(xall, me, q), tx, rxs(3 - n1kind, q, c), n2).start()

    def load_x(b):
        kind, q = order1(b)
        slot = _rem(b, 2)

        @pl.when(kind == 0)
        def _():
            _copy(own(q), xg.at[slot, pl.ds(pl.multiple_of(c * LANE, LANE), LANE)], xl_sem.at[slot]).start()
            _copy(xrows(0, q, oc), xg.at[slot, pl.ds(pl.multiple_of(oc * LANE, LANE), LANE)], xl_sem.at[slot]).start()

        @pl.when(kind != 0)
        def _():
            _copy(xblock(kind, q), xg.at[slot], xl_sem.at[slot]).start()

    def wait_rows(kind, q, part):
        _copy(xrows(kind, q, part), xrows(kind, q, part), rxs(kind, q, part)).wait()

    def take_rows(kind, q):
        wait_rows(kind, q, c)
        _send(xrows(kind, q, c), xrows(kind, q, c), tx, rxs(kind, q, c), partner).start()

        @pl.when(kind == n1kind)
        def _():
            _send(xrows(kind, q, c), xrows(kind, q, c), tx, rxs(3, q, c), n2).start()

    def part_load(b, part):
        kind, q = order1(b)
        return _copy(xrows(kind, q, part), xg.at[_rem(b, 2), pl.ds(pl.multiple_of(part * LANE, LANE), LANE)], xl_sem.at[_rem(b, 2)])

    def zcopy(b, h):
        kind, q = order1(b)
        return _copy(zb.at[h], zst.at[block_id(kind, q), h], zo_sem.at[h])

    def own_store(b):
        slot = _rem(b, 2)
        return _copy(xg.at[slot, pl.ds(pl.multiple_of(c * LANE, LANE), LANE)], xrows(0, _rem(b, 4), c), xs_sem.at[slot])

    def label_column(blk, part):
        return _column(lab_v[2 * _div(blk, 4) + part, pl.ds(_rem(blk, 4), 1), :])

    def lane_stats(col, h, r):
        rows = pl.ds(r, 8)
        z = zb[h, rows, :]
        m = ml[h, rows, :]
        hit = _wide(col[rows, :] - (me * VOC + h * HALF)) == lax.broadcasted_iota(I32, (8, HALF), 1)
        s = _fold(jnp.exp(z - _wide(m)))
        t = _fold(jnp.where(hit, z, 0.0))
        if h == 1:
            m0 = mk[0, rows, :]
            mm = jnp.maximum(m0, m)
            s = sl[0, rows, :] * jnp.exp(m0 - mm) + s * jnp.exp(m - mm)
            t = tl[0, rows, :] + t
            m = mm
        mk[h, rows, :] = m
        sl[h, rows, :] = s
        tl[h, rows, :] = t

    def label_columns(blk, col, part):
        col[pl.ds(part * LANE, LANE), :] = label_column(blk, part)

    def row_stats(part):
        rows = pl.ds(part * LANE, LANE)
        m = jnp.transpose(mk[1, rows, :])
        top = jnp.max(m, axis=0, keepdims=True)
        st_new[part : part + 1, :] = top
        st_new[2 + part : 3 + part, :] = jnp.sum(jnp.transpose(sl[1, rows, :]) * jnp.exp(m - top), axis=0, keepdims=True)
        st_new[4 + part : 5 + part, :] = jnp.sum(jnp.transpose(tl[1, rows, :]), axis=0, keepdims=True)

    def send_stats(blk):
        for d in range(1, 8):
            _send(st_loc.at[blk], st_all.at[blk, me], sttx_sem, st_sem.at[blk], _rem(me + d, 8)).start()

    def keep_stats(blk):
        st_loc[blk] = st_new[...]
        st_all[blk, me] = st_new[...]

    def combine(blk):
        top = st_all[blk, 0, 0:2, :]
        for d in range(1, 8):
            top = jnp.maximum(top, st_all[blk, d, 0:2, :])
        s = jnp.zeros((2, LANE), F32)
        t = jnp.zeros((2, LANE), F32)
        for d in range(8):
            s = s + st_all[blk, d, 2:4, :] * jnp.exp(st_all[blk, d, 0:2, :] - top)
            t = t + st_all[blk, d, 4:6, :]
        comb[0:2, :] = top
        comb[2:4, :] = INV / s
        return top + jnp.log(s) - t

    def stats_arrived(blk):
        _copy(st_all.at[blk, pl.ds(0, 7)], st_all.at[blk, pl.ds(0, 7)], st_sem.at[blk]).wait()

    def columns(blk, par, part):
        rows = pl.ds(part * LANE, LANE)
        c_lab[par, rows, :] = label_column(blk, part)
        c_top[par, rows, :] = _column(comb[part : part + 1, :])
        c_scale[par, rows, :] = _column(comb[2 + part : 3 + part, :])

    def gradient(src, n, par, r, j):
        rows = pl.ds(pl.multiple_of(r, SUB), SUB)
        col = c_lab[par, rows, :] - (me * VOC + n * HALF + j)
        p = jnp.exp(src[n, rows, j : j + PIECE] - _wide(c_top[par, rows, :], 4)) * _wide(c_scale[par, rows, :], 4)
        g = jnp.where(_wide(col, 4) == lax.broadcasted_iota(I32, (SUB, PIECE), 1), p - INV, p)
        gbufs[par][rows, n * HALF + j : n * HALF + j + PIECE] = g.astype(BF16)

    def gradient_jobs(src, n, par):
        return [functools.partial(gradient, src, n, par, r, j) for r in range(0, BLK, SUB) for j in range(0, HALF, PIECE)]

    gbufs = (ga, gb)

    def gstore(k, par):
        kind, q = order2(k)
        return _copy(gbufs[par], gall.at[pl.ds(pl.multiple_of(block_id(kind, q) * BLK, BLK), BLK)], g_sem.at[par])

    def zload(k, dst, n):
        kind, q = order2(k)
        return _copy(zst.at[block_id(kind, q), n], dst.at[n], zi_sem.at[n])

    first_kind, first_q = order2(me * 0)
    first_blk = block_id(first_kind, first_q)

    def logits(b, h, jobs):
        slot = _rem(b, 2)
        def put(nt, z):
            zb[h, :, nt * PIECE : (nt + 1) * PIECE] = z
            m = z[:, :LANE]
            for j in range(1, 4):
                m = jnp.maximum(m, z[:, j * LANE : (j + 1) * LANE])
            if nt:
                m = jnp.maximum(m, ml[h])
            ml[h] = m

        _product(
            lambda kt: xg[slot, :, kt * PIECE : (kt + 1) * PIECE],
            lambda nt, kt: wv[kt * PIECE : (kt + 1) * PIECE, h * HALF + nt * PIECE : h * HALF + (nt + 1) * PIECE],
            put,
            jobs,
            False,
        )

    wait_rows(0, 0, oc)
    _copy(xrows(0, 0, oc), xg.at[0, pl.ds(pl.multiple_of(oc * LANE, LANE), LANE)], xl_sem.at[0]).start()
    _copy(lab_v, lab_v, lab_sem).wait()
    for j in FOUR:
        wcopy(j).wait()
    for j in range(4, 8):
        wcopy(j).start()

    def phase1(i, carry):
        slot = _rem(i, 2)
        kind, q = order1(i)
        kprev, qprev = order1(_rem(i + NBLK - 2, NBLK))
        kn, qn = order1(_rem(i + 1, NBLK))

        @pl.when((i == LATE + 1) | (i == NBLK - 1))
        def _():
            wait_rows(kind, q, oc)
            part_load(i, oc).start()

        _copy(xg.at[slot], xg.at[slot], xl_sem.at[slot]).wait()

        @pl.when(i < 4)
        def _():
            own_store(i).start()

        @pl.when(i > 0)
        def _():
            zcopy(i - 1, 1).start()
            zcopy(i - 1, 0).wait()

        @pl.when(i > 1)
        def _():
            keep_stats(block_id(kprev, qprev))

        @pl.when(i == NBLK - 2)
        def _():
            zload(0, pbuf, 0).start()
            zload(0, pbuf, 1).start()

        @pl.when(i == NBLK - 1)
        def _():
            stats_arrived(first_blk)
            loss_acc[...] = combine(first_blk)
            for part in PAIR:
                columns(first_blk, 0, part)
            for n in PAIR:
                zload(0, pbuf, n).wait()

                def some(r, carry, n=n):
                    for j in range(0, HALF, PIECE):
                        gradient(pbuf, n, 0, r * SUB, j)
                    return carry

                lax.fori_loop(0, SUB, some, 0)

            gstore(0, 0).start()

        @pl.when((i >= 3) & (i != LATE) & (i < NBLK - 2))
        def _():
            take_rows(kn, qn)

        jobs = [[] for _ in range(32)]
        for r in range(32):
            jobs[min(r + 1, 31)].append(functools.partial(lane_stats, la, 1, r * 8))
        for part in PAIR:
            jobs[4 + 4 * part].append(functools.partial(label_columns, block_id(kind, q), lb, part))
        logits(i, 0, jobs)

        zcopy(i, 0).start()

        @pl.when(i == 0)
        def _():
            for j in range(4, 8):
                wcopy(j).wait()

        @pl.when(i > 0)
        def _():
            zcopy(i - 1, 1).wait()

        @pl.when(i > 1)
        def _():
            send_stats(block_id(kprev, qprev))

        @pl.when((i == LATE) | (i == NBLK - 2))
        def _():
            take_rows(kn, qn)
            part_load(i + 1, c).start()

        @pl.when((i != LATE) & (i < NBLK - 2))
        def _():
            wait_rows(kn, qn, oc)

            @pl.when((i >= 1) & (i < 5))
            def _():
                own_store(i - 1).wait()

            load_x(i + 1)

        la[...] = lb[...]
        jobs = [[] for _ in range(32)]
        for r in range(32):
            jobs[min(r + 1, 31)].append(functools.partial(lane_stats, lb, 0, r * 8))
        for part in PAIR:
            jobs[8 + 8 * part].append(functools.partial(row_stats, part))
        logits(i, 1, jobs)
        return carry

    lax.fori_loop(0, NBLK, phase1, 0)
    last = NBLK - 1
    klast, qlast = order1(jnp.int32(last))
    kprev, qprev = order1(jnp.int32(last - 1))
    bprev, blast = block_id(kprev, qprev), block_id(klast, qlast)
    zcopy(last, 1).start()
    zcopy(last, 0).wait()
    zload(1, zb, 0).start()
    keep_stats(bprev)
    for r in range(32):
        lane_stats(la, 1, r * 8)
    send_stats(bprev)
    for part in PAIR:
        row_stats(part)
    keep_stats(blast)
    zcopy(last, 1).wait()
    zload(1, zb, 1).start()
    send_stats(blast)
    second_kind, second_q = order2(jnp.int32(1))
    second_blk = block_id(second_kind, second_q)
    stats_arrived(second_blk)
    loss_acc[...] += combine(second_blk)
    for part in PAIR:
        columns(second_blk, 1, part)

    def tile(ref, q, n):
        return ref.at[pl.ds(pl.multiple_of(q * LANE, LANE), LANE), pl.ds(pl.multiple_of(n * HALF, HALF), HALF)]

    def spair(k, n):
        return _send(
            pbuf.at[n, pl.ds(pl.multiple_of(oc * LANE, LANE), LANE)], rbuf.at[_rem(k + 2, 2), n], ps.at[n], rr.at[_rem(k + 2, 2) * 2 + n], partner
        )

    def sstore_start(k, n):
        kind, q = order2(k)
        sem = ss_sem.at[n]

        @pl.when(kind == 3)
        def _():
            _copy(sbuf.at[n], tile(s_d, q, n), sem).start()

        @pl.when((kind == n1kind) & (q < 2))
        def _():
            _copy(sbuf.at[n], tile(s_n1a, _rem(q, 2), n), sem).start()

        @pl.when((kind == n1kind) & (q >= 2))
        def _():
            _copy(sbuf.at[n], tile(s_n1b, _rem(q, 2), n), sem).start()

        @pl.when(kind == 3 - n1kind)
        def _():
            _copy(sbuf.at[n], tile(s_n2, q, n), sem).start()

        @pl.when(kind == 0)
        def _():
            _copy(sbuf.at[n], tile(s_self, q, n), sem).start()

    def sstore_done(k, n):
        kind, q = order2(k)
        _copy(sbuf.at[n], tile(s_d, 0, n), ss_sem.at[n]).wait()

        @pl.when(kind == 3)
        def _():
            _send(tile(s_d, q, n), tile(r1n2, q, n), s1tx, r1s.at[q * 2 + n], n1).start()

        @pl.when((kind == n1kind) & (q < 2))
        def _():
            _send(tile(s_n1a, _rem(q, 2), n), tile(r1a, _rem(q, 2), n), s1tx, r1as.at[_rem(q, 2) * 2 + n], n1).start()

    def stage2_load(q, n):
        _copy(tile(r1n2, q, n), tile(r1n2, q, n), r1s.at[q * 2 + n]).wait()
        _copy(tile(s_n2, q, n), ab.at[n], ab_sem.at[n * 2]).start()
        _copy(tile(r1n2, q, n), bb.at[n], ab_sem.at[n * 2 + 1]).start()

    def pair_sum(k, n, r):
        sbuf[n, pl.ds(r, SUB), :] = pbuf[n, pl.ds(pl.multiple_of(c * LANE + r, SUB), SUB), :] + rbuf[_rem(k + 2, 2), n, pl.ds(r, SUB), :]

    def stage2_sum(n, r):
        cb[n, pl.ds(r, SUB), :] = ab[n, pl.ds(r, SUB), :] + bb[n, pl.ds(r, SUB), :]

    def rwait(k, n):
        _copy(rbuf.at[_rem(k + 2, 2), n], rbuf.at[_rem(k + 2, 2), n], rr.at[_rem(k + 2, 2) * 2 + n]).wait()

    def loss_part(k, blk):
        loss_acc[...] += jnp.where(k < NBLK - 2, combine(blk), 0.0)

    def sub(k, cur):
        nxt = 1 - cur
        kind2, q2 = order2(_rem(k + 2, NBLK))
        blk2 = block_id(kind2, q2)

        def trip(n):
            @pl.when(k < NBLK - 1)
            def _():
                zload(k + 1, zb, n).wait()

            @pl.when(k >= 1)
            def _():
                rwait(k - 1, n)
                spair(k - 1, n).wait_send()
                if n == 0:
                    gstore(k - 1, nxt).wait()

            if n == 0:

                @pl.when(k < NBLK - 2)
                def _():
                    stats_arrived(blk2)

            @pl.when(k >= 12)
            def _():
                _copy(tile(s_n2, 0, n), ab.at[n], ab_sem.at[n * 2]).wait()
                _copy(tile(r1n2, 0, n), bb.at[n], ab_sem.at[n * 2 + 1]).wait()

            @pl.when(k >= 13)
            def _():
                _copy(cb.at[n], tile(y2, 0, n), cb_sem.at[n]).wait()

            jobs = [[] for _ in range(32)]
            for r in range(8):
                jobs[2 + r * 3 // 5].append(functools.partial(pair_sum, k - 1, n, r * SUB))
                jobs[10 + r * 5 // 2].append(functools.partial(stage2_sum, n, r * SUB))
            for r, job in enumerate(gradient_jobs(zb, n, nxt)):
                jobs[2 + r * 9 // 20].append(job)
            if n == 0:
                jobs[8].append(lambda: loss_part(k, blk2))
            else:
                for part in PAIR:
                    jobs[8 + 8 * part].append(functools.partial(columns, blk2, cur, part))

            def put(nt, acc):
                pbuf[n, :, nt * PIECE : (nt + 1) * PIECE] = acc

            _product(
                lambda kt: gbufs[cur][:, kt * PIECE : (kt + 1) * PIECE],
                lambda nt, kt: wv[pl.ds(pl.multiple_of(n * HALF + nt * PIECE, PIECE), PIECE), kt * PIECE : (kt + 1) * PIECE],
                put,
                jobs,
                True,
            )

            spair(k, n).start()

            @pl.when(k < NBLK - 2)
            def _():
                zload(k + 2, zb, n).start()

            @pl.when(k >= 2)
            def _():
                sstore_done(k - 2 + n, 1 - n)

            @pl.when(k >= 1)
            def _():
                sstore_start(k - 1, n)

            if n == 0:
                @pl.when(k == 1)
                def _():
                    sstore_done(k - 1, n)

            @pl.when(k >= 12)
            def _():
                _copy(cb.at[n], tile(y2, k - 12, n), cb_sem.at[n]).start()

            @pl.when((k >= 11) & (k < NBLK - 1))
            def _():
                stage2_load(k - 11, n)


        trip(0)
        trip(1)

        @pl.when(k < NBLK - 1)
        def _():
            gstore(k + 1, nxt).start()

    def pair(p, carry):
        sub(2 * p, 0)
        sub(2 * p + 1, 1)
        return carry

    lax.fori_loop(0, NBLK // 2, pair, 0)

    kl = jnp.int32(NBLK - 1)
    for n in PAIR:
        rwait(kl, n)
        spair(kl, n).wait_send()
        if n == 0:
            sstore_done(kl - 1, 1)
        for r in range(8):
            pair_sum(kl, n, r * SUB)
        sstore_start(kl, n)
    for n in PAIR:
        sstore_done(kl, n)
    gstore(kl, 1).wait()
    for n in PAIR:
        _copy(cb.at[n], tile(y2, 0, n), cb_sem.at[n]).wait()

    loss_out[...] = jnp.full(TILE, jnp.sum(loss_acc[...]) * INV, F32)

    for i in FOUR:
        _copy(tile(r1a, i // 2, i % 2), tile(r1a, i // 2, i % 2), r1as.at[i]).wait()
    _copy(s_d, s_d, s1tx).wait()
    _copy(s_n1a, s_n1a, s1tx).wait()
    _copy(xall.at[pl.ds(0, 28 * LANE)], xall.at[pl.ds(0, 28 * LANE)], tx).wait()
    for d in range(7):
        _copy(lab_v.at[d], lab_v.at[d], labtx_sem).wait()
        _copy(st_loc, st_loc, sttx_sem).wait()


def xrows_at(xall, dev, q):
    return xall.at[pl.ds(pl.multiple_of((dev // 2) * 1024 + q * BLK + (dev % 2) * LANE, LANE), LANE)]


def _head(hid, lab, w):
    hbm = pl.BlockSpec(memory_space=ANY)
    sd = jax.ShapeDtypeStruct
    dma = pltpu.SemaphoreType.DMA
    vmem = pltpu.VMEM
    quarter = (LANE, HALF)
    return pl.pallas_call(
        _head_kernel,
        out_shape=(
            sd((TOK, HID), BF16),
            sd((TOK, VOC), BF16),
            sd((256, HID), F32),
            sd((PIECE, HID), F32),
            sd((PIECE, HID), F32),
            sd((256, HID), F32),
            sd(TILE, F32),
            sd((NBLK, 2, BLK, HALF), F32),
            sd((PIECE, HID), F32),
            sd((256, HID), F32),
            sd((PIECE, HID), F32),
            sd((PIECE, HID), F32),
        ),
        in_specs=[hbm] * 3,
        out_specs=(hbm,) * 6 + (pl.BlockSpec(memory_space=vmem),) + (hbm,) * 5,
        scratch_shapes=[
            vmem((HID, VOC), BF16),
            vmem((2, BLK, HID), BF16),
            vmem((BLK, VOC), BF16),
            vmem((BLK, VOC), BF16),
            vmem((2, BLK, HALF), F32),
            vmem((2, BLK, HALF), F32),
            vmem((2, 2) + quarter, F32),
            vmem(TWO + quarter, F32),
            vmem(TWO + quarter, F32),
            vmem(TWO + quarter, F32),
            vmem(TWO + quarter, F32),
            vmem((8, 4, LANE), I32),
            vmem((BLK, LANE), I32),
            vmem((BLK, LANE), I32),
            vmem(TILE, F32),
            vmem((NBLK,) + TILE, F32),
            vmem((NBLK, 8) + TILE, F32),
            vmem((2, BLK, LANE), F32),
            vmem((2, BLK, LANE), F32),
            vmem((2, BLK, LANE), F32),
            vmem((2, BLK, LANE), F32),
            vmem(TILE, F32),
            vmem((2, BLK, LANE), I32),
            vmem((2, BLK, LANE), F32),
            vmem((2, BLK, LANE), F32),
            vmem((2, LANE), F32),
            dma((8,)),
            dma(()),
            dma(()),
            dma((32,)),
            dma(()),
            dma(TWO),
            dma(TWO),
            dma(TWO),
            dma((NBLK,)),
            dma(()),
            dma(TWO),
            dma((4,)),
            dma(TWO),
            dma(TWO),
            dma(()),
            dma((8,)),
            dma((4,)),
            dma((4,)),
            dma(TWO),
            dma(TWO),
        ],
        compiler_params=pltpu.CompilerParams(collective_id=0, has_side_effects=True, vmem_limit_bytes=67_043_328),
        cost_estimate=pl.CostEstimate(flops=4 * TOK * HID * VOC, bytes_accessed=400 * MIB, transcendentals=2 * TOK * VOC),
        name="head",
    )(hid, lab, w)


def _dhead_kernel(x_hbm, g_hbm, o_hbm, gv, xb, ob, x_sem, g_sem, o_sem):
    rows = HID // PIECE

    def xload(b):
        return _copy(x_hbm.at[:, pl.ds(pl.multiple_of(b * PIECE, PIECE), PIECE)], xb.at[b % 2], x_sem.at[b % 2])

    def gload(j):
        cols = pl.ds(pl.multiple_of(j * PIECE, PIECE), PIECE)
        return _copy(g_hbm.at[:, cols], gv.at[:, cols], g_sem.at[j])

    def ostore(b, n):
        dst = o_hbm.at[pl.ds(pl.multiple_of(b * PIECE, PIECE), PIECE), pl.ds(pl.multiple_of(n * HALF, HALF), HALF)]
        return _copy(ob.at[n], dst, o_sem.at[n])

    def dot(lhs, rhs):
        return lax.dot_general(lhs, rhs, (((0,), (0,)), ((), ())), preferred_element_type=F32).astype(BF16)

    xload(0).start()
    gload(0).start()
    gload(1).start()
    xload(0).wait()

    def first(j, carry):
        gload(j).wait()

        @pl.when(j < 6)
        def _():
            gload(j + 2).start()

        @pl.when(j == 6)
        def _():
            xload(1).start()

        cols = pl.ds(pl.multiple_of(j % 4 * PIECE, PIECE), PIECE)
        ob[j // 4, :, cols] = dot(xb[0], gv[:, pl.ds(pl.multiple_of(j * PIECE, PIECE), PIECE)])
        return carry

    lax.fori_loop(0, 8, first, 0)
    ostore(0, 0).start()
    ostore(0, 1).start()

    def block(b, carry):
        xload(b).wait()

        @pl.when(b < rows - 1)
        def _():
            xload(b + 1).start()

        def half(n, carry):
            ostore(b - 1, n).wait()

            @pl.when(b < rows)
            def _():
                ob[n] = dot(xb[b % 2], gv[:, pl.ds(pl.multiple_of(n * HALF, HALF), HALF)])

            ostore(b, n).start()
            return carry

        return lax.fori_loop(0, 2, half, carry)

    lax.fori_loop(1, rows, block, 0)
    ostore(rows - 1, 0).wait()
    ostore(rows - 1, 1).wait()


def _dhead(xall, gall):
    hbm = pl.BlockSpec(memory_space=ANY)
    dma = pltpu.SemaphoreType.DMA
    return pl.pallas_call(
        _dhead_kernel,
        in_specs=[hbm, hbm],
        out_specs=hbm,
        out_shape=jax.ShapeDtypeStruct((HID, VOC), BF16),
        scratch_shapes=[
            pltpu.VMEM((TOK, VOC), BF16),
            pltpu.VMEM((2, TOK, PIECE), BF16),
            pltpu.VMEM((2, PIECE, HALF), BF16),
            dma(TWO),
            dma((8,)),
            dma(TWO),
        ],
        compiler_params=pltpu.CompilerParams(vmem_limit_bytes=60 * MIB),
        cost_estimate=pl.CostEstimate(flops=2 * TOK * HID * VOC, bytes_accessed=200 * MIB, transcendentals=0),
        name="dhead",
    )(xall, gall)


def _final_kernel(s_hbm, a_hbm, b_hbm, r_hbm, l_ref, o_hbm, loss_ref, terms, ov, in_sem, o_sem):
    rows = PIECE // SUB

    def chunk(ref, i):
        return ref.at[pl.ds(pl.multiple_of(i * rows, rows), rows)]

    for i in range(SUB):
        half = (a_hbm, b_hbm)[i * 2 // SUB]
        for t, src in enumerate((chunk(s_hbm, i), chunk(half, i % (SUB // 2)), chunk(r_hbm, i))):
            _copy(src, chunk(terms.at[t], i), in_sem.at[t, i]).start()
    loss_ref[0] = l_ref[0, 0]

    def add(i, carry):
        for t in range(3):
            _copy(chunk(s_hbm, i), chunk(terms.at[t], i), in_sem.at[t, i]).wait()
        rs = pl.ds(pl.multiple_of(i * rows, rows), rows)
        ov[rs, :] = (terms[0, rs, :] + terms[1, rs, :] + terms[2, rs, :]).astype(BF16)
        _copy(chunk(ov, i), chunk(o_hbm, i), o_sem).start()
        return carry

    lax.fori_loop(0, SUB, add, 0)
    _copy(ov, o_hbm, o_sem).wait()


def _final(s_self, r1a, r1b, r2, loss):
    hbm = pl.BlockSpec(memory_space=ANY)
    dma = pltpu.SemaphoreType.DMA
    return pl.pallas_call(
        _final_kernel,
        in_specs=[hbm] * 4 + [pl.BlockSpec(memory_space=pltpu.VMEM)],
        out_specs=(hbm, pl.BlockSpec(memory_space=pltpu.SMEM)),
        out_shape=(jax.ShapeDtypeStruct((PIECE, HID), BF16), jax.ShapeDtypeStruct((1,), F32)),
        scratch_shapes=[
            pltpu.VMEM((3, PIECE, HID), F32),
            pltpu.VMEM((PIECE, HID), BF16),
            dma((3, SUB)),
            dma(()),
        ],
        compiler_params=pltpu.CompilerParams(vmem_limit_bytes=62 * MIB),
        cost_estimate=pl.CostEstimate(flops=3 * PIECE * HID, bytes_accessed=28 * MIB, transcendentals=0),
        name="final",
    )(s_self, r1a, r1b, r2, loss)


def solution(mesh):
    def device(y, x, core):
        return (y % 2) * 4 + (x % 2) * 2 + core

    first, second = [], []
    for yy in PAIR:
        for xx in PAIR:
            along_x = [(device(yy, xx, k), device(yy, xx + 1, k)) for k in PAIR]
            along_y = [(device(yy, xx, k), device(yy + 1, xx, k)) for k in PAIR]
            first += [along_x[0], along_y[1]]
            second += [along_y[0], along_x[1]]

    def local_step(hid, w, lab):
        xall, gall, s_n1b, s_self, y2, r1a, loss = _head(hid, lab.reshape(4, LANE), w)[:7]
        r1b = lax.ppermute(s_n1b, "tp", first)
        r2 = lax.ppermute(y2, "tp", second)
        d_head = _dhead(xall, gall)
        d_hidden, mean_loss = _final(s_self, r1a, r1b, r2, loss)
        return mean_loss, d_hidden, d_head

    return jax.shard_map(
        local_step,
        mesh=mesh,
        in_specs=(P(("dp", "tp"), None), P(None, "tp"), P(("dp", "tp"))),
        out_specs=(P("dp"), P(("dp", "tp"), None), P("dp", "tp")),
        check_vma=False,
    )
```

```python
import functools

import jax
import jax.numpy as jnp
from jax import lax
from jax.experimental import pallas as pl
from jax.experimental.pallas import tpu as pltpu
from jax.sharding import PartitionSpec as P

F32, BF16, I32 = jnp.float32, jnp.bfloat16, jnp.int32
MESH = pl.DeviceIdType.MESH
ANY = pl.ANY

TOK = 4096
HID = 4096
VOC = 4096
BLK = 256
HALF = 2048
NBLK = TOK // BLK
LANE = 128
MIB = 1 << 20
TWO = (2,)
PAIR = (0, 1)
TILE = (8, LANE)
SUB = 16
FOUR = range(4)
CORNER = 6
LATE = 9
PIECE = 512
INV = 1.0 / TOK


def _div(a, b):
    return lax.div(jnp.int32(a), jnp.int32(b))


def _rem(a, b):
    return lax.rem(jnp.int32(a), jnp.int32(b))


def _odd(a):
    return _rem(a, 2)


def _half(a):
    return _div(a, 2)


def _copy(src, dst, sem):
    return pltpu.make_async_copy(src, dst, sem)


def _send(src, dst, send_sem, recv_sem, dev):
    return pltpu.make_async_remote_copy(
        src_ref=src, dst_ref=dst, send_sem=send_sem, recv_sem=recv_sem, device_id={"tp": dev}, device_id_type=MESH
    )


def _product(lhs, rhs, put, jobs, transposed):
    pl.when(lax.axis_index("tp") < 8)(functools.partial(_pieces, lhs, rhs, put, jobs, transposed))


def _pieces(lhs, rhs, put, jobs, transposed):
    dims = (((1,), (1,)), ((), ())) if transposed else (((1,), (0,)), ((), ()))
    pieces = HALF // PIECE
    deep = 8
    for nt in range(pieces):
        acc = None
        for kt in range(deep):
            part = lax.dot_general(lhs(kt), rhs(nt, kt), dims, preferred_element_type=F32)
            acc = part if acc is None else acc + part
            for job in jobs[nt * deep + kt]:
                job()
        put(nt, acc)


def _wide(v, times=HALF // LANE):
    return jnp.concatenate([v] * times, axis=1)


def _fold(v):
    width = v.shape[1] // 2
    while width >= LANE:
        v = v[:, :width] + v[:, width:]
        width //= 2
    return v


def _column(row):
    return jnp.transpose(jnp.broadcast_to(row, (LANE, LANE)))


def _head_kernel(
    x_hbm, lab_hbm, w_hbm,
    xall, gall, s_n1b, s_self, y2, r1a, loss_out,
    zst, s_d, s_n1a, s_n2, r1n2,
    wv, xg, ga, gb, zb, pbuf, rbuf, sbuf, ab, bb, cb, lab_v, la, lb, st_new, st_loc, st_all, ml, mk, sl, tl, comb, c_lab, c_top, c_scale, loss_acc,
    w_sem, lab_sem, labtx_sem, rx, tx, xl_sem, xs_sem, zo_sem, st_sem, sttx_sem,
    zi_sem, rr, ps, ss_sem, s1tx, r1s, r1as, ab_sem, cb_sem, g_sem,
):
    me = lax.axis_index("tp")
    chip = _half(me)
    c = _odd(me)
    x = _odd(chip)
    y = _half(chip)
    oc = 1 - c
    partner = me + 1 - 2 * c
    dx, dy = 2 - 4 * x, 4 - 8 * y
    n1 = me + oc * dx + c * dy
    n2 = me + c * dx + oc * dy
    n1kind = 1 + c

    def chip_of(kind):
        return chip + _odd(kind) * (1 - 2 * x) + _half(kind) * (2 - 4 * y)

    def order(i, first, last):
        a = _div(i, 4)
        mid, end = _rem(_half(a + 1), 2), _div(a, 3)
        kind = mid * (1 + _odd(i)) + first * (1 - mid) * (1 - end) + last * end
        return kind, mid * _half(i - 4) + (1 - mid) * _rem(i, 4)

    def order1(i):
        return order(i, 0, 3)

    def order2(i):
        return order(i, 3, 0)

    def block_id(kind, q):
        return chip_of(kind) * 4 + q

    def xrows(kind, q, part):
        return xall.at[pl.ds(pl.multiple_of(block_id(kind, q) * BLK + part * LANE, LANE), LANE)]

    def xblock(kind, q):
        return xall.at[pl.ds(pl.multiple_of(block_id(kind, q) * BLK, BLK), BLK)]

    def own(q):
        return x_hbm.at[pl.ds(pl.multiple_of(q * LANE, LANE), LANE)]

    def rxs(kind, q, part):
        return rx.at[kind * 8 + q * 2 + part]

    def wcopy(j):
        cols = pl.ds(j * PIECE, PIECE)
        return _copy(w_hbm.at[:, cols], wv.at[:, cols], w_sem.at[j])

    _copy(own(0), xg.at[0, pl.ds(pl.multiple_of(c * LANE, LANE), LANE)], xl_sem.at[0]).start()
    for j in FOUR:
        wcopy(j).start()

    barrier = pltpu.get_barrier_semaphore()
    for d in range(1, 8):
        pl.semaphore_signal(barrier, inc=1, device_id={"tp": _rem(me + d, 8)}, device_id_type=MESH)
    pl.semaphore_wait(barrier, 7)

    for d in range(1, 8):
        _send(lab_hbm, lab_v.at[me], labtx_sem, lab_sem, _rem(me + d, 8)).start()
    _copy(lab_hbm, lab_v.at[me], lab_sem).start()
    for q in FOUR:
        _send(own(q), xrows(0, q, c), tx, rxs(0, q, c), partner).start()
    for q in FOUR:
        _send(own(q), xrows_at(xall, me, q), tx, rxs(n1kind, q, c), n1).start()
        _send(own(q), xrows_at(xall, me, q), tx, rxs(3 - n1kind, q, c), n2).start()

    def load_x(b):
        kind, q = order1(b)
        slot = _odd(b)

        @pl.when(kind == 0)
        def _():
            _copy(own(q), xg.at[slot, pl.ds(pl.multiple_of(c * LANE, LANE), LANE)], xl_sem.at[slot]).start()
            _copy(xrows(0, q, oc), xg.at[slot, pl.ds(pl.multiple_of(oc * LANE, LANE), LANE)], xl_sem.at[slot]).start()

        @pl.when(kind != 0)
        def _():
            _copy(xblock(kind, q), xg.at[slot], xl_sem.at[slot]).start()

    def wait_rows(kind, q, part):
        _copy(xrows(kind, q, part), xrows(kind, q, part), rxs(kind, q, part)).wait()

    def take_rows(kind, q):
        wait_rows(kind, q, c)
        _send(xrows(kind, q, c), xrows(kind, q, c), tx, rxs(kind, q, c), partner).start()

        @pl.when(kind == n1kind)
        def _():
            _send(xrows(kind, q, c), xrows(kind, q, c), tx, rxs(3, q, c), n2).start()

    def part_load(b, part):
        kind, q = order1(b)
        return _copy(xrows(kind, q, part), xg.at[_odd(b), pl.ds(pl.multiple_of(part * LANE, LANE), LANE)], xl_sem.at[_odd(b)])

    def zcopy(b, h):
        kind, q = order1(b)
        return _copy(zb.at[h], zst.at[block_id(kind, q), h], zo_sem.at[h])

    def own_store(b):
        slot = _odd(b)
        return _copy(xg.at[slot, pl.ds(pl.multiple_of(c * LANE, LANE), LANE)], xrows(0, _rem(b, 4), c), xs_sem.at[slot])

    def label_column(blk, part):
        return _column(lab_v[2 * _div(blk, 4) + part, pl.ds(_rem(blk, 4), 1), :])

    def lane_stats(col, h, r):
        rows = pl.ds(r, 8)
        z = zb[h, rows, :]
        m = ml[h, rows, :]
        hit = _wide(col[rows, :] - (me * VOC + h * HALF)) == lax.broadcasted_iota(I32, (8, HALF), 1)
        s = _fold(jnp.exp(z - _wide(m)))
        t = _fold(jnp.where(hit, z, 0.0))
        if h == 1:
            m0 = mk[0, rows, :]
            mm = jnp.maximum(m0, m)
            s = sl[0, rows, :] * jnp.exp(m0 - mm) + s * jnp.exp(m - mm)
            t = tl[0, rows, :] + t
            m = mm
        mk[h, rows, :] = m
        sl[h, rows, :] = s
        tl[h, rows, :] = t

    def label_columns(blk, col, part):
        col[pl.ds(part * LANE, LANE), :] = label_column(blk, part)

    def row_stats(part):
        rows = pl.ds(part * LANE, LANE)
        m = jnp.transpose(mk[1, rows, :])
        top = jnp.max(m, axis=0, keepdims=True)
        st_new[part : part + 1, :] = top
        st_new[2 + part : 3 + part, :] = jnp.sum(jnp.transpose(sl[1, rows, :]) * jnp.exp(m - top), axis=0, keepdims=True)
        st_new[4 + part : 5 + part, :] = jnp.sum(jnp.transpose(tl[1, rows, :]), axis=0, keepdims=True)

    def send_stats(blk):
        for d in range(1, 8):
            _send(st_loc.at[blk], st_all.at[blk, me], sttx_sem, st_sem.at[blk], _rem(me + d, 8)).start()

    def keep_stats(blk):
        st_loc[blk] = st_new[...]
        st_all[blk, me] = st_new[...]

    def combine(blk):
        top = st_all[blk, 0, 0:2, :]
        for d in range(1, 8):
            top = jnp.maximum(top, st_all[blk, d, 0:2, :])
        s = jnp.zeros((2, LANE), F32)
        t = jnp.zeros((2, LANE), F32)
        for d in range(8):
            s = s + st_all[blk, d, 2:4, :] * jnp.exp(st_all[blk, d, 0:2, :] - top)
            t = t + st_all[blk, d, 4:6, :]
        comb[0:2, :] = top
        comb[2:4, :] = INV / s
        return top + jnp.log(s) - t

    def stats_arrived(blk):
        _copy(st_all.at[blk, pl.ds(0, 7)], st_all.at[blk, pl.ds(0, 7)], st_sem.at[blk]).wait()

    def columns(blk, par, part):
        rows = pl.ds(part * LANE, LANE)
        c_lab[par, rows, :] = label_column(blk, part)
        c_top[par, rows, :] = _column(comb[part : part + 1, :])
        c_scale[par, rows, :] = _column(comb[2 + part : 3 + part, :])

    def gradient(src, n, par, r, j):
        rows = pl.ds(pl.multiple_of(r, SUB), SUB)
        col = c_lab[par, rows, :] - (me * VOC + n * HALF + j)
        p = jnp.exp(src[n, rows, j : j + PIECE] - _wide(c_top[par, rows, :], 4)) * _wide(c_scale[par, rows, :], 4)
        g = jnp.where(_wide(col, 4) == lax.broadcasted_iota(I32, (SUB, PIECE), 1), p - INV, p)
        gbufs[par][rows, n * HALF + j : n * HALF + j + PIECE] = g.astype(BF16)

    def gradient_jobs(src, n, par):
        return [functools.partial(gradient, src, n, par, r, j) for r in range(0, BLK, SUB) for j in range(0, HALF, PIECE)]

    gbufs = (ga, gb)

    def gstore(k, par):
        kind, q = order2(k)
        return _copy(gbufs[par], gall.at[pl.ds(pl.multiple_of(block_id(kind, q) * BLK, BLK), BLK)], g_sem.at[par])

    def zload(k, dst, n):
        kind, q = order2(k)
        return _copy(zst.at[block_id(kind, q), n], dst.at[n], zi_sem.at[n])

    first_kind, first_q = order2(me * 0)
    first_blk = block_id(first_kind, first_q)

    def logits(b, h, jobs):
        slot = _odd(b)
        def put(nt, z):
            zb[h, :, nt * PIECE : (nt + 1) * PIECE] = z
            m = z[:, :LANE]
            for j in range(1, 4):
                m = jnp.maximum(m, z[:, j * LANE : (j + 1) * LANE])
            if nt:
                m = jnp.maximum(m, ml[h])
            ml[h] = m

        _product(
            lambda kt: xg[slot, :, kt * PIECE : (kt + 1) * PIECE],
            lambda nt, kt: wv[kt * PIECE : (kt + 1) * PIECE, h * HALF + nt * PIECE : h * HALF + (nt + 1) * PIECE],
            put,
            jobs,
            False,
        )

    wait_rows(0, 0, oc)
    _copy(xrows(0, 0, oc), xg.at[0, pl.ds(pl.multiple_of(oc * LANE, LANE), LANE)], xl_sem.at[0]).start()
    _copy(lab_v, lab_v, lab_sem).wait()
    for j in FOUR:
        wcopy(j).wait()
    for j in range(4, 8):
        wcopy(j).start()

    def phase1(i, carry):
        slot = _odd(i)
        kind, q = order1(i)
        kprev, qprev = order1(_rem(i + NBLK - 2, NBLK))
        kn, qn = order1(_rem(i + 1, NBLK))

        @pl.when((i == LATE + 1) | (i == NBLK - 1))
        def _():
            wait_rows(kind, q, oc)
            part_load(i, oc).start()

        _copy(xg.at[slot], xg.at[slot], xl_sem.at[slot]).wait()

        @pl.when(i < 4)
        def _():
            own_store(i).start()

        @pl.when(i > 0)
        def _():
            zcopy(i - 1, 1).start()
            zcopy(i - 1, 0).wait()

        @pl.when(i > 1)
        def _():
            keep_stats(block_id(kprev, qprev))

        @pl.when(i == NBLK - 2)
        def _():
            zload(0, pbuf, 0).start()
            zload(0, pbuf, 1).start()

        @pl.when(i == NBLK - 1)
        def _():
            stats_arrived(first_blk)
            loss_acc[...] = combine(first_blk)
            for part in PAIR:
                columns(first_blk, 0, part)
            for n in PAIR:
                zload(0, pbuf, n).wait()

                def some(r, carry, n=n):
                    for j in range(0, HALF, PIECE):
                        gradient(pbuf, n, 0, r * SUB, j)
                    return carry

                lax.fori_loop(0, SUB, some, 0)

            gstore(0, 0).start()

        @pl.when((i >= 3) & (i != LATE) & (i < NBLK - 2))
        def _():
            take_rows(kn, qn)

        jobs = [[] for _ in range(32)]
        for r in range(32):
            jobs[min(r + 1, 31)].append(functools.partial(lane_stats, la, 1, r * 8))
        for part in PAIR:
            jobs[4 + 4 * part].append(functools.partial(label_columns, block_id(kind, q), lb, part))
        logits(i, 0, jobs)

        zcopy(i, 0).start()

        @pl.when(i == 0)
        def _():
            for j in range(4, 8):
                wcopy(j).wait()

        @pl.when(i > 0)
        def _():
            zcopy(i - 1, 1).wait()

        @pl.when(i > 1)
        def _():
            send_stats(block_id(kprev, qprev))

        @pl.when((i == LATE) | (i == NBLK - 2))
        def _():
            take_rows(kn, qn)
            part_load(i + 1, c).start()

        @pl.when((i != LATE) & (i < NBLK - 2))
        def _():
            wait_rows(kn, qn, oc)

            @pl.when((i >= 1) & (i < 5))
            def _():
                own_store(i - 1).wait()

            load_x(i + 1)

        la[...] = lb[...]
        jobs = [[] for _ in range(32)]
        for r in range(32):
            jobs[min(r + 1, 31)].append(functools.partial(lane_stats, lb, 0, r * 8))
        for part in PAIR:
            jobs[8 + 8 * part].append(functools.partial(row_stats, part))
        logits(i, 1, jobs)
        return carry

    lax.fori_loop(0, NBLK, phase1, 0)
    last = NBLK - 1
    klast, qlast = order1(jnp.int32(last))
    kprev, qprev = order1(jnp.int32(last - 1))
    bprev, blast = block_id(kprev, qprev), block_id(klast, qlast)
    zcopy(last, 1).start()
    zcopy(last, 0).wait()
    zload(1, zb, 0).start()
    keep_stats(bprev)
    for r in range(32):
        lane_stats(la, 1, r * 8)
    send_stats(bprev)
    for part in PAIR:
        row_stats(part)
    keep_stats(blast)
    zcopy(last, 1).wait()
    zload(1, zb, 1).start()
    send_stats(blast)
    second_kind, second_q = order2(jnp.int32(1))
    second_blk = block_id(second_kind, second_q)
    stats_arrived(second_blk)
    loss_acc[...] += combine(second_blk)
    for part in PAIR:
        columns(second_blk, 1, part)

    def tile(ref, q, n):
        return ref.at[pl.ds(pl.multiple_of(q * LANE, LANE), LANE), pl.ds(pl.multiple_of(n * HALF, HALF), HALF)]

    def spair(k, n):
        return _send(
            pbuf.at[n, pl.ds(pl.multiple_of(oc * LANE, LANE), LANE)], rbuf.at[_odd(k + 2), n], ps.at[n], rr.at[_odd(k + 2) * 2 + n], partner
        )

    def sstore_start(k, n):
        kind, q = order2(k)
        sem = ss_sem.at[n]

        @pl.when(kind == 3)
        def _():
            _copy(sbuf.at[n], tile(s_d, q, n), sem).start()

        @pl.when((kind == n1kind) & (q < 2))
        def _():
            _copy(sbuf.at[n], tile(s_n1a, _odd(q), n), sem).start()

        @pl.when((kind == n1kind) & (q >= 2))
        def _():
            _copy(sbuf.at[n], tile(s_n1b, _odd(q), n), sem).start()

        @pl.when(kind == 3 - n1kind)
        def _():
            _copy(sbuf.at[n], tile(s_n2, q, n), sem).start()

        @pl.when(kind == 0)
        def _():
            _copy(sbuf.at[n], tile(s_self, q, n), sem).start()

    def sstore_done(k, n):
        kind, q = order2(k)
        _copy(sbuf.at[n], tile(s_d, 0, n), ss_sem.at[n]).wait()

        @pl.when(kind == 3)
        def _():
            _send(tile(s_d, q, n), tile(r1n2, q, n), s1tx, r1s.at[q * 2 + n], n1).start()

        @pl.when((kind == n1kind) & (q < 2))
        def _():
            _send(tile(s_n1a, _odd(q), n), tile(r1a, _odd(q), n), s1tx, r1as.at[_odd(q) * 2 + n], n1).start()

    def stage2_load(q, n):
        _copy(tile(r1n2, q, n), tile(r1n2, q, n), r1s.at[q * 2 + n]).wait()
        _copy(tile(s_n2, q, n), ab.at[n], ab_sem.at[n * 2]).start()
        _copy(tile(r1n2, q, n), bb.at[n], ab_sem.at[n * 2 + 1]).start()

    def pair_sum(k, n, r):
        sbuf[n, pl.ds(r, SUB), :] = pbuf[n, pl.ds(pl.multiple_of(c * LANE + r, SUB), SUB), :] + rbuf[_odd(k + 2), n, pl.ds(r, SUB), :]

    def stage2_sum(n, r):
        cb[n, pl.ds(r, SUB), :] = ab[n, pl.ds(r, SUB), :] + bb[n, pl.ds(r, SUB), :]

    def rwait(k, n):
        _copy(rbuf.at[_odd(k + 2), n], rbuf.at[_odd(k + 2), n], rr.at[_odd(k + 2) * 2 + n]).wait()

    def loss_part(k, blk):
        loss_acc[...] += jnp.where(k < NBLK - 2, combine(blk), 0.0)

    def sub(k, cur):
        nxt = 1 - cur
        kind2, q2 = order2(_rem(k + 2, NBLK))
        blk2 = block_id(kind2, q2)

        def trip(n):
            @pl.when(k < NBLK - 1)
            def _():
                zload(k + 1, zb, n).wait()

            @pl.when(k >= 1)
            def _():
                rwait(k - 1, n)
                spair(k - 1, n).wait_send()
                if n == 0:
                    gstore(k - 1, nxt).wait()

            if n == 0:

                @pl.when(k < NBLK - 2)
                def _():
                    stats_arrived(blk2)

            @pl.when(k >= 12)
            def _():
                _copy(tile(s_n2, 0, n), ab.at[n], ab_sem.at[n * 2]).wait()
                _copy(tile(r1n2, 0, n), bb.at[n], ab_sem.at[n * 2 + 1]).wait()

            @pl.when(k >= 13)
            def _():
                _copy(cb.at[n], tile(y2, 0, n), cb_sem.at[n]).wait()

            jobs = [[] for _ in range(32)]
            for r in range(8):
                jobs[2 + r * 3 // 5].append(functools.partial(pair_sum, k - 1, n, r * SUB))
                jobs[10 + r * 5 // 2].append(functools.partial(stage2_sum, n, r * SUB))
            for r, job in enumerate(gradient_jobs(zb, n, nxt)):
                jobs[2 + r * 9 // 20].append(job)
            if n == 0:
                jobs[8].append(lambda: loss_part(k, blk2))
            else:
                for part in PAIR:
                    jobs[8 + 8 * part].append(functools.partial(columns, blk2, cur, part))

            def put(nt, acc):
                pbuf[n, :, nt * PIECE : (nt + 1) * PIECE] = acc

            _product(
                lambda kt: gbufs[cur][:, kt * PIECE : (kt + 1) * PIECE],
                lambda nt, kt: wv[pl.ds(pl.multiple_of(n * HALF + nt * PIECE, PIECE), PIECE), kt * PIECE : (kt + 1) * PIECE],
                put,
                jobs,
                True,
            )

            spair(k, n).start()

            @pl.when(k < NBLK - 2)
            def _():
                zload(k + 2, zb, n).start()

            @pl.when(k >= 2)
            def _():
                sstore_done(k - 2 + n, 1 - n)

            @pl.when(k >= 1)
            def _():
                sstore_start(k - 1, n)

            if n == 0:
                @pl.when(k == 1)
                def _():
                    sstore_done(k - 1, n)

            @pl.when(k >= 12)
            def _():
                _copy(cb.at[n], tile(y2, k - 12, n), cb_sem.at[n]).start()

            @pl.when((k >= 11) & (k < NBLK - 1))
            def _():
                stage2_load(k - 11, n)


        trip(0)
        trip(1)

        @pl.when(k < NBLK - 1)
        def _():
            gstore(k + 1, nxt).start()

    def pair(p, carry):
        sub(2 * p, 0)
        sub(2 * p + 1, 1)
        return carry

    lax.fori_loop(0, NBLK // 2, pair, 0)

    kl = jnp.int32(NBLK - 1)
    for n in PAIR:
        rwait(kl, n)
        spair(kl, n).wait_send()
        if n == 0:
            sstore_done(kl - 1, 1)
        for r in range(8):
            pair_sum(kl, n, r * SUB)
        sstore_start(kl, n)
    for n in PAIR:
        sstore_done(kl, n)
    gstore(kl, 1).wait()
    for n in PAIR:
        _copy(cb.at[n], tile(y2, 0, n), cb_sem.at[n]).wait()

    loss_out[...] = jnp.full(TILE, jnp.sum(loss_acc[...]) * INV, F32)

    for i in FOUR:
        _copy(tile(r1a, i // 2, i % 2), tile(r1a, i // 2, i % 2), r1as.at[i]).wait()
    _copy(s_d, s_d, s1tx).wait()
    _copy(s_n1a, s_n1a, s1tx).wait()
    _copy(xall.at[pl.ds(0, 28 * LANE)], xall.at[pl.ds(0, 28 * LANE)], tx).wait()
    for d in range(7):
        _copy(lab_v.at[d], lab_v.at[d], labtx_sem).wait()
        _copy(st_loc, st_loc, sttx_sem).wait()


def xrows_at(xall, dev, q):
    return xall.at[pl.ds(pl.multiple_of((dev // 2) * 1024 + q * BLK + (dev % 2) * LANE, LANE), LANE)]


def _head(hid, lab, w):
    hbm = pl.BlockSpec(memory_space=ANY)
    sd = jax.ShapeDtypeStruct
    dma = pltpu.SemaphoreType.DMA
    vmem = pltpu.VMEM
    quarter = (LANE, HALF)
    return pl.pallas_call(
        _head_kernel,
        out_shape=(
            sd((TOK, HID), BF16),
            sd((TOK, VOC), BF16),
            sd((256, HID), F32),
            sd((PIECE, HID), F32),
            sd((PIECE, HID), F32),
            sd((256, HID), F32),
            sd(TILE, F32),
            sd((NBLK, 2, BLK, HALF), F32),
            sd((PIECE, HID), F32),
            sd((256, HID), F32),
            sd((PIECE, HID), F32),
            sd((PIECE, HID), F32),
        ),
        in_specs=[hbm] * 3,
        out_specs=(hbm,) * 6 + (pl.BlockSpec(memory_space=vmem),) + (hbm,) * 5,
        scratch_shapes=[
            vmem((HID, VOC), BF16),
            vmem((2, BLK, HID), BF16),
            vmem((BLK, VOC), BF16),
            vmem((BLK, VOC), BF16),
            vmem((2, BLK, HALF), F32),
            vmem((2, BLK, HALF), F32),
            vmem((2, 2) + quarter, F32),
            vmem(TWO + quarter, F32),
            vmem(TWO + quarter, F32),
            vmem(TWO + quarter, F32),
            vmem(TWO + quarter, F32),
            vmem((8, 4, LANE), I32),
            vmem((BLK, LANE), I32),
            vmem((BLK, LANE), I32),
            vmem(TILE, F32),
            vmem((NBLK,) + TILE, F32),
            vmem((NBLK, 8) + TILE, F32),
            vmem((2, BLK, LANE), F32),
            vmem((2, BLK, LANE), F32),
            vmem((2, BLK, LANE), F32),
            vmem((2, BLK, LANE), F32),
            vmem(TILE, F32),
            vmem((2, BLK, LANE), I32),
            vmem((2, BLK, LANE), F32),
            vmem((2, BLK, LANE), F32),
            vmem((2, LANE), F32),
            dma((8,)),
            dma(()),
            dma(()),
            dma((32,)),
            dma(()),
            dma(TWO),
            dma(TWO),
            dma(TWO),
            dma((NBLK,)),
            dma(()),
            dma(TWO),
            dma((4,)),
            dma(TWO),
            dma(TWO),
            dma(()),
            dma((8,)),
            dma((4,)),
            dma((4,)),
            dma(TWO),
            dma(TWO),
        ],
        compiler_params=pltpu.CompilerParams(collective_id=0, has_side_effects=True, vmem_limit_bytes=67_043_328),
        cost_estimate=pl.CostEstimate(flops=4 * TOK * HID * VOC, bytes_accessed=400 * MIB, transcendentals=2 * TOK * VOC),
        name="head",
    )(hid, lab, w)


def _outer(lhs, rhs):
    return lax.dot_general(lhs, rhs, (((0,), (0,)), ((), ())), preferred_element_type=F32).astype(BF16)


def _cols(j, width=PIECE):
    return pl.ds(pl.multiple_of(j * width, width), width)


def _dhead_kernel(x_hbm, g_hbm, o_hbm, gv, xb, ob, x_sem, g_sem, o_sem):
    blocks = HID // PIECE

    def xload(b):
        return _copy(x_hbm.at[:, _cols(b)], xb.at[_odd(b)], x_sem.at[_odd(b)])

    def gload(j):
        return _copy(g_hbm.at[:, _cols(j)], gv.at[:, _cols(j)], g_sem.at[j])

    def ostore(b, n):
        return _copy(ob.at[n], o_hbm.at[_cols(b), _cols(n, HALF)], o_sem.at[n])

    def short_store(b):
        return _copy(ob.at[1, :, pl.ds(0, 2 * PIECE)], o_hbm.at[_cols(b), pl.ds(HALF, 2 * PIECE)], o_sem.at[1])

    def stored(b, n):
        short = (b >= CORNER) & (n == 1)
        pl.when(short)(lambda: short_store(b).wait())
        pl.when(jnp.logical_not(short))(lambda: ostore(b, n).wait())

    def piece(b, j):
        ob[_div(j, 4), :, _cols(_rem(j, 4))] = _outer(xb[_odd(b)], gv[:, _cols(j)])

    xload(0).start()
    gload(0).start()
    gload(1).start()

    def block(b, carry):
        xload(b).wait()

        @pl.when((b > 0) & (b < blocks - 1))
        def _():
            xload(b + 1).start()

        def half(n, carry):
            stored(b - 1, n)

            @pl.when(b < blocks)
            def _():
                ob[n] = _outer(xb[_odd(b)], gv[:, _cols(n, HALF)])

            ostore(b, n).start()
            return carry

        lax.fori_loop(0, jnp.where(b == 0, 0, jnp.where(b < CORNER, 2, 1)), half, 0)

        @pl.when(b >= CORNER)
        def _():
            stored(b - 1, 1)

        def small(j, carry):
            @pl.when(b == 0)
            def _():
                gload(j).wait()

                @pl.when(j < 6)
                def _():
                    gload(j + 2).start()

                @pl.when(j == 6)
                def _():
                    xload(1).start()

            pl.when(b < blocks)(lambda: piece(b, j))
            return carry

        part = (b == 0) | (b >= CORNER)
        low = jnp.where(b == 0, 0, 4)
        lax.fori_loop(low, jnp.where(part, jnp.where(b == 0, 8, 6), low), small, 0)

        @pl.when(b == 0)
        def _():
            ostore(0, 0).start()
            ostore(0, 1).start()

        @pl.when(b >= CORNER)
        def _():
            short_store(b).start()

        return carry

    lax.fori_loop(0, blocks, block, 0)
    last = jnp.int32(blocks - 1)
    stored(last, 0)
    stored(last, 1)


def _dhead(xall, gall):
    hbm = pl.BlockSpec(memory_space=ANY)
    dma = pltpu.SemaphoreType.DMA
    return pl.pallas_call(
        _dhead_kernel,
        in_specs=[hbm, hbm],
        out_specs=hbm,
        out_shape=jax.ShapeDtypeStruct((HID, VOC), BF16),
        scratch_shapes=[
            pltpu.VMEM((TOK, VOC), BF16),
            pltpu.VMEM((2, TOK, PIECE), BF16),
            pltpu.VMEM((2, PIECE, HALF), BF16),
            dma(TWO),
            dma((8,)),
            dma(TWO),
        ],
        compiler_params=pltpu.CompilerParams(vmem_limit_bytes=60 * MIB),
        cost_estimate=pl.CostEstimate(flops=2 * TOK * HID * VOC, bytes_accessed=200 * MIB, transcendentals=0),
        name="dhead",
    )(xall, gall)


def _tail_kernel(
    x_hbm, g_hbm, d_hbm, s_hbm, a_hbm, b_hbm, r_hbm, l_ref, do_hbm, o_hbm, loss_ref,
    gv, xb, ob, terms, ov, x_sem, g_sem, d_sem, in_sem, o_sem,
):
    steps = 2 * (HID // PIECE - CORNER)
    rows = PIECE // steps

    def xload(b):
        return _copy(x_hbm.at[:, _cols(CORNER + b)], xb.at[_odd(b)], x_sem.at[_odd(b)])

    def gload(j):
        return _copy(g_hbm.at[:, _cols(6 + j)], gv.at[:, _cols(j)], g_sem.at[j])

    def dstore(m):
        dst = do_hbm.at[_cols(CORNER + _half(m)), _cols(6 + _odd(m))]
        return _copy(ob.at[_odd(m)], dst, d_sem.at[_odd(m)])

    def chunk(ref, i):
        return ref.at[_cols(i, rows)]

    def load_terms(i):
        half = (a_hbm, b_hbm)[i * 2 // steps]
        for t, src in enumerate((chunk(s_hbm, i), chunk(half, i % (steps // 2)), chunk(r_hbm, i))):
            _copy(src, chunk(terms.at[t], i), in_sem.at[t, i]).start()

    xload(0).start()
    gload(0).start()
    load_terms(0)
    gload(1).start()
    xload(1).start()
    for i in range(1, steps):
        load_terms(i)
    loss_ref[0] = l_ref[0, 0]

    def add(i):
        for t in range(3):
            _copy(chunk(s_hbm, i), chunk(terms.at[t], i), in_sem.at[t, i]).wait()
        for r in range(0, rows, SUB):
            rs = pl.ds(pl.multiple_of(i * rows + r, SUB), SUB)
            ov[rs, :] = (terms[0, rs, :] + terms[1, rs, :] + terms[2, rs, :]).astype(BF16)
        _copy(chunk(ov, i), chunk(o_hbm, i), o_sem).start()

    def step(m, carry):
        b, j = _half(m), _odd(m)

        @pl.when(j == 0)
        def _():
            xload(b).wait()

        @pl.when(b == 0)
        def _():
            gload(j).wait()

        @pl.when(m > 1)
        def _():
            dstore(m - 2).wait()

        @pl.when(m < steps)
        def _():
            ob[j] = _outer(xb[_odd(b)], gv[:, _cols(j)])

        dstore(m).start()

        @pl.when((j == 1) & (m < steps - 3))
        def _():
            xload(b + 2).start()

        pl.when(m > 0)(lambda: add(m - 1))
        return carry

    lax.fori_loop(0, steps, step, 0)
    add(jnp.int32(steps - 1))
    dstore(steps - 2).wait()
    dstore(steps - 1).wait()
    _copy(ov, o_hbm, o_sem).wait()


def _tail(xall, gall, d_head, s_self, r1a, r1b, r2, loss):
    hbm = pl.BlockSpec(memory_space=ANY)
    dma = pltpu.SemaphoreType.DMA
    steps = 2 * (HID // PIECE - CORNER)
    return pl.pallas_call(
        _tail_kernel,
        in_specs=[hbm] * 7 + [pl.BlockSpec(memory_space=pltpu.VMEM)],
        out_specs=(hbm, hbm, pl.BlockSpec(memory_space=pltpu.SMEM)),
        out_shape=(
            jax.ShapeDtypeStruct((HID, VOC), BF16),
            jax.ShapeDtypeStruct((PIECE, HID), BF16),
            jax.ShapeDtypeStruct((1,), F32),
        ),
        input_output_aliases={2: 0},
        scratch_shapes=[
            pltpu.VMEM((TOK, 2 * PIECE), BF16),
            pltpu.VMEM((2, TOK, PIECE), BF16),
            pltpu.VMEM((2, PIECE, PIECE), BF16),
            pltpu.VMEM((3, PIECE, HID), F32),
            pltpu.VMEM((PIECE, HID), BF16),
            dma(TWO),
            dma(TWO),
            dma(TWO),
            dma((3, steps)),
            dma(()),
        ],
        compiler_params=pltpu.CompilerParams(vmem_limit_bytes=62 * MIB),
        cost_estimate=pl.CostEstimate(flops=TOK * HID * VOC // 8, bytes_accessed=46 * MIB, transcendentals=0),
        name="tail",
    )(xall, gall, d_head, s_self, r1a, r1b, r2, loss)


def solution(mesh):
    def device(y, x, core):
        return (y % 2) * 4 + (x % 2) * 2 + core

    first, second = [], []
    for yy in PAIR:
        for xx in PAIR:
            along_x = [(device(yy, xx, k), device(yy, xx + 1, k)) for k in PAIR]
            along_y = [(device(yy, xx, k), device(yy + 1, xx, k)) for k in PAIR]
            first += [along_x[0], along_y[1]]
            second += [along_y[0], along_x[1]]

    def local_step(hid, w, lab):
        xall, gall, s_n1b, s_self, y2, r1a, loss = _head(hid, lab.reshape(4, LANE), w)[:7]
        r1b = lax.ppermute(s_n1b, "tp", first)
        r2 = lax.ppermute(y2, "tp", second)
        d_head = _dhead(xall, gall)
        d_head, d_hidden, mean_loss = _tail(xall, gall, d_head, s_self, r1a, r1b, r2, loss)
        return mean_loss, d_hidden, d_head

    return jax.shard_map(
        local_step,
        mesh=mesh,
        in_specs=(P(("dp", "tp"), None), P(None, "tp"), P(("dp", "tp"))),
        out_specs=(P("dp"), P(("dp", "tp"), None), P("dp", "tp")),
        check_vma=False,
    )
```

```python
import functools

import jax
import jax.numpy as jnp
from jax import lax
from jax.experimental import pallas as pl
from jax.experimental.pallas import tpu as pltpu
from jax.sharding import PartitionSpec as P

F32, BF16, I32 = jnp.float32, jnp.bfloat16, jnp.int32
MESH = pl.DeviceIdType.MESH
ANY = pl.ANY

TOK = 4096
HID = 4096
VOC = 4096
BLK = 256
HALF = 2048
NBLK = TOK // BLK
LANE = 128
MIB = 1 << 20
TWO = (2,)
PAIR = (0, 1)
TILE = (8, LANE)
SUB = 16
FOUR = range(4)
CORNER = 6
LATE = 9
PIECE = 512
INV = 1.0 / TOK


def _div(a, b):
    return lax.div(jnp.int32(a), jnp.int32(b))


def _rem(a, b):
    return lax.rem(jnp.int32(a), jnp.int32(b))


def _odd(a):
    return _rem(a, 2)


def _half(a):
    return _div(a, 2)


def _copy(src, dst, sem):
    return pltpu.make_async_copy(src, dst, sem)


def _send(src, dst, send_sem, recv_sem, dev):
    return pltpu.make_async_remote_copy(
        src_ref=src, dst_ref=dst, send_sem=send_sem, recv_sem=recv_sem, device_id={"tp": dev}, device_id_type=MESH
    )


def _product(lhs, rhs, put, jobs, transposed):
    pl.when(lax.axis_index("tp") < 8)(functools.partial(_pieces, lhs, rhs, put, jobs, transposed))


def _pieces(lhs, rhs, put, jobs, transposed):
    dims = (((1,), (1,)), ((), ())) if transposed else (((1,), (0,)), ((), ()))
    pieces = HALF // PIECE
    deep = 8
    for nt in range(pieces):
        acc = None
        for kt in range(deep):
            part = lax.dot_general(lhs(kt), rhs(nt, kt), dims, preferred_element_type=F32)
            acc = part if acc is None else acc + part
            for job in jobs[nt * deep + kt]:
                job()
        put(nt, acc)


def _wide(v, times=HALF // LANE):
    return jnp.concatenate([v] * times, axis=1)


def _fold(v):
    width = v.shape[1] // 2
    while width >= LANE:
        v = v[:, :width] + v[:, width:]
        width //= 2
    return v


def _column(row):
    return jnp.transpose(jnp.broadcast_to(row, (LANE, LANE)))


def _head_kernel(
    x_hbm, lab_hbm, w_hbm,
    xall, gall, s_n1b, s_self, y2, r1a, loss_out,
    zst, s_d, s_n1a, s_n2, r1n2,
    wv, xg, ga, gb, zb, pbuf, rbuf, sbuf, ab, bb, cb, lab_v, la, lb, st_new, st_loc, st_all, ml, mk, sl, tl, comb, c_lab, c_top, c_scale, loss_acc,
    w_sem, lab_sem, labtx_sem, rx, tx, xl_sem, xs_sem, zo_sem, st_sem, sttx_sem,
    zi_sem, rr, ps, ss_sem, s1tx, r1s, r1as, ab_sem, cb_sem, g_sem,
):
    me = lax.axis_index("tp")
    chip = _half(me)
    c = _odd(me)
    x = _odd(chip)
    y = _half(chip)
    oc = 1 - c
    partner = me + 1 - 2 * c
    dx, dy = 2 - 4 * x, 4 - 8 * y
    n1 = me + oc * dx + c * dy
    n2 = me + c * dx + oc * dy
    n1kind = 1 + c

    def chip_of(kind):
        return chip + _odd(kind) * (1 - 2 * x) + _half(kind) * (2 - 4 * y)

    def order(i, first, last):
        a = _div(i, 4)
        mid, end = _rem(_half(a + 1), 2), _div(a, 3)
        kind = mid * (1 + _odd(i)) + first * (1 - mid) * (1 - end) + last * end
        return kind, mid * _half(i - 4) + (1 - mid) * _rem(i, 4)

    def order1(i):
        return order(i, 0, 3)

    def order2(i):
        return order(i, 3, 0)

    def block_id(kind, q):
        return chip_of(kind) * 4 + q

    def xrows(kind, q, part):
        return xall.at[pl.ds(pl.multiple_of(block_id(kind, q) * BLK + part * LANE, LANE), LANE)]

    def xblock(kind, q):
        return xall.at[pl.ds(pl.multiple_of(block_id(kind, q) * BLK, BLK), BLK)]

    def own(q):
        return x_hbm.at[pl.ds(pl.multiple_of(q * LANE, LANE), LANE)]

    def rxs(kind, q, part):
        return rx.at[kind * 8 + q * 2 + part]

    def wcopy(j):
        cols = pl.ds(j * PIECE, PIECE)
        return _copy(w_hbm.at[:, cols], wv.at[:, cols], w_sem.at[j])

    _copy(own(0), xg.at[0, pl.ds(pl.multiple_of(c * LANE, LANE), LANE)], xl_sem.at[0]).start()
    for j in FOUR:
        wcopy(j).start()

    barrier = pltpu.get_barrier_semaphore()
    for d in range(1, 8):
        pl.semaphore_signal(barrier, inc=1, device_id={"tp": _rem(me + d, 8)}, device_id_type=MESH)
    pl.semaphore_wait(barrier, 7)

    for d in range(1, 8):
        _send(lab_hbm, lab_v.at[me], labtx_sem, lab_sem, _rem(me + d, 8)).start()
    _copy(lab_hbm, lab_v.at[me], lab_sem).start()
    for q in FOUR:
        _send(own(q), xrows(0, q, c), tx, rxs(0, q, c), partner).start()
    for q in FOUR:
        _send(own(q), xrows_at(xall, me, q), tx, rxs(n1kind, q, c), n1).start()
        _send(own(q), xrows_at(xall, me, q), tx, rxs(3 - n1kind, q, c), n2).start()

    def load_x(b):
        kind, q = order1(b)
        slot = _odd(b)

        @pl.when(kind == 0)
        def _():
            _copy(own(q), xg.at[slot, pl.ds(pl.multiple_of(c * LANE, LANE), LANE)], xl_sem.at[slot]).start()
            _copy(xrows(0, q, oc), xg.at[slot, pl.ds(pl.multiple_of(oc * LANE, LANE), LANE)], xl_sem.at[slot]).start()

        @pl.when(kind != 0)
        def _():
            _copy(xblock(kind, q), xg.at[slot], xl_sem.at[slot]).start()

    def wait_rows(kind, q, part):
        _copy(xrows(kind, q, part), xrows(kind, q, part), rxs(kind, q, part)).wait()

    def take_rows(kind, q):
        wait_rows(kind, q, c)
        _send(xrows(kind, q, c), xrows(kind, q, c), tx, rxs(kind, q, c), partner).start()

        @pl.when(kind == n1kind)
        def _():
            _send(xrows(kind, q, c), xrows(kind, q, c), tx, rxs(3, q, c), n2).start()

    def part_load(b, part):
        kind, q = order1(b)
        return _copy(xrows(kind, q, part), xg.at[_odd(b), pl.ds(pl.multiple_of(part * LANE, LANE), LANE)], xl_sem.at[_odd(b)])

    def zcopy(b, h):
        kind, q = order1(b)
        return _copy(zb.at[h], zst.at[block_id(kind, q), h], zo_sem.at[h])

    def own_store(b):
        slot = _odd(b)
        return _copy(xg.at[slot, pl.ds(pl.multiple_of(c * LANE, LANE), LANE)], xrows(0, _rem(b, 4), c), xs_sem.at[slot])

    def label_column(blk, part):
        return _column(lab_v[2 * _div(blk, 4) + part, pl.ds(_rem(blk, 4), 1), :])

    def lane_stats(col, h, r):
        rows = pl.ds(r, 8)
        z = zb[h, rows, :]
        m = ml[h, rows, :]
        hit = _wide(col[rows, :] - (me * VOC + h * HALF)) == lax.broadcasted_iota(I32, (8, HALF), 1)
        s = _fold(jnp.exp(z - _wide(m)))
        t = _fold(jnp.where(hit, z, 0.0))
        if h == 1:
            m0 = mk[0, rows, :]
            mm = jnp.maximum(m0, m)
            s = sl[0, rows, :] * jnp.exp(m0 - mm) + s * jnp.exp(m - mm)
            t = tl[0, rows, :] + t
            m = mm
        mk[h, rows, :] = m
        sl[h, rows, :] = s
        tl[h, rows, :] = t

    def label_columns(blk, col, part):
        col[pl.ds(part * LANE, LANE), :] = label_column(blk, part)

    def row_stats(part):
        rows = pl.ds(part * LANE, LANE)
        m = jnp.transpose(mk[1, rows, :])
        top = jnp.max(m, axis=0, keepdims=True)
        st_new[part : part + 1, :] = top
        st_new[2 + part : 3 + part, :] = jnp.sum(jnp.transpose(sl[1, rows, :]) * jnp.exp(m - top), axis=0, keepdims=True)
        st_new[4 + part : 5 + part, :] = jnp.sum(jnp.transpose(tl[1, rows, :]), axis=0, keepdims=True)

    def send_stats(blk):
        for d in range(1, 8):
            _send(st_loc.at[blk], st_all.at[blk, me], sttx_sem, st_sem.at[blk], _rem(me + d, 8)).start()

    def keep_stats(blk):
        st_loc[blk] = st_new[...]
        st_all[blk, me] = st_new[...]

    def combine(blk):
        top = st_all[blk, 0, 0:2, :]
        for d in range(1, 8):
            top = jnp.maximum(top, st_all[blk, d, 0:2, :])
        s = jnp.zeros((2, LANE), F32)
        t = jnp.zeros((2, LANE), F32)
        for d in range(8):
            s = s + st_all[blk, d, 2:4, :] * jnp.exp(st_all[blk, d, 0:2, :] - top)
            t = t + st_all[blk, d, 4:6, :]
        comb[0:2, :] = top
        comb[2:4, :] = INV / s
        return top + jnp.log(s) - t

    def stats_arrived(blk):
        _copy(st_all.at[blk, pl.ds(0, 7)], st_all.at[blk, pl.ds(0, 7)], st_sem.at[blk]).wait()

    def columns(blk, par, part):
        rows = pl.ds(part * LANE, LANE)
        c_lab[par, rows, :] = label_column(blk, part)
        c_top[par, rows, :] = _column(comb[part : part + 1, :])
        c_scale[par, rows, :] = _column(comb[2 + part : 3 + part, :])

    def gradient(src, n, par, r, j):
        rows = pl.ds(pl.multiple_of(r, SUB), SUB)
        col = c_lab[par, rows, :] - (me * VOC + n * HALF + j)
        p = jnp.exp(src[n, rows, j : j + PIECE] - _wide(c_top[par, rows, :], 4)) * _wide(c_scale[par, rows, :], 4)
        g = jnp.where(_wide(col, 4) == lax.broadcasted_iota(I32, (SUB, PIECE), 1), p - INV, p)
        gbufs[par][rows, n * HALF + j : n * HALF + j + PIECE] = g.astype(BF16)

    def gradient_jobs(src, n, par):
        return [functools.partial(gradient, src, n, par, r, j) for r in range(0, BLK, SUB) for j in range(0, HALF, PIECE)]

    gbufs = (ga, gb)

    def gstore(k, par):
        kind, q = order2(k)
        return _copy(gbufs[par], gall.at[pl.ds(pl.multiple_of(block_id(kind, q) * BLK, BLK), BLK)], g_sem.at[par])

    def zload(k, dst, n):
        kind, q = order2(k)
        return _copy(zst.at[block_id(kind, q), n], dst.at[n], zi_sem.at[n])

    first_kind, first_q = order2(me * 0)
    first_blk = block_id(first_kind, first_q)

    def logits(b, h, jobs):
        slot = _odd(b)
        def put(nt, z):
            zb[h, :, nt * PIECE : (nt + 1) * PIECE] = z
            m = z[:, :LANE]
            for j in range(1, 4):
                m = jnp.maximum(m, z[:, j * LANE : (j + 1) * LANE])
            if nt:
                m = jnp.maximum(m, ml[h])
            ml[h] = m

        _product(
            lambda kt: xg[slot, :, kt * PIECE : (kt + 1) * PIECE],
            lambda nt, kt: wv[kt * PIECE : (kt + 1) * PIECE, h * HALF + nt * PIECE : h * HALF + (nt + 1) * PIECE],
            put,
            jobs,
            False,
        )

    wait_rows(0, 0, oc)
    _copy(xrows(0, 0, oc), xg.at[0, pl.ds(pl.multiple_of(oc * LANE, LANE), LANE)], xl_sem.at[0]).start()
    _copy(lab_v, lab_v, lab_sem).wait()
    for j in FOUR:
        wcopy(j).wait()
    for j in range(4, 8):
        wcopy(j).start()

    def phase1(i, carry):
        slot = _odd(i)
        kind, q = order1(i)
        kprev, qprev = order1(_rem(i + NBLK - 2, NBLK))
        kn, qn = order1(_rem(i + 1, NBLK))

        @pl.when((i == LATE + 1) | (i == NBLK - 1))
        def _():
            wait_rows(kind, q, oc)
            part_load(i, oc).start()

        _copy(xg.at[slot], xg.at[slot], xl_sem.at[slot]).wait()

        @pl.when(i < 4)
        def _():
            own_store(i).start()

        @pl.when(i > 0)
        def _():
            zcopy(i - 1, 1).start()
            zcopy(i - 1, 0).wait()

        @pl.when(i > 1)
        def _():
            keep_stats(block_id(kprev, qprev))

        @pl.when(i == NBLK - 2)
        def _():
            zload(0, pbuf, 0).start()
            zload(0, pbuf, 1).start()

        @pl.when(i == NBLK - 1)
        def _():
            stats_arrived(first_blk)
            loss_acc[...] = combine(first_blk)
            for part in PAIR:
                columns(first_blk, 0, part)
            for n in PAIR:
                zload(0, pbuf, n).wait()

                def some(r, carry, n=n):
                    for j in range(0, HALF, PIECE):
                        gradient(pbuf, n, 0, r * SUB, j)
                    return carry

                lax.fori_loop(0, SUB, some, 0)

            gstore(0, 0).start()

        @pl.when((i >= 3) & (i != LATE) & (i < NBLK - 2))
        def _():
            take_rows(kn, qn)

        jobs = [[] for _ in range(32)]
        for r in range(32):
            jobs[min(r + 1, 31)].append(functools.partial(lane_stats, la, 1, r * 8))
        for part in PAIR:
            jobs[4 + 4 * part].append(functools.partial(label_columns, block_id(kind, q), lb, part))
        logits(i, 0, jobs)

        zcopy(i, 0).start()

        @pl.when(i == 0)
        def _():
            for j in range(4, 8):
                wcopy(j).wait()

        @pl.when(i > 0)
        def _():
            zcopy(i - 1, 1).wait()

        @pl.when(i > 1)
        def _():
            send_stats(block_id(kprev, qprev))

        @pl.when((i == LATE) | (i == NBLK - 2))
        def _():
            take_rows(kn, qn)
            part_load(i + 1, c).start()

        @pl.when((i != LATE) & (i < NBLK - 2))
        def _():
            wait_rows(kn, qn, oc)

            @pl.when((i >= 1) & (i < 5))
            def _():
                own_store(i - 1).wait()

            load_x(i + 1)

        la[...] = lb[...]
        jobs = [[] for _ in range(32)]
        for r in range(32):
            jobs[min(r + 1, 31)].append(functools.partial(lane_stats, lb, 0, r * 8))
        for part in PAIR:
            jobs[8 + 8 * part].append(functools.partial(row_stats, part))
        logits(i, 1, jobs)
        return carry

    lax.fori_loop(0, NBLK, phase1, 0)
    last = NBLK - 1
    klast, qlast = order1(jnp.int32(last))
    kprev, qprev = order1(jnp.int32(last - 1))
    bprev, blast = block_id(kprev, qprev), block_id(klast, qlast)
    zcopy(last, 1).start()
    zcopy(last, 0).wait()
    zload(1, zb, 0).start()
    keep_stats(bprev)
    for r in range(32):
        lane_stats(la, 1, r * 8)
    send_stats(bprev)
    for part in PAIR:
        row_stats(part)
    keep_stats(blast)
    zcopy(last, 1).wait()
    zload(1, zb, 1).start()
    send_stats(blast)
    second_kind, second_q = order2(jnp.int32(1))
    second_blk = block_id(second_kind, second_q)
    stats_arrived(second_blk)
    loss_acc[...] += combine(second_blk)
    for part in PAIR:
        columns(second_blk, 1, part)

    def tile(ref, q, n):
        return ref.at[pl.ds(pl.multiple_of(q * LANE, LANE), LANE), pl.ds(pl.multiple_of(n * HALF, HALF), HALF)]

    def spair(k, n):
        return _send(
            pbuf.at[n, pl.ds(pl.multiple_of(oc * LANE, LANE), LANE)], rbuf.at[_odd(k + 2), n], ps.at[n], rr.at[_odd(k + 2) * 2 + n], partner
        )

    def sstore_start(k, n):
        kind, q = order2(k)
        sem = ss_sem.at[n]

        @pl.when(kind == 3)
        def _():
            _copy(sbuf.at[n], tile(s_d, q, n), sem).start()

        @pl.when((kind == n1kind) & (q < 2))
        def _():
            _copy(sbuf.at[n], tile(s_n1a, _odd(q), n), sem).start()

        @pl.when((kind == n1kind) & (q >= 2))
        def _():
            _copy(sbuf.at[n], tile(s_n1b, _odd(q), n), sem).start()

        @pl.when(kind == 3 - n1kind)
        def _():
            _copy(sbuf.at[n], tile(s_n2, q, n), sem).start()

        @pl.when(kind == 0)
        def _():
            _copy(sbuf.at[n], tile(s_self, q, n), sem).start()

    def sstore_done(k, n):
        kind, q = order2(k)
        _copy(sbuf.at[n], tile(s_d, 0, n), ss_sem.at[n]).wait()

        @pl.when(kind == 3)
        def _():
            _send(tile(s_d, q, n), tile(r1n2, q, n), s1tx, r1s.at[q * 2 + n], n1).start()

        @pl.when((kind == n1kind) & (q < 2))
        def _():
            _send(tile(s_n1a, _odd(q), n), tile(r1a, _odd(q), n), s1tx, r1as.at[_odd(q) * 2 + n], n1).start()

    def stage2_load(q, n):
        _copy(tile(r1n2, q, n), tile(r1n2, q, n), r1s.at[q * 2 + n]).wait()
        _copy(tile(s_n2, q, n), ab.at[n], ab_sem.at[n * 2]).start()
        _copy(tile(r1n2, q, n), bb.at[n], ab_sem.at[n * 2 + 1]).start()

    def pair_sum(k, n, r):
        sbuf[n, pl.ds(r, SUB), :] = pbuf[n, pl.ds(pl.multiple_of(c * LANE + r, SUB), SUB), :] + rbuf[_odd(k + 2), n, pl.ds(r, SUB), :]

    def stage2_sum(n, r):
        cb[n, pl.ds(r, SUB), :] = ab[n, pl.ds(r, SUB), :] + bb[n, pl.ds(r, SUB), :]

    def rwait(k, n):
        _copy(rbuf.at[_odd(k + 2), n], rbuf.at[_odd(k + 2), n], rr.at[_odd(k + 2) * 2 + n]).wait()

    def loss_part(k, blk):
        loss_acc[...] += jnp.where(k < NBLK - 2, combine(blk), 0.0)

    def sub(k, cur):
        nxt = 1 - cur
        kind2, q2 = order2(_rem(k + 2, NBLK))
        blk2 = block_id(kind2, q2)

        def trip(n):
            @pl.when(k < NBLK - 1)
            def _():
                zload(k + 1, zb, n).wait()

            @pl.when(k >= 1)
            def _():
                rwait(k - 1, n)
                spair(k - 1, n).wait_send()
                if n == 0:
                    gstore(k - 1, nxt).wait()

            if n == 0:

                @pl.when(k < NBLK - 2)
                def _():
                    stats_arrived(blk2)

            @pl.when(k >= 12)
            def _():
                _copy(tile(s_n2, 0, n), ab.at[n], ab_sem.at[n * 2]).wait()
                _copy(tile(r1n2, 0, n), bb.at[n], ab_sem.at[n * 2 + 1]).wait()

            @pl.when(k >= 13)
            def _():
                _copy(cb.at[n], tile(y2, 0, n), cb_sem.at[n]).wait()

            jobs = [[] for _ in range(32)]
            for r in range(8):
                jobs[2 + r * 3 // 5].append(functools.partial(pair_sum, k - 1, n, r * SUB))
                jobs[10 + r * 5 // 2].append(functools.partial(stage2_sum, n, r * SUB))
            for r, job in enumerate(gradient_jobs(zb, n, nxt)):
                jobs[2 + r * 9 // 20].append(job)
            if n == 0:
                jobs[8].append(lambda: loss_part(k, blk2))
            else:
                for part in PAIR:
                    jobs[8 + 8 * part].append(functools.partial(columns, blk2, cur, part))

            def put(nt, acc):
                pbuf[n, :, nt * PIECE : (nt + 1) * PIECE] = acc

            _product(
                lambda kt: gbufs[cur][:, kt * PIECE : (kt + 1) * PIECE],
                lambda nt, kt: wv[pl.ds(pl.multiple_of(n * HALF + nt * PIECE, PIECE), PIECE), kt * PIECE : (kt + 1) * PIECE],
                put,
                jobs,
                True,
            )

            spair(k, n).start()

            @pl.when(k < NBLK - 2)
            def _():
                zload(k + 2, zb, n).start()

            @pl.when(k >= 2)
            def _():
                sstore_done(k - 2 + n, 1 - n)

            @pl.when(k >= 1)
            def _():
                sstore_start(k - 1, n)

            if n == 0:
                @pl.when(k == 1)
                def _():
                    sstore_done(k - 1, n)

            @pl.when(k >= 12)
            def _():
                _copy(cb.at[n], tile(y2, k - 12, n), cb_sem.at[n]).start()

            @pl.when((k >= 11) & (k < NBLK - 1))
            def _():
                stage2_load(k - 11, n)


        trip(0)
        trip(1)

        @pl.when(k < NBLK - 1)
        def _():
            gstore(k + 1, nxt).start()

    def pair(p, carry):
        sub(2 * p, 0)
        sub(2 * p + 1, 1)
        return carry

    lax.fori_loop(0, NBLK // 2, pair, 0)

    kl = jnp.int32(NBLK - 1)
    for n in PAIR:
        rwait(kl, n)
        spair(kl, n).wait_send()
        if n == 0:
            sstore_done(kl - 1, 1)
        for r in range(8):
            pair_sum(kl, n, r * SUB)
        sstore_start(kl, n)
    for n in PAIR:
        sstore_done(kl, n)
    gstore(kl, 1).wait()
    for n in PAIR:
        _copy(cb.at[n], tile(y2, 0, n), cb_sem.at[n]).wait()

    loss_out[...] = jnp.full(TILE, jnp.sum(loss_acc[...]) * INV, F32)

    for i in FOUR:
        _copy(tile(r1a, i // 2, i % 2), tile(r1a, i // 2, i % 2), r1as.at[i]).wait()
    _copy(s_d, s_d, s1tx).wait()
    _copy(s_n1a, s_n1a, s1tx).wait()
    _copy(xall.at[pl.ds(0, 28 * LANE)], xall.at[pl.ds(0, 28 * LANE)], tx).wait()
    for d in range(7):
        _copy(lab_v.at[d], lab_v.at[d], labtx_sem).wait()
        _copy(st_loc, st_loc, sttx_sem).wait()


def xrows_at(xall, dev, q):
    return xall.at[pl.ds(pl.multiple_of((dev // 2) * 1024 + q * BLK + (dev % 2) * LANE, LANE), LANE)]


def _head(hid, lab, w):
    hbm = pl.BlockSpec(memory_space=ANY)
    sd = jax.ShapeDtypeStruct
    dma = pltpu.SemaphoreType.DMA
    vmem = pltpu.VMEM
    quarter = (LANE, HALF)
    return pl.pallas_call(
        _head_kernel,
        out_shape=(
            sd((TOK, HID), BF16),
            sd((TOK, VOC), BF16),
            sd((256, HID), F32),
            sd((PIECE, HID), F32),
            sd((PIECE, HID), F32),
            sd((256, HID), F32),
            sd(TILE, F32),
            sd((NBLK, 2, BLK, HALF), F32),
            sd((PIECE, HID), F32),
            sd((256, HID), F32),
            sd((PIECE, HID), F32),
            sd((PIECE, HID), F32),
        ),
        in_specs=[hbm] * 3,
        out_specs=(hbm,) * 6 + (pl.BlockSpec(memory_space=vmem),) + (hbm,) * 5,
        scratch_shapes=[
            vmem((HID, VOC), BF16),
            vmem((2, BLK, HID), BF16),
            vmem((BLK, VOC), BF16),
            vmem((BLK, VOC), BF16),
            vmem((2, BLK, HALF), F32),
            vmem((2, BLK, HALF), F32),
            vmem((2, 2) + quarter, F32),
            vmem(TWO + quarter, F32),
            vmem(TWO + quarter, F32),
            vmem(TWO + quarter, F32),
            vmem(TWO + quarter, F32),
            vmem((8, 4, LANE), I32),
            vmem((BLK, LANE), I32),
            vmem((BLK, LANE), I32),
            vmem(TILE, F32),
            vmem((NBLK,) + TILE, F32),
            vmem((NBLK, 8) + TILE, F32),
            vmem((2, BLK, LANE), F32),
            vmem((2, BLK, LANE), F32),
            vmem((2, BLK, LANE), F32),
            vmem((2, BLK, LANE), F32),
            vmem(TILE, F32),
            vmem((2, BLK, LANE), I32),
            vmem((2, BLK, LANE), F32),
            vmem((2, BLK, LANE), F32),
            vmem((2, LANE), F32),
            dma((8,)),
            dma(()),
            dma(()),
            dma((32,)),
            dma(()),
            dma(TWO),
            dma(TWO),
            dma(TWO),
            dma((NBLK,)),
            dma(()),
            dma(TWO),
            dma((4,)),
            dma(TWO),
            dma(TWO),
            dma(()),
            dma((8,)),
            dma((4,)),
            dma((4,)),
            dma(TWO),
            dma(TWO),
        ],
        compiler_params=pltpu.CompilerParams(collective_id=0, has_side_effects=True, vmem_limit_bytes=67_043_328),
        cost_estimate=pl.CostEstimate(flops=4 * TOK * HID * VOC, bytes_accessed=400 * MIB, transcendentals=2 * TOK * VOC),
        name="head",
    )(hid, lab, w)


def _outer(lhs, rhs):
    return lax.dot_general(lhs, rhs, (((0,), (0,)), ((), ())), preferred_element_type=F32).astype(BF16)


def _cols(j, width=PIECE):
    return pl.ds(pl.multiple_of(j * width, width), width)


def _dhead_kernel(x_hbm, g_hbm, o_hbm, gv, xb, ob, x_sem, g_sem, o_sem):
    blocks = HID // PIECE

    def xload(b):
        return _copy(x_hbm.at[:, _cols(b)], xb.at[_odd(b)], x_sem.at[_odd(b)])

    def gload(j):
        return _copy(g_hbm.at[:, _cols(j)], gv.at[:, _cols(j)], g_sem.at[j])

    def ostore(b, n):
        return _copy(ob.at[n], o_hbm.at[_cols(b), _cols(n, HALF)], o_sem.at[n])

    def short_store(b):
        return _copy(ob.at[1, :, pl.ds(0, 2 * PIECE)], o_hbm.at[_cols(b), pl.ds(HALF, 2 * PIECE)], o_sem.at[1])

    def stored(b, n):
        short = (b >= CORNER) & (n == 1)
        pl.when(short)(lambda: short_store(b).wait())
        pl.when(jnp.logical_not(short))(lambda: ostore(b, n).wait())

    def piece(b, j):
        ob[_div(j, 4), :, _cols(_rem(j, 4))] = _outer(xb[_odd(b)], gv[:, _cols(j)])

    xload(0).start()
    gload(0).start()

    def block(b, carry):
        xload(b).wait()

        @pl.when((b > 0) & (b < blocks - 1))
        def _():
            xload(b + 1).start()

        def half(n, carry):
            stored(b - 1, n)

            @pl.when(b < blocks)
            def _():
                ob[n] = _outer(xb[_odd(b)], gv[:, _cols(n, HALF)])

            ostore(b, n).start()
            return carry

        lax.fori_loop(0, jnp.where(b == 0, 0, jnp.where(b < CORNER, 2, 1)), half, 0)

        @pl.when(b >= CORNER)
        def _():
            stored(b - 1, 1)

        def small(j, carry):
            @pl.when(b == 0)
            def _():
                gload(j).wait()

                @pl.when(j == 0)
                def _():
                    gload(1).start()

                @pl.when(j < 6)
                def _():
                    gload(j + 2).start()

                @pl.when(j == 6)
                def _():
                    xload(1).start()

            pl.when(b < blocks)(lambda: piece(b, j))
            return carry

        part = (b == 0) | (b >= CORNER)
        low = jnp.where(b == 0, 0, 4)
        lax.fori_loop(low, jnp.where(part, jnp.where(b == 0, 8, 6), low), small, 0)

        @pl.when(b == 0)
        def _():
            ostore(0, 0).start()
            ostore(0, 1).start()

        @pl.when(b >= CORNER)
        def _():
            short_store(b).start()

        return carry

    lax.fori_loop(0, blocks, block, 0)
    last = jnp.int32(blocks - 1)
    stored(last, 0)
    stored(last, 1)


def _dhead(xall, gall):
    hbm = pl.BlockSpec(memory_space=ANY)
    dma = pltpu.SemaphoreType.DMA
    return pl.pallas_call(
        _dhead_kernel,
        in_specs=[hbm, hbm],
        out_specs=hbm,
        out_shape=jax.ShapeDtypeStruct((HID, VOC), BF16),
        scratch_shapes=[
            pltpu.VMEM((TOK, VOC), BF16),
            pltpu.VMEM((2, TOK, PIECE), BF16),
            pltpu.VMEM((2, PIECE, HALF), BF16),
            dma(TWO),
            dma((8,)),
            dma(TWO),
        ],
        compiler_params=pltpu.CompilerParams(vmem_limit_bytes=60 * MIB),
        cost_estimate=pl.CostEstimate(flops=2 * TOK * HID * VOC, bytes_accessed=200 * MIB, transcendentals=0),
        name="dhead",
    )(xall, gall)


def _tail_kernel(
    x_hbm, g_hbm, d_hbm, s_hbm, a_hbm, b_hbm, r_hbm, l_ref, do_hbm, o_hbm, loss_ref,
    gv, xb, ob, terms, ov, x_sem, g_sem, d_sem, in_sem, o_sem,
):
    steps = 2 * (HID // PIECE - CORNER)
    rows = PIECE // steps

    def xload(b):
        return _copy(x_hbm.at[:, _cols(CORNER + b)], xb.at[_odd(b)], x_sem.at[_odd(b)])

    def gload(j):
        return _copy(g_hbm.at[:, _cols(6 + j)], gv.at[:, _cols(j)], g_sem.at[j])

    def dstore(m):
        dst = do_hbm.at[_cols(CORNER + _half(m)), _cols(6 + _odd(m))]
        return _copy(ob.at[_odd(m)], dst, d_sem.at[_odd(m)])

    def chunk(ref, i):
        return ref.at[_cols(i, rows)]

    def load_terms(i):
        _copy(chunk(s_hbm, i), chunk(terms.at[0], i), in_sem.at[0, i]).start()
        _copy(chunk(r_hbm, i), chunk(terms.at[2], i), in_sem.at[2, i]).start()
        row = _rem(i, steps // 2)
        pl.when(i < steps // 2)(lambda: _copy(chunk(a_hbm, row), chunk(terms.at[1], i), in_sem.at[1, i]).start())
        pl.when(i >= steps // 2)(lambda: _copy(chunk(b_hbm, row), chunk(terms.at[1], i), in_sem.at[1, i]).start())

    xload(0).start()
    gload(0).start()
    loss_ref[0] = l_ref[0, 0]

    def add(i):
        for t in range(3):
            _copy(chunk(s_hbm, i), chunk(terms.at[t], i), in_sem.at[t, i]).wait()
        for r in range(0, rows, SUB):
            rs = pl.ds(pl.multiple_of(i * rows + r, SUB), SUB)
            ov[rs, :] = (terms[0, rs, :] + terms[1, rs, :] + terms[2, rs, :]).astype(BF16)
        _copy(chunk(ov, i), chunk(o_hbm, i), o_sem).start()

    def step(m, carry):
        b, j = _half(m), _odd(m)

        @pl.when(j == 0)
        def _():
            xload(b).wait()

        @pl.when(b == 0)
        def _():
            gload(j).wait()

        @pl.when(m == 0)
        def _():
            gload(1).start()

        @pl.when(m == 1)
        def _():
            xload(1).start()

        load_terms(m)

        @pl.when(m > 1)
        def _():
            dstore(m - 2).wait()

        @pl.when(m < steps)
        def _():
            ob[j] = _outer(xb[_odd(b)], gv[:, _cols(j)])

        dstore(m).start()

        @pl.when((j == 1) & (m < steps - 3))
        def _():
            xload(b + 2).start()

        pl.when(m > 0)(lambda: add(m - 1))
        return carry

    lax.fori_loop(0, steps, step, 0)
    add(jnp.int32(steps - 1))
    dstore(steps - 2).wait()
    dstore(steps - 1).wait()
    _copy(ov, o_hbm, o_sem).wait()


def _tail(xall, gall, d_head, s_self, r1a, r1b, r2, loss):
    hbm = pl.BlockSpec(memory_space=ANY)
    dma = pltpu.SemaphoreType.DMA
    steps = 2 * (HID // PIECE - CORNER)
    return pl.pallas_call(
        _tail_kernel,
        in_specs=[hbm] * 7 + [pl.BlockSpec(memory_space=pltpu.VMEM)],
        out_specs=(hbm, hbm, pl.BlockSpec(memory_space=pltpu.SMEM)),
        out_shape=(
            jax.ShapeDtypeStruct((HID, VOC), BF16),
            jax.ShapeDtypeStruct((PIECE, HID), BF16),
            jax.ShapeDtypeStruct((1,), F32),
        ),
        input_output_aliases={2: 0},
        scratch_shapes=[
            pltpu.VMEM((TOK, 2 * PIECE), BF16),
            pltpu.VMEM((2, TOK, PIECE), BF16),
            pltpu.VMEM((2, PIECE, PIECE), BF16),
            pltpu.VMEM((3, PIECE, HID), F32),
            pltpu.VMEM((PIECE, HID), BF16),
            dma(TWO),
            dma(TWO),
            dma(TWO),
            dma((3, steps)),
            dma(()),
        ],
        compiler_params=pltpu.CompilerParams(vmem_limit_bytes=62 * MIB),
        cost_estimate=pl.CostEstimate(flops=TOK * HID * VOC // 8, bytes_accessed=46 * MIB, transcendentals=0),
        name="tail",
    )(xall, gall, d_head, s_self, r1a, r1b, r2, loss)


def solution(mesh):
    def device(y, x, core):
        return (y % 2) * 4 + (x % 2) * 2 + core

    first, second = [], []
    for yy in PAIR:
        for xx in PAIR:
            along_x = [(device(yy, xx, k), device(yy, xx + 1, k)) for k in PAIR]
            along_y = [(device(yy, xx, k), device(yy + 1, xx, k)) for k in PAIR]
            first += [along_x[0], along_y[1]]
            second += [along_y[0], along_x[1]]

    def local_step(hid, w, lab):
        xall, gall, s_n1b, s_self, y2, r1a, loss = _head(hid, lab.reshape(4, LANE), w)[:7]
        r1b = lax.ppermute(s_n1b, "tp", first)
        r2 = lax.ppermute(y2, "tp", second)
        d_head = _dhead(xall, gall)
        d_head, d_hidden, mean_loss = _tail(xall, gall, d_head, s_self, r1a, r1b, r2, loss)
        return mean_loss, d_hidden, d_head

    return jax.shard_map(
        local_step,
        mesh=mesh,
        in_specs=(P(("dp", "tp"), None), P(None, "tp"), P(("dp", "tp"))),
        out_specs=(P("dp"), P(("dp", "tp"), None), P("dp", "tp")),
        check_vma=False,
    )
```

```python
import functools

import jax
import jax.numpy as jnp
from jax import lax
from jax.experimental import pallas as pl
from jax.experimental.pallas import tpu as pltpu
from jax.sharding import PartitionSpec as P

F32, BF16, I32 = jnp.float32, jnp.bfloat16, jnp.int32
MESH = pl.DeviceIdType.MESH
ANY = pl.ANY

TOK = 4096
HID = 4096
VOC = 4096
BLK = 256
HALF = 2048
NBLK = TOK // BLK
LANE = 128
MIB = 1 << 20
TWO = (2,)
PAIR = (0, 1)
TILE = (8, LANE)
SUB = 16
FOUR = range(4)
LATE = 9
PIECE = 512
INV = 1.0 / TOK


def _div(a, b):
    return lax.div(jnp.int32(a), jnp.int32(b))


def _rem(a, b):
    return lax.rem(jnp.int32(a), jnp.int32(b))


def _copy(src, dst, sem):
    return pltpu.make_async_copy(src, dst, sem)


def _send(src, dst, send_sem, recv_sem, dev):
    return pltpu.make_async_remote_copy(
        src_ref=src, dst_ref=dst, send_sem=send_sem, recv_sem=recv_sem, device_id={"tp": dev}, device_id_type=MESH
    )


def _product(lhs, rhs, put, jobs, transposed):
    pl.when(lax.axis_index("tp") < 8)(functools.partial(_pieces, lhs, rhs, put, jobs, transposed))


def _pieces(lhs, rhs, put, jobs, transposed):
    dims = (((1,), (1,)), ((), ())) if transposed else (((1,), (0,)), ((), ()))
    pieces = HALF // PIECE
    deep = 8
    for nt in range(pieces):
        acc = None
        for kt in range(deep):
            part = lax.dot_general(lhs(kt), rhs(nt, kt), dims, preferred_element_type=F32)
            acc = part if acc is None else acc + part
            for job in jobs[nt * deep + kt]:
                job()
        put(nt, acc)


def _wide(v, times=HALF // LANE):
    return jnp.concatenate([v] * times, axis=1)


def _fold(v):
    width = v.shape[1] // 2
    while width >= LANE:
        v = v[:, :width] + v[:, width:]
        width //= 2
    return v


def _column(row):
    return jnp.transpose(jnp.broadcast_to(row, (LANE, LANE)))


def _head_kernel(
    x_hbm, lab_hbm, w_hbm,
    xall, gall, s_n1b, s_self, y2, r1a, loss_out,
    zst, s_d, s_n1a, s_n2, r1n2,
    wv, xg, ga, gb, zb, pbuf, rbuf, sbuf, ab, bb, cb, lab_v, la, lb, st_new, st_loc, st_all, ml, mk, sl, tl, comb, c_lab, c_top, c_scale, loss_acc,
    w_sem, lab_sem, labtx_sem, rx, tx, xl_sem, xs_sem, zo_sem, st_sem, sttx_sem,
    zi_sem, rr, ps, ss_sem, s1tx, r1s, r1as, ab_sem, cb_sem, g_sem,
):
    me = lax.axis_index("tp")
    chip = _div(me, 2)
    c = _rem(me, 2)
    x = _rem(chip, 2)
    y = _div(chip, 2)
    oc = 1 - c
    partner = me + 1 - 2 * c
    dx, dy = 2 - 4 * x, 4 - 8 * y
    n1 = me + oc * dx + c * dy
    n2 = me + c * dx + oc * dy
    n1kind = 1 + c

    def chip_of(kind):
        return chip + _rem(kind, 2) * (1 - 2 * x) + _div(kind, 2) * (2 - 4 * y)

    def order(i, first, last):
        a = _div(i, 4)
        mid, end = _rem(_div(a + 1, 2), 2), _div(a, 3)
        kind = mid * (1 + _rem(i, 2)) + first * (1 - mid) * (1 - end) + last * end
        return kind, mid * _div(i - 4, 2) + (1 - mid) * _rem(i, 4)

    def order1(i):
        return order(i, 0, 3)

    def order2(i):
        return order(i, 3, 0)

    def block_id(kind, q):
        return chip_of(kind) * 4 + q

    def xrows(kind, q, part):
        return xall.at[pl.ds(pl.multiple_of(block_id(kind, q) * BLK + part * LANE, LANE), LANE)]

    def xblock(kind, q):
        return xall.at[pl.ds(pl.multiple_of(block_id(kind, q) * BLK, BLK), BLK)]

    def own(q):
        return x_hbm.at[pl.ds(pl.multiple_of(q * LANE, LANE), LANE)]

    def rxs(kind, q, part):
        return rx.at[kind * 8 + q * 2 + part]

    def wcopy(j):
        cols = pl.ds(j * PIECE, PIECE)
        return _copy(w_hbm.at[:, cols], wv.at[:, cols], w_sem.at[j])

    _copy(own(0), xg.at[0, pl.ds(pl.multiple_of(c * LANE, LANE), LANE)], xl_sem.at[0]).start()
    for j in FOUR:
        wcopy(j).start()

    barrier = pltpu.get_barrier_semaphore()
    for d in range(1, 8):
        pl.semaphore_signal(barrier, inc=1, device_id={"tp": _rem(me + d, 8)}, device_id_type=MESH)
    pl.semaphore_wait(barrier, 7)

    for d in range(1, 8):
        _send(lab_hbm, lab_v.at[me], labtx_sem, lab_sem, _rem(me + d, 8)).start()
    _copy(lab_hbm, lab_v.at[me], lab_sem).start()
    for q in FOUR:
        _send(own(q), xrows(0, q, c), tx, rxs(0, q, c), partner).start()
    for q in FOUR:
        _send(own(q), xrows_at(xall, me, q), tx, rxs(n1kind, q, c), n1).start()
        _send(own(q), xrows_at(xall, me, q), tx, rxs(3 - n1kind, q, c), n2).start()

    def load_x(b):
        kind, q = order1(b)
        slot = _rem(b, 2)

        @pl.when(kind == 0)
        def _():
            _copy(own(q), xg.at[slot, pl.ds(pl.multiple_of(c * LANE, LANE), LANE)], xl_sem.at[slot]).start()
            _copy(xrows(0, q, oc), xg.at[slot, pl.ds(pl.multiple_of(oc * LANE, LANE), LANE)], xl_sem.at[slot]).start()

        @pl.when(kind != 0)
        def _():
            _copy(xblock(kind, q), xg.at[slot], xl_sem.at[slot]).start()

    def wait_rows(kind, q, part):
        _copy(xrows(kind, q, part), xrows(kind, q, part), rxs(kind, q, part)).wait()

    def take_rows(kind, q):
        wait_rows(kind, q, c)
        _send(xrows(kind, q, c), xrows(kind, q, c), tx, rxs(kind, q, c), partner).start()

        @pl.when(kind == n1kind)
        def _():
            _send(xrows(kind, q, c), xrows(kind, q, c), tx, rxs(3, q, c), n2).start()

    def part_load(b, part):
        kind, q = order1(b)
        return _copy(xrows(kind, q, part), xg.at[_rem(b, 2), pl.ds(pl.multiple_of(part * LANE, LANE), LANE)], xl_sem.at[_rem(b, 2)])

    def zcopy(b, h):
        kind, q = order1(b)
        return _copy(zb.at[h], zst.at[block_id(kind, q), h], zo_sem.at[h])

    def own_store(b):
        slot = _rem(b, 2)
        return _copy(xg.at[slot, pl.ds(pl.multiple_of(c * LANE, LANE), LANE)], xrows(0, _rem(b, 4), c), xs_sem.at[slot])

    def label_column(blk, part):
        return _column(lab_v[2 * _div(blk, 4) + part, pl.ds(_rem(blk, 4), 1), :])

    def lane_stats(col, h, r):
        rows = pl.ds(r, 8)
        z = zb[h, rows, :]
        m = ml[h, rows, :]
        hit = _wide(col[rows, :] - (me * VOC + h * HALF)) == lax.broadcasted_iota(I32, (8, HALF), 1)
        s = _fold(jnp.exp(z - _wide(m)))
        t = _fold(jnp.where(hit, z, 0.0))
        if h == 1:
            m0 = mk[0, rows, :]
            mm = jnp.maximum(m0, m)
            s = sl[0, rows, :] * jnp.exp(m0 - mm) + s * jnp.exp(m - mm)
            t = tl[0, rows, :] + t
            m = mm
        mk[h, rows, :] = m
        sl[h, rows, :] = s
        tl[h, rows, :] = t

    def label_columns(blk, col, part):
        col[pl.ds(part * LANE, LANE), :] = label_column(blk, part)

    def row_stats(part):
        rows = pl.ds(part * LANE, LANE)
        m = jnp.transpose(mk[1, rows, :])
        top = jnp.max(m, axis=0, keepdims=True)
        st_new[part : part + 1, :] = top
        st_new[2 + part : 3 + part, :] = jnp.sum(jnp.transpose(sl[1, rows, :]) * jnp.exp(m - top), axis=0, keepdims=True)
        st_new[4 + part : 5 + part, :] = jnp.sum(jnp.transpose(tl[1, rows, :]), axis=0, keepdims=True)

    def send_stats(blk):
        for d in range(1, 8):
            _send(st_loc.at[blk], st_all.at[blk, me], sttx_sem, st_sem.at[blk], _rem(me + d, 8)).start()

    def keep_stats(blk):
        st_loc[blk] = st_new[...]
        st_all[blk, me] = st_new[...]

    def combine(blk):
        top = st_all[blk, 0, 0:2, :]
        for d in range(1, 8):
            top = jnp.maximum(top, st_all[blk, d, 0:2, :])
        s = jnp.zeros((2, LANE), F32)
        t = jnp.zeros((2, LANE), F32)
        for d in range(8):
            s = s + st_all[blk, d, 2:4, :] * jnp.exp(st_all[blk, d, 0:2, :] - top)
            t = t + st_all[blk, d, 4:6, :]
        comb[0:2, :] = top
        comb[2:4, :] = INV / s
        return top + jnp.log(s) - t

    def stats_arrived(blk):
        _copy(st_all.at[blk, pl.ds(0, 7)], st_all.at[blk, pl.ds(0, 7)], st_sem.at[blk]).wait()

    def columns(blk, par, part):
        rows = pl.ds(part * LANE, LANE)
        c_lab[par, rows, :] = label_column(blk, part)
        c_top[par, rows, :] = _column(comb[part : part + 1, :])
        c_scale[par, rows, :] = _column(comb[2 + part : 3 + part, :])

    def gradient(src, n, par, r, j):
        rows = pl.ds(pl.multiple_of(r, SUB), SUB)
        col = c_lab[par, rows, :] - (me * VOC + n * HALF + j)
        p = jnp.exp(src[n, rows, j : j + PIECE] - _wide(c_top[par, rows, :], 4)) * _wide(c_scale[par, rows, :], 4)
        g = jnp.where(_wide(col, 4) == lax.broadcasted_iota(I32, (SUB, PIECE), 1), p - INV, p)
        gbufs[par][rows, n * HALF + j : n * HALF + j + PIECE] = g.astype(BF16)

    def gradient_jobs(src, n, par):
        return [functools.partial(gradient, src, n, par, r, j) for r in range(0, BLK, SUB) for j in range(0, HALF, PIECE)]

    gbufs = (ga, gb)

    def gstore(k, par):
        kind, q = order2(k)
        return _copy(gbufs[par], gall.at[pl.ds(pl.multiple_of(block_id(kind, q) * BLK, BLK), BLK)], g_sem.at[par])

    def zload(k, dst, n):
        kind, q = order2(k)
        return _copy(zst.at[block_id(kind, q), n], dst.at[n], zi_sem.at[n])

    first_kind, first_q = order2(me * 0)
    first_blk = block_id(first_kind, first_q)

    def logits(b, h, jobs):
        slot = _rem(b, 2)
        def put(nt, z):
            zb[h, :, nt * PIECE : (nt + 1) * PIECE] = z
            m = z[:, :LANE]
            for j in range(1, 4):
                m = jnp.maximum(m, z[:, j * LANE : (j + 1) * LANE])
            if nt:
                m = jnp.maximum(m, ml[h])
            ml[h] = m

        _product(
            lambda kt: xg[slot, :, kt * PIECE : (kt + 1) * PIECE],
            lambda nt, kt: wv[kt * PIECE : (kt + 1) * PIECE, h * HALF + nt * PIECE : h * HALF + (nt + 1) * PIECE],
            put,
            jobs,
            False,
        )

    wait_rows(0, 0, oc)
    _copy(xrows(0, 0, oc), xg.at[0, pl.ds(pl.multiple_of(oc * LANE, LANE), LANE)], xl_sem.at[0]).start()
    _copy(lab_v, lab_v, lab_sem).wait()
    for j in FOUR:
        wcopy(j).wait()
    for j in range(4, 8):
        wcopy(j).start()

    def phase1(i, carry):
        slot = _rem(i, 2)
        kind, q = order1(i)
        kprev, qprev = order1(_rem(i + NBLK - 2, NBLK))
        kn, qn = order1(_rem(i + 1, NBLK))

        @pl.when((i == LATE + 1) | (i == NBLK - 1))
        def _():
            wait_rows(kind, q, oc)
            part_load(i, oc).start()

        _copy(xg.at[slot], xg.at[slot], xl_sem.at[slot]).wait()

        @pl.when(i < 4)
        def _():
            own_store(i).start()

        @pl.when(i > 0)
        def _():
            zcopy(i - 1, 1).start()
            zcopy(i - 1, 0).wait()

        @pl.when(i > 1)
        def _():
            keep_stats(block_id(kprev, qprev))

        @pl.when(i == NBLK - 2)
        def _():
            zload(0, pbuf, 0).start()
            zload(0, pbuf, 1).start()

        @pl.when(i == NBLK - 1)
        def _():
            stats_arrived(first_blk)
            loss_acc[...] = combine(first_blk)
            for part in PAIR:
                columns(first_blk, 0, part)
            for n in PAIR:
                zload(0, pbuf, n).wait()

                def some(r, carry, n=n):
                    for j in range(0, HALF, PIECE):
                        gradient(pbuf, n, 0, r * SUB, j)
                    return carry

                lax.fori_loop(0, SUB, some, 0)

            gstore(0, 0).start()

        @pl.when((i >= 3) & (i != LATE) & (i < NBLK - 2))
        def _():
            take_rows(kn, qn)

        jobs = [[] for _ in range(32)]
        for r in range(32):
            jobs[min(r + 1, 31)].append(functools.partial(lane_stats, la, 1, r * 8))
        for part in PAIR:
            jobs[4 + 4 * part].append(functools.partial(label_columns, block_id(kind, q), lb, part))
        logits(i, 0, jobs)

        zcopy(i, 0).start()

        @pl.when(i == 0)
        def _():
            for j in range(4, 8):
                wcopy(j).wait()

        @pl.when(i > 0)
        def _():
            zcopy(i - 1, 1).wait()

        @pl.when(i > 1)
        def _():
            send_stats(block_id(kprev, qprev))

        @pl.when((i == LATE) | (i == NBLK - 2))
        def _():
            take_rows(kn, qn)
            part_load(i + 1, c).start()

        @pl.when((i != LATE) & (i < NBLK - 2))
        def _():
            wait_rows(kn, qn, oc)

            @pl.when((i >= 1) & (i < 5))
            def _():
                own_store(i - 1).wait()

            load_x(i + 1)

        la[...] = lb[...]
        jobs = [[] for _ in range(32)]
        for r in range(32):
            jobs[min(r + 1, 31)].append(functools.partial(lane_stats, lb, 0, r * 8))
        for part in PAIR:
            jobs[8 + 8 * part].append(functools.partial(row_stats, part))
        logits(i, 1, jobs)
        return carry

    lax.fori_loop(0, NBLK, phase1, 0)
    last = NBLK - 1
    klast, qlast = order1(jnp.int32(last))
    kprev, qprev = order1(jnp.int32(last - 1))
    bprev, blast = block_id(kprev, qprev), block_id(klast, qlast)
    zcopy(last, 1).start()
    zcopy(last, 0).wait()
    zload(1, zb, 0).start()
    keep_stats(bprev)
    for r in range(32):
        lane_stats(la, 1, r * 8)
    send_stats(bprev)
    for part in PAIR:
        row_stats(part)
    keep_stats(blast)
    zcopy(last, 1).wait()
    zload(1, zb, 1).start()
    send_stats(blast)
    second_kind, second_q = order2(jnp.int32(1))
    second_blk = block_id(second_kind, second_q)
    stats_arrived(second_blk)
    loss_acc[...] += combine(second_blk)
    for part in PAIR:
        columns(second_blk, 1, part)

    def tile(ref, q, n):
        return ref.at[pl.ds(pl.multiple_of(q * LANE, LANE), LANE), pl.ds(pl.multiple_of(n * HALF, HALF), HALF)]

    def spair(k, n):
        return _send(
            pbuf.at[n, pl.ds(pl.multiple_of(oc * LANE, LANE), LANE)], rbuf.at[_rem(k + 2, 2), n], ps.at[n], rr.at[_rem(k + 2, 2) * 2 + n], partner
        )

    def sstore_start(k, n):
        kind, q = order2(k)
        sem = ss_sem.at[n]

        @pl.when(kind == 3)
        def _():
            _copy(sbuf.at[n], tile(s_d, q, n), sem).start()

        @pl.when((kind == n1kind) & (q < 2))
        def _():
            _copy(sbuf.at[n], tile(s_n1a, _rem(q, 2), n), sem).start()

        @pl.when((kind == n1kind) & (q >= 2))
        def _():
            _copy(sbuf.at[n], tile(s_n1b, _rem(q, 2), n), sem).start()

        @pl.when(kind == 3 - n1kind)
        def _():
            _copy(sbuf.at[n], tile(s_n2, q, n), sem).start()

        @pl.when(kind == 0)
        def _():
            _copy(sbuf.at[n], tile(s_self, q, n), sem).start()

    def sstore_done(k, n):
        kind, q = order2(k)
        _copy(sbuf.at[n], tile(s_d, 0, n), ss_sem.at[n]).wait()

        @pl.when(kind == 3)
        def _():
            _send(tile(s_d, q, n), tile(r1n2, q, n), s1tx, r1s.at[q * 2 + n], n1).start()

        @pl.when((kind == n1kind) & (q < 2))
        def _():
            _send(tile(s_n1a, _rem(q, 2), n), tile(r1a, _rem(q, 2), n), s1tx, r1as.at[_rem(q, 2) * 2 + n], n1).start()

    def stage2_load(q, n):
        _copy(tile(r1n2, q, n), tile(r1n2, q, n), r1s.at[q * 2 + n]).wait()
        _copy(tile(s_n2, q, n), ab.at[n], ab_sem.at[n * 2]).start()
        _copy(tile(r1n2, q, n), bb.at[n], ab_sem.at[n * 2 + 1]).start()

    def pair_sum(k, n, r):
        sbuf[n, pl.ds(r, SUB), :] = pbuf[n, pl.ds(pl.multiple_of(c * LANE + r, SUB), SUB), :] + rbuf[_rem(k + 2, 2), n, pl.ds(r, SUB), :]

    def stage2_sum(n, r):
        cb[n, pl.ds(r, SUB), :] = ab[n, pl.ds(r, SUB), :] + bb[n, pl.ds(r, SUB), :]

    def rwait(k, n):
        _copy(rbuf.at[_rem(k + 2, 2), n], rbuf.at[_rem(k + 2, 2), n], rr.at[_rem(k + 2, 2) * 2 + n]).wait()

    def loss_part(k, blk):
        loss_acc[...] += jnp.where(k < NBLK - 2, combine(blk), 0.0)

    def sub(k, cur):
        nxt = 1 - cur
        kind2, q2 = order2(_rem(k + 2, NBLK))
        blk2 = block_id(kind2, q2)

        def trip(n):
            @pl.when(k < NBLK - 1)
            def _():
                zload(k + 1, zb, n).wait()

            @pl.when(k >= 1)
            def _():
                rwait(k - 1, n)
                spair(k - 1, n).wait_send()
                if n == 0:
                    gstore(k - 1, nxt).wait()

            if n == 0:

                @pl.when(k < NBLK - 2)
                def _():
                    stats_arrived(blk2)

            @pl.when(k >= 12)
            def _():
                _copy(tile(s_n2, 0, n), ab.at[n], ab_sem.at[n * 2]).wait()
                _copy(tile(r1n2, 0, n), bb.at[n], ab_sem.at[n * 2 + 1]).wait()

            @pl.when(k >= 13)
            def _():
                _copy(cb.at[n], tile(y2, 0, n), cb_sem.at[n]).wait()

            jobs = [[] for _ in range(32)]
            for r in range(8):
                jobs[2 + r * 3 // 5].append(functools.partial(pair_sum, k - 1, n, r * SUB))
                jobs[10 + r * 5 // 2].append(functools.partial(stage2_sum, n, r * SUB))
            for r, job in enumerate(gradient_jobs(zb, n, nxt)):
                jobs[2 + r * 9 // 20].append(job)
            if n == 0:
                jobs[8].append(lambda: loss_part(k, blk2))
            else:
                for part in PAIR:
                    jobs[8 + 8 * part].append(functools.partial(columns, blk2, cur, part))

            def put(nt, acc):
                pbuf[n, :, nt * PIECE : (nt + 1) * PIECE] = acc

            _product(
                lambda kt: gbufs[cur][:, kt * PIECE : (kt + 1) * PIECE],
                lambda nt, kt: wv[pl.ds(pl.multiple_of(n * HALF + nt * PIECE, PIECE), PIECE), kt * PIECE : (kt + 1) * PIECE],
                put,
                jobs,
                True,
            )

            spair(k, n).start()

            @pl.when(k < NBLK - 2)
            def _():
                zload(k + 2, zb, n).start()

            @pl.when(k >= 2)
            def _():
                sstore_done(k - 2 + n, 1 - n)

            @pl.when(k >= 1)
            def _():
                sstore_start(k - 1, n)

            if n == 0:
                @pl.when(k == 1)
                def _():
                    sstore_done(k - 1, n)

            @pl.when(k >= 12)
            def _():
                _copy(cb.at[n], tile(y2, k - 12, n), cb_sem.at[n]).start()

            @pl.when((k >= 11) & (k < NBLK - 1))
            def _():
                stage2_load(k - 11, n)


        trip(0)
        trip(1)

        @pl.when(k < NBLK - 1)
        def _():
            gstore(k + 1, nxt).start()

    def pair(p, carry):
        sub(2 * p, 0)
        sub(2 * p + 1, 1)
        return carry

    lax.fori_loop(0, NBLK // 2, pair, 0)

    kl = jnp.int32(NBLK - 1)
    for n in PAIR:
        rwait(kl, n)
        spair(kl, n).wait_send()
        if n == 0:
            sstore_done(kl - 1, 1)
        for r in range(8):
            pair_sum(kl, n, r * SUB)
        sstore_start(kl, n)
    for n in PAIR:
        sstore_done(kl, n)
    gstore(kl, 1).wait()
    for n in PAIR:
        _copy(cb.at[n], tile(y2, 0, n), cb_sem.at[n]).wait()

    loss_out[...] = jnp.full(TILE, jnp.sum(loss_acc[...]) * INV, F32)

    for i in FOUR:
        _copy(tile(r1a, i // 2, i % 2), tile(r1a, i // 2, i % 2), r1as.at[i]).wait()
    _copy(s_d, s_d, s1tx).wait()
    _copy(s_n1a, s_n1a, s1tx).wait()
    _copy(xall.at[pl.ds(0, 28 * LANE)], xall.at[pl.ds(0, 28 * LANE)], tx).wait()
    for d in range(7):
        _copy(lab_v.at[d], lab_v.at[d], labtx_sem).wait()
        _copy(st_loc, st_loc, sttx_sem).wait()


def xrows_at(xall, dev, q):
    return xall.at[pl.ds(pl.multiple_of((dev // 2) * 1024 + q * BLK + (dev % 2) * LANE, LANE), LANE)]


def _head(hid, lab, w):
    hbm = pl.BlockSpec(memory_space=ANY)
    sd = jax.ShapeDtypeStruct
    dma = pltpu.SemaphoreType.DMA
    vmem = pltpu.VMEM
    quarter = (LANE, HALF)
    return pl.pallas_call(
        _head_kernel,
        out_shape=(
            sd((TOK, HID), BF16),
            sd((TOK, VOC), BF16),
            sd((256, HID), F32),
            sd((PIECE, HID), F32),
            sd((PIECE, HID), F32),
            sd((256, HID), F32),
            sd(TILE, F32),
            sd((NBLK, 2, BLK, HALF), F32),
            sd((PIECE, HID), F32),
            sd((256, HID), F32),
            sd((PIECE, HID), F32),
            sd((PIECE, HID), F32),
        ),
        in_specs=[hbm] * 3,
        out_specs=(hbm,) * 6 + (pl.BlockSpec(memory_space=vmem),) + (hbm,) * 5,
        scratch_shapes=[
            vmem((HID, VOC), BF16),
            vmem((2, BLK, HID), BF16),
            vmem((BLK, VOC), BF16),
            vmem((BLK, VOC), BF16),
            vmem((2, BLK, HALF), F32),
            vmem((2, BLK, HALF), F32),
            vmem((2, 2) + quarter, F32),
            vmem(TWO + quarter, F32),
            vmem(TWO + quarter, F32),
            vmem(TWO + quarter, F32),
            vmem(TWO + quarter, F32),
            vmem((8, 4, LANE), I32),
            vmem((BLK, LANE), I32),
            vmem((BLK, LANE), I32),
            vmem(TILE, F32),
            vmem((NBLK,) + TILE, F32),
            vmem((NBLK, 8) + TILE, F32),
            vmem((2, BLK, LANE), F32),
            vmem((2, BLK, LANE), F32),
            vmem((2, BLK, LANE), F32),
            vmem((2, BLK, LANE), F32),
            vmem(TILE, F32),
            vmem((2, BLK, LANE), I32),
            vmem((2, BLK, LANE), F32),
            vmem((2, BLK, LANE), F32),
            vmem((2, LANE), F32),
            dma((8,)),
            dma(()),
            dma(()),
            dma((32,)),
            dma(()),
            dma(TWO),
            dma(TWO),
            dma(TWO),
            dma((NBLK,)),
            dma(()),
            dma(TWO),
            dma((4,)),
            dma(TWO),
            dma(TWO),
            dma(()),
            dma((8,)),
            dma((4,)),
            dma((4,)),
            dma(TWO),
            dma(TWO),
        ],
        compiler_params=pltpu.CompilerParams(collective_id=0, has_side_effects=True, vmem_limit_bytes=67_043_328),
        cost_estimate=pl.CostEstimate(flops=4 * TOK * HID * VOC, bytes_accessed=400 * MIB, transcendentals=2 * TOK * VOC),
        name="head",
    )(hid, lab, w)


def _dhead_kernel(x_hbm, g_hbm, o_hbm, gv, xb, ob, x_sem, g_sem, o_sem):
    rows = HID // PIECE

    def xload(b):
        return _copy(x_hbm.at[:, pl.ds(pl.multiple_of(b * PIECE, PIECE), PIECE)], xb.at[b % 2], x_sem.at[b % 2])

    def gload(j):
        cols = pl.ds(pl.multiple_of(j * PIECE, PIECE), PIECE)
        return _copy(g_hbm.at[:, cols], gv.at[:, cols], g_sem.at[j])

    def ostore(b, n):
        dst = o_hbm.at[pl.ds(pl.multiple_of(b * PIECE, PIECE), PIECE), pl.ds(pl.multiple_of(n * HALF, HALF), HALF)]
        return _copy(ob.at[n], dst, o_sem.at[n])

    def dot(lhs, rhs):
        return lax.dot_general(lhs, rhs, (((0,), (0,)), ((), ())), preferred_element_type=F32).astype(BF16)

    xload(0).start()
    gload(0).start()
    xload(0).wait()
    gload(1).start()

    def first(j, carry):
        gload(j).wait()

        @pl.when(j < 6)
        def _():
            gload(j + 2).start()

        @pl.when(j == 6)
        def _():
            xload(1).start()

        cols = pl.ds(pl.multiple_of(j % 4 * PIECE, PIECE), PIECE)
        ob[j // 4, :, cols] = dot(xb[0], gv[:, pl.ds(pl.multiple_of(j * PIECE, PIECE), PIECE)])

        @pl.when(j == 3)
        def _():
            ostore(0, 0).start()

        return carry

    lax.fori_loop(0, 8, first, 0)
    ostore(0, 1).start()

    def block(b, carry):
        xload(b).wait()

        @pl.when(b < rows - 1)
        def _():
            xload(b + 1).start()

        def half(n, carry):
            ostore(b - 1, n).wait()

            @pl.when(b < rows)
            def _():
                ob[n] = dot(xb[b % 2], gv[:, pl.ds(pl.multiple_of(n * HALF, HALF), HALF)])

            ostore(b, n).start()
            return carry

        return lax.fori_loop(0, 2, half, carry)

    lax.fori_loop(1, rows, block, 0)
    ostore(rows - 1, 0).wait()
    ostore(rows - 1, 1).wait()


def _dhead(xall, gall):
    hbm = pl.BlockSpec(memory_space=ANY)
    dma = pltpu.SemaphoreType.DMA
    return pl.pallas_call(
        _dhead_kernel,
        in_specs=[hbm, hbm],
        out_specs=hbm,
        out_shape=jax.ShapeDtypeStruct((HID, VOC), BF16),
        scratch_shapes=[
            pltpu.VMEM((TOK, VOC), BF16),
            pltpu.VMEM((2, TOK, PIECE), BF16),
            pltpu.VMEM((2, PIECE, HALF), BF16),
            dma(TWO),
            dma((8,)),
            dma(TWO),
        ],
        compiler_params=pltpu.CompilerParams(vmem_limit_bytes=60 * MIB),
        cost_estimate=pl.CostEstimate(flops=2 * TOK * HID * VOC, bytes_accessed=200 * MIB, transcendentals=0),
        name="dhead",
    )(xall, gall)


def _final_kernel(s_hbm, a_hbm, b_hbm, r_hbm, l_ref, o_hbm, loss_ref, terms, ov, in_sem, o_sem):
    rows = PIECE // SUB
    ahead = 6

    def chunk(ref, i):
        return ref.at[pl.ds(pl.multiple_of(i * rows, rows), rows)]

    def load(i):
        row = _rem(i, SUB // 2)
        _copy(chunk(s_hbm, i), chunk(terms.at[0], i), in_sem.at[0, i]).start()
        pl.when(i < SUB // 2)(lambda: _copy(chunk(a_hbm, row), chunk(terms.at[1], i), in_sem.at[1, i]).start())
        pl.when(i >= SUB // 2)(lambda: _copy(chunk(b_hbm, row), chunk(terms.at[1], i), in_sem.at[1, i]).start())
        _copy(chunk(r_hbm, i), chunk(terms.at[2], i), in_sem.at[2, i]).start()

    def first(i, carry):
        load(i)
        return carry

    lax.fori_loop(0, ahead, first, 0)
    loss_ref[0] = l_ref[0, 0]

    def add(i, carry):
        for t in range(3):
            _copy(chunk(s_hbm, i), chunk(terms.at[t], i), in_sem.at[t, i]).wait()
        pl.when(i < SUB - ahead)(lambda: load(i + ahead))
        rs = pl.ds(pl.multiple_of(i * rows, rows), rows)
        ov[rs, :] = (terms[0, rs, :] + terms[1, rs, :] + terms[2, rs, :]).astype(BF16)
        _copy(chunk(ov, i), chunk(o_hbm, i), o_sem).start()
        return carry

    lax.fori_loop(0, SUB, add, 0)
    _copy(ov, o_hbm, o_sem).wait()


def _final(s_self, r1a, r1b, r2, loss):
    hbm = pl.BlockSpec(memory_space=ANY)
    dma = pltpu.SemaphoreType.DMA
    return pl.pallas_call(
        _final_kernel,
        in_specs=[hbm] * 4 + [pl.BlockSpec(memory_space=pltpu.VMEM)],
        out_specs=(hbm, pl.BlockSpec(memory_space=pltpu.SMEM)),
        out_shape=(jax.ShapeDtypeStruct((PIECE, HID), BF16), jax.ShapeDtypeStruct((1,), F32)),
        scratch_shapes=[
            pltpu.VMEM((3, PIECE, HID), F32),
            pltpu.VMEM((PIECE, HID), BF16),
            dma((3, SUB)),
            dma(()),
        ],
        compiler_params=pltpu.CompilerParams(vmem_limit_bytes=62 * MIB),
        cost_estimate=pl.CostEstimate(flops=3 * PIECE * HID, bytes_accessed=28 * MIB, transcendentals=0),
        name="final",
    )(s_self, r1a, r1b, r2, loss)


def solution(mesh):
    def device(y, x, core):
        return (y % 2) * 4 + (x % 2) * 2 + core

    first, second = [], []
    for yy in PAIR:
        for xx in PAIR:
            along_x = [(device(yy, xx, k), device(yy, xx + 1, k)) for k in PAIR]
            along_y = [(device(yy, xx, k), device(yy + 1, xx, k)) for k in PAIR]
            first += [along_x[0], along_y[1]]
            second += [along_y[0], along_x[1]]

    def local_step(hid, w, lab):
        xall, gall, s_n1b, s_self, y2, r1a, loss = _head(hid, lab.reshape(4, LANE), w)[:7]
        r1b = lax.ppermute(s_n1b, "tp", first)
        r2 = lax.ppermute(y2, "tp", second)
        d_head = _dhead(xall, gall)
        d_hidden, mean_loss = _final(s_self, r1a, r1b, r2, loss)
        return mean_loss, d_hidden, d_head

    return jax.shard_map(
        local_step,
        mesh=mesh,
        in_specs=(P(("dp", "tp"), None), P(None, "tp"), P(("dp", "tp"))),
        out_specs=(P("dp"), P(("dp", "tp"), None), P("dp", "tp")),
        check_vma=False,
    )
```

```python
import functools

import jax
import jax.numpy as jnp
from jax import lax
from jax.experimental import pallas as pl
from jax.experimental.pallas import tpu as pltpu
from jax.sharding import PartitionSpec as P

F32, BF16, I32 = jnp.float32, jnp.bfloat16, jnp.int32
MESH = pl.DeviceIdType.MESH
ANY = pl.ANY

TOK = 4096
HID = 4096
VOC = 4096
BLK = 256
HALF = 2048
NBLK = TOK // BLK
LANE = 128
MIB = 1 << 20
TWO = (2,)
PAIR = (0, 1)
TILE = (8, LANE)
SUB = 16
FOUR = range(4)
OTHERS = range(1, 8)
SEVEN = pl.ds(0, 7)
LATE = 9
PIECE = 512
INV = 1.0 / TOK


def _div(a, b):
    return lax.div(jnp.int32(a), jnp.int32(b))


def _rem(a, b):
    return lax.rem(jnp.int32(a), jnp.int32(b))


def _loop(count, body):
    lax.fori_loop(0, count, body, 0)


def _copy(src, dst, sem):
    return pltpu.make_async_copy(src, dst, sem)


def _send(src, dst, send_sem, recv_sem, dev):
    return pltpu.make_async_remote_copy(
        src_ref=src, dst_ref=dst, send_sem=send_sem, recv_sem=recv_sem, device_id={"tp": dev}, device_id_type=MESH
    )


def _product(lhs, rhs, put, jobs, transposed):
    pl.when(lax.axis_index("tp") < 8)(functools.partial(_pieces, lhs, rhs, put, jobs, transposed))


def _pieces(lhs, rhs, put, jobs, transposed):
    dims = (((1,), (1,)), ((), ())) if transposed else (((1,), (0,)), ((), ()))
    pieces = HALF // PIECE
    deep = 8
    for nt in range(pieces):
        acc = None
        for kt in range(deep):
            part = lax.dot_general(lhs(kt), rhs(nt, kt), dims, preferred_element_type=F32)
            acc = part if acc is None else acc + part
            for job in jobs[nt * deep + kt]:
                job()
        put(nt, acc)


def _wide(v, times=HALF // LANE):
    return jnp.concatenate([v] * times, axis=1)


def _fold(v):
    width = v.shape[1] // 2
    while width >= LANE:
        v = v[:, :width] + v[:, width:]
        width //= 2
    return v


def _column(row):
    return jnp.transpose(jnp.broadcast_to(row, (LANE, LANE)))


def _head_kernel(
    x_hbm, lab_hbm, w_hbm,
    xall, gall, s_n1b, s_self, y2, r1a, loss_out,
    zst, s_d, s_n1a, s_n2, r1n2,
    wv, xg, ga, gb, zb, pbuf, rbuf, sbuf, ab, bb, cb, lab_v, la, lb, st_new, st_loc, st_all, ml, mk, sl, tl, comb, c_lab, c_top, c_scale, loss_acc,
    w_sem, lab_sem, labtx_sem, rx, tx, xl_sem, xs_sem, zo_sem, st_sem, sttx_sem,
    zi_sem, rr, ps, ss_sem, s1tx, r1s, r1as, ab_sem, cb_sem, g_sem,
):
    me = lax.axis_index("tp")
    chip = _div(me, 2)
    c = _rem(me, 2)
    x = _rem(chip, 2)
    y = _div(chip, 2)
    oc = 1 - c
    partner = me + 1 - 2 * c
    dx, dy = 2 - 4 * x, 4 - 8 * y
    n1 = me + oc * dx + c * dy
    n2 = me + c * dx + oc * dy
    n1kind = 1 + c

    def chip_of(kind):
        return chip + _rem(kind, 2) * (1 - 2 * x) + _div(kind, 2) * (2 - 4 * y)

    def order(i, first, last):
        a = _div(i, 4)
        mid, end = _rem(_div(a + 1, 2), 2), _div(a, 3)
        kind = mid * (1 + _rem(i, 2)) + first * (1 - mid) * (1 - end) + last * end
        return kind, mid * _div(i - 4, 2) + (1 - mid) * _rem(i, 4)

    def order1(i):
        return order(i, 0, 3)

    def order2(i):
        return order(i, 3, 0)

    def block_id(kind, q):
        return chip_of(kind) * 4 + q

    def xrows(kind, q, part):
        return xall.at[pl.ds(pl.multiple_of(block_id(kind, q) * BLK + part * LANE, LANE), LANE)]

    def xblock(kind, q):
        return xall.at[pl.ds(pl.multiple_of(block_id(kind, q) * BLK, BLK), BLK)]

    def own(q):
        return x_hbm.at[pl.ds(pl.multiple_of(q * LANE, LANE), LANE)]

    def rxs(kind, q, part):
        return rx.at[kind * 8 + q * 2 + part]

    def wcopy(j):
        cols = pl.ds(j * PIECE, PIECE)
        return _copy(w_hbm.at[:, cols], wv.at[:, cols], w_sem.at[j])

    _copy(own(0), xg.at[0, pl.ds(pl.multiple_of(c * LANE, LANE), LANE)], xl_sem.at[0]).start()
    for j in FOUR:
        wcopy(j).start()

    barrier = pltpu.get_barrier_semaphore()
    for d in OTHERS:
        pl.semaphore_signal(barrier, inc=1, device_id={"tp": _rem(me + d, 8)}, device_id_type=MESH)
    pl.semaphore_wait(barrier, 7)

    for d in OTHERS:
        _send(lab_hbm, lab_v.at[me], labtx_sem, lab_sem, _rem(me + d, 8)).start()
    _copy(lab_hbm, lab_v.at[me], lab_sem).start()
    for q in FOUR:
        _send(own(q), xrows(0, q, c), tx, rxs(0, q, c), partner).start()
    for q in FOUR:
        _send(own(q), xrows_at(xall, me, q), tx, rxs(n1kind, q, c), n1).start()
        _send(own(q), xrows_at(xall, me, q), tx, rxs(3 - n1kind, q, c), n2).start()

    def load_x(b):
        kind, q = order1(b)
        slot = _rem(b, 2)

        @pl.when(kind == 0)
        def _():
            _copy(own(q), xg.at[slot, pl.ds(pl.multiple_of(c * LANE, LANE), LANE)], xl_sem.at[slot]).start()
            _copy(xrows(0, q, oc), xg.at[slot, pl.ds(pl.multiple_of(oc * LANE, LANE), LANE)], xl_sem.at[slot]).start()

        @pl.when(kind != 0)
        def _():
            _copy(xblock(kind, q), xg.at[slot], xl_sem.at[slot]).start()

    def wait_rows(kind, q, part):
        _copy(xrows(kind, q, part), xrows(kind, q, part), rxs(kind, q, part)).wait()

    def take_rows(kind, q):
        wait_rows(kind, q, c)
        _send(xrows(kind, q, c), xrows(kind, q, c), tx, rxs(kind, q, c), partner).start()

        @pl.when(kind == n1kind)
        def _():
            _send(xrows(kind, q, c), xrows(kind, q, c), tx, rxs(3, q, c), n2).start()

    def part_load(b, part):
        kind, q = order1(b)
        return _copy(xrows(kind, q, part), xg.at[_rem(b, 2), pl.ds(pl.multiple_of(part * LANE, LANE), LANE)], xl_sem.at[_rem(b, 2)])

    def zcopy(b, h):
        kind, q = order1(b)
        return _copy(zb.at[h], zst.at[block_id(kind, q), h], zo_sem.at[h])

    def own_store(b):
        slot = _rem(b, 2)
        return _copy(xg.at[slot, pl.ds(pl.multiple_of(c * LANE, LANE), LANE)], xrows(0, _rem(b, 4), c), xs_sem.at[slot])

    def label_column(blk, part):
        return _column(lab_v[2 * _div(blk, 4) + part, pl.ds(_rem(blk, 4), 1), :])

    def lane_stats(col, h, r):
        rows = pl.ds(r, 8)
        z = zb[h, rows, :]
        m = ml[h, rows, :]
        hit = _wide(col[rows, :] - (me * VOC + h * HALF)) == lax.broadcasted_iota(I32, (8, HALF), 1)
        s = _fold(jnp.exp(z - _wide(m)))
        t = _fold(jnp.where(hit, z, 0.0))
        if h == 1:
            m0 = mk[0, rows, :]
            mm = jnp.maximum(m0, m)
            s = sl[0, rows, :] * jnp.exp(m0 - mm) + s * jnp.exp(m - mm)
            t = tl[0, rows, :] + t
            m = mm
        mk[h, rows, :] = m
        sl[h, rows, :] = s
        tl[h, rows, :] = t

    def label_columns(blk, col, part):
        col[pl.ds(part * LANE, LANE), :] = label_column(blk, part)

    def row_stats(part):
        rows = pl.ds(part * LANE, LANE)
        m = jnp.transpose(mk[1, rows, :])
        top = jnp.max(m, axis=0, keepdims=True)
        st_new[part : part + 1, :] = top
        st_new[2 + part : 3 + part, :] = jnp.sum(jnp.transpose(sl[1, rows, :]) * jnp.exp(m - top), axis=0, keepdims=True)
        st_new[4 + part : 5 + part, :] = jnp.sum(jnp.transpose(tl[1, rows, :]), axis=0, keepdims=True)

    def entry(kind, q):
        diagonal = _div(kind, 3)
        return diagonal * (NBLK + q) + (1 - diagonal) * block_id(kind, q)

    def send_stats(kind, q):
        def start(dev):
            _send(st_loc.at[block_id(kind, q)], st_all.at[NBLK + q, me], sttx_sem, st_sem.at[q], dev).start()

        for core in PAIR:
            dev = 2 * chip_of(3 - kind) + core
            pl.when(dev != me)(functools.partial(start, dev))

    def send_late():
        for d in OTHERS:
            _send(st_loc, st_all.at[pl.ds(0, NBLK), me], sttx_sem, st_sem.at[4], _rem(me + d, 8)).start()

    def keep_stats(kind, q):
        st_loc[block_id(kind, q)] = st_new[...]
        st_all[block_id(kind, q), me] = st_new[...]
        st_all[entry(kind, q), me] = st_new[...]

    def combine(place):
        top = st_all[place, 0, 0:2, :]
        for d in OTHERS:
            top = jnp.maximum(top, st_all[place, d, 0:2, :])
        s = jnp.zeros((2, LANE), F32)
        t = jnp.zeros((2, LANE), F32)
        for d in range(8):
            s = s + st_all[place, d, 2:4, :] * jnp.exp(st_all[place, d, 0:2, :] - top)
            t = t + st_all[place, d, 4:6, :]
        comb[0:2, :] = top
        comb[2:4, :] = INV / s
        return top + jnp.log(s) - t

    def stats_arrived(q):
        _copy(st_all.at[0, SEVEN], st_all.at[0, SEVEN], st_sem.at[q]).wait()

    def late_arrived():
        _copy(st_all.at[pl.ds(0, 14)], st_all.at[pl.ds(0, 14)], st_sem.at[4]).wait()

    def columns(blk, par, part):
        rows = pl.ds(part * LANE, LANE)
        c_lab[par, rows, :] = label_column(blk, part)
        c_top[par, rows, :] = _column(comb[part : part + 1, :])
        c_scale[par, rows, :] = _column(comb[2 + part : 3 + part, :])

    def gradient(src, n, par, r, j):
        rows = pl.ds(pl.multiple_of(r, SUB), SUB)
        col = c_lab[par, rows, :] - (me * VOC + n * HALF + j)
        p = jnp.exp(src[n, rows, j : j + PIECE] - _wide(c_top[par, rows, :], 4)) * _wide(c_scale[par, rows, :], 4)
        g = jnp.where(_wide(col, 4) == lax.broadcasted_iota(I32, (SUB, PIECE), 1), p - INV, p)
        gbufs[par][rows, n * HALF + j : n * HALF + j + PIECE] = g.astype(BF16)

    def gradient_jobs(src, n, par):
        return [functools.partial(gradient, src, n, par, r, j) for r in range(0, BLK, SUB) for j in range(0, HALF, PIECE)]

    gbufs = (ga, gb)

    def gstore(k, par):
        kind, q = order2(k)
        return _copy(gbufs[par], gall.at[pl.ds(pl.multiple_of(block_id(kind, q) * BLK, BLK), BLK)], g_sem.at[par])

    def zload(k, dst, n):
        kind, q = order2(k)
        return _copy(zst.at[block_id(kind, q), n], dst.at[n], zi_sem.at[n])

    first_kind, first_q = order2(me * 0)
    first_blk = block_id(first_kind, first_q)

    def logits(b, h, jobs):
        slot = _rem(b, 2)
        def put(nt, z):
            zb[h, :, nt * PIECE : (nt + 1) * PIECE] = z
            m = z[:, :LANE]
            for j in range(1, 4):
                m = jnp.maximum(m, z[:, j * LANE : (j + 1) * LANE])
            if nt:
                m = jnp.maximum(m, ml[h])
            ml[h] = m

        _product(
            lambda kt: xg[slot, :, kt * PIECE : (kt + 1) * PIECE],
            lambda nt, kt: wv[kt * PIECE : (kt + 1) * PIECE, h * HALF + nt * PIECE : h * HALF + (nt + 1) * PIECE],
            put,
            jobs,
            False,
        )

    wait_rows(0, 0, oc)
    _copy(xrows(0, 0, oc), xg.at[0, pl.ds(pl.multiple_of(oc * LANE, LANE), LANE)], xl_sem.at[0]).start()
    _copy(lab_v, lab_v, lab_sem).wait()
    for j in FOUR:
        wcopy(j).wait()
    for j in range(4, 8):
        wcopy(j).start()

    def phase1(i, carry):
        slot = _rem(i, 2)
        kind, q = order1(i)
        kprev, qprev = order1(_rem(i + NBLK - 2, NBLK))
        kn, qn = order1(_rem(i + 1, NBLK))

        @pl.when((i == LATE + 1) | (i == NBLK - 1))
        def _():
            wait_rows(kind, q, oc)
            part_load(i, oc).start()

        @pl.when(i > 0)
        def _():
            zcopy(i - 1, 1).start()
            zcopy(i - 1, 0).wait()

        @pl.when(i > 1)
        def _():
            keep_stats(kprev, qprev)

        @pl.when(i == NBLK - 2)
        def _():
            zload(0, pbuf, 0).start()
            zload(0, pbuf, 1).start()

        @pl.when(i == NBLK - 1)
        def _():
            stats_arrived(0)
            loss_acc[...] = combine(entry(first_kind, first_q))
            for part in PAIR:
                columns(first_blk, 0, part)
            for n in PAIR:
                zload(0, pbuf, n).wait()

                def some(r, carry, n=n):
                    for j in range(0, HALF, PIECE):
                        gradient(pbuf, n, 0, r * SUB, j)
                    return carry

                _loop(SUB, some)

            gstore(0, 0).start()

        @pl.when((i >= 3) & (i != LATE) & (i < NBLK - 2))
        def _():
            take_rows(kn, qn)

        _copy(xg.at[slot], xg.at[slot], xl_sem.at[slot]).wait()

        @pl.when(i < 4)
        def _():
            own_store(i).start()

        jobs = [[] for _ in range(32)]
        for r in range(32):
            jobs[min(r + 1, 31)].append(functools.partial(lane_stats, la, 1, r * 8))
        for part in PAIR:
            jobs[4 + 4 * part].append(functools.partial(label_columns, block_id(kind, q), lb, part))
        logits(i, 0, jobs)

        zcopy(i, 0).start()

        @pl.when(i == 0)
        def _():
            for j in range(4, 8):
                wcopy(j).wait()

        @pl.when(i > 0)
        def _():
            zcopy(i - 1, 1).wait()

        @pl.when(i > 1)
        def _():
            send_stats(kprev, qprev)

        @pl.when((i == LATE) | (i == NBLK - 2))
        def _():
            take_rows(kn, qn)
            part_load(i + 1, c).start()

        @pl.when((i != LATE) & (i < NBLK - 2))
        def _():
            wait_rows(kn, qn, oc)

            @pl.when((i >= 1) & (i < 5))
            def _():
                own_store(i - 1).wait()

            load_x(i + 1)

        la[...] = lb[...]
        jobs = [[] for _ in range(32)]
        for r in range(32):
            jobs[min(r + 1, 31)].append(functools.partial(lane_stats, lb, 0, r * 8))
        for part in PAIR:
            jobs[8 + 8 * part].append(functools.partial(row_stats, part))
        logits(i, 1, jobs)
        return carry

    _loop(NBLK, phase1)
    last = NBLK - 1
    klast, qlast = order1(jnp.int32(last))
    kprev, qprev = order1(jnp.int32(last - 1))
    zcopy(last, 1).start()
    zcopy(last, 0).wait()
    zload(1, zb, 0).start()
    keep_stats(kprev, qprev)
    for r in range(32):
        lane_stats(la, 1, r * 8)
    send_stats(kprev, qprev)
    for part in PAIR:
        row_stats(part)
    keep_stats(klast, qlast)
    zcopy(last, 1).wait()
    zload(1, zb, 1).start()
    send_stats(klast, qlast)
    second_kind, second_q = order2(jnp.int32(1))
    second_blk = block_id(second_kind, second_q)
    stats_arrived(1)
    loss_acc[...] += combine(entry(second_kind, second_q))
    for part in PAIR:
        columns(second_blk, 1, part)

    def tile(ref, q, n):
        return ref.at[pl.ds(pl.multiple_of(q * LANE, LANE), LANE), pl.ds(pl.multiple_of(n * HALF, HALF), HALF)]

    def spair(k, n):
        return _send(
            pbuf.at[n, pl.ds(pl.multiple_of(oc * LANE, LANE), LANE)], rbuf.at[_rem(k + 2, 2), n], ps.at[n], rr.at[_rem(k + 2, 2) * 2 + n], partner
        )

    def sstore_start(k, n):
        kind, q = order2(k)
        sem = ss_sem.at[n]

        @pl.when(kind == 3)
        def _():
            _copy(sbuf.at[n], tile(s_d, q, n), sem).start()

        @pl.when((kind == n1kind) & (q < 2))
        def _():
            _copy(sbuf.at[n], tile(s_n1a, _rem(q, 2), n), sem).start()

        @pl.when((kind == n1kind) & (q >= 2))
        def _():
            _copy(sbuf.at[n], tile(s_n1b, _rem(q, 2), n), sem).start()

        @pl.when(kind == 3 - n1kind)
        def _():
            _copy(sbuf.at[n], tile(s_n2, q, n), sem).start()

        @pl.when(kind == 0)
        def _():
            _copy(sbuf.at[n], tile(s_self, q, n), sem).start()

    def sstore_done(k, n):
        kind, q = order2(k)
        _copy(sbuf.at[n], tile(s_d, 0, n), ss_sem.at[n]).wait()

        @pl.when(kind == 3)
        def _():
            _send(tile(s_d, q, n), tile(r1n2, q, n), s1tx, r1s.at[q * 2 + n], n1).start()

        @pl.when((kind == n1kind) & (q < 2))
        def _():
            _send(tile(s_n1a, _rem(q, 2), n), tile(r1a, _rem(q, 2), n), s1tx, r1as.at[_rem(q, 2) * 2 + n], n1).start()

    def stage2_load(q, n):
        _copy(tile(r1n2, q, n), tile(r1n2, q, n), r1s.at[q * 2 + n]).wait()
        _copy(tile(s_n2, q, n), ab.at[n], ab_sem.at[n * 2]).start()
        _copy(tile(r1n2, q, n), bb.at[n], ab_sem.at[n * 2 + 1]).start()

    def pair_sum(k, n, r):
        sbuf[n, pl.ds(r, SUB), :] = pbuf[n, pl.ds(pl.multiple_of(c * LANE + r, SUB), SUB), :] + rbuf[_rem(k + 2, 2), n, pl.ds(r, SUB), :]

    def stage2_sum(n, r):
        cb[n, pl.ds(r, SUB), :] = ab[n, pl.ds(r, SUB), :] + bb[n, pl.ds(r, SUB), :]

    def rwait(k, n):
        _copy(rbuf.at[_rem(k + 2, 2), n], rbuf.at[_rem(k + 2, 2), n], rr.at[_rem(k + 2, 2) * 2 + n]).wait()

    def loss_part(k, place):
        loss_acc[...] += jnp.where(k < NBLK - 2, combine(place), 0.0)

    def sub(k, cur):
        nxt = 1 - cur
        kind2, q2 = order2(_rem(k + 2, NBLK))
        blk2 = block_id(kind2, q2)

        def trip(n):
            @pl.when(k < NBLK - 1)
            def _():
                zload(k + 1, zb, n).wait()

            @pl.when(k >= 1)
            def _():
                rwait(k - 1, n)
                spair(k - 1, n).wait_send()
                if n == 0:
                    gstore(k - 1, nxt).wait()

            if n == 0:

                @pl.when(k < 2)
                def _():
                    stats_arrived(k + 2)

                @pl.when(k == 2)
                def _():
                    late_arrived()

            @pl.when(k >= 12)
            def _():
                _copy(tile(s_n2, 0, n), ab.at[n], ab_sem.at[n * 2]).wait()
                _copy(tile(r1n2, 0, n), bb.at[n], ab_sem.at[n * 2 + 1]).wait()

            @pl.when(k >= 13)
            def _():
                _copy(cb.at[n], tile(y2, 0, n), cb_sem.at[n]).wait()

            jobs = [[] for _ in range(32)]
            for r in range(8):
                jobs[2 + r * 3 // 5].append(functools.partial(pair_sum, k - 1, n, r * SUB))
                jobs[10 + r * 5 // 2].append(functools.partial(stage2_sum, n, r * SUB))
            for r, job in enumerate(gradient_jobs(zb, n, nxt)):
                jobs[2 + r * 9 // 20].append(job)
            if n == 0:
                jobs[8].append(lambda: loss_part(k, entry(kind2, q2)))
            else:
                for part in PAIR:
                    jobs[8 + 8 * part].append(functools.partial(columns, blk2, cur, part))

            def put(nt, acc):
                pbuf[n, :, nt * PIECE : (nt + 1) * PIECE] = acc

            _product(
                lambda kt: gbufs[cur][:, kt * PIECE : (kt + 1) * PIECE],
                lambda nt, kt: wv[pl.ds(pl.multiple_of(n * HALF + nt * PIECE, PIECE), PIECE), kt * PIECE : (kt + 1) * PIECE],
                put,
                jobs,
                True,
            )

            spair(k, n).start()

            if cur == n == 0:
                pl.when(k == 0)(send_late)

            @pl.when(k < NBLK - 2)
            def _():
                zload(k + 2, zb, n).start()

            @pl.when(k >= 2)
            def _():
                sstore_done(k - 2 + n, 1 - n)

            @pl.when(k >= 1)
            def _():
                sstore_start(k - 1, n)

            if n == 0:
                @pl.when(k == 1)
                def _():
                    sstore_done(k - 1, n)

            @pl.when(k >= 12)
            def _():
                _copy(cb.at[n], tile(y2, k - 12, n), cb_sem.at[n]).start()

            @pl.when((k >= 11) & (k < NBLK - 1))
            def _():
                stage2_load(k - 11, n)


        trip(0)
        trip(1)

        @pl.when(k < NBLK - 1)
        def _():
            gstore(k + 1, nxt).start()

    def pair(p, carry):
        sub(2 * p, 0)
        sub(2 * p + 1, 1)
        return carry

    _loop(NBLK // 2, pair)

    kl = jnp.int32(NBLK - 1)
    for n in PAIR:
        rwait(kl, n)
        spair(kl, n).wait_send()
        if n == 0:
            sstore_done(kl - 1, 1)
        for r in range(8):
            pair_sum(kl, n, r * SUB)
        sstore_start(kl, n)
    for n in PAIR:
        sstore_done(kl, n)
    gstore(kl, 1).wait()
    for n in PAIR:
        _copy(cb.at[n], tile(y2, 0, n), cb_sem.at[n]).wait()

    loss_out[...] = jnp.full(TILE, jnp.sum(loss_acc[...]) * INV, F32)

    for i in FOUR:
        _copy(tile(r1a, i // 2, i % 2), tile(r1a, i // 2, i % 2), r1as.at[i]).wait()
    _copy(s_d, s_d, s1tx).wait()
    _copy(s_n1a, s_n1a, s1tx).wait()
    _copy(xall.at[pl.ds(0, 28 * LANE)], xall.at[pl.ds(0, 28 * LANE)], tx).wait()
    for d in range(7):
        _copy(lab_v.at[d], lab_v.at[d], labtx_sem).wait()
        _copy(st_loc, st_loc, sttx_sem).wait()
    for d in FOUR:
        _copy(st_all.at[d, SEVEN], st_all.at[d, SEVEN], sttx_sem).wait()


def xrows_at(xall, dev, q):
    return xall.at[pl.ds(pl.multiple_of((dev // 2) * 1024 + q * BLK + (dev % 2) * LANE, LANE), LANE)]


def _head(hid, lab, w):
    hbm = pl.BlockSpec(memory_space=ANY)
    sd = jax.ShapeDtypeStruct
    dma = pltpu.SemaphoreType.DMA
    vmem = pltpu.VMEM
    quarter = (LANE, HALF)
    return pl.pallas_call(
        _head_kernel,
        out_shape=(
            sd((TOK, HID), BF16),
            sd((TOK, VOC), BF16),
            sd((256, HID), F32),
            sd((PIECE, HID), F32),
            sd((PIECE, HID), F32),
            sd((256, HID), F32),
            sd(TILE, F32),
            sd((NBLK, 2, BLK, HALF), F32),
            sd((PIECE, HID), F32),
            sd((256, HID), F32),
            sd((PIECE, HID), F32),
            sd((PIECE, HID), F32),
        ),
        in_specs=[hbm] * 3,
        out_specs=(hbm,) * 6 + (pl.BlockSpec(memory_space=vmem),) + (hbm,) * 5,
        scratch_shapes=[
            vmem((HID, VOC), BF16),
            vmem((2, BLK, HID), BF16),
            vmem((BLK, VOC), BF16),
            vmem((BLK, VOC), BF16),
            vmem((2, BLK, HALF), F32),
            vmem((2, BLK, HALF), F32),
            vmem((2, 2) + quarter, F32),
            vmem(TWO + quarter, F32),
            vmem(TWO + quarter, F32),
            vmem(TWO + quarter, F32),
            vmem(TWO + quarter, F32),
            vmem((8, 4, LANE), I32),
            vmem((BLK, LANE), I32),
            vmem((BLK, LANE), I32),
            vmem(TILE, F32),
            vmem((NBLK,) + TILE, F32),
            vmem((NBLK + 4, 8) + TILE, F32),
            vmem((2, BLK, LANE), F32),
            vmem((2, BLK, LANE), F32),
            vmem((2, BLK, LANE), F32),
            vmem((2, BLK, LANE), F32),
            vmem(TILE, F32),
            vmem((2, BLK, LANE), I32),
            vmem((2, BLK, LANE), F32),
            vmem((2, BLK, LANE), F32),
            vmem((2, LANE), F32),
            dma((8,)),
            dma(()),
            dma(()),
            dma((32,)),
            dma(()),
            dma(TWO),
            dma(TWO),
            dma(TWO),
            dma((5,)),
            dma(()),
            dma(TWO),
            dma((4,)),
            dma(TWO),
            dma(TWO),
            dma(()),
            dma((8,)),
            dma((4,)),
            dma((4,)),
            dma(TWO),
            dma(TWO),
        ],
        compiler_params=pltpu.CompilerParams(collective_id=0, has_side_effects=True, vmem_limit_bytes=67_043_328),
        cost_estimate=pl.CostEstimate(flops=4 * TOK * HID * VOC, bytes_accessed=400 * MIB, transcendentals=2 * TOK * VOC),
        name="head",
    )(hid, lab, w)


def _dhead_kernel(x_hbm, g_hbm, o_hbm, gv, xb, ob, x_sem, g_sem, o_sem):
    rows = HID // PIECE

    def xload(b):
        return _copy(x_hbm.at[:, pl.ds(pl.multiple_of(b * PIECE, PIECE), PIECE)], xb.at[b % 2], x_sem.at[b % 2])

    def gload(j):
        cols = pl.ds(pl.multiple_of(j * PIECE, PIECE), PIECE)
        return _copy(g_hbm.at[:, cols], gv.at[:, cols], g_sem.at[j])

    def ostore(b, n):
        dst = o_hbm.at[pl.ds(pl.multiple_of(b * PIECE, PIECE), PIECE), pl.ds(pl.multiple_of(n * HALF, HALF), HALF)]
        return _copy(ob.at[n], dst, o_sem.at[n])

    def dot(lhs, rhs):
        return lax.dot_general(lhs, rhs, (((0,), (0,)), ((), ())), preferred_element_type=F32).astype(BF16)

    xload(0).start()
    gload(0).start()
    xload(0).wait()
    gload(1).start()

    def first(j, carry):
        gload(j).wait()

        @pl.when(j < 6)
        def _():
            gload(j + 2).start()

        @pl.when(j == 6)
        def _():
            xload(1).start()

        cols = pl.ds(pl.multiple_of(j % 4 * PIECE, PIECE), PIECE)
        ob[j // 4, :, cols] = dot(xb[0], gv[:, pl.ds(pl.multiple_of(j * PIECE, PIECE), PIECE)])

        @pl.when(j == 3)
        def _():
            ostore(0, 0).start()

        return carry

    _loop(8, first)
    ostore(0, 1).start()

    def block(b, carry):
        xload(b).wait()

        @pl.when(b < rows - 1)
        def _():
            xload(b + 1).start()

        def half(n, carry):
            ostore(b - 1, n).wait()

            @pl.when(b < rows)
            def _():
                ob[n] = dot(xb[b % 2], gv[:, pl.ds(pl.multiple_of(n * HALF, HALF), HALF)])

            ostore(b, n).start()
            return carry

        return lax.fori_loop(0, 2, half, carry)

    lax.fori_loop(1, rows, block, 0)
    ostore(rows - 1, 0).wait()
    ostore(rows - 1, 1).wait()


def _dhead(xall, gall):
    hbm = pl.BlockSpec(memory_space=ANY)
    dma = pltpu.SemaphoreType.DMA
    return pl.pallas_call(
        _dhead_kernel,
        in_specs=[hbm, hbm],
        out_specs=hbm,
        out_shape=jax.ShapeDtypeStruct((HID, VOC), BF16),
        scratch_shapes=[
            pltpu.VMEM((TOK, VOC), BF16),
            pltpu.VMEM((2, TOK, PIECE), BF16),
            pltpu.VMEM((2, PIECE, HALF), BF16),
            dma(TWO),
            dma((8,)),
            dma(TWO),
        ],
        compiler_params=pltpu.CompilerParams(vmem_limit_bytes=60 * MIB),
        cost_estimate=pl.CostEstimate(flops=2 * TOK * HID * VOC, bytes_accessed=200 * MIB, transcendentals=0),
        name="dhead",
    )(xall, gall)


def _final_kernel(s_hbm, a_hbm, b_hbm, r_hbm, l_ref, o_hbm, loss_ref, terms, ov, in_sem, o_sem):
    rows = PIECE // SUB
    ahead = 6

    def chunk(ref, i):
        return ref.at[pl.ds(pl.multiple_of(i * rows, rows), rows)]

    def load(i):
        row = _rem(i, SUB // 2)
        _copy(chunk(s_hbm, i), chunk(terms.at[0], i), in_sem.at[0, i]).start()
        pl.when(i < SUB // 2)(lambda: _copy(chunk(a_hbm, row), chunk(terms.at[1], i), in_sem.at[1, i]).start())
        pl.when(i >= SUB // 2)(lambda: _copy(chunk(b_hbm, row), chunk(terms.at[1], i), in_sem.at[1, i]).start())
        _copy(chunk(r_hbm, i), chunk(terms.at[2], i), in_sem.at[2, i]).start()

    def first(i, carry):
        load(i)
        return carry

    _loop(ahead, first)
    loss_ref[0] = l_ref[0, 0]

    def add(i, carry):
        for t in range(3):
            _copy(chunk(s_hbm, i), chunk(terms.at[t], i), in_sem.at[t, i]).wait()
        pl.when(i < SUB - ahead)(lambda: load(i + ahead))
        rs = pl.ds(pl.multiple_of(i * rows, rows), rows)
        ov[rs, :] = (terms[0, rs, :] + terms[1, rs, :] + terms[2, rs, :]).astype(BF16)
        _copy(chunk(ov, i), chunk(o_hbm, i), o_sem).start()
        return carry

    _loop(SUB, add)
    _copy(ov, o_hbm, o_sem).wait()


def _final(s_self, r1a, r1b, r2, loss):
    hbm = pl.BlockSpec(memory_space=ANY)
    dma = pltpu.SemaphoreType.DMA
    return pl.pallas_call(
        _final_kernel,
        in_specs=[hbm] * 4 + [pl.BlockSpec(memory_space=pltpu.VMEM)],
        out_specs=(hbm, pl.BlockSpec(memory_space=pltpu.SMEM)),
        out_shape=(jax.ShapeDtypeStruct((PIECE, HID), BF16), jax.ShapeDtypeStruct((1,), F32)),
        scratch_shapes=[
            pltpu.VMEM((3, PIECE, HID), F32),
            pltpu.VMEM((PIECE, HID), BF16),
            dma((3, SUB)),
            dma(()),
        ],
        compiler_params=pltpu.CompilerParams(vmem_limit_bytes=62 * MIB),
        cost_estimate=pl.CostEstimate(flops=3 * PIECE * HID, bytes_accessed=28 * MIB, transcendentals=0),
        name="final",
    )(s_self, r1a, r1b, r2, loss)


def solution(mesh):
    def device(y, x, core):
        return (y % 2) * 4 + (x % 2) * 2 + core

    first, second = [], []
    for yy in PAIR:
        for xx in PAIR:
            along_x = [(device(yy, xx, k), device(yy, xx + 1, k)) for k in PAIR]
            along_y = [(device(yy, xx, k), device(yy + 1, xx, k)) for k in PAIR]
            first += [along_x[0], along_y[1]]
            second += [along_y[0], along_x[1]]

    def local_step(hid, w, lab):
        xall, gall, s_n1b, s_self, y2, r1a, loss = _head(hid, lab.reshape(4, LANE), w)[:7]
        r1b = lax.ppermute(s_n1b, "tp", first)
        r2 = lax.ppermute(y2, "tp", second)
        d_head = _dhead(xall, gall)
        d_hidden, mean_loss = _final(s_self, r1a, r1b, r2, loss)
        return mean_loss, d_hidden, d_head

    return jax.shard_map(
        local_step,
        mesh=mesh,
        in_specs=(P(("dp", "tp"), None), P(None, "tp"), P(("dp", "tp"))),
        out_specs=(P("dp"), P(("dp", "tp"), None), P("dp", "tp")),
        check_vma=False,
    )
```

```python
import functools

import jax
import jax.numpy as jnp
from jax import lax
from jax.experimental import pallas as pl
from jax.experimental.pallas import tpu as pltpu
from jax.sharding import PartitionSpec as P

F32, BF16, I32 = jnp.float32, jnp.bfloat16, jnp.int32
MESH = pl.DeviceIdType.MESH
ANY = pl.ANY

TOK = 4096
HID = 4096
VOC = 4096
BLK = 256
HALF = 2048
NBLK = TOK // BLK
LANE = 128
MIB = 1 << 20
TWO = (2,)
PAIR = (0, 1)
TILE = (8, LANE)
SUB = 16
FOUR = range(4)
OTHERS = range(1, 8)
SEVEN = pl.ds(0, 7)
LATE = 9
PIECE = 512
INV = 1.0 / TOK


def _div(a, b):
    return lax.div(jnp.int32(a), jnp.int32(b))


def _rem(a, b):
    return lax.rem(jnp.int32(a), jnp.int32(b))


def _odd(a):
    return _rem(a, 2)


def _loop(count, body):
    lax.fori_loop(0, count, body, 0)


def _copy(src, dst, sem):
    return pltpu.make_async_copy(src, dst, sem)


def _send(src, dst, send_sem, recv_sem, dev):
    return pltpu.make_async_remote_copy(
        src_ref=src, dst_ref=dst, send_sem=send_sem, recv_sem=recv_sem, device_id={"tp": dev}, device_id_type=MESH
    )


def _product(lhs, rhs, put, jobs, transposed):
    pl.when(lax.axis_index("tp") < 8)(functools.partial(_pieces, lhs, rhs, put, jobs, transposed))


def _pieces(lhs, rhs, put, jobs, transposed):
    dims = (((1,), (1,)), ((), ())) if transposed else (((1,), (0,)), ((), ()))
    pieces = HALF // PIECE
    deep = 8
    for nt in range(pieces):
        acc = None
        for kt in range(deep):
            part = lax.dot_general(lhs(kt), rhs(nt, kt), dims, preferred_element_type=F32)
            acc = part if acc is None else acc + part
            for job in jobs[nt * deep + kt]:
                job()
        put(nt, acc)


def _wide(v, times=HALF // LANE):
    return jnp.concatenate([v] * times, axis=1)


def _fold(v):
    width = v.shape[1] // 2
    while width >= LANE:
        v = v[:, :width] + v[:, width:]
        width //= 2
    return v


def _column(row):
    return jnp.transpose(jnp.broadcast_to(row, (LANE, LANE)))


def _head_kernel(
    x_hbm, lab_hbm, w_hbm,
    xall, gall, s_n1b, s_self, y2, r1a, loss_out,
    zst, s_d, s_n1a, s_n2, r1n2,
    wv, xg, ga, gb, zb, pbuf, rbuf, sbuf, ab, bb, cb, lab_v, la, lb, st_new, st_loc, st_all, ml, mk, sl, tl, comb, c_lab, c_top, c_scale, loss_acc,
    w_sem, lab_sem, labtx_sem, rx, tx, xl_sem, xs_sem, zo_sem, st_sem, sttx_sem,
    zi_sem, rr, ps, ss_sem, s1tx, r1s, r1as, ab_sem, cb_sem, g_sem,
):
    me = lax.axis_index("tp")
    chip = _div(me, 2)
    c = _odd(me)
    x = _odd(chip)
    y = _div(chip, 2)
    oc = 1 - c
    partner = me + 1 - 2 * c
    dx, dy = 2 - 4 * x, 4 - 8 * y
    n1 = me + oc * dx + c * dy
    n2 = me + c * dx + oc * dy
    n1kind = 1 + c

    def chip_of(kind):
        return chip + _odd(kind) * (1 - 2 * x) + _div(kind, 2) * (2 - 4 * y)

    def order(i, first, last):
        a = _div(i, 4)
        mid, end = _rem(_div(a + 1, 2), 2), _div(a, 3)
        kind = mid * (1 + _odd(i)) + first * (1 - mid) * (1 - end) + last * end
        return kind, mid * _div(i - 4, 2) + (1 - mid) * _rem(i, 4)

    def order1(i):
        return order(i, 0, 3)

    def order2(i):
        return order(i, 3, 0)

    def block_id(kind, q):
        return chip_of(kind) * 4 + q

    def xrows(kind, q, part):
        return xall.at[pl.ds(pl.multiple_of(block_id(kind, q) * BLK + part * LANE, LANE), LANE)]

    def xblock(kind, q):
        return xall.at[pl.ds(pl.multiple_of(block_id(kind, q) * BLK, BLK), BLK)]

    def own(q):
        return x_hbm.at[pl.ds(pl.multiple_of(q * LANE, LANE), LANE)]

    def rxs(kind, q, part):
        return rx.at[kind * 8 + q * 2 + part]

    def wcopy(j):
        cols = pl.ds(j * PIECE, PIECE)
        return _copy(w_hbm.at[:, cols], wv.at[:, cols], w_sem.at[j])

    _copy(own(0), xg.at[0, pl.ds(pl.multiple_of(c * LANE, LANE), LANE)], xl_sem.at[0]).start()
    for j in FOUR:
        wcopy(j).start()

    barrier = pltpu.get_barrier_semaphore()
    for d in OTHERS:
        pl.semaphore_signal(barrier, inc=1, device_id={"tp": _rem(me + d, 8)}, device_id_type=MESH)
    pl.semaphore_wait(barrier, 7)

    for d in OTHERS:
        _send(lab_hbm, lab_v.at[me], labtx_sem, lab_sem, _rem(me + d, 8)).start()
    _copy(lab_hbm, lab_v.at[me], lab_sem).start()
    for q in FOUR:
        _send(own(q), xrows(0, q, c), tx, rxs(0, q, c), partner).start()
    for q in FOUR:
        _send(own(q), xrows_at(xall, me, q), tx, rxs(n1kind, q, c), n1).start()
        _send(own(q), xrows_at(xall, me, q), tx, rxs(3 - n1kind, q, c), n2).start()

    def load_x(b):
        kind, q = order1(b)
        slot = _odd(b)

        @pl.when(kind == 0)
        def _():
            _copy(own(q), xg.at[slot, pl.ds(pl.multiple_of(c * LANE, LANE), LANE)], xl_sem.at[slot]).start()
            _copy(xrows(0, q, oc), xg.at[slot, pl.ds(pl.multiple_of(oc * LANE, LANE), LANE)], xl_sem.at[slot]).start()

        @pl.when(kind != 0)
        def _():
            _copy(xblock(kind, q), xg.at[slot], xl_sem.at[slot]).start()

    def wait_rows(kind, q, part):
        _copy(xrows(kind, q, part), xrows(kind, q, part), rxs(kind, q, part)).wait()

    def take_rows(kind, q):
        wait_rows(kind, q, c)
        _send(xrows(kind, q, c), xrows(kind, q, c), tx, rxs(kind, q, c), partner).start()

        @pl.when(kind == n1kind)
        def _():
            _send(xrows(kind, q, c), xrows(kind, q, c), tx, rxs(3, q, c), n2).start()

    def part_load(b, part):
        kind, q = order1(b)
        return _copy(xrows(kind, q, part), xg.at[_odd(b), pl.ds(pl.multiple_of(part * LANE, LANE), LANE)], xl_sem.at[_odd(b)])

    def zcopy(b, h):
        kind, q = order1(b)
        return _copy(zb.at[h], zst.at[block_id(kind, q), h], zo_sem.at[h])

    def own_store(b):
        slot = _odd(b)
        return _copy(xg.at[slot, pl.ds(pl.multiple_of(c * LANE, LANE), LANE)], xrows(0, _rem(b, 4), c), xs_sem.at[slot])

    def label_column(blk, part):
        return _column(lab_v[2 * _div(blk, 4) + part, pl.ds(_rem(blk, 4), 1), :])

    def lane_stats(col, h, r):
        rows = pl.ds(r, 8)
        z = zb[h, rows, :]
        m = ml[h, rows, :]
        hit = _wide(col[rows, :] - (me * VOC + h * HALF)) == lax.broadcasted_iota(I32, (8, HALF), 1)
        s = _fold(jnp.exp(z - _wide(m)))
        t = _fold(jnp.where(hit, z, 0.0))
        if h == 1:
            m0 = mk[0, rows, :]
            mm = jnp.maximum(m0, m)
            s = sl[0, rows, :] * jnp.exp(m0 - mm) + s * jnp.exp(m - mm)
            t = tl[0, rows, :] + t
            m = mm
        mk[h, rows, :] = m
        sl[h, rows, :] = s
        tl[h, rows, :] = t

    def label_columns(blk, col, part):
        col[pl.ds(part * LANE, LANE), :] = label_column(blk, part)

    def row_stats(part):
        rows = pl.ds(part * LANE, LANE)
        m = jnp.transpose(mk[1, rows, :])
        top = jnp.max(m, axis=0, keepdims=True)
        st_new[part : part + 1, :] = top
        st_new[2 + part : 3 + part, :] = jnp.sum(jnp.transpose(sl[1, rows, :]) * jnp.exp(m - top), axis=0, keepdims=True)
        st_new[4 + part : 5 + part, :] = jnp.sum(jnp.transpose(tl[1, rows, :]), axis=0, keepdims=True)

    def entry(kind, q):
        diagonal = _div(kind, 3)
        return diagonal * (NBLK + q) + (1 - diagonal) * block_id(kind, q)

    def send_stats(kind, q):
        def start(dev):
            _send(st_loc.at[block_id(kind, q)], st_all.at[NBLK + q, me], sttx_sem, st_sem.at[q], dev).start()

        for core in PAIR:
            dev = 2 * chip_of(3 - kind) + core
            pl.when(dev != me)(functools.partial(start, dev))

    def send_late():
        for d in OTHERS:
            _send(st_loc, st_all.at[pl.ds(0, NBLK), me], sttx_sem, st_sem.at[4], _rem(me + d, 8)).start()

    def keep_stats(kind, q):
        st_loc[block_id(kind, q)] = st_new[...]
        st_all[block_id(kind, q), me] = st_new[...]
        st_all[entry(kind, q), me] = st_new[...]

    def combine(place):
        top = st_all[place, 0, 0:2, :]
        for d in OTHERS:
            top = jnp.maximum(top, st_all[place, d, 0:2, :])
        s = jnp.zeros((2, LANE), F32)
        t = jnp.zeros((2, LANE), F32)
        for d in range(8):
            s = s + st_all[place, d, 2:4, :] * jnp.exp(st_all[place, d, 0:2, :] - top)
            t = t + st_all[place, d, 4:6, :]
        comb[0:2, :] = top
        comb[2:4, :] = INV / s
        return top + jnp.log(s) - t

    def stats_arrived(q):
        _copy(st_all.at[0, SEVEN], st_all.at[0, SEVEN], st_sem.at[q]).wait()

    def late_arrived():
        _copy(st_all.at[pl.ds(0, 14)], st_all.at[pl.ds(0, 14)], st_sem.at[4]).wait()

    def columns(blk, par, part):
        rows = pl.ds(part * LANE, LANE)
        c_lab[par, rows, :] = label_column(blk, part)
        c_top[par, rows, :] = _column(comb[part : part + 1, :])
        c_scale[par, rows, :] = _column(comb[2 + part : 3 + part, :])

    def gradient(src, n, par, r, j):
        rows = pl.ds(pl.multiple_of(r, SUB), SUB)
        col = c_lab[par, rows, :] - (me * VOC + n * HALF + j)
        p = jnp.exp(src[n, rows, j : j + PIECE] - _wide(c_top[par, rows, :], 4)) * _wide(c_scale[par, rows, :], 4)
        g = jnp.where(_wide(col, 4) == lax.broadcasted_iota(I32, (SUB, PIECE), 1), p - INV, p)
        gbufs[par][rows, n * HALF + j : n * HALF + j + PIECE] = g.astype(BF16)

    def gradient_jobs(src, n, par):
        return [functools.partial(gradient, src, n, par, r, j) for r in range(0, BLK, SUB) for j in range(0, HALF, PIECE)]

    gbufs = (ga, gb)

    def gstore(k, par):
        kind, q = order2(k)
        return _copy(gbufs[par], gall.at[pl.ds(pl.multiple_of(block_id(kind, q) * BLK, BLK), BLK)], g_sem.at[par])

    def zload(k, dst, n):
        kind, q = order2(k)
        return _copy(zst.at[block_id(kind, q), n], dst.at[n], zi_sem.at[n])

    first_kind, first_q = order2(me * 0)
    first_blk = block_id(first_kind, first_q)

    def logits(b, h, jobs):
        slot = _odd(b)
        def put(nt, z):
            zb[h, :, nt * PIECE : (nt + 1) * PIECE] = z
            m = z[:, :LANE]
            for j in range(1, 4):
                m = jnp.maximum(m, z[:, j * LANE : (j + 1) * LANE])
            if nt:
                m = jnp.maximum(m, ml[h])
            ml[h] = m

        _product(
            lambda kt: xg[slot, :, kt * PIECE : (kt + 1) * PIECE],
            lambda nt, kt: wv[kt * PIECE : (kt + 1) * PIECE, h * HALF + nt * PIECE : h * HALF + (nt + 1) * PIECE],
            put,
            jobs,
            False,
        )

    wait_rows(0, 0, oc)
    _copy(xrows(0, 0, oc), xg.at[0, pl.ds(pl.multiple_of(oc * LANE, LANE), LANE)], xl_sem.at[0]).start()
    _copy(lab_v, lab_v, lab_sem).wait()
    for j in FOUR:
        wcopy(j).wait()
    for j in range(4, 8):
        wcopy(j).start()

    def phase1(i, carry):
        slot = _odd(i)
        kind, q = order1(i)
        kprev, qprev = order1(_rem(i + NBLK - 2, NBLK))
        kn, qn = order1(_rem(i + 1, NBLK))

        @pl.when((i == LATE + 1) | (i == NBLK - 1))
        def _():
            wait_rows(kind, q, oc)
            part_load(i, oc).start()

        @pl.when(i > 0)
        def _():
            zcopy(i - 1, 1).start()
            zcopy(i - 1, 0).wait()

        @pl.when(i > 1)
        def _():
            keep_stats(kprev, qprev)

        @pl.when(i == NBLK - 2)
        def _():
            zload(0, pbuf, 0).start()
            zload(0, pbuf, 1).start()

        @pl.when(i == NBLK - 1)
        def _():
            stats_arrived(0)
            loss_acc[...] = combine(entry(first_kind, first_q))
            for part in PAIR:
                columns(first_blk, 0, part)
            for n in PAIR:
                zload(0, pbuf, n).wait()

                def some(r, carry, n=n):
                    for j in range(0, HALF, PIECE):
                        gradient(pbuf, n, 0, r * SUB, j)
                    return carry

                _loop(SUB, some)

            gstore(0, 0).start()

        @pl.when((i >= 3) & (i != LATE) & (i < NBLK - 2))
        def _():
            take_rows(kn, qn)

        _copy(xg.at[slot], xg.at[slot], xl_sem.at[slot]).wait()

        @pl.when(i < 4)
        def _():
            own_store(i).start()

        jobs = [[] for _ in range(32)]
        for r in range(32):
            jobs[min(r + 1, 31)].append(functools.partial(lane_stats, la, 1, r * 8))
        for part in PAIR:
            jobs[4 + 4 * part].append(functools.partial(label_columns, block_id(kind, q), lb, part))
        logits(i, 0, jobs)

        zcopy(i, 0).start()

        @pl.when(i == 0)
        def _():
            for j in range(4, 8):
                wcopy(j).wait()

        @pl.when(i > 0)
        def _():
            zcopy(i - 1, 1).wait()

        @pl.when(i > 1)
        def _():
            send_stats(kprev, qprev)

        @pl.when((i == LATE) | (i == NBLK - 2))
        def _():
            take_rows(kn, qn)
            part_load(i + 1, c).start()

        @pl.when((i != LATE) & (i < NBLK - 2))
        def _():
            wait_rows(kn, qn, oc)

            @pl.when((i >= 1) & (i < 5))
            def _():
                own_store(i - 1).wait()

            load_x(i + 1)

        la[...] = lb[...]
        jobs = [[] for _ in range(32)]
        for r in range(32):
            jobs[min(r + 1, 31)].append(functools.partial(lane_stats, lb, 0, r * 8))
        for part in PAIR:
            jobs[8 + 8 * part].append(functools.partial(row_stats, part))
        logits(i, 1, jobs)
        return carry

    _loop(NBLK, phase1)
    last = NBLK - 1
    klast, qlast = order1(jnp.int32(last))
    kprev, qprev = order1(jnp.int32(last - 1))
    zcopy(last, 1).start()
    zcopy(last, 0).wait()
    zload(1, zb, 0).start()
    keep_stats(kprev, qprev)
    for r in range(32):
        lane_stats(la, 1, r * 8)
    send_stats(kprev, qprev)
    for part in PAIR:
        row_stats(part)
    keep_stats(klast, qlast)
    zcopy(last, 1).wait()
    zload(1, zb, 1).start()
    send_stats(klast, qlast)
    second_kind, second_q = order2(jnp.int32(1))
    second_blk = block_id(second_kind, second_q)
    stats_arrived(1)
    loss_acc[...] += combine(entry(second_kind, second_q))
    for part in PAIR:
        columns(second_blk, 1, part)

    def tile(ref, q, n):
        return ref.at[pl.ds(pl.multiple_of(q * LANE, LANE), LANE), pl.ds(pl.multiple_of(n * HALF, HALF), HALF)]

    def spair(k, n):
        return _send(
            pbuf.at[n, pl.ds(pl.multiple_of(oc * LANE, LANE), LANE)], rbuf.at[_odd(k + 2), n], ps.at[n], rr.at[_odd(k + 2) * 2 + n], partner
        )

    def sstore_start(k, n):
        kind, q = order2(k)
        sem = ss_sem.at[n]

        @pl.when(kind == 3)
        def _():
            _copy(sbuf.at[n], tile(s_d, q, n), sem).start()

        @pl.when((kind == n1kind) & (q < 2))
        def _():
            _copy(sbuf.at[n], tile(s_n1a, _odd(q), n), sem).start()

        @pl.when((kind == n1kind) & (q >= 2))
        def _():
            _copy(sbuf.at[n], tile(s_n1b, _odd(q), n), sem).start()

        @pl.when(kind == 3 - n1kind)
        def _():
            _copy(sbuf.at[n], tile(s_n2, q, n), sem).start()

        @pl.when(kind == 0)
        def _():
            _copy(sbuf.at[n], tile(s_self, q, n), sem).start()

    def sstore_done(k, n):
        kind, q = order2(k)
        _copy(sbuf.at[n], tile(s_d, 0, n), ss_sem.at[n]).wait()

        @pl.when(kind == 3)
        def _():
            _send(tile(s_d, q, n), tile(r1n2, q, n), s1tx, r1s.at[q * 2 + n], n1).start()

        @pl.when((kind == n1kind) & (q < 2))
        def _():
            _send(tile(s_n1a, _odd(q), n), tile(r1a, _odd(q), n), s1tx, r1as.at[_odd(q) * 2 + n], n1).start()

    def stage2_load(q, n):
        _copy(tile(r1n2, q, n), tile(r1n2, q, n), r1s.at[q * 2 + n]).wait()
        _copy(tile(s_n2, q, n), ab.at[n], ab_sem.at[n * 2]).start()
        _copy(tile(r1n2, q, n), bb.at[n], ab_sem.at[n * 2 + 1]).start()

    def pair_sum(k, n, r):
        sbuf[n, pl.ds(r, SUB), :] = pbuf[n, pl.ds(pl.multiple_of(c * LANE + r, SUB), SUB), :] + rbuf[_odd(k + 2), n, pl.ds(r, SUB), :]

    def stage2_sum(n, r):
        cb[n, pl.ds(r, SUB), :] = ab[n, pl.ds(r, SUB), :] + bb[n, pl.ds(r, SUB), :]

    def rwait(k, n):
        _copy(rbuf.at[_odd(k + 2), n], rbuf.at[_odd(k + 2), n], rr.at[_odd(k + 2) * 2 + n]).wait()

    def loss_part(k, place):
        loss_acc[...] += jnp.where(k < NBLK - 2, combine(place), 0.0)

    def sub(k, cur):
        nxt = 1 - cur
        kind2, q2 = order2(_rem(k + 2, NBLK))
        blk2 = block_id(kind2, q2)

        def trip(n):
            @pl.when(k < NBLK - 1)
            def _():
                zload(k + 1, zb, n).wait()

            @pl.when(k >= 1)
            def _():
                rwait(k - 1, n)
                spair(k - 1, n).wait_send()
                if n == 0:
                    gstore(k - 1, nxt).wait()

            if n == 0:

                @pl.when(k < 2)
                def _():
                    stats_arrived(k + 2)

                @pl.when(k == 2)
                def _():
                    late_arrived()

            @pl.when(k >= 12)
            def _():
                _copy(tile(s_n2, 0, n), ab.at[n], ab_sem.at[n * 2]).wait()
                _copy(tile(r1n2, 0, n), bb.at[n], ab_sem.at[n * 2 + 1]).wait()

            @pl.when(k >= 13)
            def _():
                _copy(cb.at[n], tile(y2, 0, n), cb_sem.at[n]).wait()

            jobs = [[] for _ in range(32)]
            for r in range(8):
                jobs[2 + r * 3 // 5].append(functools.partial(pair_sum, k - 1, n, r * SUB))
                jobs[10 + r * 5 // 2].append(functools.partial(stage2_sum, n, r * SUB))
            for r, job in enumerate(gradient_jobs(zb, n, nxt)):
                jobs[2 + r * 9 // 20].append(job)
            if n == 0:
                jobs[8].append(lambda: loss_part(k, entry(kind2, q2)))
            else:
                for part in PAIR:
                    jobs[8 + 8 * part].append(functools.partial(columns, blk2, cur, part))

            def put(nt, acc):
                pbuf[n, :, nt * PIECE : (nt + 1) * PIECE] = acc

            _product(
                lambda kt: gbufs[cur][:, kt * PIECE : (kt + 1) * PIECE],
                lambda nt, kt: wv[pl.ds(pl.multiple_of(n * HALF + nt * PIECE, PIECE), PIECE), kt * PIECE : (kt + 1) * PIECE],
                put,
                jobs,
                True,
            )

            spair(k, n).start()

            if cur == n == 0:
                pl.when(k == 0)(send_late)

            @pl.when(k < NBLK - 2)
            def _():
                zload(k + 2, zb, n).start()

            @pl.when(k >= 2)
            def _():
                sstore_done(k - 2 + n, 1 - n)

            @pl.when(k >= 1)
            def _():
                sstore_start(k - 1, n)

            if n == 0:
                @pl.when(k == 1)
                def _():
                    sstore_done(k - 1, n)

            @pl.when(k >= 12)
            def _():
                _copy(cb.at[n], tile(y2, k - 12, n), cb_sem.at[n]).start()

            @pl.when((k >= 11) & (k < NBLK - 1))
            def _():
                stage2_load(k - 11, n)


        trip(0)
        trip(1)

        @pl.when(k < NBLK - 1)
        def _():
            gstore(k + 1, nxt).start()

    def pair(p, carry):
        sub(2 * p, 0)
        sub(2 * p + 1, 1)
        return carry

    _loop(NBLK // 2, pair)

    kl = jnp.int32(NBLK - 1)
    for n in PAIR:
        rwait(kl, n)
        spair(kl, n).wait_send()
        if n == 0:
            sstore_done(kl - 1, 1)
        for r in range(8):
            pair_sum(kl, n, r * SUB)
        sstore_start(kl, n)
    for n in PAIR:
        sstore_done(kl, n)
    gstore(kl, 1).wait()
    for n in PAIR:
        _copy(cb.at[n], tile(y2, 0, n), cb_sem.at[n]).wait()

    loss_out[...] = jnp.full(TILE, jnp.sum(loss_acc[...]) * INV, F32)

    for i in FOUR:
        _copy(tile(r1a, i // 2, i % 2), tile(r1a, i // 2, i % 2), r1as.at[i]).wait()
    _copy(s_d, s_d, s1tx).wait()
    _copy(s_n1a, s_n1a, s1tx).wait()
    _copy(xall.at[pl.ds(0, 28 * LANE)], xall.at[pl.ds(0, 28 * LANE)], tx).wait()
    for d in range(7):
        _copy(lab_v.at[d], lab_v.at[d], labtx_sem).wait()
        _copy(st_loc, st_loc, sttx_sem).wait()
    for d in FOUR:
        _copy(st_all.at[d, SEVEN], st_all.at[d, SEVEN], sttx_sem).wait()


def xrows_at(xall, dev, q):
    return xall.at[pl.ds(pl.multiple_of((dev // 2) * 1024 + q * BLK + (dev % 2) * LANE, LANE), LANE)]


def _head(hid, lab, w):
    hbm = pl.BlockSpec(memory_space=ANY)
    sd = jax.ShapeDtypeStruct
    dma = pltpu.SemaphoreType.DMA
    vmem = pltpu.VMEM
    quarter = (LANE, HALF)
    return pl.pallas_call(
        _head_kernel,
        out_shape=(
            sd((TOK, HID), BF16),
            sd((TOK, VOC), BF16),
            sd((256, HID), F32),
            sd((PIECE, HID), F32),
            sd((PIECE, HID), F32),
            sd((256, HID), F32),
            sd(TILE, F32),
            sd((NBLK, 2, BLK, HALF), F32),
            sd((PIECE, HID), F32),
            sd((256, HID), F32),
            sd((PIECE, HID), F32),
            sd((PIECE, HID), F32),
        ),
        in_specs=[hbm] * 3,
        out_specs=(hbm,) * 6 + (pl.BlockSpec(memory_space=vmem),) + (hbm,) * 5,
        scratch_shapes=[
            vmem((HID, VOC), BF16),
            vmem((2, BLK, HID), BF16),
            vmem((BLK, VOC), BF16),
            vmem((BLK, VOC), BF16),
            vmem((2, BLK, HALF), F32),
            vmem((2, BLK, HALF), F32),
            vmem((2, 2) + quarter, F32),
            vmem(TWO + quarter, F32),
            vmem(TWO + quarter, F32),
            vmem(TWO + quarter, F32),
            vmem(TWO + quarter, F32),
            vmem((8, 4, LANE), I32),
            vmem((BLK, LANE), I32),
            vmem((BLK, LANE), I32),
            vmem(TILE, F32),
            vmem((NBLK,) + TILE, F32),
            vmem((NBLK + 4, 8) + TILE, F32),
            vmem((2, BLK, LANE), F32),
            vmem((2, BLK, LANE), F32),
            vmem((2, BLK, LANE), F32),
            vmem((2, BLK, LANE), F32),
            vmem(TILE, F32),
            vmem((2, BLK, LANE), I32),
            vmem((2, BLK, LANE), F32),
            vmem((2, BLK, LANE), F32),
            vmem((2, LANE), F32),
            dma((8,)),
            dma(()),
            dma(()),
            dma((32,)),
            dma(()),
            dma(TWO),
            dma(TWO),
            dma(TWO),
            dma((5,)),
            dma(()),
            dma(TWO),
            dma((4,)),
            dma(TWO),
            dma(TWO),
            dma(()),
            dma((8,)),
            dma((4,)),
            dma((4,)),
            dma(TWO),
            dma(TWO),
        ],
        compiler_params=pltpu.CompilerParams(collective_id=0, has_side_effects=True, vmem_limit_bytes=67_043_328),
        cost_estimate=pl.CostEstimate(flops=4 * TOK * HID * VOC, bytes_accessed=400 * MIB, transcendentals=2 * TOK * VOC),
        name="head",
    )(hid, lab, w)


def _cols(j, width=PIECE):
    return pl.ds(pl.multiple_of(j * width, width), width)


def _dhead_kernel(
    x_hbm, g_hbm, s_hbm, a_hbm, o_hbm, t_hbm, gv, xb, ob, sv, av, x_sem, g_sem, o_sem, s_sem, a_sem, t_sem
):
    blocks = HID // PIECE
    rows = BLK // 4

    def xload(b):
        return _copy(x_hbm.at[:, _cols(b)], xb.at[_odd(b)], x_sem.at[_odd(b)])

    def gload(j):
        return _copy(g_hbm.at[:, _cols(j)], gv.at[:, _cols(j)], g_sem.at[j])

    def ostore(b, n):
        return _copy(ob.at[n], o_hbm.at[_cols(b), _cols(n, HALF)], o_sem.at[n])

    def dot(lhs, rhs):
        return lax.dot_general(lhs, rhs, (((0,), (0,)), ((), ())), preferred_element_type=F32).astype(BF16)

    def terms(p):
        slot = _odd(p)
        src = _cols(p, rows)
        return _copy(s_hbm.at[src], sv.at[slot], s_sem.at[slot]), _copy(a_hbm.at[src], av.at[slot], a_sem.at[slot])

    def tstore(p):
        return _copy(sv.at[_odd(p)], t_hbm.at[_cols(p, rows)], t_sem.at[_odd(p)])

    xload(0).start()
    gload(0).start()
    xload(0).wait()
    gload(1).start()

    def first(j, carry):
        gload(j).wait()

        @pl.when(j == 0)
        def _():
            gload(2).start()

        @pl.when(j > 0)
        def _():
            gload(2 * j + 1).start()

        @pl.when((j > 0) & (j < 3))
        def _():
            gload(2 * j + 2).start()

        ob[0, :, _cols(j)] = dot(xb[0], gv[:, _cols(j)])
        return carry

    _loop(4, first)
    ostore(0, 0).start()
    xload(1).start()
    for j in range(4, 8):
        gload(j).wait()

    def block(b, carry):
        @pl.when(b > 0)
        def _():
            xload(b).wait()

        @pl.when((b > 0) & (b < blocks - 1))
        def _():
            xload(b + 1).start()

        @pl.when((b > 1) & (b < 6))
        def _():
            for copy in terms(b - 2):
                copy.wait()
            sv[_odd(b)] = sv[_odd(b)] + av[_odd(b)]
            tstore(b - 2).start()

        @pl.when((b > 0) & (b < 5))
        def _():
            pl.when(b > 2)(lambda: tstore(b - 3).wait())
            for copy in terms(b - 1):
                copy.start()

        def half(n, carry):
            pl.when(b > 0)(lambda: ostore(b - 1, n).wait())

            @pl.when(b < blocks)
            def _():
                ob[n] = dot(xb[_odd(b)], gv[:, _cols(n, HALF)])

            ostore(b, n).start()
            return carry

        return lax.fori_loop(jnp.where(b == 0, 1, 0), 2, half, carry)

    _loop(blocks, block)
    for n in PAIR:
        ostore(blocks - 1, n).wait()
        tstore(n).wait()


def _dhead(xall, gall, s_self, r1a):
    hbm = pl.BlockSpec(memory_space=ANY)
    dma = pltpu.SemaphoreType.DMA
    return pl.pallas_call(
        _dhead_kernel,
        in_specs=[hbm] * 4,
        out_specs=(hbm, hbm),
        out_shape=(jax.ShapeDtypeStruct((HID, VOC), BF16), jax.ShapeDtypeStruct((BLK, HID), F32)),
        scratch_shapes=[
            pltpu.VMEM((TOK, VOC), BF16),
            pltpu.VMEM((2, TOK, PIECE), BF16),
            pltpu.VMEM((2, PIECE, HALF), BF16),
            pltpu.VMEM((2, BLK // 4, HID), F32),
            pltpu.VMEM((2, BLK // 4, HID), F32),
            dma(TWO),
            dma((8,)),
            dma(TWO),
            dma(TWO),
            dma(TWO),
            dma(TWO),
        ],
        compiler_params=pltpu.CompilerParams(vmem_limit_bytes=60 * MIB),
        cost_estimate=pl.CostEstimate(flops=2 * TOK * HID * VOC, bytes_accessed=200 * MIB, transcendentals=0),
        name="dhead",
    )(xall, gall, s_self, r1a)


def _final_kernel(t_hbm, s_hbm, b_hbm, r_hbm, l_ref, o_hbm, loss_ref, terms, ov, in_sem, o_sem):
    rows = PIECE // SUB
    ahead = 6
    half = SUB // 2

    def load(t, ref, i, dst):
        return _copy(ref.at[_cols(i, rows)], terms.at[t, _cols(dst, rows)], in_sem.at[t, dst])

    def start(i):
        @pl.when(i < half)
        def _():
            load(0, t_hbm, i, i).start()

        @pl.when(i >= half)
        def _():
            load(0, s_hbm, i, i).start()
            load(1, b_hbm, i - half, i).start()

        load(2, r_hbm, i, i).start()

    def begin(i, carry):
        start(i)
        return carry

    _loop(ahead, begin)
    loss_ref[0] = l_ref[0, 0]

    def add(i, carry):
        rs = _cols(i, rows)
        load(0, s_hbm, i, i).wait()
        load(2, r_hbm, i, i).wait()
        pl.when(i < SUB - ahead)(lambda: start(i + ahead))

        @pl.when(i < half)
        def _():
            ov[rs, :] = (terms[0, rs, :] + terms[2, rs, :]).astype(BF16)

        @pl.when(i >= half)
        def _():
            load(1, b_hbm, i - half, i).wait()
            ov[rs, :] = (terms[0, rs, :] + terms[1, rs, :] + terms[2, rs, :]).astype(BF16)

        _copy(ov.at[rs], o_hbm.at[rs], o_sem).start()
        return carry

    _loop(SUB, add)
    _copy(ov, o_hbm, o_sem).wait()


def _final(t, s_self, r1b, r2, loss):
    hbm = pl.BlockSpec(memory_space=ANY)
    dma = pltpu.SemaphoreType.DMA
    return pl.pallas_call(
        _final_kernel,
        in_specs=[hbm] * 4 + [pl.BlockSpec(memory_space=pltpu.VMEM)],
        out_specs=(hbm, pl.BlockSpec(memory_space=pltpu.SMEM)),
        out_shape=(jax.ShapeDtypeStruct((PIECE, HID), BF16), jax.ShapeDtypeStruct((1,), F32)),
        scratch_shapes=[
            pltpu.VMEM((3, PIECE, HID), F32),
            pltpu.VMEM((PIECE, HID), BF16),
            dma((3, SUB)),
            dma(()),
        ],
        compiler_params=pltpu.CompilerParams(vmem_limit_bytes=62 * MIB),
        cost_estimate=pl.CostEstimate(flops=3 * PIECE * HID, bytes_accessed=24 * MIB, transcendentals=0),
        name="final",
    )(t, s_self, r1b, r2, loss)


def solution(mesh):
    def device(y, x, core):
        return (y % 2) * 4 + (x % 2) * 2 + core

    first, second = [], []
    for yy in PAIR:
        for xx in PAIR:
            along_x = [(device(yy, xx, k), device(yy, xx + 1, k)) for k in PAIR]
            along_y = [(device(yy, xx, k), device(yy + 1, xx, k)) for k in PAIR]
            first += [along_x[0], along_y[1]]
            second += [along_y[0], along_x[1]]

    def local_step(hid, w, lab):
        xall, gall, s_n1b, s_self, y2, r1a, loss = _head(hid, lab.reshape(4, LANE), w)[:7]
        r1b = lax.ppermute(s_n1b, "tp", first)
        r2 = lax.ppermute(y2, "tp", second)
        d_head, t = _dhead(xall, gall, s_self, r1a)
        d_hidden, mean_loss = _final(t, s_self, r1b, r2, loss)
        return mean_loss, d_hidden, d_head

    return jax.shard_map(
        local_step,
        mesh=mesh,
        in_specs=(P(("dp", "tp"), None), P(None, "tp"), P(("dp", "tp"))),
        out_specs=(P("dp"), P(("dp", "tp"), None), P("dp", "tp")),
        check_vma=False,
    )
```

```python
import functools

import jax
import jax.numpy as jnp
from jax import lax
from jax.experimental import pallas as pl
from jax.experimental.pallas import tpu as pltpu
from jax.sharding import PartitionSpec as P

F32, BF16, I32 = jnp.float32, jnp.bfloat16, jnp.int32
MESH = pl.DeviceIdType.MESH
ANY = pl.ANY

TOK = 4096
HID = 4096
VOC = 4096
BLK = 256
HALF = 2048
NBLK = TOK // BLK
LANE = 128
MIB = 1 << 20
TWO = (2,)
PAIR = (0, 1)
TILE = (8, LANE)
SUB = 16
FIRST_DIMS = (((0,), (0,)), ((), ()))
FOUR = range(4)
OTHERS = range(1, 8)
SEVEN = pl.ds(0, 7)
LATE = 9
PIECE = 512
INV = 1.0 / TOK


def _div(a, b):
    return lax.div(jnp.int32(a), jnp.int32(b))


def _rem(a, b):
    return lax.rem(jnp.int32(a), jnp.int32(b))


def _odd(a):
    return _rem(a, 2)


def _loop(count, body):
    lax.fori_loop(0, count, body, 0)


def _copy(src, dst, sem):
    return pltpu.make_async_copy(src, dst, sem)


def _send(src, dst, send_sem, recv_sem, dev):
    return pltpu.make_async_remote_copy(
        src_ref=src, dst_ref=dst, send_sem=send_sem, recv_sem=recv_sem, device_id={"tp": dev}, device_id_type=MESH
    )


def _product(lhs, rhs, put, jobs, transposed):
    pl.when(lax.axis_index("tp") < 8)(functools.partial(_pieces, lhs, rhs, put, jobs, transposed))


def _pieces(lhs, rhs, put, jobs, transposed):
    dims = (((1,), (1,)), ((), ())) if transposed else (((1,), (0,)), ((), ()))
    pieces = HALF // PIECE
    deep = 8
    for nt in range(pieces):
        acc = None
        for kt in range(deep):
            part = lax.dot_general(lhs(kt), rhs(nt, kt), dims, preferred_element_type=F32)
            acc = part if acc is None else acc + part
            for job in jobs[nt * deep + kt]:
                job()
        put(nt, acc)


def _wide(v, times=HALF // LANE):
    return jnp.concatenate([v] * times, axis=1)


def _fold(v):
    width = v.shape[1] // 2
    while width >= LANE:
        v = v[:, :width] + v[:, width:]
        width //= 2
    return v


def _column(row):
    return jnp.transpose(jnp.broadcast_to(row, (LANE, LANE)))


def _head_kernel(
    x_hbm, lab_hbm, w_hbm,
    xall, gall, s_n1b, s_self, y2, r1a, loss_out,
    zst, s_d, s_n1a, s_n2, r1n2,
    wv, xg, ga, gb, zb, pbuf, rbuf, sbuf, ab, bb, cb, lab_v, la, lb, st_new, st_loc, st_all, ml, mk, sl, tl, comb, c_lab, c_top, c_scale, loss_acc,
    w_sem, lab_sem, labtx_sem, rx, tx, xl_sem, xs_sem, zo_sem, st_sem, sttx_sem,
    zi_sem, rr, ps, ss_sem, s1tx, r1s, r1as, ab_sem, cb_sem, g_sem,
):
    me = lax.axis_index("tp")
    chip = _div(me, 2)
    c = _odd(me)
    x = _odd(chip)
    y = _div(chip, 2)
    oc = 1 - c
    partner = me + 1 - 2 * c
    dx, dy = 2 - 4 * x, 4 - 8 * y
    n1 = me + oc * dx + c * dy
    n2 = me + c * dx + oc * dy
    n1kind = 1 + c

    def chip_of(kind):
        return chip + _odd(kind) * (1 - 2 * x) + _div(kind, 2) * (2 - 4 * y)

    def order(i, first, last):
        a = _div(i, 4)
        mid, end = _rem(_div(a + 1, 2), 2), _div(a, 3)
        kind = mid * (1 + _odd(i)) + first * (1 - mid) * (1 - end) + last * end
        return kind, mid * _div(i - 4, 2) + (1 - mid) * _rem(i, 4)

    def order1(i):
        return order(i, 0, 3)

    def order2(i):
        return order(i, 3, 0)

    def block_id(kind, q):
        return chip_of(kind) * 4 + q

    def xrows(kind, q, part):
        return xall.at[pl.ds(pl.multiple_of(block_id(kind, q) * BLK + part * LANE, LANE), LANE)]

    def xblock(kind, q):
        return xall.at[pl.ds(pl.multiple_of(block_id(kind, q) * BLK, BLK), BLK)]

    def own(q):
        return x_hbm.at[pl.ds(pl.multiple_of(q * LANE, LANE), LANE)]

    def rxs(kind, q, part):
        return rx.at[kind * 8 + q * 2 + part]

    def wcopy(j):
        cols = pl.ds(j * PIECE, PIECE)
        return _copy(w_hbm.at[:, cols], wv.at[:, cols], w_sem.at[j])

    _copy(own(0), xg.at[0, pl.ds(pl.multiple_of(c * LANE, LANE), LANE)], xl_sem.at[0]).start()
    for j in FOUR:
        wcopy(j).start()

    barrier = pltpu.get_barrier_semaphore()
    for d in OTHERS:
        pl.semaphore_signal(barrier, inc=1, device_id={"tp": _rem(me + d, 8)}, device_id_type=MESH)
    pl.semaphore_wait(barrier, 7)

    for d in OTHERS:
        _send(lab_hbm, lab_v.at[me], labtx_sem, lab_sem, _rem(me + d, 8)).start()
    _copy(lab_hbm, lab_v.at[me], lab_sem).start()
    for q in FOUR:
        _send(own(q), xrows(0, q, c), tx, rxs(0, q, c), partner).start()
    for q in FOUR:
        _send(own(q), xrows_at(xall, me, q), tx, rxs(n1kind, q, c), n1).start()
        _send(own(q), xrows_at(xall, me, q), tx, rxs(3 - n1kind, q, c), n2).start()

    def load_x(b):
        kind, q = order1(b)
        slot = _odd(b)

        @pl.when(kind == 0)
        def _():
            _copy(own(q), xg.at[slot, pl.ds(pl.multiple_of(c * LANE, LANE), LANE)], xl_sem.at[slot]).start()
            _copy(xrows(0, q, oc), xg.at[slot, pl.ds(pl.multiple_of(oc * LANE, LANE), LANE)], xl_sem.at[slot]).start()

        @pl.when(kind != 0)
        def _():
            _copy(xblock(kind, q), xg.at[slot], xl_sem.at[slot]).start()

    def wait_rows(kind, q, part):
        _copy(xrows(kind, q, part), xrows(kind, q, part), rxs(kind, q, part)).wait()

    def take_rows(kind, q):
        wait_rows(kind, q, c)
        _send(xrows(kind, q, c), xrows(kind, q, c), tx, rxs(kind, q, c), partner).start()

        @pl.when(kind == n1kind)
        def _():
            _send(xrows(kind, q, c), xrows(kind, q, c), tx, rxs(3, q, c), n2).start()

    def part_load(b, part):
        kind, q = order1(b)
        return _copy(xrows(kind, q, part), xg.at[_odd(b), pl.ds(pl.multiple_of(part * LANE, LANE), LANE)], xl_sem.at[_odd(b)])

    def zcopy(b, h):
        kind, q = order1(b)
        return _copy(zb.at[h], zst.at[block_id(kind, q), h], zo_sem.at[h])

    def own_store(b):
        slot = _odd(b)
        return _copy(xg.at[slot, pl.ds(pl.multiple_of(c * LANE, LANE), LANE)], xrows(0, _rem(b, 4), c), xs_sem.at[slot])

    def label_column(blk, part):
        return _column(lab_v[2 * _div(blk, 4) + part, pl.ds(_rem(blk, 4), 1), :])

    def lane_stats(col, h, r):
        rows = pl.ds(r, 8)
        z = zb[h, rows, :]
        m = ml[h, rows, :]
        hit = _wide(col[rows, :] - (me * VOC + h * HALF)) == lax.broadcasted_iota(I32, (8, HALF), 1)
        s = _fold(jnp.exp(z - _wide(m)))
        t = _fold(jnp.where(hit, z, 0.0))
        if h == 1:
            m0 = mk[0, rows, :]
            mm = jnp.maximum(m0, m)
            s = sl[0, rows, :] * jnp.exp(m0 - mm) + s * jnp.exp(m - mm)
            t = tl[0, rows, :] + t
            m = mm
        mk[h, rows, :] = m
        sl[h, rows, :] = s
        tl[h, rows, :] = t

    def label_columns(blk, col, part):
        col[pl.ds(part * LANE, LANE), :] = label_column(blk, part)

    def row_stats(part):
        rows = pl.ds(part * LANE, LANE)
        m = jnp.transpose(mk[1, rows, :])
        top = jnp.max(m, axis=0, keepdims=True)
        st_new[part : part + 1, :] = top
        st_new[2 + part : 3 + part, :] = jnp.sum(jnp.transpose(sl[1, rows, :]) * jnp.exp(m - top), axis=0, keepdims=True)
        st_new[4 + part : 5 + part, :] = jnp.sum(jnp.transpose(tl[1, rows, :]), axis=0, keepdims=True)

    def entry(kind, q):
        diagonal = _div(kind, 3)
        return diagonal * (NBLK + q) + (1 - diagonal) * block_id(kind, q)

    def send_stats(kind, q):
        def start(dev):
            _send(st_loc.at[block_id(kind, q)], st_all.at[NBLK + q, me], sttx_sem, st_sem.at[q], dev).start()

        for core in PAIR:
            dev = 2 * chip_of(3 - kind) + core
            pl.when(dev != me)(functools.partial(start, dev))

    def send_late():
        for d in OTHERS:
            _send(st_loc, st_all.at[pl.ds(0, NBLK), me], sttx_sem, st_sem.at[4], _rem(me + d, 8)).start()

    def keep_stats(kind, q):
        st_loc[block_id(kind, q)] = st_new[...]
        st_all[block_id(kind, q), me] = st_new[...]
        st_all[entry(kind, q), me] = st_new[...]

    def combine(place):
        top = st_all[place, 0, 0:2, :]
        for d in OTHERS:
            top = jnp.maximum(top, st_all[place, d, 0:2, :])
        s = jnp.zeros((2, LANE), F32)
        t = jnp.zeros((2, LANE), F32)
        for d in range(8):
            s = s + st_all[place, d, 2:4, :] * jnp.exp(st_all[place, d, 0:2, :] - top)
            t = t + st_all[place, d, 4:6, :]
        comb[0:2, :] = top
        comb[2:4, :] = INV / s
        return top + jnp.log(s) - t

    def stats_arrived(q):
        _copy(st_all.at[0, SEVEN], st_all.at[0, SEVEN], st_sem.at[q]).wait()

    def late_arrived():
        _copy(st_all.at[pl.ds(0, 14)], st_all.at[pl.ds(0, 14)], st_sem.at[4]).wait()

    def columns(blk, par, part):
        rows = pl.ds(part * LANE, LANE)
        c_lab[par, rows, :] = label_column(blk, part)
        c_top[par, rows, :] = _column(comb[part : part + 1, :])
        c_scale[par, rows, :] = _column(comb[2 + part : 3 + part, :])

    def gradient(src, n, par, r, j):
        rows = pl.ds(pl.multiple_of(r, SUB), SUB)
        col = c_lab[par, rows, :] - (me * VOC + n * HALF + j)
        p = jnp.exp(src[n, rows, j : j + PIECE] - _wide(c_top[par, rows, :], 4)) * _wide(c_scale[par, rows, :], 4)
        g = jnp.where(_wide(col, 4) == lax.broadcasted_iota(I32, (SUB, PIECE), 1), p - INV, p)
        gbufs[par][rows, n * HALF + j : n * HALF + j + PIECE] = g.astype(BF16)

    def gradient_jobs(src, n, par):
        return [functools.partial(gradient, src, n, par, r, j) for r in range(0, BLK, SUB) for j in range(0, HALF, PIECE)]

    gbufs = (ga, gb)

    def gstore(k, par):
        kind, q = order2(k)
        return _copy(gbufs[par], gall.at[pl.ds(pl.multiple_of(block_id(kind, q) * BLK, BLK), BLK)], g_sem.at[par])

    def zload(k, dst, n):
        kind, q = order2(k)
        return _copy(zst.at[block_id(kind, q), n], dst.at[n], zi_sem.at[n])

    first_kind, first_q = order2(me * 0)
    first_blk = block_id(first_kind, first_q)

    def logits(b, h, jobs):
        slot = _odd(b)
        def put(nt, z):
            zb[h, :, nt * PIECE : (nt + 1) * PIECE] = z
            m = z[:, :LANE]
            for j in range(1, 4):
                m = jnp.maximum(m, z[:, j * LANE : (j + 1) * LANE])
            if nt:
                m = jnp.maximum(m, ml[h])
            ml[h] = m

        _product(
            lambda kt: xg[slot, :, kt * PIECE : (kt + 1) * PIECE],
            lambda nt, kt: wv[kt * PIECE : (kt + 1) * PIECE, h * HALF + nt * PIECE : h * HALF + (nt + 1) * PIECE],
            put,
            jobs,
            False,
        )

    wait_rows(0, 0, oc)
    _copy(xrows(0, 0, oc), xg.at[0, pl.ds(pl.multiple_of(oc * LANE, LANE), LANE)], xl_sem.at[0]).start()
    _copy(lab_v, lab_v, lab_sem).wait()
    for j in FOUR:
        wcopy(j).wait()
    for j in range(4, 8):
        wcopy(j).start()

    def phase1(i, carry):
        slot = _odd(i)
        kind, q = order1(i)
        kprev, qprev = order1(_rem(i + NBLK - 2, NBLK))
        kn, qn = order1(_rem(i + 1, NBLK))

        @pl.when((i == LATE + 1) | (i == NBLK - 1))
        def _():
            wait_rows(kind, q, oc)
            part_load(i, oc).start()

        @pl.when(i > 0)
        def _():
            zcopy(i - 1, 1).start()
            zcopy(i - 1, 0).wait()

        @pl.when(i > 1)
        def _():
            keep_stats(kprev, qprev)

        @pl.when(i == NBLK - 2)
        def _():
            zload(0, pbuf, 0).start()
            zload(0, pbuf, 1).start()

        @pl.when(i == NBLK - 1)
        def _():
            stats_arrived(0)
            loss_acc[...] = combine(entry(first_kind, first_q))
            for part in PAIR:
                columns(first_blk, 0, part)
            for n in PAIR:
                zload(0, pbuf, n).wait()

                def some(r, carry, n=n):
                    for j in range(0, HALF, PIECE):
                        gradient(pbuf, n, 0, r * SUB, j)
                    return carry

                _loop(SUB, some)

            gstore(0, 0).start()

        @pl.when((i >= 3) & (i != LATE) & (i < NBLK - 2))
        def _():
            take_rows(kn, qn)

        _copy(xg.at[slot], xg.at[slot], xl_sem.at[slot]).wait()

        @pl.when(i < 4)
        def _():
            own_store(i).start()

        jobs = [[] for _ in range(32)]
        for r in range(32):
            jobs[min(r + 1, 31)].append(functools.partial(lane_stats, la, 1, r * 8))
        for part in PAIR:
            jobs[4 + 4 * part].append(functools.partial(label_columns, block_id(kind, q), lb, part))
        logits(i, 0, jobs)

        zcopy(i, 0).start()

        @pl.when(i == 0)
        def _():
            for j in range(4, 8):
                wcopy(j).wait()

        @pl.when(i > 0)
        def _():
            zcopy(i - 1, 1).wait()

        @pl.when(i > 1)
        def _():
            send_stats(kprev, qprev)

        @pl.when((i == LATE) | (i == NBLK - 2))
        def _():
            take_rows(kn, qn)
            part_load(i + 1, c).start()

        @pl.when((i != LATE) & (i < NBLK - 2))
        def _():
            wait_rows(kn, qn, oc)

            @pl.when((i >= 1) & (i < 5))
            def _():
                own_store(i - 1).wait()

            load_x(i + 1)

        la[...] = lb[...]
        jobs = [[] for _ in range(32)]
        for r in range(32):
            jobs[min(r + 1, 31)].append(functools.partial(lane_stats, lb, 0, r * 8))
        for part in PAIR:
            jobs[8 + 8 * part].append(functools.partial(row_stats, part))
        logits(i, 1, jobs)
        return carry

    _loop(NBLK, phase1)
    last = NBLK - 1
    klast, qlast = order1(jnp.int32(last))
    kprev, qprev = order1(jnp.int32(last - 1))
    zcopy(last, 1).start()
    zcopy(last, 0).wait()
    zload(1, zb, 0).start()
    keep_stats(kprev, qprev)
    for r in range(32):
        lane_stats(la, 1, r * 8)
    send_stats(kprev, qprev)
    for part in PAIR:
        row_stats(part)
    keep_stats(klast, qlast)
    zcopy(last, 1).wait()
    zload(1, zb, 1).start()
    send_stats(klast, qlast)
    second_kind, second_q = order2(jnp.int32(1))
    second_blk = block_id(second_kind, second_q)
    stats_arrived(1)
    loss_acc[...] += combine(entry(second_kind, second_q))
    for part in PAIR:
        columns(second_blk, 1, part)

    def tile(ref, q, n):
        return ref.at[pl.ds(pl.multiple_of(q * LANE, LANE), LANE), pl.ds(pl.multiple_of(n * HALF, HALF), HALF)]

    def spair(k, n):
        return _send(
            pbuf.at[n, pl.ds(pl.multiple_of(oc * LANE, LANE), LANE)], rbuf.at[_odd(k + 2), n], ps.at[n], rr.at[_odd(k + 2) * 2 + n], partner
        )

    def sstore_start(k, n):
        kind, q = order2(k)
        sem = ss_sem.at[n]

        @pl.when(kind == 3)
        def _():
            _copy(sbuf.at[n], tile(s_d, q, n), sem).start()

        @pl.when((kind == n1kind) & (q < 2))
        def _():
            _copy(sbuf.at[n], tile(s_n1a, _odd(q), n), sem).start()

        @pl.when((kind == n1kind) & (q >= 2))
        def _():
            _copy(sbuf.at[n], tile(s_n1b, _odd(q), n), sem).start()

        @pl.when(kind == 3 - n1kind)
        def _():
            _copy(sbuf.at[n], tile(s_n2, q, n), sem).start()

        @pl.when(kind == 0)
        def _():
            _copy(sbuf.at[n], tile(s_self, q, n), sem).start()

    def sstore_done(k, n):
        kind, q = order2(k)
        _copy(sbuf.at[n], tile(s_d, 0, n), ss_sem.at[n]).wait()

        @pl.when(kind == 3)
        def _():
            _send(tile(s_d, q, n), tile(r1n2, q, n), s1tx, r1s.at[q * 2 + n], n1).start()

        @pl.when((kind == n1kind) & (q < 2))
        def _():
            _send(tile(s_n1a, _odd(q), n), tile(r1a, _odd(q), n), s1tx, r1as.at[_odd(q) * 2 + n], n1).start()

    def stage2_load(q, n):
        _copy(tile(r1n2, q, n), tile(r1n2, q, n), r1s.at[q * 2 + n]).wait()
        _copy(tile(s_n2, q, n), ab.at[n], ab_sem.at[n * 2]).start()
        _copy(tile(r1n2, q, n), bb.at[n], ab_sem.at[n * 2 + 1]).start()

    def pair_sum(k, n, r):
        sbuf[n, pl.ds(r, SUB), :] = pbuf[n, pl.ds(pl.multiple_of(c * LANE + r, SUB), SUB), :] + rbuf[_odd(k + 2), n, pl.ds(r, SUB), :]

    def stage2_sum(n, r):
        cb[n, pl.ds(r, SUB), :] = ab[n, pl.ds(r, SUB), :] + bb[n, pl.ds(r, SUB), :]

    def rwait(k, n):
        _copy(rbuf.at[_odd(k + 2), n], rbuf.at[_odd(k + 2), n], rr.at[_odd(k + 2) * 2 + n]).wait()

    def loss_part(k, place):
        loss_acc[...] += jnp.where(k < NBLK - 2, combine(place), 0.0)

    def sub(k, cur):
        nxt = 1 - cur
        kind2, q2 = order2(_rem(k + 2, NBLK))
        blk2 = block_id(kind2, q2)

        def trip(n):
            @pl.when(k < NBLK - 1)
            def _():
                zload(k + 1, zb, n).wait()

            @pl.when(k >= 1)
            def _():
                rwait(k - 1, n)
                spair(k - 1, n).wait_send()
                if n == 0:
                    gstore(k - 1, nxt).wait()

            if n == 0:

                @pl.when(k < 2)
                def _():
                    stats_arrived(k + 2)

                @pl.when(k == 2)
                def _():
                    late_arrived()

            @pl.when(k >= 12)
            def _():
                _copy(tile(s_n2, 0, n), ab.at[n], ab_sem.at[n * 2]).wait()
                _copy(tile(r1n2, 0, n), bb.at[n], ab_sem.at[n * 2 + 1]).wait()

            @pl.when(k >= 13)
            def _():
                _copy(cb.at[n], tile(y2, 0, n), cb_sem.at[n]).wait()

            jobs = [[] for _ in range(32)]
            for r in range(8):
                jobs[2 + r * 3 // 5].append(functools.partial(pair_sum, k - 1, n, r * SUB))
                jobs[10 + r * 5 // 2].append(functools.partial(stage2_sum, n, r * SUB))
            for r, job in enumerate(gradient_jobs(zb, n, nxt)):
                jobs[2 + r * 9 // 20].append(job)
            if n == 0:
                jobs[8].append(lambda: loss_part(k, entry(kind2, q2)))
            else:
                for part in PAIR:
                    jobs[8 + 8 * part].append(functools.partial(columns, blk2, cur, part))

            def put(nt, acc):
                pbuf[n, :, nt * PIECE : (nt + 1) * PIECE] = acc

            _product(
                lambda kt: gbufs[cur][:, kt * PIECE : (kt + 1) * PIECE],
                lambda nt, kt: wv[pl.ds(pl.multiple_of(n * HALF + nt * PIECE, PIECE), PIECE), kt * PIECE : (kt + 1) * PIECE],
                put,
                jobs,
                True,
            )

            spair(k, n).start()

            if cur == n == 0:
                pl.when(k == 0)(send_late)

            @pl.when(k < NBLK - 2)
            def _():
                zload(k + 2, zb, n).start()

            @pl.when(k >= 2)
            def _():
                sstore_done(k - 2 + n, 1 - n)

            @pl.when(k >= 1)
            def _():
                sstore_start(k - 1, n)

            if n == 0:
                @pl.when(k == 1)
                def _():
                    sstore_done(k - 1, n)

            @pl.when(k >= 12)
            def _():
                _copy(cb.at[n], tile(y2, k - 12, n), cb_sem.at[n]).start()

            @pl.when((k >= 11) & (k < NBLK - 1))
            def _():
                stage2_load(k - 11, n)


        trip(0)
        trip(1)

        @pl.when(k < NBLK - 1)
        def _():
            gstore(k + 1, nxt).start()

    def pair(p, carry):
        sub(2 * p, 0)
        sub(2 * p + 1, 1)
        return carry

    _loop(NBLK // 2, pair)

    kl = jnp.int32(NBLK - 1)
    for n in PAIR:
        rwait(kl, n)
        spair(kl, n).wait_send()
        if n == 0:
            sstore_done(kl - 1, 1)
        for r in range(8):
            pair_sum(kl, n, r * SUB)
        sstore_start(kl, n)
    for n in PAIR:
        sstore_done(kl, n)
    gstore(kl, 1).wait()
    for n in PAIR:
        _copy(cb.at[n], tile(y2, 0, n), cb_sem.at[n]).wait()

    loss_out[...] = jnp.full(TILE, jnp.sum(loss_acc[...]) * INV, F32)

    for i in FOUR:
        _copy(tile(r1a, i // 2, i % 2), tile(r1a, i // 2, i % 2), r1as.at[i]).wait()
    _copy(s_d, s_d, s1tx).wait()
    _copy(s_n1a, s_n1a, s1tx).wait()
    _copy(xall.at[pl.ds(0, 28 * LANE)], xall.at[pl.ds(0, 28 * LANE)], tx).wait()
    for d in range(7):
        _copy(lab_v.at[d], lab_v.at[d], labtx_sem).wait()
        _copy(st_loc, st_loc, sttx_sem).wait()
    for d in FOUR:
        _copy(st_all.at[d, SEVEN], st_all.at[d, SEVEN], sttx_sem).wait()


def xrows_at(xall, dev, q):
    return xall.at[pl.ds(pl.multiple_of((dev // 2) * 1024 + q * BLK + (dev % 2) * LANE, LANE), LANE)]


def _head(hid, lab, w):
    hbm = pl.BlockSpec(memory_space=ANY)
    sd = jax.ShapeDtypeStruct
    dma = pltpu.SemaphoreType.DMA
    vmem = pltpu.VMEM
    quarter = (LANE, HALF)
    return pl.pallas_call(
        _head_kernel,
        out_shape=(
            sd((TOK, HID), BF16),
            sd((TOK, VOC), BF16),
            sd((256, HID), F32),
            sd((PIECE, HID), F32),
            sd((PIECE, HID), F32),
            sd((256, HID), F32),
            sd(TILE, F32),
            sd((NBLK, 2, BLK, HALF), F32),
            sd((PIECE, HID), F32),
            sd((256, HID), F32),
            sd((PIECE, HID), F32),
            sd((PIECE, HID), F32),
        ),
        in_specs=[hbm] * 3,
        out_specs=(hbm,) * 6 + (pl.BlockSpec(memory_space=vmem),) + (hbm,) * 5,
        scratch_shapes=[
            vmem((HID, VOC), BF16),
            vmem((2, BLK, HID), BF16),
            vmem((BLK, VOC), BF16),
            vmem((BLK, VOC), BF16),
            vmem((2, BLK, HALF), F32),
            vmem((2, BLK, HALF), F32),
            vmem((2, 2) + quarter, F32),
            vmem(TWO + quarter, F32),
            vmem(TWO + quarter, F32),
            vmem(TWO + quarter, F32),
            vmem(TWO + quarter, F32),
            vmem((8, 4, LANE), I32),
            vmem((BLK, LANE), I32),
            vmem((BLK, LANE), I32),
            vmem(TILE, F32),
            vmem((NBLK,) + TILE, F32),
            vmem((NBLK + 4, 8) + TILE, F32),
            vmem((2, BLK, LANE), F32),
            vmem((2, BLK, LANE), F32),
            vmem((2, BLK, LANE), F32),
            vmem((2, BLK, LANE), F32),
            vmem(TILE, F32),
            vmem((2, BLK, LANE), I32),
            vmem((2, BLK, LANE), F32),
            vmem((2, BLK, LANE), F32),
            vmem((2, LANE), F32),
            dma((8,)),
            dma(()),
            dma(()),
            dma((32,)),
            dma(()),
            dma(TWO),
            dma(TWO),
            dma(TWO),
            dma((5,)),
            dma(()),
            dma(TWO),
            dma((4,)),
            dma(TWO),
            dma(TWO),
            dma(()),
            dma((8,)),
            dma((4,)),
            dma((4,)),
            dma(TWO),
            dma(TWO),
        ],
        compiler_params=pltpu.CompilerParams(collective_id=0, has_side_effects=True, vmem_limit_bytes=67_043_328),
        cost_estimate=pl.CostEstimate(flops=4 * TOK * HID * VOC, bytes_accessed=400 * MIB, transcendentals=2 * TOK * VOC),
        name="head",
    )(hid, lab, w)


def _cols(j, width=PIECE):
    return pl.ds(pl.multiple_of(j * width, width), width)


def _dhead_kernel(
    x_hbm, g_hbm, s_hbm, a_hbm, o_hbm, t_hbm,
    gv, xb, ob, acc, sv, av, x_sem, g_sem, o_sem, s_sem, a_sem, t_sem, f_sem,
):
    blocks = HID // PIECE
    rows = BLK // 4

    def xload(b):
        return _copy(x_hbm.at[:, _cols(b)], xb.at[_odd(b)], x_sem.at[_odd(b)])

    def gload(j):
        return _copy(g_hbm.at[:, _cols(j)], gv.at[:, _cols(j)], g_sem.at[j])

    def ostore(b, n):
        return _copy(ob.at[n], o_hbm.at[_cols(b), _cols(n, HALF)], o_sem.at[n])

    def dot(lhs, rhs):
        return lax.dot_general(lhs, rhs, FIRST_DIMS, preferred_element_type=F32).astype(BF16)

    def terms(p):
        slot = _odd(p)
        src = _cols(p, rows)
        return _copy(s_hbm.at[src], sv.at[slot], s_sem.at[slot]), _copy(a_hbm.at[src], av.at[slot], a_sem.at[slot])

    def tstore(p):
        return _copy(sv.at[_odd(p)], t_hbm.at[_cols(p, rows)], t_sem.at[_odd(p)])

    def part(h):
        tokens = pl.ds(h * HALF, HALF)
        return (
            _copy(x_hbm.at[tokens, _cols(0)], xb.at[0, tokens], f_sem.at[h, 0]),
            _copy(g_hbm.at[tokens, _cols(0)], gv.at[tokens, _cols(0)], f_sem.at[h, 1]),
        )

    def part_dot(h):
        tokens = slice(h * HALF, (h + 1) * HALF)
        return lax.dot_general(
            xb[0, tokens, :], gv[tokens, :PIECE], FIRST_DIMS, preferred_element_type=F32
        )

    for h in PAIR:
        for copy in part(h):
            copy.start()
    for copy in part(0):
        copy.wait()
    gload(1).start()

    @pl.when(lax.axis_index("tp") < 8)
    def _():
        acc[...] = part_dot(0)

    for copy in part(1):
        copy.wait()
    gload(2).start()

    @pl.when(lax.axis_index("tp") < 8)
    def _():
        ob[0, :, :PIECE] = (acc[...] + part_dot(1)).astype(BF16)

    def first(j, carry):
        gload(j).wait()
        gload(2 * j + 1).start()

        @pl.when(j < 3)
        def _():
            gload(2 * j + 2).start()

        ob[0, :, _cols(j)] = dot(xb[0], gv[:, _cols(j)])
        return carry

    lax.fori_loop(1, 4, first, 0)
    ostore(0, 0).start()
    xload(1).start()
    for j in range(4, 8):
        gload(j).wait()

    def block(b, carry):
        @pl.when(b > 0)
        def _():
            xload(b).wait()

        @pl.when((b > 0) & (b < blocks - 1))
        def _():
            xload(b + 1).start()

        @pl.when((b > 1) & (b < 6))
        def _():
            for copy in terms(b - 2):
                copy.wait()
            sv[_odd(b)] = sv[_odd(b)] + av[_odd(b)]
            tstore(b - 2).start()

        @pl.when((b > 0) & (b < 5))
        def _():
            pl.when(b > 2)(lambda: tstore(b - 3).wait())
            for copy in terms(b - 1):
                copy.start()

        def half(n, carry):
            pl.when(b > 0)(lambda: ostore(b - 1, n).wait())

            @pl.when(b < blocks)
            def _():
                ob[n] = dot(xb[_odd(b)], gv[:, _cols(n, HALF)])

            ostore(b, n).start()
            return carry

        return lax.fori_loop(jnp.where(b == 0, 1, 0), 2, half, carry)

    _loop(blocks, block)
    for n in PAIR:
        ostore(blocks - 1, n).wait()
        tstore(n).wait()


def _dhead(xall, gall, s_self, r1a):
    hbm = pl.BlockSpec(memory_space=ANY)
    dma = pltpu.SemaphoreType.DMA
    return pl.pallas_call(
        _dhead_kernel,
        in_specs=[hbm] * 4,
        out_specs=(hbm, hbm),
        out_shape=(jax.ShapeDtypeStruct((HID, VOC), BF16), jax.ShapeDtypeStruct((BLK, HID), F32)),
        scratch_shapes=[
            pltpu.VMEM((TOK, VOC), BF16),
            pltpu.VMEM((2, TOK, PIECE), BF16),
            pltpu.VMEM((2, PIECE, HALF), BF16),
            pltpu.VMEM((PIECE, PIECE), F32),
            pltpu.VMEM((2, BLK // 4, HID), F32),
            pltpu.VMEM((2, BLK // 4, HID), F32),
            dma(TWO),
            dma((8,)),
            dma(TWO),
            dma(TWO),
            dma(TWO),
            dma(TWO),
            dma(TWO + TWO),
        ],
        compiler_params=pltpu.CompilerParams(vmem_limit_bytes=60 * MIB),
        cost_estimate=pl.CostEstimate(flops=2 * TOK * HID * VOC, bytes_accessed=200 * MIB, transcendentals=0),
        name="dhead",
    )(xall, gall, s_self, r1a)


def _final_kernel(t_hbm, s_hbm, b_hbm, r_hbm, l_ref, o_hbm, loss_ref, terms, ov, in_sem, o_sem):
    rows = PIECE // SUB
    ahead = 6
    half = SUB // 2

    def load(t, ref, i, dst):
        return _copy(ref.at[_cols(i, rows)], terms.at[t, _cols(dst, rows)], in_sem.at[t, dst])

    def start(i):
        @pl.when(i < half)
        def _():
            load(0, t_hbm, i, i).start()

        @pl.when(i >= half)
        def _():
            load(0, s_hbm, i, i).start()
            load(1, b_hbm, i - half, i).start()

        load(2, r_hbm, i, i).start()

    def begin(i, carry):
        start(i)
        return carry

    _loop(ahead, begin)
    loss_ref[0] = l_ref[0, 0]

    def add(i, carry):
        rs = _cols(i, rows)
        load(0, s_hbm, i, i).wait()
        load(2, r_hbm, i, i).wait()
        pl.when(i < SUB - ahead)(lambda: start(i + ahead))

        @pl.when(i < half)
        def _():
            ov[rs, :] = (terms[0, rs, :] + terms[2, rs, :]).astype(BF16)

        @pl.when(i >= half)
        def _():
            load(1, b_hbm, i - half, i).wait()
            ov[rs, :] = (terms[0, rs, :] + terms[1, rs, :] + terms[2, rs, :]).astype(BF16)

        _copy(ov.at[rs], o_hbm.at[rs], o_sem).start()
        return carry

    _loop(SUB, add)
    _copy(ov, o_hbm, o_sem).wait()


def _final(t, s_self, r1b, r2, loss):
    hbm = pl.BlockSpec(memory_space=ANY)
    dma = pltpu.SemaphoreType.DMA
    return pl.pallas_call(
        _final_kernel,
        in_specs=[hbm] * 4 + [pl.BlockSpec(memory_space=pltpu.VMEM)],
        out_specs=(hbm, pl.BlockSpec(memory_space=pltpu.SMEM)),
        out_shape=(jax.ShapeDtypeStruct((PIECE, HID), BF16), jax.ShapeDtypeStruct((1,), F32)),
        scratch_shapes=[
            pltpu.VMEM((3, PIECE, HID), F32),
            pltpu.VMEM((PIECE, HID), BF16),
            dma((3, SUB)),
            dma(()),
        ],
        compiler_params=pltpu.CompilerParams(vmem_limit_bytes=62 * MIB),
        cost_estimate=pl.CostEstimate(flops=3 * PIECE * HID, bytes_accessed=24 * MIB, transcendentals=0),
        name="final",
    )(t, s_self, r1b, r2, loss)


def solution(mesh):
    def device(y, x, core):
        return (y % 2) * 4 + (x % 2) * 2 + core

    first, second = [], []
    for yy in PAIR:
        for xx in PAIR:
            along_x = [(device(yy, xx, k), device(yy, xx + 1, k)) for k in PAIR]
            along_y = [(device(yy, xx, k), device(yy + 1, xx, k)) for k in PAIR]
            first += [along_x[0], along_y[1]]
            second += [along_y[0], along_x[1]]

    def local_step(hid, w, lab):
        xall, gall, s_n1b, s_self, y2, r1a, loss = _head(hid, lab.reshape(4, LANE), w)[:7]
        r2 = lax.ppermute(y2, "tp", second)
        r1b = lax.ppermute(s_n1b, "tp", first)
        d_head, t = _dhead(xall, gall, s_self, r1a)
        d_hidden, mean_loss = _final(t, s_self, r1b, r2, loss)
        return mean_loss, d_hidden, d_head

    return jax.shard_map(
        local_step,
        mesh=mesh,
        in_specs=(P(("dp", "tp"), None), P(None, "tp"), P(("dp", "tp"))),
        out_specs=(P("dp"), P(("dp", "tp"), None), P("dp", "tp")),
        check_vma=False,
    )
```

```python
import functools

import jax
import jax.numpy as jnp
from jax import lax
from jax.experimental import pallas as pl
from jax.experimental.pallas import tpu as pltpu
from jax.sharding import PartitionSpec as P

F32, BF16, I32 = jnp.float32, jnp.bfloat16, jnp.int32
MESH = pl.DeviceIdType.MESH
ANY = pl.ANY

TOK = 4096
HID = 4096
VOC = 4096
BLK = 256
HALF = 2048
NBLK = TOK // BLK
LANE = 128
MIB = 1 << 20
TWO = (2,)
PAIR = (0, 1)
TILE = (8, LANE)
SUB = 16
FIRST_DIMS = (((0,), (0,)), ((), ()))
FOUR = range(4)
OTHERS = range(1, 8)
SEVEN = pl.ds(0, 7)
LATE = 9
PIECE = 512
INV = 1.0 / TOK


def _div(a, b):
    return lax.div(jnp.int32(a), jnp.int32(b))


def _rem(a, b):
    return lax.rem(jnp.int32(a), jnp.int32(b))


def _odd(a):
    return _rem(a, 2)


def _loop(count, body):
    lax.fori_loop(0, count, body, 0)


def _copy(src, dst, sem):
    return pltpu.make_async_copy(src, dst, sem)


def _send(src, dst, send_sem, recv_sem, dev):
    return pltpu.make_async_remote_copy(
        src_ref=src, dst_ref=dst, send_sem=send_sem, recv_sem=recv_sem, device_id={"tp": dev}, device_id_type=MESH
    )


def _product(lhs, rhs, put, jobs, transposed):
    pl.when(lax.axis_index("tp") < 8)(functools.partial(_pieces, lhs, rhs, put, jobs, transposed))


def _pieces(lhs, rhs, put, jobs, transposed):
    dims = (((1,), (1,)), ((), ())) if transposed else (((1,), (0,)), ((), ()))
    pieces = HALF // PIECE
    deep = HID // BLK
    for nt in range(pieces):
        acc = None
        for kt in range(deep):
            part = lax.dot_general(lhs(kt), rhs(nt, kt), dims, preferred_element_type=F32)
            acc = part if acc is None else acc + part
            if kt % 2:
                for job in jobs[(nt * deep + kt) // 2]:
                    job()
        put(nt, acc)


def _wide(v, times=HALF // LANE):
    return jnp.concatenate([v] * times, axis=1)


def _fold(v):
    width = v.shape[1] // 2
    while width >= LANE:
        v = v[:, :width] + v[:, width:]
        width //= 2
    return v


def _column(row):
    return jnp.transpose(jnp.broadcast_to(row, (LANE, LANE)))


def _head_kernel(
    x_hbm, lab_hbm, w_hbm,
    xall, gall, s_n1b, s_self, y2, r1a, loss_out,
    zst, s_d, s_n1a, s_n2, r1n2,
    wv, xg, ga, gb, zb, pbuf, rbuf, sbuf, ab, bb, cb, lab_v, la, lb, st_new, st_loc, st_all, ml, mk, sl, tl, comb, c_lab, c_top, c_scale, loss_acc,
    w_sem, lab_sem, labtx_sem, rx, tx, xl_sem, xs_sem, zo_sem, st_sem, sttx_sem,
    zi_sem, rr, ps, ss_sem, s1tx, r1s, r1as, ab_sem, cb_sem, g_sem,
):
    me = lax.axis_index("tp")
    chip = _div(me, 2)
    c = _odd(me)
    x = _odd(chip)
    y = _div(chip, 2)
    oc = 1 - c
    partner = me + 1 - 2 * c
    dx, dy = 2 - 4 * x, 4 - 8 * y
    n1 = me + oc * dx + c * dy
    n2 = me + c * dx + oc * dy
    n1kind = 1 + c

    def chip_of(kind):
        return chip + _odd(kind) * (1 - 2 * x) + _div(kind, 2) * (2 - 4 * y)

    def order(i, first, last):
        a = _div(i, 4)
        mid, end = _rem(_div(a + 1, 2), 2), _div(a, 3)
        kind = mid * (1 + _odd(i)) + first * (1 - mid) * (1 - end) + last * end
        return kind, mid * _div(i - 4, 2) + (1 - mid) * _rem(i, 4)

    def order1(i):
        return order(i, 0, 3)

    def order2(i):
        return order(i, 3, 0)

    def block_id(kind, q):
        return chip_of(kind) * 4 + q

    def xrows(kind, q, part):
        return xall.at[pl.ds(pl.multiple_of(block_id(kind, q) * BLK + part * LANE, LANE), LANE)]

    def xblock(kind, q):
        return xall.at[pl.ds(pl.multiple_of(block_id(kind, q) * BLK, BLK), BLK)]

    def own(q):
        return x_hbm.at[pl.ds(pl.multiple_of(q * LANE, LANE), LANE)]

    def rxs(kind, q, part):
        return rx.at[kind * 8 + q * 2 + part]

    def wcopy(j):
        cols = pl.ds(j * PIECE, PIECE)
        return _copy(w_hbm.at[:, cols], wv.at[:, cols], w_sem.at[j])

    _copy(own(0), xg.at[0, pl.ds(pl.multiple_of(c * LANE, LANE), LANE)], xl_sem.at[0]).start()
    for j in FOUR:
        wcopy(j).start()

    barrier = pltpu.get_barrier_semaphore()
    for d in OTHERS:
        pl.semaphore_signal(barrier, inc=1, device_id={"tp": _rem(me + d, 8)}, device_id_type=MESH)
    pl.semaphore_wait(barrier, 7)

    for d in OTHERS:
        _send(lab_hbm, lab_v.at[me], labtx_sem, lab_sem, _rem(me + d, 8)).start()
    _copy(lab_hbm, lab_v.at[me], lab_sem).start()
    for q in FOUR:
        _send(own(q), xrows(0, q, c), tx, rxs(0, q, c), partner).start()
    for q in FOUR:
        _send(own(q), xrows_at(xall, me, q), tx, rxs(n1kind, q, c), n1).start()
        _send(own(q), xrows_at(xall, me, q), tx, rxs(3 - n1kind, q, c), n2).start()

    def load_x(b):
        kind, q = order1(b)
        slot = _odd(b)

        @pl.when(kind == 0)
        def _():
            _copy(own(q), xg.at[slot, pl.ds(pl.multiple_of(c * LANE, LANE), LANE)], xl_sem.at[slot]).start()
            _copy(xrows(0, q, oc), xg.at[slot, pl.ds(pl.multiple_of(oc * LANE, LANE), LANE)], xl_sem.at[slot]).start()

        @pl.when(kind != 0)
        def _():
            _copy(xblock(kind, q), xg.at[slot], xl_sem.at[slot]).start()

    def wait_rows(kind, q, part):
        _copy(xrows(kind, q, part), xrows(kind, q, part), rxs(kind, q, part)).wait()

    def take_rows(kind, q):
        wait_rows(kind, q, c)
        _send(xrows(kind, q, c), xrows(kind, q, c), tx, rxs(kind, q, c), partner).start()

        @pl.when(kind == n1kind)
        def _():
            _send(xrows(kind, q, c), xrows(kind, q, c), tx, rxs(3, q, c), n2).start()

    def part_load(b, part):
        kind, q = order1(b)
        return _copy(xrows(kind, q, part), xg.at[_odd(b), pl.ds(pl.multiple_of(part * LANE, LANE), LANE)], xl_sem.at[_odd(b)])

    def zcopy(b, h):
        kind, q = order1(b)
        return _copy(zb.at[h], zst.at[block_id(kind, q), h], zo_sem.at[h])

    def own_store(b):
        slot = _odd(b)
        return _copy(xg.at[slot, pl.ds(pl.multiple_of(c * LANE, LANE), LANE)], xrows(0, _rem(b, 4), c), xs_sem.at[slot])

    def label_column(blk, part):
        return _column(lab_v[2 * _div(blk, 4) + part, pl.ds(_rem(blk, 4), 1), :])

    def lane_stats(col, h, r):
        rows = pl.ds(r, 8)
        z = zb[h, rows, :]
        m = ml[h, rows, :]
        hit = _wide(col[rows, :] - (me * VOC + h * HALF)) == lax.broadcasted_iota(I32, (8, HALF), 1)
        s = _fold(jnp.exp(z - _wide(m)))
        t = _fold(jnp.where(hit, z, 0.0))
        if h == 1:
            m0 = mk[0, rows, :]
            mm = jnp.maximum(m0, m)
            s = sl[0, rows, :] * jnp.exp(m0 - mm) + s * jnp.exp(m - mm)
            t = tl[0, rows, :] + t
            m = mm
        mk[h, rows, :] = m
        sl[h, rows, :] = s
        tl[h, rows, :] = t

    def label_columns(blk, col, part):
        col[pl.ds(part * LANE, LANE), :] = label_column(blk, part)

    def row_stats(part):
        rows = pl.ds(part * LANE, LANE)
        m = jnp.transpose(mk[1, rows, :])
        top = jnp.max(m, axis=0, keepdims=True)
        st_new[part : part + 1, :] = top
        st_new[2 + part : 3 + part, :] = jnp.sum(jnp.transpose(sl[1, rows, :]) * jnp.exp(m - top), axis=0, keepdims=True)
        st_new[4 + part : 5 + part, :] = jnp.sum(jnp.transpose(tl[1, rows, :]), axis=0, keepdims=True)

    def entry(kind, q):
        diagonal = _div(kind, 3)
        return diagonal * (NBLK + q) + (1 - diagonal) * block_id(kind, q)

    def send_stats(kind, q):
        def start(dev):
            _send(st_loc.at[block_id(kind, q)], st_all.at[NBLK + q, me], sttx_sem, st_sem.at[q], dev).start()

        for core in PAIR:
            dev = 2 * chip_of(3 - kind) + core
            pl.when(dev != me)(functools.partial(start, dev))

    def send_late():
        for d in OTHERS:
            _send(st_loc, st_all.at[pl.ds(0, NBLK), me], sttx_sem, st_sem.at[4], _rem(me + d, 8)).start()

    def keep_stats(kind, q):
        st_loc[block_id(kind, q)] = st_new[...]
        st_all[block_id(kind, q), me] = st_new[...]
        st_all[entry(kind, q), me] = st_new[...]

    def combine(place):
        top = st_all[place, 0, 0:2, :]
        for d in OTHERS:
            top = jnp.maximum(top, st_all[place, d, 0:2, :])
        s = jnp.zeros((2, LANE), F32)
        t = jnp.zeros((2, LANE), F32)
        for d in range(8):
            s = s + st_all[place, d, 2:4, :] * jnp.exp(st_all[place, d, 0:2, :] - top)
            t = t + st_all[place, d, 4:6, :]
        comb[0:2, :] = top
        comb[2:4, :] = INV / s
        return top + jnp.log(s) - t

    def stats_arrived(q):
        _copy(st_all.at[0, SEVEN], st_all.at[0, SEVEN], st_sem.at[q]).wait()

    def late_arrived():
        _copy(st_all.at[pl.ds(0, 14)], st_all.at[pl.ds(0, 14)], st_sem.at[4]).wait()

    def columns(blk, par, part):
        rows = pl.ds(part * LANE, LANE)
        c_lab[par, rows, :] = label_column(blk, part)
        c_top[par, rows, :] = _column(comb[part : part + 1, :])
        c_scale[par, rows, :] = _column(comb[2 + part : 3 + part, :])

    def gradient(src, n, par, r, j):
        rows = pl.ds(pl.multiple_of(r, SUB), SUB)
        col = c_lab[par, rows, :] - (me * VOC + n * HALF + j)
        p = jnp.exp(src[n, rows, j : j + PIECE] - _wide(c_top[par, rows, :], 4)) * _wide(c_scale[par, rows, :], 4)
        g = jnp.where(_wide(col, 4) == lax.broadcasted_iota(I32, (SUB, PIECE), 1), p - INV, p)
        gbufs[par][rows, n * HALF + j : n * HALF + j + PIECE] = g.astype(BF16)

    def gradient_jobs(src, n, par):
        return [functools.partial(gradient, src, n, par, r, j) for r in range(0, BLK, SUB) for j in range(0, HALF, PIECE)]

    gbufs = (ga, gb)

    def gstore(k, par):
        kind, q = order2(k)
        return _copy(gbufs[par], gall.at[pl.ds(pl.multiple_of(block_id(kind, q) * BLK, BLK), BLK)], g_sem.at[par])

    def zload(k, dst, n):
        kind, q = order2(k)
        return _copy(zst.at[block_id(kind, q), n], dst.at[n], zi_sem.at[n])

    first_kind, first_q = order2(me * 0)
    first_blk = block_id(first_kind, first_q)

    def logits(b, h, jobs):
        slot = _odd(b)
        def put(nt, z):
            zb[h, :, nt * PIECE : (nt + 1) * PIECE] = z
            m = z[:, :LANE]
            for j in range(1, 4):
                m = jnp.maximum(m, z[:, j * LANE : (j + 1) * LANE])
            if nt:
                m = jnp.maximum(m, ml[h])
            ml[h] = m

        _product(
            lambda kt: xg[slot, :, kt * BLK : (kt + 1) * BLK],
            lambda nt, kt: wv[kt * BLK : (kt + 1) * BLK, h * HALF + nt * PIECE : h * HALF + (nt + 1) * PIECE],
            put,
            jobs,
            False,
        )

    wait_rows(0, 0, oc)
    _copy(xrows(0, 0, oc), xg.at[0, pl.ds(pl.multiple_of(oc * LANE, LANE), LANE)], xl_sem.at[0]).start()
    _copy(lab_v, lab_v, lab_sem).wait()
    for j in FOUR:
        wcopy(j).wait()
    for j in FOUR:
        wcopy(4 + j).start()

    def phase1(i, carry):
        slot = _odd(i)
        kind, q = order1(i)
        kprev, qprev = order1(_rem(i + NBLK - 2, NBLK))
        kn, qn = order1(_rem(i + 1, NBLK))

        @pl.when((i == LATE + 1) | (i == NBLK - 1))
        def _():
            wait_rows(kind, q, oc)
            part_load(i, oc).start()

        @pl.when(i > 0)
        def _():
            zcopy(i - 1, 1).start()
            zcopy(i - 1, 0).wait()

        @pl.when(i > 1)
        def _():
            keep_stats(kprev, qprev)

        @pl.when(i == NBLK - 2)
        def _():
            zload(0, pbuf, 0).start()
            zload(0, pbuf, 1).start()

        @pl.when(i == NBLK - 1)
        def _():
            stats_arrived(0)
            loss_acc[...] = combine(entry(first_kind, first_q))
            for part in PAIR:
                columns(first_blk, 0, part)
            for n in PAIR:
                zload(0, pbuf, n).wait()

                def some(r, carry, n=n):
                    for j in range(0, HALF, PIECE):
                        gradient(pbuf, n, 0, r * SUB, j)
                    return carry

                _loop(SUB, some)

            gstore(0, 0).start()

        @pl.when((i >= 3) & (i != LATE) & (i < NBLK - 2))
        def _():
            take_rows(kn, qn)

        _copy(xg.at[slot], xg.at[slot], xl_sem.at[slot]).wait()

        @pl.when(i < 4)
        def _():
            own_store(i).start()

        jobs = [[] for _ in range(32)]
        for r in range(32):
            jobs[min(r + 1, 31)].append(functools.partial(lane_stats, la, 1, r * 8))
        for part in PAIR:
            jobs[4 + 4 * part].append(functools.partial(label_columns, block_id(kind, q), lb, part))
        logits(i, 0, jobs)

        zcopy(i, 0).start()

        @pl.when(i == 0)
        def _():
            for j in FOUR:
                wcopy(4 + j).wait()

        @pl.when(i > 0)
        def _():
            zcopy(i - 1, 1).wait()

        @pl.when(i > 1)
        def _():
            send_stats(kprev, qprev)

        @pl.when((i == LATE) | (i == NBLK - 2))
        def _():
            take_rows(kn, qn)
            part_load(i + 1, c).start()

        @pl.when((i != LATE) & (i < NBLK - 2))
        def _():
            wait_rows(kn, qn, oc)

            @pl.when((i >= 1) & (i < 5))
            def _():
                own_store(i - 1).wait()

            load_x(i + 1)

        la[...] = lb[...]
        jobs = [[] for _ in range(32)]
        for r in range(32):
            jobs[min(r + 1, 31)].append(functools.partial(lane_stats, lb, 0, r * 8))
        for part in PAIR:
            jobs[8 + 8 * part].append(functools.partial(row_stats, part))
        logits(i, 1, jobs)
        return carry

    _loop(NBLK, phase1)
    last = NBLK - 1
    klast, qlast = order1(jnp.int32(last))
    kprev, qprev = order1(jnp.int32(last - 1))
    zcopy(last, 1).start()
    zcopy(last, 0).wait()
    zload(1, zb, 0).start()
    keep_stats(kprev, qprev)
    for r in range(32):
        lane_stats(la, 1, r * 8)
    send_stats(kprev, qprev)
    for part in PAIR:
        row_stats(part)
    keep_stats(klast, qlast)
    zcopy(last, 1).wait()
    zload(1, zb, 1).start()
    send_stats(klast, qlast)
    second_kind, second_q = order2(jnp.int32(1))
    second_blk = block_id(second_kind, second_q)
    stats_arrived(1)
    loss_acc[...] += combine(entry(second_kind, second_q))
    for part in PAIR:
        columns(second_blk, 1, part)

    def tile(ref, q, n):
        return ref.at[pl.ds(pl.multiple_of(q * LANE, LANE), LANE), pl.ds(pl.multiple_of(n * HALF, HALF), HALF)]

    def spair(k, n):
        return _send(
            pbuf.at[n, pl.ds(pl.multiple_of(oc * LANE, LANE), LANE)], rbuf.at[_odd(k + 2), n], ps.at[n], rr.at[_odd(k + 2) * 2 + n], partner
        )

    def sstore_start(k, n):
        kind, q = order2(k)
        sem = ss_sem.at[n]

        @pl.when(kind == 3)
        def _():
            _copy(sbuf.at[n], tile(s_d, q, n), sem).start()

        @pl.when((kind == n1kind) & (q < 2))
        def _():
            _copy(sbuf.at[n], tile(s_n1a, _odd(q), n), sem).start()

        @pl.when((kind == n1kind) & (q >= 2))
        def _():
            _copy(sbuf.at[n], tile(s_n1b, _odd(q), n), sem).start()

        @pl.when(kind == 3 - n1kind)
        def _():
            _copy(sbuf.at[n], tile(s_n2, q, n), sem).start()

        @pl.when(kind == 0)
        def _():
            _copy(sbuf.at[n], tile(s_self, q, n), sem).start()

    def sstore_done(k, n):
        kind, q = order2(k)
        _copy(sbuf.at[n], tile(s_d, 0, n), ss_sem.at[n]).wait()

        @pl.when(kind == 3)
        def _():
            _send(tile(s_d, q, n), tile(r1n2, q, n), s1tx, r1s.at[q * 2 + n], n1).start()

        @pl.when((kind == n1kind) & (q < 2))
        def _():
            _send(tile(s_n1a, _odd(q), n), tile(r1a, _odd(q), n), s1tx, r1as.at[_odd(q) * 2 + n], n1).start()

    def stage2_load(q, n):
        _copy(tile(r1n2, q, n), tile(r1n2, q, n), r1s.at[q * 2 + n]).wait()
        _copy(tile(s_n2, q, n), ab.at[n], ab_sem.at[n * 2]).start()
        _copy(tile(r1n2, q, n), bb.at[n], ab_sem.at[n * 2 + 1]).start()

    def pair_sum(k, n, r):
        sbuf[n, pl.ds(r, SUB), :] = pbuf[n, pl.ds(pl.multiple_of(c * LANE + r, SUB), SUB), :] + rbuf[_odd(k + 2), n, pl.ds(r, SUB), :]

    def stage2_sum(n, r):
        cb[n, pl.ds(r, SUB), :] = ab[n, pl.ds(r, SUB), :] + bb[n, pl.ds(r, SUB), :]

    def rwait(k, n):
        _copy(rbuf.at[_odd(k + 2), n], rbuf.at[_odd(k + 2), n], rr.at[_odd(k + 2) * 2 + n]).wait()

    def loss_part(k, place):
        loss_acc[...] += jnp.where(k < NBLK - 2, combine(place), 0.0)

    def sub(k, cur):
        nxt = 1 - cur
        kind2, q2 = order2(_rem(k + 2, NBLK))
        blk2 = block_id(kind2, q2)

        def trip(n):
            @pl.when(k < NBLK - 1)
            def _():
                zload(k + 1, zb, n).wait()

            @pl.when(k >= 1)
            def _():
                rwait(k - 1, n)
                spair(k - 1, n).wait_send()
                if n == 0:
                    gstore(k - 1, nxt).wait()

            if n == 0:

                @pl.when(k < 2)
                def _():
                    stats_arrived(k + 2)

                @pl.when(k == 2)
                def _():
                    late_arrived()

            @pl.when(k >= 12)
            def _():
                _copy(tile(s_n2, 0, n), ab.at[n], ab_sem.at[n * 2]).wait()
                _copy(tile(r1n2, 0, n), bb.at[n], ab_sem.at[n * 2 + 1]).wait()

            @pl.when(k >= 13)
            def _():
                _copy(cb.at[n], tile(y2, 0, n), cb_sem.at[n]).wait()

            jobs = [[] for _ in range(32)]
            for r in range(8):
                jobs[2 + r * 3 // 5].append(functools.partial(pair_sum, k - 1, n, r * SUB))
                jobs[10 + r * 5 // 2].append(functools.partial(stage2_sum, n, r * SUB))
            for r, job in enumerate(gradient_jobs(zb, n, nxt)):
                jobs[2 + r * 9 // 20].append(job)
            if n == 0:
                jobs[8].append(lambda: loss_part(k, entry(kind2, q2)))
            else:
                for part in PAIR:
                    jobs[8 + 8 * part].append(functools.partial(columns, blk2, cur, part))

            def put(nt, acc):
                pbuf[n, :, nt * PIECE : (nt + 1) * PIECE] = acc

            _product(
                lambda kt: gbufs[cur][:, kt * BLK : (kt + 1) * BLK],
                lambda nt, kt: wv[pl.ds(pl.multiple_of(n * HALF + nt * PIECE, PIECE), PIECE), kt * BLK : (kt + 1) * BLK],
                put,
                jobs,
                True,
            )

            spair(k, n).start()

            if cur == n == 0:
                pl.when(k == 0)(send_late)

            @pl.when(k < NBLK - 2)
            def _():
                zload(k + 2, zb, n).start()

            @pl.when(k >= 2)
            def _():
                sstore_done(k - 2 + n, 1 - n)

            @pl.when(k >= 1)
            def _():
                sstore_start(k - 1, n)

            if n == 0:
                @pl.when(k == 1)
                def _():
                    sstore_done(k - 1, n)

            @pl.when(k >= 12)
            def _():
                _copy(cb.at[n], tile(y2, k - 12, n), cb_sem.at[n]).start()

            @pl.when((k >= 11) & (k < NBLK - 1))
            def _():
                stage2_load(k - 11, n)


        trip(0)
        trip(1)

        @pl.when(k < NBLK - 1)
        def _():
            gstore(k + 1, nxt).start()

    def pair(p, carry):
        sub(2 * p, 0)
        sub(2 * p + 1, 1)
        return carry

    _loop(NBLK // 2, pair)

    kl = jnp.int32(NBLK - 1)
    for n in PAIR:
        rwait(kl, n)
        spair(kl, n).wait_send()
        if n == 0:
            sstore_done(kl - 1, 1)
        for r in range(8):
            pair_sum(kl, n, r * SUB)
        sstore_start(kl, n)
    for n in PAIR:
        sstore_done(kl, n)
    gstore(kl, 1).wait()
    for n in PAIR:
        _copy(cb.at[n], tile(y2, 0, n), cb_sem.at[n]).wait()

    loss_out[...] = jnp.full(TILE, jnp.sum(loss_acc[...]) * INV, F32)

    for i in FOUR:
        _copy(tile(r1a, i // 2, i % 2), tile(r1a, i // 2, i % 2), r1as.at[i]).wait()
    _copy(s_d, s_d, s1tx).wait()
    _copy(s_n1a, s_n1a, s1tx).wait()
    _copy(xall.at[pl.ds(0, 28 * LANE)], xall.at[pl.ds(0, 28 * LANE)], tx).wait()
    for d in range(7):
        _copy(lab_v.at[d], lab_v.at[d], labtx_sem).wait()
        _copy(st_loc, st_loc, sttx_sem).wait()
    for d in FOUR:
        _copy(st_all.at[d, SEVEN], st_all.at[d, SEVEN], sttx_sem).wait()


def xrows_at(xall, dev, q):
    return xall.at[pl.ds(pl.multiple_of((dev // 2) * 1024 + q * BLK + (dev % 2) * LANE, LANE), LANE)]


def _head(hid, lab, w):
    hbm = pl.BlockSpec(memory_space=ANY)
    sd = jax.ShapeDtypeStruct
    dma = pltpu.SemaphoreType.DMA
    vmem = pltpu.VMEM
    quarter = (LANE, HALF)
    return pl.pallas_call(
        _head_kernel,
        out_shape=(
            sd((TOK, HID), BF16),
            sd((TOK, VOC), BF16),
            sd((256, HID), F32),
            sd((PIECE, HID), F32),
            sd((PIECE, HID), F32),
            sd((256, HID), F32),
            sd(TILE, F32),
            sd((NBLK, 2, BLK, HALF), F32),
            sd((PIECE, HID), F32),
            sd((256, HID), F32),
            sd((PIECE, HID), F32),
            sd((PIECE, HID), F32),
        ),
        in_specs=[hbm] * 3,
        out_specs=(hbm,) * 6 + (pl.BlockSpec(memory_space=vmem),) + (hbm,) * 5,
        scratch_shapes=[
            vmem((HID, VOC), BF16),
            vmem((2, BLK, HID), BF16),
            vmem((BLK, VOC), BF16),
            vmem((BLK, VOC), BF16),
            vmem((2, BLK, HALF), F32),
            vmem((2, BLK, HALF), F32),
            vmem((2, 2) + quarter, F32),
            vmem(TWO + quarter, F32),
            vmem(TWO + quarter, F32),
            vmem(TWO + quarter, F32),
            vmem(TWO + quarter, F32),
            vmem((8, 4, LANE), I32),
            vmem((BLK, LANE), I32),
            vmem((BLK, LANE), I32),
            vmem(TILE, F32),
            vmem((NBLK,) + TILE, F32),
            vmem((NBLK + 4, 8) + TILE, F32),
            vmem((2, BLK, LANE), F32),
            vmem((2, BLK, LANE), F32),
            vmem((2, BLK, LANE), F32),
            vmem((2, BLK, LANE), F32),
            vmem(TILE, F32),
            vmem((2, BLK, LANE), I32),
            vmem((2, BLK, LANE), F32),
            vmem((2, BLK, LANE), F32),
            vmem((2, LANE), F32),
            dma((8,)),
            dma(()),
            dma(()),
            dma((32,)),
            dma(()),
            dma(TWO),
            dma(TWO),
            dma(TWO),
            dma((5,)),
            dma(()),
            dma(TWO),
            dma((4,)),
            dma(TWO),
            dma(TWO),
            dma(()),
            dma((8,)),
            dma((4,)),
            dma((4,)),
            dma(TWO),
            dma(TWO),
        ],
        compiler_params=pltpu.CompilerParams(collective_id=0, has_side_effects=True, vmem_limit_bytes=67_043_328),
        cost_estimate=pl.CostEstimate(flops=4 * TOK * HID * VOC, bytes_accessed=400 * MIB, transcendentals=2 * TOK * VOC),
        name="head",
    )(hid, lab, w)


def _cols(j, width=PIECE):
    return pl.ds(pl.multiple_of(j * width, width), width)


def _dhead_kernel(
    x_hbm, g_hbm, s_hbm, a_hbm, o_hbm, t_hbm,
    gv, xb, ob, acc, sv, av, x_sem, g_sem, o_sem, s_sem, a_sem, t_sem, f_sem,
):
    blocks = HID // PIECE
    rows = BLK // 4

    def xload(b):
        return _copy(x_hbm.at[:, _cols(b)], xb.at[_odd(b)], x_sem.at[_odd(b)])

    def gload(j):
        return _copy(g_hbm.at[:, _cols(j)], gv.at[:, _cols(j)], g_sem.at[j])

    def ostore(b, n):
        return _copy(ob.at[n], o_hbm.at[_cols(b), _cols(n, HALF)], o_sem.at[n])

    def dot(lhs, rhs):
        return lax.dot_general(lhs, rhs, FIRST_DIMS, preferred_element_type=F32).astype(BF16)

    def terms(p):
        slot = _odd(p)
        src = _cols(p, rows)
        return _copy(s_hbm.at[src], sv.at[slot], s_sem.at[slot]), _copy(a_hbm.at[src], av.at[slot], a_sem.at[slot])

    def tstore(p):
        return _copy(sv.at[_odd(p)], t_hbm.at[_cols(p, rows)], t_sem.at[_odd(p)])

    def part(h):
        tokens = pl.ds(h * HALF, HALF)
        return (
            _copy(x_hbm.at[tokens, _cols(0)], xb.at[0, tokens], f_sem.at[h, 0]),
            _copy(g_hbm.at[tokens, _cols(0)], gv.at[tokens, _cols(0)], f_sem.at[h, 1]),
        )

    def part_dot(h):
        tokens = slice(h * HALF, (h + 1) * HALF)
        return lax.dot_general(
            xb[0, tokens, :], gv[tokens, :PIECE], FIRST_DIMS, preferred_element_type=F32
        )

    for h in PAIR:
        for copy in part(h):
            copy.start()
    for copy in part(0):
        copy.wait()
    gload(1).start()

    @pl.when(lax.axis_index("tp") < 8)
    def _():
        acc[...] = part_dot(0)

    for copy in part(1):
        copy.wait()
    gload(2).start()

    @pl.when(lax.axis_index("tp") < 8)
    def _():
        ob[0, :, :PIECE] = (acc[...] + part_dot(1)).astype(BF16)

    def first(j, carry):
        gload(j).wait()
        gload(2 * j + 1).start()

        @pl.when(j < 3)
        def _():
            gload(2 * j + 2).start()

        ob[0, :, _cols(j)] = dot(xb[0], gv[:, _cols(j)])
        return carry

    lax.fori_loop(1, 4, first, 0)
    ostore(0, 0).start()
    xload(1).start()
    for j in FOUR:
        gload(4 + j).wait()

    def block(b, carry):
        @pl.when(b > 0)
        def _():
            xload(b).wait()

        @pl.when((b > 0) & (b < blocks - 1))
        def _():
            xload(b + 1).start()

        @pl.when((b > 1) & (b < 6))
        def _():
            for copy in terms(b - 2):
                copy.wait()
            sv[_odd(b)] = sv[_odd(b)] + av[_odd(b)]
            tstore(b - 2).start()

        @pl.when((b > 0) & (b < 5))
        def _():
            pl.when(b > 2)(lambda: tstore(b - 3).wait())
            for copy in terms(b - 1):
                copy.start()

        def half(n, carry):
            pl.when(b > 0)(lambda: ostore(b - 1, n).wait())

            @pl.when(b < blocks)
            def _():
                ob[n] = dot(xb[_odd(b)], gv[:, _cols(n, HALF)])

            ostore(b, n).start()
            return carry

        return lax.fori_loop(jnp.where(b == 0, 1, 0), 2, half, carry)

    _loop(blocks, block)
    for n in PAIR:
        ostore(blocks - 1, n).wait()
        tstore(n).wait()


def _dhead(xall, gall, s_self, r1a):
    hbm = pl.BlockSpec(memory_space=ANY)
    dma = pltpu.SemaphoreType.DMA
    return pl.pallas_call(
        _dhead_kernel,
        in_specs=[hbm] * 4,
        out_specs=(hbm, hbm),
        out_shape=(jax.ShapeDtypeStruct((HID, VOC), BF16), jax.ShapeDtypeStruct((BLK, HID), F32)),
        scratch_shapes=[
            pltpu.VMEM((TOK, VOC), BF16),
            pltpu.VMEM((2, TOK, PIECE), BF16),
            pltpu.VMEM((2, PIECE, HALF), BF16),
            pltpu.VMEM((PIECE, PIECE), F32),
            pltpu.VMEM((2, BLK // 4, HID), F32),
            pltpu.VMEM((2, BLK // 4, HID), F32),
            dma(TWO),
            dma((8,)),
            dma(TWO),
            dma(TWO),
            dma(TWO),
            dma(TWO),
            dma(TWO + TWO),
        ],
        compiler_params=pltpu.CompilerParams(vmem_limit_bytes=60 * MIB),
        cost_estimate=pl.CostEstimate(flops=2 * TOK * HID * VOC, bytes_accessed=200 * MIB, transcendentals=0),
        name="dhead",
    )(xall, gall, s_self, r1a)


def _final_kernel(t_hbm, s_hbm, b_hbm, r_hbm, l_ref, o_hbm, loss_ref, terms, ov, in_sem, o_sem):
    rows = PIECE // SUB
    ahead = 6
    half = SUB // 2

    def load(t, ref, i, dst):
        return _copy(ref.at[_cols(i, rows)], terms.at[t, _cols(dst, rows)], in_sem.at[t, dst])

    def start(i):
        @pl.when(i < half)
        def _():
            load(0, t_hbm, i, i).start()

        @pl.when(i >= half)
        def _():
            load(0, s_hbm, i, i).start()
            load(1, b_hbm, i - half, i).start()

        load(2, r_hbm, i, i).start()

    def begin(i, carry):
        start(i)
        return carry

    _loop(ahead, begin)
    loss_ref[0] = l_ref[0, 0]

    def add(i, carry):
        rs = _cols(i, rows)
        load(0, s_hbm, i, i).wait()
        load(2, r_hbm, i, i).wait()
        pl.when(i < SUB - ahead)(lambda: start(i + ahead))

        @pl.when(i < half)
        def _():
            ov[rs, :] = (terms[0, rs, :] + terms[2, rs, :]).astype(BF16)

        @pl.when(i >= half)
        def _():
            load(1, b_hbm, i - half, i).wait()
            ov[rs, :] = (terms[0, rs, :] + terms[1, rs, :] + terms[2, rs, :]).astype(BF16)

        _copy(ov.at[rs], o_hbm.at[rs], o_sem).start()
        return carry

    _loop(SUB, add)
    _copy(ov, o_hbm, o_sem).wait()


def _final(t, s_self, r1b, r2, loss):
    hbm = pl.BlockSpec(memory_space=ANY)
    dma = pltpu.SemaphoreType.DMA
    return pl.pallas_call(
        _final_kernel,
        in_specs=[hbm] * 4 + [pl.BlockSpec(memory_space=pltpu.VMEM)],
        out_specs=(hbm, pl.BlockSpec(memory_space=pltpu.SMEM)),
        out_shape=(jax.ShapeDtypeStruct((PIECE, HID), BF16), jax.ShapeDtypeStruct((1,), F32)),
        scratch_shapes=[
            pltpu.VMEM((3, PIECE, HID), F32),
            pltpu.VMEM((PIECE, HID), BF16),
            dma((3, SUB)),
            dma(()),
        ],
        compiler_params=pltpu.CompilerParams(vmem_limit_bytes=62 * MIB),
        cost_estimate=pl.CostEstimate(flops=3 * PIECE * HID, bytes_accessed=24 * MIB, transcendentals=0),
        name="final",
    )(t, s_self, r1b, r2, loss)


def solution(mesh):
    def device(y, x, core):
        return (y % 2) * 4 + (x % 2) * 2 + core

    first, second = [], []
    for yy in PAIR:
        for xx in PAIR:
            along_x = [(device(yy, xx, k), device(yy, xx + 1, k)) for k in PAIR]
            along_y = [(device(yy, xx, k), device(yy + 1, xx, k)) for k in PAIR]
            first += [along_x[0], along_y[1]]
            second += [along_y[0], along_x[1]]

    def local_step(hid, w, lab):
        xall, gall, s_n1b, s_self, y2, r1a, loss = _head(hid, lab.reshape(4, LANE), w)[:7]
        r2 = lax.ppermute(y2, "tp", second)
        r1b = lax.ppermute(s_n1b, "tp", first)
        d_head, t = _dhead(xall, gall, s_self, r1a)
        d_hidden, mean_loss = _final(t, s_self, r1b, r2, loss)
        return mean_loss, d_hidden, d_head

    return jax.shard_map(
        local_step,
        mesh=mesh,
        in_specs=(P(("dp", "tp"), None), P(None, "tp"), P(("dp", "tp"))),
        out_specs=(P("dp"), P(("dp", "tp"), None), P("dp", "tp")),
        check_vma=False,
    )
```

```python
import functools

import jax
import jax.numpy as jnp
from jax import lax
from jax.experimental import pallas as pl
from jax.experimental.pallas import tpu as pltpu
from jax.sharding import PartitionSpec as P

F32, BF16, I32 = jnp.float32, jnp.bfloat16, jnp.int32
MESH = pl.DeviceIdType.MESH
ANY = pl.ANY

TOK = 4096
HID = 4096
VOC = 4096
BLK = 256
HALF = 2048
NBLK = TOK // BLK
LANE = 128
MIB = 1 << 20
TWO = (2,)
PAIR = (0, 1)
TILE = (8, LANE)
SUB = 16
FIRST_DIMS = (((0,), (0,)), ((), ()))
FOUR = range(4)
OTHERS = range(1, 8)
SEVEN = pl.ds(0, 7)
LATE = 9
PIECE = 512
INV = 1.0 / TOK


def _div(a, b):
    return lax.div(jnp.int32(a), jnp.int32(b))


def _rem(a, b):
    return lax.rem(jnp.int32(a), jnp.int32(b))


def _odd(a):
    return _rem(a, 2)


def _loop(count, body):
    lax.fori_loop(0, count, body, 0)


def _copy(src, dst, sem):
    return pltpu.make_async_copy(src, dst, sem)


def _send(src, dst, send_sem, recv_sem, dev):
    return pltpu.make_async_remote_copy(
        src_ref=src, dst_ref=dst, send_sem=send_sem, recv_sem=recv_sem, device_id={"tp": dev}, device_id_type=MESH
    )


def _product(lhs, rhs, put, jobs, transposed):
    pl.when(lax.axis_index("tp") < 8)(functools.partial(_pieces, lhs, rhs, put, jobs, transposed))


def _pieces(lhs, rhs, put, jobs, transposed):
    dims = (((1,), (1,)), ((), ())) if transposed else (((1,), (0,)), ((), ()))
    pieces = HALF // PIECE
    deep = HID // BLK
    for nt in range(pieces):
        acc = None
        for kt in range(deep):
            part = lax.dot_general(lhs(kt), rhs(nt, kt), dims, preferred_element_type=F32)
            acc = part if acc is None else acc + part
            if kt % 2:
                for job in jobs[(nt * deep + kt) // 2]:
                    job()
        put(nt, acc)


def _wide(v, times=HALF // LANE):
    return jnp.concatenate([v] * times, axis=1)


def _fold(v):
    width = v.shape[1] // 2
    while width >= LANE:
        v = v[:, :width] + v[:, width:]
        width //= 2
    return v


def _column(row):
    return jnp.transpose(jnp.broadcast_to(row, (LANE, LANE)))


def _head_kernel(
    x_hbm, lab_hbm, w_hbm,
    xall, gall, s_n1b, s_self, y2, r1a, loss_out,
    zst, s_d, s_n1a, s_n2, r1n2,
    wv, xg, ga, gb, zb, pbuf, rbuf, sbuf, ab, bb, cb, lab_v, la, lb, st_new, st_loc, st_all, ml, mk, sl, tl, comb, c_lab, c_top, c_scale, loss_acc,
    w_sem, lab_sem, labtx_sem, rx, tx, xl_sem, xs_sem, zo_sem, st_sem, sttx_sem,
    zi_sem, rr, ps, ss_sem, s1tx, r1s, r1as, ab_sem, cb_sem, g_sem,
):
    me = lax.axis_index("tp")
    chip = _div(me, 2)
    c = _odd(me)
    x = _odd(chip)
    y = _div(chip, 2)
    oc = 1 - c
    partner = me + 1 - 2 * c
    dx, dy = 2 - 4 * x, 4 - 8 * y
    n1 = me + oc * dx + c * dy
    n2 = me + c * dx + oc * dy
    n1kind = 1 + c

    def chip_of(kind):
        return chip + _odd(kind) * (1 - 2 * x) + _div(kind, 2) * (2 - 4 * y)

    def order(i, first, last):
        a = _div(i, 4)
        mid, end = _rem(_div(a + 1, 2), 2), _div(a, 3)
        kind = mid * (1 + _odd(i)) + first * (1 - mid) * (1 - end) + last * end
        return kind, mid * _div(i - 4, 2) + (1 - mid) * _rem(i, 4)

    def order1(i):
        return order(i, 0, 3)

    def order2(i):
        return order(i, 3, 0)

    def block_id(kind, q):
        return chip_of(kind) * 4 + q

    def xrows(kind, q, part):
        return xall.at[pl.ds(pl.multiple_of(block_id(kind, q) * BLK + part * LANE, LANE), LANE)]

    def xblock(kind, q):
        return xall.at[pl.ds(pl.multiple_of(block_id(kind, q) * BLK, BLK), BLK)]

    def own(q):
        return x_hbm.at[pl.ds(pl.multiple_of(q * LANE, LANE), LANE)]

    def rxs(kind, q, part):
        return rx.at[kind * 8 + q * 2 + part]

    def wcopy(j):
        cols = pl.ds(j * PIECE, PIECE)
        return _copy(w_hbm.at[:, cols], wv.at[:, cols], w_sem.at[j])

    _copy(own(0), xg.at[0, pl.ds(pl.multiple_of(c * LANE, LANE), LANE)], xl_sem.at[0]).start()
    for j in FOUR:
        wcopy(j).start()

    barrier = pltpu.get_barrier_semaphore()
    for d in OTHERS:
        pl.semaphore_signal(barrier, inc=1, device_id={"tp": _rem(me + d, 8)}, device_id_type=MESH)
    pl.semaphore_wait(barrier, 7)

    for d in OTHERS:
        _send(lab_hbm, lab_v.at[me], labtx_sem, lab_sem, _rem(me + d, 8)).start()
    _copy(lab_hbm, lab_v.at[me], lab_sem).start()
    for q in FOUR:
        _send(own(q), xrows(0, q, c), tx, rxs(0, q, c), partner).start()
    for q in FOUR:
        _send(own(q), xrows_at(xall, me, q), tx, rxs(n1kind, q, c), n1).start()
        _send(own(q), xrows_at(xall, me, q), tx, rxs(3 - n1kind, q, c), n2).start()

    def load_x(b):
        kind, q = order1(b)
        slot = _odd(b)

        @pl.when(kind == 0)
        def _():
            _copy(own(q), xg.at[slot, pl.ds(pl.multiple_of(c * LANE, LANE), LANE)], xl_sem.at[slot]).start()
            _copy(xrows(0, q, oc), xg.at[slot, pl.ds(pl.multiple_of(oc * LANE, LANE), LANE)], xl_sem.at[slot]).start()

        @pl.when(kind != 0)
        def _():
            _copy(xblock(kind, q), xg.at[slot], xl_sem.at[slot]).start()

    def wait_rows(kind, q, part):
        _copy(xrows(kind, q, part), xrows(kind, q, part), rxs(kind, q, part)).wait()

    def take_rows(kind, q):
        wait_rows(kind, q, c)
        _send(xrows(kind, q, c), xrows(kind, q, c), tx, rxs(kind, q, c), partner).start()

        @pl.when(kind == n1kind)
        def _():
            _send(xrows(kind, q, c), xrows(kind, q, c), tx, rxs(3, q, c), n2).start()

    def part_load(b, part):
        kind, q = order1(b)
        return _copy(xrows(kind, q, part), xg.at[_odd(b), pl.ds(pl.multiple_of(part * LANE, LANE), LANE)], xl_sem.at[_odd(b)])

    def zcopy(b, h):
        kind, q = order1(b)
        return _copy(zb.at[h], zst.at[block_id(kind, q), h], zo_sem.at[h])

    def own_store(b):
        slot = _odd(b)
        return _copy(xg.at[slot, pl.ds(pl.multiple_of(c * LANE, LANE), LANE)], xrows(0, _rem(b, 4), c), xs_sem.at[slot])

    def label_column(blk, part):
        return _column(lab_v[2 * _div(blk, 4) + part, pl.ds(_rem(blk, 4), 1), :])

    def lane_stats(col, h, r):
        rows = pl.ds(r, 8)
        z = zb[h, rows, :]
        m = ml[h, rows, :]
        hit = _wide(col[rows, :] - (me * VOC + h * HALF)) == lax.broadcasted_iota(I32, (8, HALF), 1)
        s = _fold(jnp.exp(z - _wide(m)))
        t = _fold(jnp.where(hit, z, 0.0))
        if h == 1:
            m0 = mk[0, rows, :]
            mm = jnp.maximum(m0, m)
            s = sl[0, rows, :] * jnp.exp(m0 - mm) + s * jnp.exp(m - mm)
            t = tl[0, rows, :] + t
            m = mm
        mk[h, rows, :] = m
        sl[h, rows, :] = s
        tl[h, rows, :] = t

    def label_columns(blk, col, part):
        col[pl.ds(part * LANE, LANE), :] = label_column(blk, part)

    def row_stats(part):
        rows = pl.ds(part * LANE, LANE)
        m = jnp.transpose(mk[1, rows, :])
        top = jnp.max(m, axis=0, keepdims=True)
        st_new[part : part + 1, :] = top
        st_new[2 + part : 3 + part, :] = jnp.sum(jnp.transpose(sl[1, rows, :]) * jnp.exp(m - top), axis=0, keepdims=True)
        st_new[4 + part : 5 + part, :] = jnp.sum(jnp.transpose(tl[1, rows, :]), axis=0, keepdims=True)

    def entry(kind, q):
        diagonal = _div(kind, 3)
        return diagonal * (NBLK + q) + (1 - diagonal) * block_id(kind, q)

    def send_stats(kind, q):
        def start(dev):
            _send(st_loc.at[block_id(kind, q)], st_all.at[NBLK + q, me], sttx_sem, st_sem.at[q], dev).start()

        for core in PAIR:
            dev = 2 * chip_of(3 - kind) + core
            pl.when(dev != me)(functools.partial(start, dev))

    def send_late():
        for d in OTHERS:
            _send(st_loc, st_all.at[pl.ds(0, NBLK), me], sttx_sem, st_sem.at[4], _rem(me + d, 8)).start()

    def keep_stats(kind, q):
        st_loc[block_id(kind, q)] = st_new[...]
        st_all[block_id(kind, q), me] = st_new[...]
        st_all[entry(kind, q), me] = st_new[...]

    def combine(place):
        top = st_all[place, 0, 0:2, :]
        for d in OTHERS:
            top = jnp.maximum(top, st_all[place, d, 0:2, :])
        s = jnp.zeros((2, LANE), F32)
        t = jnp.zeros((2, LANE), F32)
        for d in range(8):
            s = s + st_all[place, d, 2:4, :] * jnp.exp(st_all[place, d, 0:2, :] - top)
            t = t + st_all[place, d, 4:6, :]
        comb[0:2, :] = top
        comb[2:4, :] = INV / s
        return top + jnp.log(s) - t

    def stats_arrived(q):
        _copy(st_all.at[0, SEVEN], st_all.at[0, SEVEN], st_sem.at[q]).wait()

    def late_arrived():
        _copy(st_all.at[pl.ds(0, 14)], st_all.at[pl.ds(0, 14)], st_sem.at[4]).wait()

    def columns(blk, par, part):
        rows = pl.ds(part * LANE, LANE)
        c_lab[par, rows, :] = label_column(blk, part)
        c_top[par, rows, :] = _column(comb[part : part + 1, :])
        c_scale[par, rows, :] = _column(comb[2 + part : 3 + part, :])

    def gradient(src, n, par, r, j):
        rows = pl.ds(pl.multiple_of(r, SUB), SUB)
        col = c_lab[par, rows, :] - (me * VOC + n * HALF + j)
        p = jnp.exp(src[n, rows, j : j + PIECE] - _wide(c_top[par, rows, :], 4)) * _wide(c_scale[par, rows, :], 4)
        g = jnp.where(_wide(col, 4) == lax.broadcasted_iota(I32, (SUB, PIECE), 1), p - INV, p)
        gbufs[par][rows, n * HALF + j : n * HALF + j + PIECE] = g.astype(BF16)

    def gradient_jobs(src, n, par):
        return [functools.partial(gradient, src, n, par, r, j) for r in range(0, BLK, SUB) for j in range(0, HALF, PIECE)]

    gbufs = (ga, gb)

    def gstore(k, par):
        kind, q = order2(k)
        return _copy(gbufs[par], gall.at[pl.ds(pl.multiple_of(block_id(kind, q) * BLK, BLK), BLK)], g_sem.at[par])

    def zload(k, dst, n):
        kind, q = order2(k)
        return _copy(zst.at[block_id(kind, q), n], dst.at[n], zi_sem.at[n])

    first_kind, first_q = order2(me * 0)
    first_blk = block_id(first_kind, first_q)

    def logits(b, h, jobs):
        slot = _odd(b)
        def put(nt, z):
            zb[h, :, nt * PIECE : (nt + 1) * PIECE] = z
            m = z[:, :LANE]
            for j in range(1, 4):
                m = jnp.maximum(m, z[:, j * LANE : (j + 1) * LANE])
            if nt:
                m = jnp.maximum(m, ml[h])
            ml[h] = m

        _product(
            lambda kt: xg[slot, :, kt * BLK : (kt + 1) * BLK],
            lambda nt, kt: wv[kt * BLK : (kt + 1) * BLK, h * HALF + nt * PIECE : h * HALF + (nt + 1) * PIECE],
            put,
            jobs,
            False,
        )

    wait_rows(0, 0, oc)
    _copy(xrows(0, 0, oc), xg.at[0, pl.ds(pl.multiple_of(oc * LANE, LANE), LANE)], xl_sem.at[0]).start()
    _copy(lab_v, lab_v, lab_sem).wait()
    for j in FOUR:
        wcopy(j).wait()
    for j in FOUR:
        wcopy(4 + j).start()

    def phase1(i, carry):
        slot = _odd(i)
        kind, q = order1(i)
        kprev, qprev = order1(_rem(i + NBLK - 2, NBLK))
        kn, qn = order1(_rem(i + 1, NBLK))

        @pl.when((i == LATE + 1) | (i == NBLK - 1))
        def _():
            wait_rows(kind, q, oc)
            part_load(i, oc).start()

        @pl.when(i > 0)
        def _():
            zcopy(i - 1, 1).start()
            zcopy(i - 1, 0).wait()

        @pl.when(i > 1)
        def _():
            keep_stats(kprev, qprev)

        @pl.when(i == NBLK - 2)
        def _():
            zload(0, pbuf, 0).start()
            zload(0, pbuf, 1).start()

        @pl.when(i == NBLK - 1)
        def _():
            stats_arrived(0)
            loss_acc[...] = combine(entry(first_kind, first_q))
            for part in PAIR:
                columns(first_blk, 0, part)
            for n in PAIR:
                zload(0, pbuf, n).wait()

                def some(r, carry, n=n):
                    for j in range(0, HALF, PIECE):
                        gradient(pbuf, n, 0, r * SUB, j)
                    return carry

                _loop(SUB, some)

            gstore(0, 0).start()

        @pl.when((i >= 3) & (i != LATE) & (i < NBLK - 2))
        def _():
            take_rows(kn, qn)

        _copy(xg.at[slot], xg.at[slot], xl_sem.at[slot]).wait()

        @pl.when(i < 4)
        def _():
            own_store(i).start()

        jobs = [[] for _ in range(32)]
        for r in range(32):
            jobs[min(r + 1, 31)].append(functools.partial(lane_stats, la, 1, r * 8))
        for part in PAIR:
            jobs[4 + 4 * part].append(functools.partial(label_columns, block_id(kind, q), lb, part))
        logits(i, 0, jobs)

        zcopy(i, 0).start()

        @pl.when(i == 0)
        def _():
            for j in FOUR:
                wcopy(4 + j).wait()

        @pl.when(i > 0)
        def _():
            zcopy(i - 1, 1).wait()

        @pl.when(i > 1)
        def _():
            send_stats(kprev, qprev)

        @pl.when((i == LATE) | (i == NBLK - 2))
        def _():
            take_rows(kn, qn)
            part_load(i + 1, c).start()

        @pl.when((i != LATE) & (i < NBLK - 2))
        def _():
            wait_rows(kn, qn, oc)

            @pl.when((i >= 1) & (i < 5))
            def _():
                own_store(i - 1).wait()

            load_x(i + 1)

        la[...] = lb[...]
        jobs = [[] for _ in range(32)]
        for r in range(32):
            jobs[min(r + 1, 31)].append(functools.partial(lane_stats, lb, 0, r * 8))
        for part in PAIR:
            jobs[8 + 8 * part].append(functools.partial(row_stats, part))
        logits(i, 1, jobs)
        return carry

    _loop(NBLK, phase1)
    last = NBLK - 1
    klast, qlast = order1(jnp.int32(last))
    kprev, qprev = order1(jnp.int32(last - 1))
    keep_stats(kprev, qprev)
    zcopy(last, 1).start()
    zcopy(last, 0).wait()
    zload(1, zb, 0).start()
    send_stats(kprev, qprev)
    for r in range(32):
        lane_stats(la, 1, r * 8)
    for part in PAIR:
        row_stats(part)
    keep_stats(klast, qlast)
    second_kind, second_q = order2(jnp.int32(1))
    second_blk = block_id(second_kind, second_q)
    stats_arrived(1)
    loss_acc[...] += combine(entry(second_kind, second_q))
    for part in PAIR:
        columns(second_blk, 1, part)
    send_stats(klast, qlast)
    zcopy(last, 1).wait()
    zload(1, zb, 1).start()

    def tile(ref, q, n):
        return ref.at[pl.ds(pl.multiple_of(q * LANE, LANE), LANE), pl.ds(pl.multiple_of(n * HALF, HALF), HALF)]

    def spair(k, n):
        return _send(
            pbuf.at[n, pl.ds(pl.multiple_of(oc * LANE, LANE), LANE)], rbuf.at[_odd(k + 2), n], ps.at[n], rr.at[_odd(k + 2) * 2 + n], partner
        )

    def sstore_start(k, n):
        kind, q = order2(k)
        sem = ss_sem.at[n]

        @pl.when(kind == 3)
        def _():
            _copy(sbuf.at[n], tile(s_d, q, n), sem).start()

        @pl.when((kind == n1kind) & (q < 2))
        def _():
            _copy(sbuf.at[n], tile(s_n1a, _odd(q), n), sem).start()

        @pl.when((kind == n1kind) & (q >= 2))
        def _():
            _copy(sbuf.at[n], tile(s_n1b, _odd(q), n), sem).start()

        @pl.when(kind == 3 - n1kind)
        def _():
            _copy(sbuf.at[n], tile(s_n2, q, n), sem).start()

        @pl.when(kind == 0)
        def _():
            _copy(sbuf.at[n], tile(s_self, q, n), sem).start()

    def sstore_done(k, n):
        kind, q = order2(k)
        _copy(sbuf.at[n], tile(s_d, 0, n), ss_sem.at[n]).wait()

        @pl.when(kind == 3)
        def _():
            _send(tile(s_d, q, n), tile(r1n2, q, n), s1tx, r1s.at[q * 2 + n], n1).start()

        @pl.when((kind == n1kind) & (q < 2))
        def _():
            _send(tile(s_n1a, _odd(q), n), tile(r1a, _odd(q), n), s1tx, r1as.at[_odd(q) * 2 + n], n1).start()

    def stage2_load(q, n):
        _copy(tile(r1n2, q, n), tile(r1n2, q, n), r1s.at[q * 2 + n]).wait()
        _copy(tile(s_n2, q, n), ab.at[n], ab_sem.at[n * 2]).start()
        _copy(tile(r1n2, q, n), bb.at[n], ab_sem.at[n * 2 + 1]).start()

    def pair_sum(k, n, r):
        sbuf[n, pl.ds(r, SUB), :] = pbuf[n, pl.ds(pl.multiple_of(c * LANE + r, SUB), SUB), :] + rbuf[_odd(k + 2), n, pl.ds(r, SUB), :]

    def stage2_sum(n, r):
        cb[n, pl.ds(r, SUB), :] = ab[n, pl.ds(r, SUB), :] + bb[n, pl.ds(r, SUB), :]

    def rwait(k, n):
        _copy(rbuf.at[_odd(k + 2), n], rbuf.at[_odd(k + 2), n], rr.at[_odd(k + 2) * 2 + n]).wait()

    def loss_part(k, place):
        loss_acc[...] += jnp.where(k < NBLK - 2, combine(place), 0.0)

    def sub(k, cur):
        nxt = 1 - cur
        kind2, q2 = order2(_rem(k + 2, NBLK))
        blk2 = block_id(kind2, q2)

        def trip(n):
            @pl.when(k < NBLK - 1)
            def _():
                zload(k + 1, zb, n).wait()

            @pl.when(k >= 1)
            def _():
                rwait(k - 1, n)
                spair(k - 1, n).wait_send()
                if n == 0:
                    gstore(k - 1, nxt).wait()

            if n == 0:

                @pl.when(k < 2)
                def _():
                    stats_arrived(k + 2)

                @pl.when(k == 2)
                def _():
                    late_arrived()

            @pl.when(k >= 12)
            def _():
                _copy(tile(s_n2, 0, n), ab.at[n], ab_sem.at[n * 2]).wait()
                _copy(tile(r1n2, 0, n), bb.at[n], ab_sem.at[n * 2 + 1]).wait()

            @pl.when(k >= 13)
            def _():
                _copy(cb.at[n], tile(y2, 0, n), cb_sem.at[n]).wait()

            jobs = [[] for _ in range(32)]
            for r in range(8):
                jobs[2 + r * 3 // 5].append(functools.partial(pair_sum, k - 1, n, r * SUB))
                jobs[10 + r * 5 // 2].append(functools.partial(stage2_sum, n, r * SUB))
            for r, job in enumerate(gradient_jobs(zb, n, nxt)):
                jobs[2 + r * 9 // 20].append(job)
            if n == 0:
                jobs[8].append(lambda: loss_part(k, entry(kind2, q2)))
            else:
                for part in PAIR:
                    jobs[8 + 8 * part].append(functools.partial(columns, blk2, cur, part))

            def put(nt, acc):
                pbuf[n, :, nt * PIECE : (nt + 1) * PIECE] = acc

            _product(
                lambda kt: gbufs[cur][:, kt * BLK : (kt + 1) * BLK],
                lambda nt, kt: wv[pl.ds(pl.multiple_of(n * HALF + nt * PIECE, PIECE), PIECE), kt * BLK : (kt + 1) * BLK],
                put,
                jobs,
                True,
            )

            spair(k, n).start()

            if cur == n == 0:
                pl.when(k == 0)(send_late)

            @pl.when(k < NBLK - 2)
            def _():
                zload(k + 2, zb, n).start()

            @pl.when(k >= 2)
            def _():
                sstore_done(k - 2 + n, 1 - n)

            @pl.when(k >= 1)
            def _():
                sstore_start(k - 1, n)

            if n == 0:
                @pl.when(k == 1)
                def _():
                    sstore_done(k - 1, n)

            @pl.when(k >= 12)
            def _():
                _copy(cb.at[n], tile(y2, k - 12, n), cb_sem.at[n]).start()

            @pl.when((k >= 11) & (k < NBLK - 1))
            def _():
                stage2_load(k - 11, n)


        trip(0)
        trip(1)

        @pl.when(k < NBLK - 1)
        def _():
            gstore(k + 1, nxt).start()

    def pair(p, carry):
        sub(2 * p, 0)
        sub(2 * p + 1, 1)
        return carry

    _loop(NBLK // 2, pair)

    kl = jnp.int32(NBLK - 1)
    for n in PAIR:
        rwait(kl, n)
        spair(kl, n).wait_send()
        if n == 0:
            sstore_done(kl - 1, 1)
        for r in range(8):
            pair_sum(kl, n, r * SUB)
        sstore_start(kl, n)
    for n in PAIR:
        sstore_done(kl, n)
    gstore(kl, 1).wait()
    for n in PAIR:
        _copy(cb.at[n], tile(y2, 0, n), cb_sem.at[n]).wait()

    loss_out[...] = jnp.full(TILE, jnp.sum(loss_acc[...]) * INV, F32)

    for i in FOUR:
        _copy(tile(r1a, i // 2, i % 2), tile(r1a, i // 2, i % 2), r1as.at[i]).wait()
    _copy(s_d, s_d, s1tx).wait()
    _copy(s_n1a, s_n1a, s1tx).wait()
    _copy(xall.at[pl.ds(0, 28 * LANE)], xall.at[pl.ds(0, 28 * LANE)], tx).wait()
    for d in range(7):
        _copy(lab_v.at[d], lab_v.at[d], labtx_sem).wait()
        _copy(st_loc, st_loc, sttx_sem).wait()
    for d in FOUR:
        _copy(st_all.at[d, SEVEN], st_all.at[d, SEVEN], sttx_sem).wait()


def xrows_at(xall, dev, q):
    return xall.at[pl.ds(pl.multiple_of((dev // 2) * 1024 + q * BLK + (dev % 2) * LANE, LANE), LANE)]


def _head(hid, lab, w):
    hbm = pl.BlockSpec(memory_space=ANY)
    sd = jax.ShapeDtypeStruct
    dma = pltpu.SemaphoreType.DMA
    vmem = pltpu.VMEM
    quarter = (LANE, HALF)
    return pl.pallas_call(
        _head_kernel,
        out_shape=(
            sd((TOK, HID), BF16),
            sd((TOK, VOC), BF16),
            sd((256, HID), F32),
            sd((PIECE, HID), F32),
            sd((PIECE, HID), F32),
            sd((256, HID), F32),
            sd(TILE, F32),
            sd((NBLK, 2, BLK, HALF), F32),
            sd((PIECE, HID), F32),
            sd((256, HID), F32),
            sd((PIECE, HID), F32),
            sd((PIECE, HID), F32),
        ),
        in_specs=[hbm] * 3,
        out_specs=(hbm,) * 6 + (pl.BlockSpec(memory_space=vmem),) + (hbm,) * 5,
        scratch_shapes=[
            vmem((HID, VOC), BF16),
            vmem((2, BLK, HID), BF16),
            vmem((BLK, VOC), BF16),
            vmem((BLK, VOC), BF16),
            vmem((2, BLK, HALF), F32),
            vmem((2, BLK, HALF), F32),
            vmem((2, 2) + quarter, F32),
            vmem(TWO + quarter, F32),
            vmem(TWO + quarter, F32),
            vmem(TWO + quarter, F32),
            vmem(TWO + quarter, F32),
            vmem((8, 4, LANE), I32),
            vmem((BLK, LANE), I32),
            vmem((BLK, LANE), I32),
            vmem(TILE, F32),
            vmem((NBLK,) + TILE, F32),
            vmem((NBLK + 4, 8) + TILE, F32),
            vmem((2, BLK, LANE), F32),
            vmem((2, BLK, LANE), F32),
            vmem((2, BLK, LANE), F32),
            vmem((2, BLK, LANE), F32),
            vmem(TILE, F32),
            vmem((2, BLK, LANE), I32),
            vmem((2, BLK, LANE), F32),
            vmem((2, BLK, LANE), F32),
            vmem((2, LANE), F32),
            dma((8,)),
            dma(()),
            dma(()),
            dma((32,)),
            dma(()),
            dma(TWO),
            dma(TWO),
            dma(TWO),
            dma((5,)),
            dma(()),
            dma(TWO),
            dma((4,)),
            dma(TWO),
            dma(TWO),
            dma(()),
            dma((8,)),
            dma((4,)),
            dma((4,)),
            dma(TWO),
            dma(TWO),
        ],
        compiler_params=pltpu.CompilerParams(collective_id=0, has_side_effects=True, vmem_limit_bytes=67_043_328),
        cost_estimate=pl.CostEstimate(flops=4 * TOK * HID * VOC, bytes_accessed=400 * MIB, transcendentals=2 * TOK * VOC),
        name="head",
    )(hid, lab, w)


def _cols(j, width=PIECE):
    return pl.ds(pl.multiple_of(j * width, width), width)


def _dhead_kernel(
    x_hbm, g_hbm, s_hbm, a_hbm, o_hbm, t_hbm,
    gv, xb, ob, acc, sv, av, x_sem, g_sem, o_sem, s_sem, a_sem, t_sem, f_sem,
):
    blocks = HID // PIECE
    rows = BLK // 4

    def xload(b):
        return _copy(x_hbm.at[:, _cols(b)], xb.at[_odd(b)], x_sem.at[_odd(b)])

    def gload(j):
        return _copy(g_hbm.at[:, _cols(j)], gv.at[:, _cols(j)], g_sem.at[j])

    def ostore(b, n):
        return _copy(ob.at[n], o_hbm.at[_cols(b), _cols(n, HALF)], o_sem.at[n])

    def dot(lhs, rhs):
        return lax.dot_general(lhs, rhs, FIRST_DIMS, preferred_element_type=F32).astype(BF16)

    def terms(p):
        slot = _odd(p)
        src = _cols(p, rows)
        return _copy(s_hbm.at[src], sv.at[slot], s_sem.at[slot]), _copy(a_hbm.at[src], av.at[slot], a_sem.at[slot])

    def tstore(p):
        return _copy(sv.at[_odd(p)], t_hbm.at[_cols(p, rows)], t_sem.at[_odd(p)])

    def part(h):
        tokens = pl.ds(h * HALF, HALF)
        return (
            _copy(x_hbm.at[tokens, _cols(0)], xb.at[0, tokens], f_sem.at[h, 0]),
            _copy(g_hbm.at[tokens, _cols(0)], gv.at[tokens, _cols(0)], f_sem.at[h, 1]),
        )

    def part_dot(h):
        tokens = slice(h * HALF, (h + 1) * HALF)
        return lax.dot_general(
            xb[0, tokens, :], gv[tokens, :PIECE], FIRST_DIMS, preferred_element_type=F32
        )

    for h in PAIR:
        for copy in part(h):
            copy.start()
    for copy in part(0):
        copy.wait()
    gload(1).start()

    @pl.when(lax.axis_index("tp") < 8)
    def _():
        acc[...] = part_dot(0)

    for copy in part(1):
        copy.wait()
    gload(2).start()

    @pl.when(lax.axis_index("tp") < 8)
    def _():
        ob[0, :, :PIECE] = (acc[...] + part_dot(1)).astype(BF16)

    def first(j, carry):
        gload(j).wait()
        gload(2 * j + 1).start()

        @pl.when(j < 3)
        def _():
            gload(2 * j + 2).start()

        ob[0, :, _cols(j)] = dot(xb[0], gv[:, _cols(j)])
        return carry

    lax.fori_loop(1, 4, first, 0)
    ostore(0, 0).start()
    xload(1).start()
    for j in FOUR:
        gload(4 + j).wait()

    def block(b, carry):
        @pl.when(b > 0)
        def _():
            xload(b).wait()

        @pl.when((b > 0) & (b < blocks - 1))
        def _():
            xload(b + 1).start()

        @pl.when((b > 1) & (b < 6))
        def _():
            for copy in terms(b - 2):
                copy.wait()
            sv[_odd(b)] = sv[_odd(b)] + av[_odd(b)]
            tstore(b - 2).start()

        @pl.when((b > 0) & (b < 5))
        def _():
            pl.when(b > 2)(lambda: tstore(b - 3).wait())
            for copy in terms(b - 1):
                copy.start()

        def half(n, carry):
            pl.when(b > 0)(lambda: ostore(b - 1, n).wait())

            @pl.when(b < blocks)
            def _():
                ob[n] = dot(xb[_odd(b)], gv[:, _cols(n, HALF)])

            ostore(b, n).start()
            return carry

        return lax.fori_loop(jnp.where(b == 0, 1, 0), 2, half, carry)

    _loop(blocks, block)
    for n in PAIR:
        ostore(blocks - 1, n).wait()
        tstore(n).wait()


def _dhead(xall, gall, s_self, r1a):
    hbm = pl.BlockSpec(memory_space=ANY)
    dma = pltpu.SemaphoreType.DMA
    return pl.pallas_call(
        _dhead_kernel,
        in_specs=[hbm] * 4,
        out_specs=(hbm, hbm),
        out_shape=(jax.ShapeDtypeStruct((HID, VOC), BF16), jax.ShapeDtypeStruct((BLK, HID), F32)),
        scratch_shapes=[
            pltpu.VMEM((TOK, VOC), BF16),
            pltpu.VMEM((2, TOK, PIECE), BF16),
            pltpu.VMEM((2, PIECE, HALF), BF16),
            pltpu.VMEM((PIECE, PIECE), F32),
            pltpu.VMEM((2, BLK // 4, HID), F32),
            pltpu.VMEM((2, BLK // 4, HID), F32),
            dma(TWO),
            dma((8,)),
            dma(TWO),
            dma(TWO),
            dma(TWO),
            dma(TWO),
            dma(TWO + TWO),
        ],
        compiler_params=pltpu.CompilerParams(vmem_limit_bytes=60 * MIB),
        cost_estimate=pl.CostEstimate(flops=2 * TOK * HID * VOC, bytes_accessed=200 * MIB, transcendentals=0),
        name="dhead",
    )(xall, gall, s_self, r1a)


def _final_kernel(t_hbm, s_hbm, b_hbm, r_hbm, l_ref, o_hbm, loss_ref, terms, ov, in_sem, o_sem):
    rows = PIECE // SUB
    ahead = 6
    half = SUB // 2

    def load(t, ref, i, dst):
        return _copy(ref.at[_cols(i, rows)], terms.at[t, _cols(dst, rows)], in_sem.at[t, dst])

    def start(i):
        @pl.when(i < half)
        def _():
            load(0, t_hbm, i, i).start()

        @pl.when(i >= half)
        def _():
            load(0, s_hbm, i, i).start()
            load(1, b_hbm, i - half, i).start()

        load(2, r_hbm, i, i).start()

    def begin(i, carry):
        start(i)
        return carry

    _loop(ahead, begin)
    loss_ref[0] = l_ref[0, 0]

    def add(i, carry):
        rs = _cols(i, rows)
        load(0, s_hbm, i, i).wait()
        load(2, r_hbm, i, i).wait()
        pl.when(i < SUB - ahead)(lambda: start(i + ahead))

        @pl.when(i < half)
        def _():
            ov[rs, :] = (terms[0, rs, :] + terms[2, rs, :]).astype(BF16)

        @pl.when(i >= half)
        def _():
            load(1, b_hbm, i - half, i).wait()
            ov[rs, :] = (terms[0, rs, :] + terms[1, rs, :] + terms[2, rs, :]).astype(BF16)

        _copy(ov.at[rs], o_hbm.at[rs], o_sem).start()
        return carry

    _loop(SUB, add)
    _copy(ov, o_hbm, o_sem).wait()


def _final(t, s_self, r1b, r2, loss):
    hbm = pl.BlockSpec(memory_space=ANY)
    dma = pltpu.SemaphoreType.DMA
    return pl.pallas_call(
        _final_kernel,
        in_specs=[hbm] * 4 + [pl.BlockSpec(memory_space=pltpu.VMEM)],
        out_specs=(hbm, pl.BlockSpec(memory_space=pltpu.SMEM)),
        out_shape=(jax.ShapeDtypeStruct((PIECE, HID), BF16), jax.ShapeDtypeStruct((1,), F32)),
        scratch_shapes=[
            pltpu.VMEM((3, PIECE, HID), F32),
            pltpu.VMEM((PIECE, HID), BF16),
            dma((3, SUB)),
            dma(()),
        ],
        compiler_params=pltpu.CompilerParams(vmem_limit_bytes=62 * MIB),
        cost_estimate=pl.CostEstimate(flops=3 * PIECE * HID, bytes_accessed=24 * MIB, transcendentals=0),
        name="final",
    )(t, s_self, r1b, r2, loss)


def solution(mesh):
    def device(y, x, core):
        return (y % 2) * 4 + (x % 2) * 2 + core

    first, second = [], []
    for yy in PAIR:
        for xx in PAIR:
            along_x = [(device(yy, xx, k), device(yy, xx + 1, k)) for k in PAIR]
            along_y = [(device(yy, xx, k), device(yy + 1, xx, k)) for k in PAIR]
            first += [along_x[0], along_y[1]]
            second += [along_y[0], along_x[1]]

    def local_step(hid, w, lab):
        xall, gall, s_n1b, s_self, y2, r1a, loss = _head(hid, lab.reshape(4, LANE), w)[:7]
        r2 = lax.ppermute(y2, "tp", second)
        r1b = lax.ppermute(s_n1b, "tp", first)
        d_head, t = _dhead(xall, gall, s_self, r1a)
        d_hidden, mean_loss = _final(t, s_self, r1b, r2, loss)
        return mean_loss, d_hidden, d_head

    return jax.shard_map(
        local_step,
        mesh=mesh,
        in_specs=(P(("dp", "tp"), None), P(None, "tp"), P(("dp", "tp"))),
        out_specs=(P("dp"), P(("dp", "tp"), None), P("dp", "tp")),
        check_vma=False,
    )
```

```python
import functools

import jax
import jax.numpy as jnp
from jax import lax
from jax.experimental import pallas as pl
from jax.experimental.pallas import tpu as pltpu
from jax.sharding import PartitionSpec as P

F32, BF16, I32 = jnp.float32, jnp.bfloat16, jnp.int32
MESH = pl.DeviceIdType.MESH
ANY = pl.ANY

TOK = 4096
HID = 4096
VOC = 4096
BLK = 256
HALF = 2048
NBLK = TOK // BLK
LANE = 128
MIB = 1 << 20
TWO = (2,)
PAIR = (0, 1)
TILE = (8, LANE)
SUB = 16
FIRST_DIMS = (((0,), (0,)), ((), ()))
FOUR = range(4)
OTHERS = range(1, 8)
SEVEN = pl.ds(0, 7)
LATE = 9
PIECE = 512
INV = 1.0 / TOK


def _div(a, b):
    return lax.div(jnp.int32(a), jnp.int32(b))


def _rem(a, b):
    return lax.rem(jnp.int32(a), jnp.int32(b))


def _odd(a):
    return _rem(a, 2)


def _loop(count, body):
    lax.fori_loop(0, count, body, 0)


def _copy(src, dst, sem):
    return pltpu.make_async_copy(src, dst, sem)


def _send(src, dst, send_sem, recv_sem, dev):
    return pltpu.make_async_remote_copy(
        src_ref=src, dst_ref=dst, send_sem=send_sem, recv_sem=recv_sem, device_id={"tp": dev}, device_id_type=MESH
    )


def _product(lhs, rhs, put, jobs, transposed):
    pl.when(lax.axis_index("tp") < 8)(functools.partial(_pieces, lhs, rhs, put, jobs, transposed))


def _pieces(lhs, rhs, put, jobs, transposed):
    dims = (((1,), (1,)), ((), ())) if transposed else (((1,), (0,)), ((), ()))
    pieces = HALF // PIECE
    deep = HID // BLK
    for nt in range(pieces):
        acc = None
        for kt in range(deep):
            part = lax.dot_general(lhs(kt), rhs(nt, kt), dims, preferred_element_type=F32)
            acc = part if acc is None else acc + part
            if kt % 2:
                for job in jobs[(nt * deep + kt) // 2]:
                    job()
        put(nt, acc)


def _wide(v, times=HALF // LANE):
    return jnp.concatenate([v] * times, axis=1)


def _fold(v):
    width = v.shape[1] // 2
    while width >= LANE:
        v = v[:, :width] + v[:, width:]
        width //= 2
    return v


def _column(row):
    return jnp.transpose(jnp.broadcast_to(row, (LANE, LANE)))


def _head_kernel(
    x_hbm, lab_hbm, w_hbm,
    xall, gall, s_n1b, s_self, y2, r1a, loss_out,
    zst, s_d, s_n1a, s_n2, r1n2,
    wv, xg, ga, gb, zb, pbuf, rbuf, sbuf, ab, bb, cb, lab_v, la, lb, st_new, st_loc, st_all, ml, mk, sl, tl, comb, c_lab, c_top, c_scale, loss_acc,
    w_sem, lab_sem, labtx_sem, rx, tx, xl_sem, xs_sem, zo_sem, st_sem, sttx_sem,
    zi_sem, rr, ps, ss_sem, s1tx, r1s, r1as, ab_sem, cb_sem, g_sem,
):
    me = lax.axis_index("tp")
    chip = _div(me, 2)
    c = _odd(me)
    x = _odd(chip)
    y = _div(chip, 2)
    oc = 1 - c
    partner = me + 1 - 2 * c
    dx, dy = 2 - 4 * x, 4 - 8 * y
    n1 = me + oc * dx + c * dy
    n2 = me + c * dx + oc * dy
    n1kind = 1 + c

    def chip_of(kind):
        return chip + _odd(kind) * (1 - 2 * x) + _div(kind, 2) * (2 - 4 * y)

    def order(i, first, last):
        a = _div(i, 4)
        mid, end = _rem(_div(a + 1, 2), 2), _div(a, 3)
        kind = mid * (1 + _odd(i)) + first * (1 - mid) * (1 - end) + last * end
        return kind, mid * _div(i - 4, 2) + (1 - mid) * _rem(i, 4)

    def order1(i):
        return order(i, 0, 3)

    def order2(i):
        return order(i, 3, 0)

    def block_id(kind, q):
        return chip_of(kind) * 4 + q

    def xrows(kind, q, part):
        return xall.at[pl.ds(pl.multiple_of(block_id(kind, q) * BLK + part * LANE, LANE), LANE)]

    def xblock(kind, q):
        return xall.at[pl.ds(pl.multiple_of(block_id(kind, q) * BLK, BLK), BLK)]

    def own(q):
        return x_hbm.at[pl.ds(pl.multiple_of(q * LANE, LANE), LANE)]

    def rxs(kind, q, part):
        return rx.at[kind * 8 + q * 2 + part]

    def wcopy(j):
        cols = pl.ds(j * HALF, HALF)
        return _copy(w_hbm.at[:, cols], wv.at[:, cols], w_sem.at[j])

    _copy(own(0), xg.at[0, pl.ds(pl.multiple_of(c * LANE, LANE), LANE)], xl_sem.at[0]).start()
    wcopy(0).start()

    barrier = pltpu.get_barrier_semaphore()
    for d in OTHERS:
        pl.semaphore_signal(barrier, inc=1, device_id={"tp": _rem(me + d, 8)}, device_id_type=MESH)
    pl.semaphore_wait(barrier, 7)

    for d in OTHERS:
        _send(lab_hbm, lab_v.at[me], labtx_sem, lab_sem, _rem(me + d, 8)).start()
    _copy(lab_hbm, lab_v.at[me], lab_sem).start()
    for q in FOUR:
        _send(own(q), xrows(0, q, c), tx, rxs(0, q, c), partner).start()
    for q in FOUR:
        _send(own(q), xrows_at(xall, me, q), tx, rxs(n1kind, q, c), n1).start()
        _send(own(q), xrows_at(xall, me, q), tx, rxs(3 - n1kind, q, c), n2).start()

    def load_x(b):
        kind, q = order1(b)
        slot = _odd(b)

        @pl.when(kind == 0)
        def _():
            _copy(own(q), xg.at[slot, pl.ds(pl.multiple_of(c * LANE, LANE), LANE)], xl_sem.at[slot]).start()
            _copy(xrows(0, q, oc), xg.at[slot, pl.ds(pl.multiple_of(oc * LANE, LANE), LANE)], xl_sem.at[slot]).start()

        @pl.when(kind != 0)
        def _():
            _copy(xblock(kind, q), xg.at[slot], xl_sem.at[slot]).start()

    def wait_rows(kind, q, part):
        _copy(xrows(kind, q, part), xrows(kind, q, part), rxs(kind, q, part)).wait()

    def take_rows(kind, q):
        wait_rows(kind, q, c)
        _send(xrows(kind, q, c), xrows(kind, q, c), tx, rxs(kind, q, c), partner).start()

        @pl.when(kind == n1kind)
        def _():
            _send(xrows(kind, q, c), xrows(kind, q, c), tx, rxs(3, q, c), n2).start()

    def part_load(b, part):
        kind, q = order1(b)
        return _copy(xrows(kind, q, part), xg.at[_odd(b), pl.ds(pl.multiple_of(part * LANE, LANE), LANE)], xl_sem.at[_odd(b)])

    def zcopy(b, h):
        kind, q = order1(b)
        return _copy(zb.at[h], zst.at[block_id(kind, q), h], zo_sem.at[h])

    def own_store(b):
        slot = _odd(b)
        return _copy(xg.at[slot, pl.ds(pl.multiple_of(c * LANE, LANE), LANE)], xrows(0, _rem(b, 4), c), xs_sem.at[slot])

    def label_column(blk, part):
        return _column(lab_v[2 * _div(blk, 4) + part, pl.ds(_rem(blk, 4), 1), :])

    def lane_stats(col, h, r):
        rows = pl.ds(r, 8)
        z = zb[h, rows, :]
        m = ml[h, rows, :]
        hit = _wide(col[rows, :] - (me * VOC + h * HALF)) == lax.broadcasted_iota(I32, (8, HALF), 1)
        s = _fold(jnp.exp(z - _wide(m)))
        t = _fold(jnp.where(hit, z, 0.0))
        if h == 1:
            m0 = mk[0, rows, :]
            mm = jnp.maximum(m0, m)
            s = sl[0, rows, :] * jnp.exp(m0 - mm) + s * jnp.exp(m - mm)
            t = tl[0, rows, :] + t
            m = mm
        mk[h, rows, :] = m
        sl[h, rows, :] = s
        tl[h, rows, :] = t

    def label_columns(blk, col, part):
        col[pl.ds(part * LANE, LANE), :] = label_column(blk, part)

    def row_stats(part):
        rows = pl.ds(part * LANE, LANE)
        m = jnp.transpose(mk[1, rows, :])
        top = jnp.max(m, axis=0, keepdims=True)
        st_new[part : part + 1, :] = top
        st_new[2 + part : 3 + part, :] = jnp.sum(jnp.transpose(sl[1, rows, :]) * jnp.exp(m - top), axis=0, keepdims=True)
        st_new[4 + part : 5 + part, :] = jnp.sum(jnp.transpose(tl[1, rows, :]), axis=0, keepdims=True)

    def entry(kind, q):
        diagonal = _div(kind, 3)
        return diagonal * (NBLK + q) + (1 - diagonal) * block_id(kind, q)

    def send_stats(kind, q):
        def start(dev):
            _send(st_loc.at[block_id(kind, q)], st_all.at[NBLK + q, me], sttx_sem, st_sem.at[q], dev).start()

        for core in PAIR:
            dev = 2 * chip_of(3 - kind) + core
            pl.when(dev != me)(functools.partial(start, dev))

    def send_late():
        for d in OTHERS:
            _send(st_loc, st_all.at[pl.ds(0, NBLK), me], sttx_sem, st_sem.at[4], _rem(me + d, 8)).start()

    def keep_stats(kind, q):
        st_loc[block_id(kind, q)] = st_new[...]
        st_all[block_id(kind, q), me] = st_new[...]
        st_all[entry(kind, q), me] = st_new[...]

    def combine(place):
        top = st_all[place, 0, 0:2, :]
        for d in OTHERS:
            top = jnp.maximum(top, st_all[place, d, 0:2, :])
        s = jnp.zeros((2, LANE), F32)
        t = jnp.zeros((2, LANE), F32)
        for d in range(8):
            s = s + st_all[place, d, 2:4, :] * jnp.exp(st_all[place, d, 0:2, :] - top)
            t = t + st_all[place, d, 4:6, :]
        comb[0:2, :] = top
        comb[2:4, :] = INV / s
        return top + jnp.log(s) - t

    def stats_arrived(q):
        _copy(st_all.at[0, SEVEN], st_all.at[0, SEVEN], st_sem.at[q]).wait()

    def late_arrived():
        _copy(st_all.at[pl.ds(0, 14)], st_all.at[pl.ds(0, 14)], st_sem.at[4]).wait()

    def columns(blk, par, part):
        rows = pl.ds(part * LANE, LANE)
        c_lab[par, rows, :] = label_column(blk, part)
        c_top[par, rows, :] = _column(comb[part : part + 1, :])
        c_scale[par, rows, :] = _column(comb[2 + part : 3 + part, :])

    def gradient(src, n, par, r, j):
        rows = pl.ds(pl.multiple_of(r, SUB), SUB)
        col = c_lab[par, rows, :] - (me * VOC + n * HALF + j)
        p = jnp.exp(src[n, rows, j : j + PIECE] - _wide(c_top[par, rows, :], 4)) * _wide(c_scale[par, rows, :], 4)
        g = jnp.where(_wide(col, 4) == lax.broadcasted_iota(I32, (SUB, PIECE), 1), p - INV, p)
        gbufs[par][rows, n * HALF + j : n * HALF + j + PIECE] = g.astype(BF16)

    def gradient_jobs(src, n, par):
        return [functools.partial(gradient, src, n, par, r, j) for r in range(0, BLK, SUB) for j in range(0, HALF, PIECE)]

    gbufs = (ga, gb)

    def gstore(k, par):
        kind, q = order2(k)
        return _copy(gbufs[par], gall.at[pl.ds(pl.multiple_of(block_id(kind, q) * BLK, BLK), BLK)], g_sem.at[par])

    def zload(k, dst, n):
        kind, q = order2(k)
        return _copy(zst.at[block_id(kind, q), n], dst.at[n], zi_sem.at[n])

    first_kind, first_q = order2(me * 0)
    first_blk = block_id(first_kind, first_q)

    def logits(b, h, jobs):
        slot = _odd(b)
        def put(nt, z):
            zb[h, :, nt * PIECE : (nt + 1) * PIECE] = z
            m = z[:, :LANE]
            for j in range(1, 4):
                m = jnp.maximum(m, z[:, j * LANE : (j + 1) * LANE])
            if nt:
                m = jnp.maximum(m, ml[h])
            ml[h] = m

        _product(
            lambda kt: xg[slot, :, kt * BLK : (kt + 1) * BLK],
            lambda nt, kt: wv[kt * BLK : (kt + 1) * BLK, h * HALF + nt * PIECE : h * HALF + (nt + 1) * PIECE],
            put,
            jobs,
            False,
        )

    wait_rows(0, 0, oc)
    _copy(xrows(0, 0, oc), xg.at[0, pl.ds(pl.multiple_of(oc * LANE, LANE), LANE)], xl_sem.at[0]).start()
    _copy(lab_v, lab_v, lab_sem).wait()
    wcopy(0).wait()
    wcopy(1).start()

    def phase1(i, carry):
        slot = _odd(i)
        kind, q = order1(i)
        kprev, qprev = order1(_rem(i + NBLK - 2, NBLK))
        kn, qn = order1(_rem(i + 1, NBLK))

        @pl.when((i == LATE + 1) | (i == NBLK - 1))
        def _():
            wait_rows(kind, q, oc)
            part_load(i, oc).start()

        @pl.when(i > 0)
        def _():
            zcopy(i - 1, 1).start()
            zcopy(i - 1, 0).wait()

        @pl.when(i > 1)
        def _():
            keep_stats(kprev, qprev)

        @pl.when(i == NBLK - 2)
        def _():
            zload(0, pbuf, 0).start()
            zload(0, pbuf, 1).start()

        @pl.when(i == NBLK - 1)
        def _():
            stats_arrived(0)
            loss_acc[...] = combine(entry(first_kind, first_q))
            for part in PAIR:
                columns(first_blk, 0, part)
            for n in PAIR:
                zload(0, pbuf, n).wait()

                def some(r, carry, n=n):
                    for j in range(0, HALF, PIECE):
                        gradient(pbuf, n, 0, r * SUB, j)
                    return carry

                _loop(SUB, some)

            gstore(0, 0).start()

        @pl.when((i >= 3) & (i != LATE) & (i < NBLK - 2))
        def _():
            take_rows(kn, qn)

        _copy(xg.at[slot], xg.at[slot], xl_sem.at[slot]).wait()

        @pl.when(i < 4)
        def _():
            own_store(i).start()

        jobs = [[] for _ in range(32)]
        for r in range(32):
            jobs[min(r + 1, 31)].append(functools.partial(lane_stats, la, 1, r * 8))
        for part in PAIR:
            jobs[4 + 4 * part].append(functools.partial(label_columns, block_id(kind, q), lb, part))
        logits(i, 0, jobs)

        zcopy(i, 0).start()

        @pl.when(i == 0)
        def _():
            wcopy(1).wait()

        @pl.when(i > 0)
        def _():
            zcopy(i - 1, 1).wait()

        @pl.when(i > 1)
        def _():
            send_stats(kprev, qprev)

        @pl.when((i == LATE) | (i == NBLK - 2))
        def _():
            take_rows(kn, qn)
            part_load(i + 1, c).start()

        @pl.when((i != LATE) & (i < NBLK - 2))
        def _():
            wait_rows(kn, qn, oc)

            @pl.when((i >= 1) & (i < 5))
            def _():
                own_store(i - 1).wait()

            load_x(i + 1)

        la[...] = lb[...]
        jobs = [[] for _ in range(32)]
        for r in range(32):
            jobs[min(r + 1, 31)].append(functools.partial(lane_stats, lb, 0, r * 8))
        for part in PAIR:
            jobs[8 + 8 * part].append(functools.partial(row_stats, part))
        logits(i, 1, jobs)
        return carry

    _loop(NBLK, phase1)
    last = NBLK - 1
    klast, qlast = order1(jnp.int32(last))
    kprev, qprev = order1(jnp.int32(last - 1))
    keep_stats(kprev, qprev)
    zcopy(last, 1).start()
    zcopy(last, 0).wait()
    zload(1, zb, 0).start()
    send_stats(kprev, qprev)
    for r in range(32):
        lane_stats(la, 1, r * 8)
    for part in PAIR:
        row_stats(part)
    keep_stats(klast, qlast)
    second_kind, second_q = order2(jnp.int32(1))
    second_blk = block_id(second_kind, second_q)
    stats_arrived(1)
    loss_acc[...] += combine(entry(second_kind, second_q))
    for part in PAIR:
        columns(second_blk, 1, part)
    send_stats(klast, qlast)
    zcopy(last, 1).wait()
    zload(1, zb, 1).start()

    def tile(ref, q, n):
        return ref.at[pl.ds(pl.multiple_of(q * LANE, LANE), LANE), pl.ds(pl.multiple_of(n * HALF, HALF), HALF)]

    def spair(k, n):
        return _send(
            pbuf.at[n, pl.ds(pl.multiple_of(oc * LANE, LANE), LANE)], rbuf.at[_odd(k + 2), n], ps.at[n], rr.at[_odd(k + 2) * 2 + n], partner
        )

    def sstore_start(k, n):
        kind, q = order2(k)
        sem = ss_sem.at[n]

        @pl.when(kind == 3)
        def _():
            _copy(sbuf.at[n], tile(s_d, q, n), sem).start()

        @pl.when((kind == n1kind) & (q < 2))
        def _():
            _copy(sbuf.at[n], tile(s_n1a, _odd(q), n), sem).start()

        @pl.when((kind == n1kind) & (q >= 2))
        def _():
            _copy(sbuf.at[n], tile(s_n1b, _odd(q), n), sem).start()

        @pl.when(kind == 3 - n1kind)
        def _():
            _copy(sbuf.at[n], tile(s_n2, q, n), sem).start()

        @pl.when(kind == 0)
        def _():
            _copy(sbuf.at[n], tile(s_self, q, n), sem).start()

    def sstore_done(k, n):
        kind, q = order2(k)
        _copy(sbuf.at[n], tile(s_d, 0, n), ss_sem.at[n]).wait()

        @pl.when(kind == 3)
        def _():
            _send(tile(s_d, q, n), tile(r1n2, q, n), s1tx, r1s.at[q * 2 + n], n1).start()

        @pl.when((kind == n1kind) & (q < 2))
        def _():
            _send(tile(s_n1a, _odd(q), n), tile(r1a, _odd(q), n), s1tx, r1as.at[_odd(q) * 2 + n], n1).start()

    def stage2_load(q, n):
        _copy(tile(r1n2, q, n), tile(r1n2, q, n), r1s.at[q * 2 + n]).wait()
        _copy(tile(s_n2, q, n), ab.at[n], ab_sem.at[n * 2]).start()
        _copy(tile(r1n2, q, n), bb.at[n], ab_sem.at[n * 2 + 1]).start()

    def pair_sum(k, n, r):
        sbuf[n, pl.ds(r, SUB), :] = pbuf[n, pl.ds(pl.multiple_of(c * LANE + r, SUB), SUB), :] + rbuf[_odd(k + 2), n, pl.ds(r, SUB), :]

    def stage2_sum(n, r):
        cb[n, pl.ds(r, SUB), :] = ab[n, pl.ds(r, SUB), :] + bb[n, pl.ds(r, SUB), :]

    def rwait(k, n):
        _copy(rbuf.at[_odd(k + 2), n], rbuf.at[_odd(k + 2), n], rr.at[_odd(k + 2) * 2 + n]).wait()

    def loss_part(k, place):
        loss_acc[...] += jnp.where(k < NBLK - 2, combine(place), 0.0)

    def sub(k, cur):
        nxt = 1 - cur
        kind2, q2 = order2(_rem(k + 2, NBLK))
        blk2 = block_id(kind2, q2)

        def trip(n):
            @pl.when(k < NBLK - 1)
            def _():
                zload(k + 1, zb, n).wait()

            @pl.when(k >= 1)
            def _():
                rwait(k - 1, n)
                spair(k - 1, n).wait_send()
                if n == 0:
                    gstore(k - 1, nxt).wait()

            if n == 0:

                @pl.when(k < 2)
                def _():
                    stats_arrived(k + 2)

                @pl.when(k == 2)
                def _():
                    late_arrived()

            @pl.when(k >= 12)
            def _():
                _copy(tile(s_n2, 0, n), ab.at[n], ab_sem.at[n * 2]).wait()
                _copy(tile(r1n2, 0, n), bb.at[n], ab_sem.at[n * 2 + 1]).wait()

            @pl.when(k >= 13)
            def _():
                _copy(cb.at[n], tile(y2, 0, n), cb_sem.at[n]).wait()

            jobs = [[] for _ in range(32)]
            for r in range(8):
                jobs[2 + r * 3 // 5].append(functools.partial(pair_sum, k - 1, n, r * SUB))
                jobs[10 + r * 5 // 2].append(functools.partial(stage2_sum, n, r * SUB))
            for r, job in enumerate(gradient_jobs(zb, n, nxt)):
                jobs[2 + r * 9 // 20].append(job)
            if n == 0:
                jobs[8].append(lambda: loss_part(k, entry(kind2, q2)))
            else:
                for part in PAIR:
                    jobs[8 + 8 * part].append(functools.partial(columns, blk2, cur, part))

            def put(nt, acc):
                pbuf[n, :, nt * PIECE : (nt + 1) * PIECE] = acc

            _product(
                lambda kt: gbufs[cur][:, kt * BLK : (kt + 1) * BLK],
                lambda nt, kt: wv[pl.ds(pl.multiple_of(n * HALF + nt * PIECE, PIECE), PIECE), kt * BLK : (kt + 1) * BLK],
                put,
                jobs,
                True,
            )

            spair(k, n).start()

            if cur == n == 0:
                pl.when(k == 0)(send_late)

            @pl.when(k < NBLK - 2)
            def _():
                zload(k + 2, zb, n).start()

            @pl.when(k >= 2)
            def _():
                sstore_done(k - 2 + n, 1 - n)

            @pl.when(k >= 1)
            def _():
                sstore_start(k - 1, n)

            if n == 0:
                @pl.when(k == 1)
                def _():
                    sstore_done(k - 1, n)

            @pl.when(k >= 12)
            def _():
                _copy(cb.at[n], tile(y2, k - 12, n), cb_sem.at[n]).start()

            @pl.when((k >= 11) & (k < NBLK - 1))
            def _():
                stage2_load(k - 11, n)


        trip(0)
        trip(1)

        @pl.when(k < NBLK - 1)
        def _():
            gstore(k + 1, nxt).start()

    def pair(p, carry):
        sub(2 * p, 0)
        sub(2 * p + 1, 1)
        return carry

    _loop(NBLK // 2, pair)

    kl = jnp.int32(NBLK - 1)
    for n in PAIR:
        rwait(kl, n)
        spair(kl, n).wait_send()
        if n == 0:
            sstore_done(kl - 1, 1)
        for r in range(8):
            pair_sum(kl, n, r * SUB)
        sstore_start(kl, n)
    for n in PAIR:
        sstore_done(kl, n)
    gstore(kl, 1).wait()
    for n in PAIR:
        _copy(cb.at[n], tile(y2, 0, n), cb_sem.at[n]).wait()

    loss_out[...] = jnp.full(TILE, jnp.sum(loss_acc[...]) * INV, F32)

    for i in FOUR:
        _copy(tile(r1a, i // 2, i % 2), tile(r1a, i // 2, i % 2), r1as.at[i]).wait()
    _copy(s_d, s_d, s1tx).wait()
    _copy(s_n1a, s_n1a, s1tx).wait()
    _copy(xall.at[pl.ds(0, 28 * LANE)], xall.at[pl.ds(0, 28 * LANE)], tx).wait()
    for d in range(7):
        _copy(lab_v.at[d], lab_v.at[d], labtx_sem).wait()
        _copy(st_loc, st_loc, sttx_sem).wait()
    for d in FOUR:
        _copy(st_all.at[d, SEVEN], st_all.at[d, SEVEN], sttx_sem).wait()


def xrows_at(xall, dev, q):
    return xall.at[pl.ds(pl.multiple_of((dev // 2) * 1024 + q * BLK + (dev % 2) * LANE, LANE), LANE)]


def _head(hid, lab, w):
    hbm = pl.BlockSpec(memory_space=ANY)
    sd = jax.ShapeDtypeStruct
    dma = pltpu.SemaphoreType.DMA
    vmem = pltpu.VMEM
    quarter = (LANE, HALF)
    return pl.pallas_call(
        _head_kernel,
        out_shape=(
            sd((TOK, HID), BF16),
            sd((TOK, VOC), BF16),
            sd((256, HID), F32),
            sd((PIECE, HID), F32),
            sd((PIECE, HID), F32),
            sd((256, HID), F32),
            sd(TILE, F32),
            sd((NBLK, 2, BLK, HALF), F32),
            sd((PIECE, HID), F32),
            sd((256, HID), F32),
            sd((PIECE, HID), F32),
            sd((PIECE, HID), F32),
        ),
        in_specs=[hbm] * 3,
        out_specs=(hbm,) * 6 + (pl.BlockSpec(memory_space=vmem),) + (hbm,) * 5,
        scratch_shapes=[
            vmem((HID, VOC), BF16),
            vmem((2, BLK, HID), BF16),
            vmem((BLK, VOC), BF16),
            vmem((BLK, VOC), BF16),
            vmem((2, BLK, HALF), F32),
            vmem((2, BLK, HALF), F32),
            vmem((2, 2) + quarter, F32),
            vmem(TWO + quarter, F32),
            vmem(TWO + quarter, F32),
            vmem(TWO + quarter, F32),
            vmem(TWO + quarter, F32),
            vmem((8, 4, LANE), I32),
            vmem((BLK, LANE), I32),
            vmem((BLK, LANE), I32),
            vmem(TILE, F32),
            vmem((NBLK,) + TILE, F32),
            vmem((NBLK + 4, 8) + TILE, F32),
            vmem((2, BLK, LANE), F32),
            vmem((2, BLK, LANE), F32),
            vmem((2, BLK, LANE), F32),
            vmem((2, BLK, LANE), F32),
            vmem(TILE, F32),
            vmem((2, BLK, LANE), I32),
            vmem((2, BLK, LANE), F32),
            vmem((2, BLK, LANE), F32),
            vmem((2, LANE), F32),
            dma(TWO),
            dma(()),
            dma(()),
            dma((32,)),
            dma(()),
            dma(TWO),
            dma(TWO),
            dma(TWO),
            dma((5,)),
            dma(()),
            dma(TWO),
            dma((4,)),
            dma(TWO),
            dma(TWO),
            dma(()),
            dma((8,)),
            dma((4,)),
            dma((4,)),
            dma(TWO),
            dma(TWO),
        ],
        compiler_params=pltpu.CompilerParams(collective_id=0, has_side_effects=True, vmem_limit_bytes=67_043_328),
        cost_estimate=pl.CostEstimate(flops=4 * TOK * HID * VOC, bytes_accessed=400 * MIB, transcendentals=2 * TOK * VOC),
        name="head",
    )(hid, lab, w)


def _cols(j, width=PIECE):
    return pl.ds(pl.multiple_of(j * width, width), width)


def _dhead_kernel(
    x_hbm, g_hbm, s_hbm, a_hbm, o_hbm, t_hbm,
    gv, xb, ob, acc, sv, av, x_sem, g_sem, o_sem, s_sem, a_sem, t_sem, f_sem,
):
    blocks = HID // PIECE
    rows = BLK // 4

    def xload(b):
        return _copy(x_hbm.at[:, _cols(b)], xb.at[_odd(b)], x_sem.at[_odd(b)])

    def gload(j):
        return _copy(g_hbm.at[:, _cols(j)], gv.at[:, _cols(j)], g_sem.at[j])

    def ostore(b, n):
        return _copy(ob.at[n], o_hbm.at[_cols(b), _cols(n, HALF)], o_sem.at[n])

    def dot(lhs, rhs):
        return lax.dot_general(lhs, rhs, FIRST_DIMS, preferred_element_type=F32).astype(BF16)

    def terms(p):
        slot = _odd(p)
        src = _cols(p, rows)
        return _copy(s_hbm.at[src], sv.at[slot], s_sem.at[slot]), _copy(a_hbm.at[src], av.at[slot], a_sem.at[slot])

    def tstore(p):
        return _copy(sv.at[_odd(p)], t_hbm.at[_cols(p, rows)], t_sem.at[_odd(p)])

    def part(h):
        tokens = pl.ds(h * HALF, HALF)
        return (
            _copy(x_hbm.at[tokens, _cols(0)], xb.at[0, tokens], f_sem.at[h, 0]),
            _copy(g_hbm.at[tokens, _cols(0)], gv.at[tokens, _cols(0)], f_sem.at[h, 1]),
        )

    def part_dot(h):
        tokens = slice(h * HALF, (h + 1) * HALF)
        return lax.dot_general(
            xb[0, tokens, :], gv[tokens, :PIECE], FIRST_DIMS, preferred_element_type=F32
        )

    for h in PAIR:
        for copy in part(h):
            copy.start()
    for copy in part(0):
        copy.wait()
    gload(1).start()

    @pl.when(lax.axis_index("tp") < 8)
    def _():
        acc[...] = part_dot(0)

    for copy in part(1):
        copy.wait()
    gload(2).start()

    @pl.when(lax.axis_index("tp") < 8)
    def _():
        ob[0, :, :PIECE] = (acc[...] + part_dot(1)).astype(BF16)

    def first(j, carry):
        gload(j).wait()
        gload(2 * j + 1).start()

        @pl.when(j < 3)
        def _():
            gload(2 * j + 2).start()

        ob[0, :, _cols(j)] = dot(xb[0], gv[:, _cols(j)])
        return carry

    lax.fori_loop(1, 4, first, 0)
    ostore(0, 0).start()
    xload(1).start()
    for j in FOUR:
        gload(4 + j).wait()

    def block(b, carry):
        @pl.when(b > 0)
        def _():
            xload(b).wait()

        @pl.when((b > 0) & (b < blocks - 1))
        def _():
            xload(b + 1).start()

        @pl.when((b > 1) & (b < 6))
        def _():
            for copy in terms(b - 2):
                copy.wait()
            sv[_odd(b)] = sv[_odd(b)] + av[_odd(b)]
            tstore(b - 2).start()

        @pl.when((b > 0) & (b < 5))
        def _():
            pl.when(b > 2)(lambda: tstore(b - 3).wait())
            for copy in terms(b - 1):
                copy.start()

        def half(n, carry):
            pl.when(b > 0)(lambda: ostore(b - 1, n).wait())

            @pl.when(b < blocks)
            def _():
                ob[n] = dot(xb[_odd(b)], gv[:, _cols(n, HALF)])

            ostore(b, n).start()
            return carry

        return lax.fori_loop(jnp.where(b == 0, 1, 0), 2, half, carry)

    _loop(blocks, block)
    for n in PAIR:
        ostore(blocks - 1, n).wait()
        tstore(n).wait()


def _dhead(xall, gall, s_self, r1a):
    hbm = pl.BlockSpec(memory_space=ANY)
    dma = pltpu.SemaphoreType.DMA
    return pl.pallas_call(
        _dhead_kernel,
        in_specs=[hbm] * 4,
        out_specs=(hbm, hbm),
        out_shape=(jax.ShapeDtypeStruct((HID, VOC), BF16), jax.ShapeDtypeStruct((BLK, HID), F32)),
        scratch_shapes=[
            pltpu.VMEM((TOK, VOC), BF16),
            pltpu.VMEM((2, TOK, PIECE), BF16),
            pltpu.VMEM((2, PIECE, HALF), BF16),
            pltpu.VMEM((PIECE, PIECE), F32),
            pltpu.VMEM((2, BLK // 4, HID), F32),
            pltpu.VMEM((2, BLK // 4, HID), F32),
            dma(TWO),
            dma((8,)),
            dma(TWO),
            dma(TWO),
            dma(TWO),
            dma(TWO),
            dma(TWO + TWO),
        ],
        compiler_params=pltpu.CompilerParams(vmem_limit_bytes=60 * MIB),
        cost_estimate=pl.CostEstimate(flops=2 * TOK * HID * VOC, bytes_accessed=200 * MIB, transcendentals=0),
        name="dhead",
    )(xall, gall, s_self, r1a)


def _final_kernel(t_hbm, s_hbm, b_hbm, r_hbm, l_ref, o_hbm, loss_ref, terms, ov, in_sem, o_sem):
    rows = PIECE // SUB
    ahead = 6
    half = SUB // 2

    def load(t, ref, i, dst):
        return _copy(ref.at[_cols(i, rows)], terms.at[t, _cols(dst, rows)], in_sem.at[t, dst])

    def start(i):
        @pl.when(i < half)
        def _():
            load(0, t_hbm, i, i).start()

        @pl.when(i >= half)
        def _():
            load(0, s_hbm, i, i).start()
            load(1, b_hbm, i - half, i).start()

        load(2, r_hbm, i, i).start()

    def begin(i, carry):
        start(i)
        return carry

    _loop(ahead, begin)
    loss_ref[0] = l_ref[0, 0]

    def add(i, carry):
        rs = _cols(i, rows)
        load(0, s_hbm, i, i).wait()
        load(2, r_hbm, i, i).wait()
        pl.when(i < SUB - ahead)(lambda: start(i + ahead))

        @pl.when(i < half)
        def _():
            ov[rs, :] = (terms[0, rs, :] + terms[2, rs, :]).astype(BF16)

        @pl.when(i >= half)
        def _():
            load(1, b_hbm, i - half, i).wait()
            ov[rs, :] = (terms[0, rs, :] + terms[1, rs, :] + terms[2, rs, :]).astype(BF16)

        _copy(ov.at[rs], o_hbm.at[rs], o_sem).start()
        return carry

    _loop(SUB, add)
    _copy(ov, o_hbm, o_sem).wait()


def _final(t, s_self, r1b, r2, loss):
    hbm = pl.BlockSpec(memory_space=ANY)
    dma = pltpu.SemaphoreType.DMA
    return pl.pallas_call(
        _final_kernel,
        in_specs=[hbm] * 4 + [pl.BlockSpec(memory_space=pltpu.VMEM)],
        out_specs=(hbm, pl.BlockSpec(memory_space=pltpu.SMEM)),
        out_shape=(jax.ShapeDtypeStruct((PIECE, HID), BF16), jax.ShapeDtypeStruct((1,), F32)),
        scratch_shapes=[
            pltpu.VMEM((3, PIECE, HID), F32),
            pltpu.VMEM((PIECE, HID), BF16),
            dma((3, SUB)),
            dma(()),
        ],
        compiler_params=pltpu.CompilerParams(vmem_limit_bytes=62 * MIB),
        cost_estimate=pl.CostEstimate(flops=3 * PIECE * HID, bytes_accessed=24 * MIB, transcendentals=0),
        name="final",
    )(t, s_self, r1b, r2, loss)


def solution(mesh):
    def device(y, x, core):
        return (y % 2) * 4 + (x % 2) * 2 + core

    first, second = [], []
    for yy in PAIR:
        for xx in PAIR:
            along_x = [(device(yy, xx, k), device(yy, xx + 1, k)) for k in PAIR]
            along_y = [(device(yy, xx, k), device(yy + 1, xx, k)) for k in PAIR]
            first += [along_x[0], along_y[1]]
            second += [along_y[0], along_x[1]]

    def local_step(hid, w, lab):
        xall, gall, s_n1b, s_self, y2, r1a, loss = _head(hid, lab.reshape(4, LANE), w)[:7]
        r2 = lax.ppermute(y2, "tp", second)
        r1b = lax.ppermute(s_n1b, "tp", first)
        d_head, t = _dhead(xall, gall, s_self, r1a)
        d_hidden, mean_loss = _final(t, s_self, r1b, r2, loss)
        return mean_loss, d_hidden, d_head

    return jax.shard_map(
        local_step,
        mesh=mesh,
        in_specs=(P(("dp", "tp"), None), P(None, "tp"), P(("dp", "tp"))),
        out_specs=(P("dp"), P(("dp", "tp"), None), P("dp", "tp")),
        check_vma=False,
    )
```

```python
import functools

import jax
import jax.numpy as jnp
from jax import lax
from jax.experimental import pallas as pl
from jax.experimental.pallas import tpu as pltpu
from jax.sharding import PartitionSpec as P

F32, BF16, I32 = jnp.float32, jnp.bfloat16, jnp.int32
MESH = pl.DeviceIdType.MESH
ANY = pl.ANY

TOK = 4096
HID = 4096
VOC = 4096
BLK = 256
HALF = 2048
NBLK = TOK // BLK
LANE = 128
MIB = 1 << 20
TWO = (2,)
PAIR = (0, 1)
TILE = (8, LANE)
SUB = 16
FIRST_DIMS = (((0,), (0,)), ((), ()))
FOUR = range(4)
OTHERS = range(1, 8)
SEVEN = pl.ds(0, 7)
LATE = 9
PIECE = 512
INV = 1.0 / TOK


def _div(a, b):
    return lax.div(jnp.int32(a), jnp.int32(b))


def _rem(a, b):
    return lax.rem(jnp.int32(a), jnp.int32(b))


def _odd(a):
    return _rem(a, 2)


def _loop(count, body):
    lax.fori_loop(0, count, body, 0)


def _copy(src, dst, sem):
    return pltpu.make_async_copy(src, dst, sem)


def _send(src, dst, send_sem, recv_sem, dev):
    return pltpu.make_async_remote_copy(
        src_ref=src, dst_ref=dst, send_sem=send_sem, recv_sem=recv_sem, device_id={"tp": dev}, device_id_type=MESH
    )


def _product(lhs, rhs, put, jobs, transposed):
    pl.when(lax.axis_index("tp") < 8)(functools.partial(_pieces, lhs, rhs, put, jobs, transposed))


def _pieces(lhs, rhs, put, jobs, transposed):
    dims = (((1,), (1,)), ((), ())) if transposed else (((1,), (0,)), ((), ()))
    pieces = HALF // PIECE
    deep = HID // BLK
    for nt in range(pieces):
        acc = None
        for kt in range(deep):
            part = lax.dot_general(lhs(kt), rhs(nt, kt), dims, preferred_element_type=F32)
            acc = part if acc is None else acc + part
            if kt % 2:
                for job in jobs[(nt * deep + kt) // 2]:
                    job()
        put(nt, acc)


def _wide(v, times=HALF // LANE):
    return jnp.concatenate([v] * times, axis=1)


def _fold(v):
    width = v.shape[1] // 2
    while width >= LANE:
        v = v[:, :width] + v[:, width:]
        width //= 2
    return v


def _column(row):
    return jnp.transpose(jnp.broadcast_to(row, (LANE, LANE)))


def _head_kernel(
    x_hbm, lab_hbm, w_hbm,
    xall, gall, s_n1b, s_self, y2, r1a, loss_out,
    zst, s_d, s_n1a, s_n2, r1n2,
    wv, xg, ga, gb, zb, pbuf, rbuf, sbuf, ab, bb, cb, lab_v, la, lb, st_new, st_loc, st_all, ml, mk, sl, tl, comb, c_lab, c_top, c_scale, loss_acc,
    w_sem, lab_sem, labtx_sem, rx, tx, xl_sem, xs_sem, zo_sem, st_sem, sttx_sem,
    zi_sem, rr, ps, ss_sem, s1tx, r1s, r1as, ab_sem, cb_sem, g_sem,
):
    me = lax.axis_index("tp")
    chip = _div(me, 2)
    c = _odd(me)
    x = _odd(chip)
    y = _div(chip, 2)
    oc = 1 - c
    partner = me + 1 - 2 * c
    dx, dy = 2 - 4 * x, 4 - 8 * y
    n1 = me + oc * dx + c * dy
    n2 = me + c * dx + oc * dy
    n1kind = 1 + c

    def chip_of(kind):
        return chip + _odd(kind) * (1 - 2 * x) + _div(kind, 2) * (2 - 4 * y)

    def order(i, first, last):
        a = _div(i, 4)
        mid, end = _rem(_div(a + 1, 2), 2), _div(a, 3)
        kind = mid * (1 + _odd(i)) + first * (1 - mid) * (1 - end) + last * end
        return kind, mid * _div(i - 4, 2) + (1 - mid) * _rem(i, 4)

    def order1(i):
        return order(i, 0, 3)

    def order2(i):
        return order(i, 3, 0)

    def block_id(kind, q):
        return chip_of(kind) * 4 + q

    def xrows(kind, q, part):
        return xall.at[pl.ds(pl.multiple_of(block_id(kind, q) * BLK + part * LANE, LANE), LANE)]

    def xblock(kind, q):
        return xall.at[pl.ds(pl.multiple_of(block_id(kind, q) * BLK, BLK), BLK)]

    def own(q):
        return x_hbm.at[pl.ds(pl.multiple_of(q * LANE, LANE), LANE)]

    def rxs(kind, q, part):
        return rx.at[kind * 8 + q * 2 + part]

    def wcopy(j):
        cols = pl.ds(j * HALF, HALF)
        return _copy(w_hbm.at[:, cols], wv.at[:, cols], w_sem.at[j])

    _copy(own(0), xg.at[0, pl.ds(pl.multiple_of(c * LANE, LANE), LANE)], xl_sem.at[0]).start()
    wcopy(0).start()

    barrier = pltpu.get_barrier_semaphore()
    for d in OTHERS:
        pl.semaphore_signal(barrier, inc=1, device_id={"tp": _rem(me + d, 8)}, device_id_type=MESH)
    pl.semaphore_wait(barrier, 7)

    for d in OTHERS:
        _send(lab_hbm, lab_v.at[me], labtx_sem, lab_sem, _rem(me + d, 8)).start()
    _copy(lab_hbm, lab_v.at[me], lab_sem).start()
    for q in FOUR:
        _send(own(q), xrows(0, q, c), tx, rxs(0, q, c), partner).start()
    for q in FOUR:
        _send(own(q), xrows_at(xall, me, q), tx, rxs(n1kind, q, c), n1).start()
        _send(own(q), xrows_at(xall, me, q), tx, rxs(3 - n1kind, q, c), n2).start()

    def load_x(b):
        kind, q = order1(b)
        slot = _odd(b)

        @pl.when(kind == 0)
        def _():
            _copy(own(q), xg.at[slot, pl.ds(pl.multiple_of(c * LANE, LANE), LANE)], xl_sem.at[slot]).start()
            _copy(xrows(0, q, oc), xg.at[slot, pl.ds(pl.multiple_of(oc * LANE, LANE), LANE)], xl_sem.at[slot]).start()

        @pl.when(kind != 0)
        def _():
            _copy(xblock(kind, q), xg.at[slot], xl_sem.at[slot]).start()

    def wait_rows(kind, q, part):
        _copy(xrows(kind, q, part), xrows(kind, q, part), rxs(kind, q, part)).wait()

    def take_rows(kind, q):
        wait_rows(kind, q, c)
        _send(xrows(kind, q, c), xrows(kind, q, c), tx, rxs(kind, q, c), partner).start()

        @pl.when(kind == n1kind)
        def _():
            _send(xrows(kind, q, c), xrows(kind, q, c), tx, rxs(3, q, c), n2).start()

    def part_load(b, part):
        kind, q = order1(b)
        return _copy(xrows(kind, q, part), xg.at[_odd(b), pl.ds(pl.multiple_of(part * LANE, LANE), LANE)], xl_sem.at[_odd(b)])

    def zcopy(b, h):
        kind, q = order1(b)
        return _copy(zb.at[h], zst.at[block_id(kind, q), h], zo_sem.at[h])

    def own_store(b):
        slot = _odd(b)
        return _copy(xg.at[slot, pl.ds(pl.multiple_of(c * LANE, LANE), LANE)], xrows(0, _rem(b, 4), c), xs_sem.at[slot])

    def label_column(blk, part):
        return _column(lab_v[2 * _div(blk, 4) + part, pl.ds(_rem(blk, 4), 1), :])

    def lane_stats(col, h, r):
        rows = pl.ds(r, 8)
        z = zb[h, rows, :]
        m = ml[h, rows, :]
        hit = _wide(col[rows, :] - (me * VOC + h * HALF)) == lax.broadcasted_iota(I32, (8, HALF), 1)
        s = _fold(jnp.exp(z - _wide(m)))
        t = _fold(jnp.where(hit, z, 0.0))
        if h == 1:
            m0 = mk[0, rows, :]
            mm = jnp.maximum(m0, m)
            s = sl[0, rows, :] * jnp.exp(m0 - mm) + s * jnp.exp(m - mm)
            t = tl[0, rows, :] + t
            m = mm
        mk[h, rows, :] = m
        sl[h, rows, :] = s
        tl[h, rows, :] = t

    def label_columns(blk, col, part):
        col[pl.ds(part * LANE, LANE), :] = label_column(blk, part)

    def row_stats(part):
        rows = pl.ds(part * LANE, LANE)
        m = jnp.transpose(mk[1, rows, :])
        top = jnp.max(m, axis=0, keepdims=True)
        st_new[part : part + 1, :] = top
        st_new[2 + part : 3 + part, :] = jnp.sum(jnp.transpose(sl[1, rows, :]) * jnp.exp(m - top), axis=0, keepdims=True)
        st_new[4 + part : 5 + part, :] = jnp.sum(jnp.transpose(tl[1, rows, :]), axis=0, keepdims=True)

    def entry(kind, q):
        diagonal = _div(kind, 3)
        return diagonal * (NBLK + q) + (1 - diagonal) * block_id(kind, q)

    def send_stats(kind, q):
        def start(dev):
            _send(st_loc.at[block_id(kind, q)], st_all.at[NBLK + q, me], sttx_sem, st_sem.at[q], dev).start()

        for core in PAIR:
            dev = 2 * chip_of(3 - kind) + core
            pl.when(dev != me)(functools.partial(start, dev))

    def send_late():
        for d in OTHERS:
            _send(st_loc, st_all.at[pl.ds(0, NBLK), me], sttx_sem, st_sem.at[4], _rem(me + d, 8)).start()

    def keep_stats(kind, q):
        st_loc[block_id(kind, q)] = st_new[...]
        st_all[block_id(kind, q), me] = st_new[...]
        st_all[entry(kind, q), me] = st_new[...]

    def combine(place):
        top = st_all[place, 0, 0:2, :]
        for d in OTHERS:
            top = jnp.maximum(top, st_all[place, d, 0:2, :])
        s = jnp.zeros((2, LANE), F32)
        t = jnp.zeros((2, LANE), F32)
        for d in range(8):
            s = s + st_all[place, d, 2:4, :] * jnp.exp(st_all[place, d, 0:2, :] - top)
            t = t + st_all[place, d, 4:6, :]
        comb[0:2, :] = top
        comb[2:4, :] = INV / s
        return top + jnp.log(s) - t

    def stats_arrived(q):
        _copy(st_all.at[0, SEVEN], st_all.at[0, SEVEN], st_sem.at[q]).wait()

    def late_arrived():
        _copy(st_all.at[pl.ds(0, 14)], st_all.at[pl.ds(0, 14)], st_sem.at[4]).wait()

    def columns(blk, par, part):
        rows = pl.ds(part * LANE, LANE)
        c_lab[par, rows, :] = label_column(blk, part)
        c_top[par, rows, :] = _column(comb[part : part + 1, :])
        c_scale[par, rows, :] = _column(comb[2 + part : 3 + part, :])

    def gradient(src, n, par, r, j):
        rows = pl.ds(pl.multiple_of(r, SUB), SUB)
        col = c_lab[par, rows, :] - (me * VOC + n * HALF + j)
        p = jnp.exp(src[n, rows, j : j + PIECE] - _wide(c_top[par, rows, :], 4)) * _wide(c_scale[par, rows, :], 4)
        g = jnp.where(_wide(col, 4) == lax.broadcasted_iota(I32, (SUB, PIECE), 1), p - INV, p)
        gbufs[par][rows, n * HALF + j : n * HALF + j + PIECE] = g.astype(BF16)

    def gradient_jobs(src, n, par):
        return [functools.partial(gradient, src, n, par, r, j) for r in range(0, BLK, SUB) for j in range(0, HALF, PIECE)]

    gbufs = (ga, gb)

    def gstore(k, par):
        kind, q = order2(k)
        return _copy(gbufs[par], gall.at[pl.ds(pl.multiple_of(block_id(kind, q) * BLK, BLK), BLK)], g_sem.at[par])

    def zload(k, dst, n):
        kind, q = order2(k)
        return _copy(zst.at[block_id(kind, q), n], dst.at[n], zi_sem.at[n])

    first_kind, first_q = order2(me * 0)
    first_blk = block_id(first_kind, first_q)

    def logits(b, h, jobs):
        slot = _odd(b)
        def put(nt, z):
            zb[h, :, nt * PIECE : (nt + 1) * PIECE] = z
            m = z[:, :LANE]
            for j in range(1, 4):
                m = jnp.maximum(m, z[:, j * LANE : (j + 1) * LANE])
            if nt:
                m = jnp.maximum(m, ml[h])
            ml[h] = m

        _product(
            lambda kt: xg[slot, :, kt * BLK : (kt + 1) * BLK],
            lambda nt, kt: wv[kt * BLK : (kt + 1) * BLK, h * HALF + nt * PIECE : h * HALF + (nt + 1) * PIECE],
            put,
            jobs,
            False,
        )

    wait_rows(0, 0, oc)
    _copy(xrows(0, 0, oc), xg.at[0, pl.ds(pl.multiple_of(oc * LANE, LANE), LANE)], xl_sem.at[0]).start()
    _copy(lab_v, lab_v, lab_sem).wait()
    wcopy(0).wait()
    wcopy(1).start()

    def phase1(i, carry):
        slot = _odd(i)
        kind, q = order1(i)
        kprev, qprev = order1(_rem(i + NBLK - 2, NBLK))
        kn, qn = order1(_rem(i + 1, NBLK))

        @pl.when((i == LATE + 1) | (i == NBLK - 1))
        def _():
            wait_rows(kind, q, oc)
            part_load(i, oc).start()

        @pl.when(i > 0)
        def _():
            zcopy(i - 1, 1).start()
            zcopy(i - 1, 0).wait()

        @pl.when(i > 1)
        def _():
            keep_stats(kprev, qprev)

        @pl.when(i == NBLK - 2)
        def _():
            zload(0, pbuf, 0).start()
            zload(0, pbuf, 1).start()

        @pl.when(i == NBLK - 1)
        def _():
            stats_arrived(0)
            loss_acc[...] = combine(entry(first_kind, first_q))
            for part in PAIR:
                columns(first_blk, 0, part)
            for n in PAIR:
                zload(0, pbuf, n).wait()

                def some(r, carry, n=n):
                    for j in range(0, HALF, PIECE):
                        gradient(pbuf, n, 0, r * SUB, j)
                    return carry

                _loop(SUB, some)

            gstore(0, 0).start()

        @pl.when((i >= 3) & (i != LATE) & (i < NBLK - 2))
        def _():
            take_rows(kn, qn)

        _copy(xg.at[slot], xg.at[slot], xl_sem.at[slot]).wait()

        @pl.when(i < 4)
        def _():
            own_store(i).start()

        jobs = [[] for _ in range(32)]
        for r in range(32):
            jobs[min(r + 1, 31)].append(functools.partial(lane_stats, la, 1, r * 8))
        for part in PAIR:
            jobs[4 + 4 * part].append(functools.partial(label_columns, block_id(kind, q), lb, part))
        logits(i, 0, jobs)

        zcopy(i, 0).start()

        @pl.when(i == 0)
        def _():
            wcopy(1).wait()

        @pl.when(i > 0)
        def _():
            zcopy(i - 1, 1).wait()

        @pl.when(i > 1)
        def _():
            send_stats(kprev, qprev)

        @pl.when((i == LATE) | (i == NBLK - 2))
        def _():
            take_rows(kn, qn)
            part_load(i + 1, c).start()

        @pl.when((i != LATE) & (i < NBLK - 2))
        def _():
            wait_rows(kn, qn, oc)

            @pl.when((i >= 1) & (i < 5))
            def _():
                own_store(i - 1).wait()

            load_x(i + 1)

        la[...] = lb[...]
        jobs = [[] for _ in range(32)]
        for r in range(32):
            jobs[min(r + 1, 31)].append(functools.partial(lane_stats, lb, 0, r * 8))
        for part in PAIR:
            jobs[8 + 8 * part].append(functools.partial(row_stats, part))
        logits(i, 1, jobs)
        return carry

    _loop(NBLK, phase1)
    last = NBLK - 1
    klast, qlast = order1(jnp.int32(last))
    kprev, qprev = order1(jnp.int32(last - 1))
    keep_stats(kprev, qprev)
    zcopy(last, 1).start()
    zcopy(last, 0).wait()
    zload(1, zb, 0).start()
    send_stats(kprev, qprev)
    for r in range(32):
        lane_stats(la, 1, r * 8)
    for part in PAIR:
        row_stats(part)
    keep_stats(klast, qlast)
    second_kind, second_q = order2(jnp.int32(1))
    second_blk = block_id(second_kind, second_q)
    stats_arrived(1)
    loss_acc[...] += combine(entry(second_kind, second_q))
    for part in PAIR:
        columns(second_blk, 1, part)
    send_stats(klast, qlast)
    zcopy(last, 1).wait()
    zload(1, zb, 1).start()

    def tile(ref, q, n):
        return ref.at[pl.ds(pl.multiple_of(q * LANE, LANE), LANE), pl.ds(pl.multiple_of(n * HALF, HALF), HALF)]

    def spair(k, n):
        return _send(
            pbuf.at[n, pl.ds(pl.multiple_of(oc * LANE, LANE), LANE)], rbuf.at[_odd(k + 2), n], ps.at[n], rr.at[_odd(k + 2) * 2 + n], partner
        )

    def sstore_start(k, n):
        kind, q = order2(k)
        sem = ss_sem.at[n]

        @pl.when(kind == 3)
        def _():
            _copy(sbuf.at[n], tile(s_d, q, n), sem).start()

        @pl.when((kind == n1kind) & (q < 2))
        def _():
            _copy(sbuf.at[n], tile(s_n1a, _odd(q), n), sem).start()

        @pl.when((kind == n1kind) & (q >= 2))
        def _():
            _copy(sbuf.at[n], tile(s_n1b, _odd(q), n), sem).start()

        @pl.when(kind == 3 - n1kind)
        def _():
            _copy(sbuf.at[n], tile(s_n2, q, n), sem).start()

        @pl.when(kind == 0)
        def _():
            _copy(sbuf.at[n], tile(s_self, q, n), sem).start()

    def sstore_done(k, n):
        kind, q = order2(k)
        _copy(sbuf.at[n], tile(s_d, 0, n), ss_sem.at[n]).wait()

        @pl.when(kind == 3)
        def _():
            _send(tile(s_d, q, n), tile(r1n2, q, n), s1tx, r1s.at[q * 2 + n], n1).start()

        @pl.when((kind == n1kind) & (q < 2))
        def _():
            _send(tile(s_n1a, _odd(q), n), tile(r1a, _odd(q), n), s1tx, r1as.at[_odd(q) * 2 + n], n1).start()

    def stage2_load(q, n):
        _copy(tile(r1n2, q, n), tile(r1n2, q, n), r1s.at[q * 2 + n]).wait()
        _copy(tile(s_n2, q, n), ab.at[n], ab_sem.at[n * 2]).start()
        _copy(tile(r1n2, q, n), bb.at[n], ab_sem.at[n * 2 + 1]).start()

    def pair_sum(k, n, r):
        sbuf[n, pl.ds(r, SUB), :] = pbuf[n, pl.ds(pl.multiple_of(c * LANE + r, SUB), SUB), :] + rbuf[_odd(k + 2), n, pl.ds(r, SUB), :]

    def stage2_sum(n, r):
        cb[n, pl.ds(r, SUB), :] = ab[n, pl.ds(r, SUB), :] + bb[n, pl.ds(r, SUB), :]

    def rwait(k, n):
        _copy(rbuf.at[_odd(k + 2), n], rbuf.at[_odd(k + 2), n], rr.at[_odd(k + 2) * 2 + n]).wait()

    def loss_part(k, place):
        loss_acc[...] += jnp.where(k < NBLK - 2, combine(place), 0.0)

    def sub(k, cur):
        nxt = 1 - cur
        kind2, q2 = order2(_rem(k + 2, NBLK))
        blk2 = block_id(kind2, q2)

        def trip(n):
            @pl.when(k < NBLK - 1)
            def _():
                zload(k + 1, zb, n).wait()

            @pl.when(k >= 1)
            def _():
                rwait(k - 1, n)
                spair(k - 1, n).wait_send()
                if n == 0:
                    gstore(k - 1, nxt).wait()

            if n == 0:

                @pl.when(k < 2)
                def _():
                    stats_arrived(k + 2)

                @pl.when(k == 2)
                def _():
                    late_arrived()

            @pl.when(k >= 12)
            def _():
                _copy(tile(s_n2, 0, n), ab.at[n], ab_sem.at[n * 2]).wait()
                _copy(tile(r1n2, 0, n), bb.at[n], ab_sem.at[n * 2 + 1]).wait()

            @pl.when(k >= 13)
            def _():
                _copy(cb.at[n], tile(y2, 0, n), cb_sem.at[n]).wait()

            jobs = [[] for _ in range(32)]
            for r in range(8):
                jobs[2 + r * 3 // 5].append(functools.partial(pair_sum, k - 1, n, r * SUB))
                jobs[10 + r * 5 // 2].append(functools.partial(stage2_sum, n, r * SUB))
            for r, job in enumerate(gradient_jobs(zb, n, nxt)):
                jobs[2 + r * 9 // 20].append(job)
            if n == 0:
                jobs[8].append(lambda: loss_part(k, entry(kind2, q2)))
            else:
                for part in PAIR:
                    jobs[8 + 8 * part].append(functools.partial(columns, blk2, cur, part))

            def put(nt, acc):
                pbuf[n, :, nt * PIECE : (nt + 1) * PIECE] = acc

            _product(
                lambda kt: gbufs[cur][:, kt * BLK : (kt + 1) * BLK],
                lambda nt, kt: wv[pl.ds(pl.multiple_of(n * HALF + nt * PIECE, PIECE), PIECE), kt * BLK : (kt + 1) * BLK],
                put,
                jobs,
                True,
            )

            spair(k, n).start()

            if cur == n == 0:
                pl.when(k == 0)(send_late)

            @pl.when(k < NBLK - 2)
            def _():
                zload(k + 2, zb, n).start()

            @pl.when(k >= 2)
            def _():
                sstore_done(k - 2 + n, 1 - n)

            @pl.when(k >= 1)
            def _():
                sstore_start(k - 1, n)

            if n == 0:
                @pl.when(k == 1)
                def _():
                    sstore_done(k - 1, n)

            @pl.when(k >= 12)
            def _():
                _copy(cb.at[n], tile(y2, k - 12, n), cb_sem.at[n]).start()

            @pl.when((k >= 11) & (k < NBLK - 1))
            def _():
                stage2_load(k - 11, n)


        trip(0)
        trip(1)

        @pl.when(k < NBLK - 1)
        def _():
            gstore(k + 1, nxt).start()

    def pair(p, carry):
        sub(2 * p, 0)
        sub(2 * p + 1, 1)
        return carry

    _loop(NBLK // 2, pair)

    kl = jnp.int32(NBLK - 1)
    for n in PAIR:
        rwait(kl, n)
        spair(kl, n).wait_send()
        if n == 0:
            sstore_done(kl - 1, 1)
        for r in range(8):
            pair_sum(kl, n, r * SUB)
        sstore_start(kl, n)
    for n in PAIR:
        sstore_done(kl, n)
    gstore(kl, 1).wait()
    for n in PAIR:
        _copy(cb.at[n], tile(y2, 0, n), cb_sem.at[n]).wait()

    loss_out[...] = jnp.full(TILE, jnp.sum(loss_acc[...]) * INV, F32)

    for i in FOUR:
        _copy(tile(r1a, i // 2, i % 2), tile(r1a, i // 2, i % 2), r1as.at[i]).wait()
    _copy(s_d, s_d, s1tx).wait()
    _copy(s_n1a, s_n1a, s1tx).wait()
    _copy(xall.at[pl.ds(0, 28 * LANE)], xall.at[pl.ds(0, 28 * LANE)], tx).wait()
    for d in range(7):
        _copy(lab_v.at[d], lab_v.at[d], labtx_sem).wait()
        _copy(st_loc, st_loc, sttx_sem).wait()
    for d in FOUR:
        _copy(st_all.at[d, SEVEN], st_all.at[d, SEVEN], sttx_sem).wait()


def xrows_at(xall, dev, q):
    return xall.at[pl.ds(pl.multiple_of((dev // 2) * 1024 + q * BLK + (dev % 2) * LANE, LANE), LANE)]


def _head(hid, lab, w):
    hbm = pl.BlockSpec(memory_space=ANY)
    sd = jax.ShapeDtypeStruct
    dma = pltpu.SemaphoreType.DMA
    vmem = pltpu.VMEM
    quarter = (LANE, HALF)
    return pl.pallas_call(
        _head_kernel,
        out_shape=(
            sd((TOK, HID), BF16),
            sd((TOK, VOC), BF16),
            sd((256, HID), F32),
            sd((PIECE, HID), F32),
            sd((PIECE, HID), F32),
            sd((256, HID), F32),
            sd(TILE, F32),
            sd((NBLK, 2, BLK, HALF), F32),
            sd((PIECE, HID), F32),
            sd((256, HID), F32),
            sd((PIECE, HID), F32),
            sd((PIECE, HID), F32),
        ),
        in_specs=[hbm] * 3,
        out_specs=(hbm,) * 6 + (pl.BlockSpec(memory_space=vmem),) + (hbm,) * 5,
        scratch_shapes=[
            vmem((HID, VOC), BF16),
            vmem((2, BLK, HID), BF16),
            vmem((BLK, VOC), BF16),
            vmem((BLK, VOC), BF16),
            vmem((2, BLK, HALF), F32),
            vmem((2, BLK, HALF), F32),
            vmem((2, 2) + quarter, F32),
            vmem(TWO + quarter, F32),
            vmem(TWO + quarter, F32),
            vmem(TWO + quarter, F32),
            vmem(TWO + quarter, F32),
            vmem((8, 4, LANE), I32),
            vmem((BLK, LANE), I32),
            vmem((BLK, LANE), I32),
            vmem(TILE, F32),
            vmem((NBLK,) + TILE, F32),
            vmem((NBLK + 4, 8) + TILE, F32),
            vmem((2, BLK, LANE), F32),
            vmem((2, BLK, LANE), F32),
            vmem((2, BLK, LANE), F32),
            vmem((2, BLK, LANE), F32),
            vmem(TILE, F32),
            vmem((2, BLK, LANE), I32),
            vmem((2, BLK, LANE), F32),
            vmem((2, BLK, LANE), F32),
            vmem((2, LANE), F32),
            dma(TWO),
            dma(()),
            dma(()),
            dma((32,)),
            dma(()),
            dma(TWO),
            dma(TWO),
            dma(TWO),
            dma((5,)),
            dma(()),
            dma(TWO),
            dma((4,)),
            dma(TWO),
            dma(TWO),
            dma(()),
            dma((8,)),
            dma((4,)),
            dma((4,)),
            dma(TWO),
            dma(TWO),
        ],
        compiler_params=pltpu.CompilerParams(collective_id=0, has_side_effects=True, vmem_limit_bytes=67_043_328),
        cost_estimate=pl.CostEstimate(flops=4 * TOK * HID * VOC, bytes_accessed=400 * MIB, transcendentals=2 * TOK * VOC),
        name="head",
    )(hid, lab, w)


def _cols(j, width=PIECE):
    return pl.ds(pl.multiple_of(j * width, width), width)


def _dhead_kernel(
    x_hbm, g_hbm, s_hbm, a_hbm, o_hbm, t_hbm,
    gv, xb, ob, acc, sv, av, x_sem, g_sem, o_sem, s_sem, a_sem, t_sem, f_sem,
):
    blocks = HID // PIECE
    rows = BLK // 4

    def xload(b):
        return _copy(x_hbm.at[:, _cols(b)], xb.at[_odd(b)], x_sem.at[_odd(b)])

    def gload(j):
        return _copy(g_hbm.at[:, _cols(j)], gv.at[:, _cols(j)], g_sem.at[j])

    def ostore(b, n):
        return _copy(ob.at[n], o_hbm.at[_cols(b), _cols(n, HALF)], o_sem.at[n])

    def dot(lhs, rhs):
        return lax.dot_general(lhs, rhs, FIRST_DIMS, preferred_element_type=F32).astype(BF16)

    def terms(p):
        slot = _odd(p)
        src = _cols(p, rows)
        return _copy(s_hbm.at[src], sv.at[slot], s_sem.at[slot]), _copy(a_hbm.at[src], av.at[slot], a_sem.at[slot])

    def tstore(p):
        return _copy(sv.at[_odd(p)], t_hbm.at[_cols(p, rows)], t_sem.at[_odd(p)])

    def part(h):
        tokens = pl.ds(h * HALF, HALF)
        return (
            _copy(x_hbm.at[tokens, _cols(0)], xb.at[0, tokens], f_sem.at[h, 0]),
            _copy(g_hbm.at[tokens, _cols(0)], gv.at[tokens, _cols(0)], f_sem.at[h, 1]),
        )

    def part_dot(h):
        tokens = slice(h * HALF, (h + 1) * HALF)
        return lax.dot_general(
            xb[0, tokens, :], gv[tokens, :PIECE], FIRST_DIMS, preferred_element_type=F32
        )

    for h in PAIR:
        for copy in part(h):
            copy.start()
    for copy in part(0):
        copy.wait()
    gload(1).start()

    @pl.when(lax.axis_index("tp") < 8)
    def _():
        acc[...] = part_dot(0)

    for copy in part(1):
        copy.wait()
    gload(2).start()

    @pl.when(lax.axis_index("tp") < 8)
    def _():
        ob[0, :, :PIECE] = (acc[...] + part_dot(1)).astype(BF16)

    def first(j, carry):
        gload(j).wait()
        gload(2 * j + 1).start()

        @pl.when(j < 3)
        def _():
            gload(2 * j + 2).start()

        ob[0, :, _cols(j)] = dot(xb[0], gv[:, _cols(j)])
        return carry

    lax.fori_loop(1, 4, first, 0)
    ostore(0, 0).start()
    xload(1).start()
    for j in FOUR:
        gload(4 + j).wait()

    def block(b, carry):
        @pl.when(b > 0)
        def _():
            xload(b).wait()

        @pl.when((b > 0) & (b < blocks - 1))
        def _():
            xload(b + 1).start()

        @pl.when((b > 1) & (b < 6))
        def _():
            for copy in terms(b - 2):
                copy.wait()
            sv[_odd(b)] = sv[_odd(b)] + av[_odd(b)]
            tstore(b - 2).start()

        @pl.when((b > 0) & (b < 5))
        def _():
            pl.when(b > 2)(lambda: tstore(b - 3).wait())
            for copy in terms(b - 1):
                copy.start()

        def half(n, carry):
            pl.when(b > 0)(lambda: ostore(b - 1, n).wait())

            @pl.when(b < blocks)
            def _():
                ob[n] = dot(xb[_odd(b)], gv[:, _cols(n, HALF)])

            ostore(b, n).start()
            return carry

        return lax.fori_loop(jnp.where(b == 0, 1, 0), 2, half, carry)

    _loop(blocks, block)
    for n in PAIR:
        ostore(blocks - 1, n).wait()
        tstore(n).wait()


def _dhead(xall, gall, s_self, r1a):
    hbm = pl.BlockSpec(memory_space=ANY)
    dma = pltpu.SemaphoreType.DMA
    return pl.pallas_call(
        _dhead_kernel,
        in_specs=[hbm] * 4,
        out_specs=(hbm, hbm),
        out_shape=(jax.ShapeDtypeStruct((HID, VOC), BF16), jax.ShapeDtypeStruct((BLK, HID), F32)),
        scratch_shapes=[
            pltpu.VMEM((TOK, VOC), BF16),
            pltpu.VMEM((2, TOK, PIECE), BF16),
            pltpu.VMEM((2, PIECE, HALF), BF16),
            pltpu.VMEM((PIECE, PIECE), F32),
            pltpu.VMEM((2, BLK // 4, HID), F32),
            pltpu.VMEM((2, BLK // 4, HID), F32),
            dma(TWO),
            dma((8,)),
            dma(TWO),
            dma(TWO),
            dma(TWO),
            dma(TWO),
            dma(TWO + TWO),
        ],
        compiler_params=pltpu.CompilerParams(vmem_limit_bytes=60 * MIB),
        cost_estimate=pl.CostEstimate(flops=2 * TOK * HID * VOC, bytes_accessed=200 * MIB, transcendentals=0),
        name="dhead",
    )(xall, gall, s_self, r1a)


def _final_kernel(t_hbm, s_hbm, b_hbm, r_hbm, l_ref, o_hbm, loss_ref, terms, ov, in_sem, o_sem):
    rows = PIECE // SUB
    ahead = 10
    half = SUB // 2

    def load(t, ref, i, dst):
        return _copy(ref.at[_cols(i, rows)], terms.at[t, _cols(dst, rows)], in_sem.at[t, dst])

    def start(i):
        @pl.when(i < half)
        def _():
            load(0, t_hbm, i, i).start()

        @pl.when(i >= half)
        def _():
            load(0, s_hbm, i, i).start()
            load(1, b_hbm, i - half, i).start()

        load(2, r_hbm, i, i).start()

    def begin(i, carry):
        start(i)
        return carry

    _loop(ahead, begin)
    loss_ref[0] = l_ref[0, 0]

    def add(i, carry):
        rs = _cols(i, rows)
        load(0, s_hbm, i, i).wait()
        load(2, r_hbm, i, i).wait()
        pl.when(i < SUB - ahead)(lambda: start(i + ahead))

        @pl.when(i < half)
        def _():
            ov[rs, :] = (terms[0, rs, :] + terms[2, rs, :]).astype(BF16)

        @pl.when(i >= half)
        def _():
            load(1, b_hbm, i - half, i).wait()
            ov[rs, :] = (terms[0, rs, :] + terms[1, rs, :] + terms[2, rs, :]).astype(BF16)

        _copy(ov.at[rs], o_hbm.at[rs], o_sem).start()
        return carry

    _loop(SUB, add)
    _copy(ov, o_hbm, o_sem).wait()


def _final(t, s_self, r1b, r2, loss):
    hbm = pl.BlockSpec(memory_space=ANY)
    dma = pltpu.SemaphoreType.DMA
    return pl.pallas_call(
        _final_kernel,
        in_specs=[hbm] * 4 + [pl.BlockSpec(memory_space=pltpu.VMEM)],
        out_specs=(hbm, pl.BlockSpec(memory_space=pltpu.SMEM)),
        out_shape=(jax.ShapeDtypeStruct((PIECE, HID), BF16), jax.ShapeDtypeStruct((1,), F32)),
        scratch_shapes=[
            pltpu.VMEM((3, PIECE, HID), F32),
            pltpu.VMEM((PIECE, HID), BF16),
            dma((3, SUB)),
            dma(()),
        ],
        compiler_params=pltpu.CompilerParams(vmem_limit_bytes=62 * MIB),
        cost_estimate=pl.CostEstimate(flops=3 * PIECE * HID, bytes_accessed=24 * MIB, transcendentals=0),
        name="final",
    )(t, s_self, r1b, r2, loss)


def solution(mesh):
    def device(y, x, core):
        return (y % 2) * 4 + (x % 2) * 2 + core

    first, second = [], []
    for yy in PAIR:
        for xx in PAIR:
            along_x = [(device(yy, xx, k), device(yy, xx + 1, k)) for k in PAIR]
            along_y = [(device(yy, xx, k), device(yy + 1, xx, k)) for k in PAIR]
            first += [along_x[0], along_y[1]]
            second += [along_y[0], along_x[1]]

    def local_step(hid, w, lab):
        xall, gall, s_n1b, s_self, y2, r1a, loss = _head(hid, lab.reshape(4, LANE), w)[:7]
        r2 = lax.ppermute(y2, "tp", second)
        r1b = lax.ppermute(s_n1b, "tp", first)
        d_head, t = _dhead(xall, gall, s_self, r1a)
        d_hidden, mean_loss = _final(t, s_self, r1b, r2, loss)
        return mean_loss, d_hidden, d_head

    return jax.shard_map(
        local_step,
        mesh=mesh,
        in_specs=(P(("dp", "tp"), None), P(None, "tp"), P(("dp", "tp"))),
        out_specs=(P("dp"), P(("dp", "tp"), None), P("dp", "tp")),
        check_vma=False,
    )
```
